8 devices in a mesh: data: 1 (over z), col: 2 (over y), row: 4 (over x, core).
Axes of the slice: x: 2, y: 2, z: 1, core: 2. Of those that a mesh axis runs over, the one named last changes fastest.
Arguments:
- image: bfloat16 [256, 128, 4], P(('data', 'row'), 'col')
- w_enc1a: bfloat16 [3, 3, 4, 320], replicated
- b_enc1a: float32 [320], replicated
- w_enc1b: bfloat16 [3, 3, 320, 320], replicated
- b_enc1b: float32 [320], replicated
- w_enc2a: bfloat16 [3, 3, 320, 640], replicated
- b_enc2a: float32 [640], replicated
- w_enc2b: bfloat16 [3, 3, 640, 640], replicated
- b_enc2b: float32 [640], replicated
- w_mid_a: bfloat16 [3, 3, 640, 1280], replicated
- b_mid_a: float32 [1280], replicated
- w_mid_b: bfloat16 [3, 3, 1280, 1280], replicated
- b_mid_b: float32 [1280], replicated
- w_up2: bfloat16 [2, 2, 1280, 640], replicated
- w_dec2a: bfloat16 [3, 3, 1280, 640], replicated
- b_dec2a: float32 [640], replicated
- w_dec2b: bfloat16 [3, 3, 640, 640], replicated
- b_dec2b: float32 [640], replicated
- w_up1: bfloat16 [2, 2, 640, 320], replicated
- w_dec1a: bfloat16 [3, 3, 640, 320], replicated
- b_dec1a: float32 [320], replicated
- w_dec1b: bfloat16 [3, 3, 320, 320], replicated
- b_dec1b: float32 [320], replicated
- w_head: bfloat16 [320, 4], replicated
- b_head: float32 [4], replicated
Outputs:
- output: float32 [256, 128, 4], P(('data', 'row'), 'col')
All inputs are finite; a program needn't handle non-finite values.
Results may differ from the reference program's by a relative error of at most 0.0171095.
Values are sent between devices in bfloat16 or wider.
A program may use at most 1 GiB of HBM per device.

```python
import jax
import jax.numpy as jnp
from jax import lax

IN_CH = 4
BASE_CH = 320
OUT_CH = 4
IMG_ROWS = 256
IMG_COLS = 128


def weight_specs():
    ch_one = BASE_CH
    ch_two = 2 * BASE_CH
    ch_four = 4 * BASE_CH
    bias_gain = 0.0625
    return [
        ("w_enc1a", (3, 3, IN_CH, ch_one), 9 * IN_CH, 2.0, jnp.bfloat16),
        ("b_enc1a", (ch_one,), 1, bias_gain, jnp.float32),
        ("w_enc1b", (3, 3, ch_one, ch_one), 9 * ch_one, 2.0, jnp.bfloat16),
        ("b_enc1b", (ch_one,), 1, bias_gain, jnp.float32),
        ("w_enc2a", (3, 3, ch_one, ch_two), 9 * ch_one, 2.0, jnp.bfloat16),
        ("b_enc2a", (ch_two,), 1, bias_gain, jnp.float32),
        ("w_enc2b", (3, 3, ch_two, ch_two), 9 * ch_two, 2.0, jnp.bfloat16),
        ("b_enc2b", (ch_two,), 1, bias_gain, jnp.float32),
        ("w_mid_a", (3, 3, ch_two, ch_four), 9 * ch_two, 2.0, jnp.bfloat16),
        ("b_mid_a", (ch_four,), 1, bias_gain, jnp.float32),
        ("w_mid_b", (3, 3, ch_four, ch_four), 9 * ch_four, 2.0, jnp.bfloat16),
        ("b_mid_b", (ch_four,), 1, bias_gain, jnp.float32),
        ("w_up2", (2, 2, ch_four, ch_two), ch_four, 1.0, jnp.bfloat16),
        ("w_dec2a", (3, 3, ch_four, ch_two), 9 * ch_four, 2.0, jnp.bfloat16),
        ("b_dec2a", (ch_two,), 1, bias_gain, jnp.float32),
        ("w_dec2b", (3, 3, ch_two, ch_two), 9 * ch_two, 2.0, jnp.bfloat16),
        ("b_dec2b", (ch_two,), 1, bias_gain, jnp.float32),
        ("w_up1", (2, 2, ch_two, ch_one), ch_two, 1.0, jnp.bfloat16),
        ("w_dec1a", (3, 3, ch_two, ch_one), 9 * ch_two, 2.0, jnp.bfloat16),
        ("b_dec1a", (ch_one,), 1, bias_gain, jnp.float32),
        ("w_dec1b", (3, 3, ch_one, ch_one), 9 * ch_one, 2.0, jnp.bfloat16),
        ("b_dec1b", (ch_one,), 1, bias_gain, jnp.float32),
        ("w_head", (ch_one, OUT_CH), ch_one, 1.0, jnp.bfloat16),
        ("b_head", (OUT_CH,), 1, bias_gain, jnp.float32),
    ]


def setup_inputs(seed: int = 0, part: int = 0) -> dict:
    root = jax.random.key(seed)
    image_key = jax.random.fold_in(jax.random.fold_in(root, 1000), part)
    pixels = jax.random.normal(image_key, (IMG_ROWS, IMG_COLS, IN_CH), jnp.float32)
    result = {"image": pixels.astype(jnp.bfloat16)}
    for index, spec in enumerate(weight_specs()):
        name, shape, fan_in, gain, dtype = spec
        values = jax.random.normal(jax.random.fold_in(root, index), shape, jnp.float32)
        result[name] = (values * (gain / fan_in) ** 0.5).astype(dtype)
    return result


def conv_relu(hidden, weight, bias):
    conv_out = lax.conv_general_dilated(hidden.astype(jnp.float32)[None], weight.astype(jnp.float32), (1, 1), "SAME", dimension_numbers=("NHWC", "HWIO", "NHWC"))[0]
    return jax.nn.relu(conv_out + bias).astype(jnp.bfloat16)


def double_conv(hidden, w_first, b_first, w_second, b_second):
    return conv_relu(conv_relu(hidden, w_first, b_first), w_second, b_second)


def max_pool(hidden):
    height, width, channels = hidden.shape
    return hidden.reshape(height // 2, 2, width // 2, 2, channels).max(axis=(1, 3))


def up_conv(hidden, weight):
    height = hidden.shape[0]
    width = hidden.shape[1]
    summed = jnp.einsum("ijc,abco->iajbo", hidden.astype(jnp.float32), weight.astype(jnp.float32))
    return summed.astype(jnp.bfloat16).reshape(2 * height, 2 * width, weight.shape[3])


def reference(image, w_enc1a, b_enc1a, w_enc1b, b_enc1b, w_enc2a, b_enc2a, w_enc2b, b_enc2b, w_mid_a, b_mid_a, w_mid_b, b_mid_b, w_up2, w_dec2a, b_dec2a, w_dec2b, b_dec2b, w_up1, w_dec1a, b_dec1a, w_dec1b, b_dec1b, w_head, b_head):
    skip_one = double_conv(image, w_enc1a, b_enc1a, w_enc1b, b_enc1b)
    skip_two = double_conv(max_pool(skip_one), w_enc2a, b_enc2a, w_enc2b, b_enc2b)
    middle = double_conv(max_pool(skip_two), w_mid_a, b_mid_a, w_mid_b, b_mid_b)
    hidden = double_conv(jnp.concatenate([up_conv(middle, w_up2), skip_two], axis=2), w_dec2a, b_dec2a, w_dec2b, b_dec2b)
    hidden = double_conv(jnp.concatenate([up_conv(hidden, w_up1), skip_one], axis=2), w_dec1a, b_dec1a, w_dec1b, b_dec1b)
    flat = hidden.reshape(-1, hidden.shape[2])
    head_out = jnp.dot(flat, w_head, preferred_element_type=jnp.float32) + b_head
    return head_out.reshape(hidden.shape[0], hidden.shape[1], w_head.shape[1])
```

```python
import functools

import jax
import jax.numpy as jnp
from jax import lax
from jax.experimental import pallas as pl
from jax.experimental.pallas import tpu as pltpu
from jax.sharding import PartitionSpec as P

BF16 = jnp.bfloat16
F32 = jnp.float32
MESH = pl.DeviceIdType.MESH
VMEM_LIMIT = 66_900_000
RING_ROWS = 11520


def strip_index():
    col = lax.axis_index("col")
    row = lax.axis_index("row")
    return row + col * (7 - 2 * row)


def strip_device(position):
    col = position // 4
    rest = position % 4
    return (lax.axis_index("data"), col, rest + col * (3 - 2 * rest))


def dot(a, b):
    return jnp.dot(a, b, preferred_element_type=F32)


def shifted(value, width, step):
    if step == 1:
        return value
    rows = value.shape[0]
    column = lax.broadcasted_iota(jnp.int32, value.shape, 0) % width
    if step == 0:
        return jnp.where(column == 0, 0.0, pltpu.roll(value, 1, axis=0))
    return jnp.where(column == width - 1, 0.0, pltpu.roll(value, rows - 1, axis=0))


def put3(dst, row0, lane0, channels, value, width):
    rows, lanes = value.shape
    for step in range(3):
        dst[pl.ds(row0, rows), pl.ds(step * channels + lane0, lanes)] = shifted(value, width, step).astype(BF16)


def put3_320(dst, row0, main, rest, width):
    rows = main.shape[0]
    for step in range(3):
        dst[pl.ds(row0, rows), pl.ds(step * 256, 256)] = shifted(main, width, step).astype(BF16)
    first = shifted(rest, width, 0) + pltpu.roll(rest, 64, axis=1)
    dst[pl.ds(row0, rows), pl.ds(768, 128)] = first.astype(BF16)
    dst[pl.ds(row0, rows), pl.ds(896, 128)] = shifted(rest, width, 2).astype(BF16)


def low_lanes(value):
    return jnp.where(lax.broadcasted_iota(jnp.int32, value.shape, 1) < 64, value, 0.0)


def pack_weights(staged, tap_rows, offset, main_ref, main0, rest_ref, rest0):
    for dj in range(3):
        for start, size, row in ((0, 256, 256 * dj), (256, 64, 768 + 64 * dj)):
            parts = []
            for di in range(3):
                base = (3 * di + dj) * tap_rows + offset + start
                main_ref[pl.ds(main0 + 1024 * di + row, size), :] = staged[pl.ds(base, size), 0:256]
                parts.append(staged[pl.ds(base, size), 256:320])
            parts.append(jnp.zeros((size, 64), BF16))
            rest_ref[pl.ds(rest0 + row, size), :] = jnp.concatenate(parts, axis=1)
    for di in range(3):
        main_ref[pl.ds(main0 + 1024 * di + 960, 64), :] = jnp.zeros((64, 256), BF16)
    rest_ref[pl.ds(rest0 + 960, 64), :] = jnp.zeros((64, 256), BF16)


def rest_sum(y_ref, row0, rows):
    total = y_ref[pl.ds(row0, rows), 0:128] + y_ref[pl.ds(row0 + 256, rows), 128:256]
    return total + pltpu.roll(y_ref[pl.ds(row0 + 128, rows), 0:128], 64, axis=1)


def valid_rows(value, first_row, width):
    row = first_row + lax.broadcasted_iota(jnp.int32, value.shape, 0) // width
    return jnp.where((row >= 0) & (row < 256), value, 0.0)


def pooled(value, width, scratch):
    rows, lanes = value.shape
    tall = jnp.concatenate(
        [jnp.maximum(value[s : s + width], value[s + width : s + 2 * width]) for s in range(0, rows, 2 * width)], axis=0
    )
    halves = []
    for start in range(0, lanes, 128):
        scratch[0 : rows // 2, :] = tall[:, start : start + 128]
        halves.append(
            jnp.maximum(scratch[pl.ds(0, rows // 4, stride=2), :], scratch[pl.ds(1, rows // 4, stride=2), :])
        )
    return jnp.concatenate(halves, axis=1) if len(halves) > 1 else halves[0]


def enc1_kernel(patch, w_a, b_a, w_b, b_b, s1_out, p1_out, x_a, y_rest, w_main, w_rest, pool_buf):
    block = pl.program_id(0)
    strip = strip_index()

    @pl.when(block == 0)
    def _():
        pack_weights(w_b, 320, 0, w_main, 0, w_rest, 0)

        def stem(i, carry):
            row0 = pl.multiple_of(i * 256, 256)
            acc = lax.dot_general(
                patch[:, pl.ds(row0, 256)], w_a[...], (((0,), (0,)), ((), ())), preferred_element_type=F32
            )
            value = valid_rows(jnp.maximum(acc + b_a[...], 0.0), 32 * strip - 3 + 2 * i, 128)
            put3_320(x_a, row0, value[:, 0:256], value[:, 256:384], 128)
            return carry

        lax.fori_loop(0, 19, stem, 0)

        def rest(i, carry):
            row0 = pl.multiple_of(i * 256, 256)
            y_rest[pl.ds(row0, 256), :] = dot(x_a[pl.ds(row0, 256), :], w_rest[...])
            return carry

        lax.fori_loop(0, 19, rest, 0)

    row0 = pl.multiple_of(block * 512, 512)
    acc = dot(x_a[pl.ds(row0, 512), :], w_main[0:1024, :])
    acc = acc + dot(x_a[pl.ds(row0 + 128, 512), :], w_main[1024:2048, :])
    acc = acc + dot(x_a[pl.ds(row0 + 256, 512), :], w_main[2048:3072, :])
    first_row = 32 * strip - 2 + 4 * block
    main = valid_rows(jnp.maximum(acc + b_b[:, 0:256], 0.0), first_row, 128)
    tail = low_lanes(valid_rows(jnp.maximum(rest_sum(y_rest, row0, 512) + b_b[:, 256:384], 0.0), first_row, 128))
    put3_320(s1_out, 0, main, tail, 128)
    put3_320(p1_out, 0, pooled(main, 128, pool_buf), pooled(tail, 128, pool_buf), 64)


def mid_kernel(
    p1, w_2a, w_2b, w_ma, w_mb, w_u2, w_d2a, w_d2b, b_2a, b_2b, b_ma, b_mb, b_d2a, b_d2b, out,
    first_w, ring, x_a, x_s, x_u, m_1, m_2, m_o, d_2, acc_ref, wide, pool_buf,
    sem_2a, sem_2b, sem_ma, sem_mb, sem_u2, sem_d2a, sem_d2b, sem_out, send_sem, recv_sem,
):
    strip = strip_index()
    prev_dev = strip_device((strip + 7) % 8)
    next_dev = strip_device((strip + 1) % 8)

    def exchange(buf, width, lane0, lanes, rows, index):
        lane = pl.ds(lane0, lanes)
        copies = []
        for side, src_row, dst_row, device in ((0, 1, rows + 1, prev_dev), (1, rows, 0, next_dev)):
            copies.append(
                pltpu.make_async_remote_copy(
                    src_ref=buf.at[pl.ds(src_row * width, width), lane],
                    dst_ref=buf.at[pl.ds(dst_row * width, width), lane],
                    send_sem=send_sem.at[index, side],
                    recv_sem=recv_sem.at[index, side],
                    device_id=device,
                    device_id_type=MESH,
                )
            )
        return copies

    def start(copies):
        for copy in copies:
            copy.start()

    def finish(copies):
        for copy in copies:
            copy.wait()

    def halo(buf, width, channels, rows, plain=False):
        for row, inside in ((0, strip > 0), (rows + 1, strip < 7)):
            lanes = pl.ds(0 if plain else channels, channels)
            value = buf[pl.ds(row * width, width), lanes].astype(F32)
            value = jnp.where(inside, value, 0.0)
            if plain:
                buf[pl.ds(row * width, width), lanes] = value.astype(BF16)
            else:
                put3(buf, row * width, 0, channels, value, width)

    copies_2a = []
    for tap in range(9):
        di, dj = tap // 3, tap % 3
        for part, (start_row, size, row) in enumerate(((0, 256, 256 * dj), (256, 64, 768 + 64 * dj))):
            copies_2a.append(
                pltpu.make_async_copy(
                    w_2a.at[pl.ds(320 * tap + start_row, size), :],
                    first_w.at[pl.ds(1024 * di + row, size), :],
                    sem_2a.at[2 * tap + part],
                )
            )

    def tap_copies(src, rows, base, sem):
        return [
            pltpu.make_async_copy(
                src.at[pl.ds(rows * tap, rows), :],
                ring.at[pl.ds(base + rows * (tap // 2), rows), pl.ds(640 * (tap % 2), 640)],
                sem.at[tap],
            )
            for tap in range(src.shape[0] // rows)
        ]

    copies_2b = tap_copies(w_2b, 640, 0, sem_2b)
    copies_ma = [
        pltpu.make_async_copy(w_ma.at[pl.ds(1920 * di, 1920), :], ring.at[pl.ds(3200 + 1920 * t, 1920), :], sem_ma.at[t])
        for t, di in enumerate((1, 0, 2))
    ]

    def mb_row(k):
        return (8960 + 1280 * k) % RING_ROWS

    copies_mb = [
        pltpu.make_async_copy(
            w_mb.at[pl.ds(1280 * (3 * (1, 0, 2)[k // 3] + k % 3), 1280), :], ring.at[pl.ds(mb_row(k), 1280), :], sem_mb.at[k]
        )
        for k in range(9)
    ]
    copies_u2 = tap_copies(w_u2, 1280, 8960, sem_u2)
    copies_d2a = tap_copies(w_d2a, 1280, 0, sem_d2a)
    copies_d2b = tap_copies(w_d2b, 640, 6400, sem_d2b)

    start(copies_2a)
    start(copies_2b)
    start(copies_ma)
    start(copies_mb[0:2])

    barrier = pltpu.get_barrier_semaphore()
    for device in (prev_dev, next_dev):
        pl.semaphore_signal(barrier, inc=1, device_id=device, device_id_type=MESH)
    pl.semaphore_wait(barrier, 2)

    for di in range(3):
        first_w[1024 * di + 960 : 1024 * di + 1024, :] = jnp.zeros((64, 640), BF16)
    finish(copies_2a)

    ex_a = exchange(x_a, 64, 640, 640, 16, 0)
    ex_s = exchange(x_s, 64, 640, 640, 16, 1)
    ex_m1 = exchange(m_1, 32, 640, 640, 8, 2)
    ex_m2 = exchange(m_2, 32, 1280, 1280, 8, 3)
    ex_u = exchange(x_u, 64, 640, 640, 16, 4)
    ex_b = exchange(x_a, 64, 640, 640, 16, 5)
    ex_d = exchange(d_2, 64, 0, 640, 16, 6)
    tiles = ((0, 256), (256, 256), (512, 128))

    def enc2a(i, carry):
        block = i + 1 - 2 * (i % 2)
        row0 = pl.multiple_of(block * 256, 256)

        @pl.when(i == 3)
        def _():
            start(ex_a)

        for lane0, lanes in tiles:
            acc = dot(p1[pl.ds(row0, 256), :], first_w[0:1024, pl.ds(lane0, lanes)])
            for di in (1, 2):
                acc = acc + dot(
                    p1[pl.ds(row0 + 64 * di, 256), :], first_w[1024 * di : 1024 * di + 1024, pl.ds(lane0, lanes)]
                )
            value = jnp.maximum(acc + b_2a[:, pl.ds(lane0, lanes)], 0.0)
            put3(x_a, row0 + 64, lane0, 640, value, 64)
        return carry

    lax.fori_loop(0, 4, enc2a, 0)
    finish(copies_2b)

    def conv640(src, row0, base, lane0, lanes):
        acc = None
        for di in range(3):
            weights = jnp.concatenate(
                [
                    ring[base + 640 * (t // 2) : base + 640 * (t // 2) + 640, pl.ds(640 * (t % 2) + lane0, lanes)]
                    for t in range(3 * di, 3 * di + 3)
                ],
                axis=0,
            )
            part = dot(src[pl.ds(row0 + 64 * di, 256), :], weights)
            acc = part if acc is None else acc + part
        return acc

    def enc2b(i, carry):
        block = i + 1 - 2 * (i % 2)
        row0 = pl.multiple_of(block * 256, 256)

        @pl.when(i == 1)
        def _():
            finish(ex_a)
            halo(x_a, 64, 640, 16)

        @pl.when(i == 3)
        def _():
            start(ex_m1)
            start(ex_s)

        for lane0, lanes in tiles:
            value = jnp.maximum(conv640(x_a, row0, 0, lane0, lanes) + b_2b[:, pl.ds(lane0, lanes)], 0.0)
            put3(x_s, row0 + 64, lane0, 640, value, 64)
            put3(m_1, pl.multiple_of(block * 64 + 32, 32), lane0, 640, pooled(value, 64, pool_buf), 32)
        return carry

    lax.fori_loop(0, 4, enc2b, 0)
    start(copies_mb[2:4])

    acc_ref[...] = jnp.zeros_like(acc_ref)
    finish(copies_ma)

    def mid_a(t, carry):
        di = (t + 1) % 2 + 2 * (t // 2) - t // 2

        @pl.when(t == 1)
        def _():
            finish(ex_m1)
            halo(m_1, 32, 640, 8)

        base = pl.multiple_of(3200 + 1920 * t, 128)
        lhs_row = pl.multiple_of(32 * di, 32)
        for lane0 in range(0, 1280, 256):
            acc_ref[:, pl.ds(lane0, 256)] += dot(
                m_1[pl.ds(lhs_row, 256), :], ring[pl.ds(base, 1920), pl.ds(lane0, 256)]
            )
        return carry

    lax.fori_loop(0, 3, mid_a, 0)
    start(copies_mb[4:9])
    for lane0 in range(0, 1280, 256):
        value = jnp.maximum(acc_ref[:, pl.ds(lane0, 256)] + b_ma[:, pl.ds(lane0, 256)], 0.0)
        put3(m_2, 32, lane0, 1280, value, 32)
    start(ex_m2)
    acc_ref[...] = jnp.zeros_like(acc_ref)

    def mid_b(k, carry):
        t = k // 3
        di = (t + 1) % 2 + 2 * (t // 2) - t // 2

        for j in range(9):
            @pl.when(k == j)
            def _(j=j):
                copies_mb[j].wait()

        @pl.when(k == 3)
        def _():
            start(copies_u2)
            finish(ex_m2)
            halo(m_2, 32, 1280, 8)

        @pl.when(k == 5)
        def _():
            start(copies_d2a[0:4])

        @pl.when(k == 8)
        def _():
            start(copies_d2a[4:9])

        base = pl.multiple_of(mb_row(k), 128)
        lhs_row = pl.multiple_of(32 * di, 32)
        lhs_lane = pl.multiple_of(1280 * (k % 3), 1280)
        for lane0 in range(0, 1280, 256):
            acc_ref[:, pl.ds(lane0, 256)] += dot(
                m_2[pl.ds(lhs_row, 256), pl.ds(lhs_lane, 1280)], ring[pl.ds(base, 1280), pl.ds(lane0, 256)]
            )
        return carry

    lax.fori_loop(0, 9, mid_b, 0)
    for lane0 in range(0, 1280, 256):
        value = jnp.maximum(acc_ref[:, pl.ds(lane0, 256)] + b_mb[:, pl.ds(lane0, 256)], 0.0)
        m_o[:, pl.ds(lane0, 256)] = value.astype(BF16)

    finish(copies_u2)
    for p in range(2):
        for q in range(2):
            for lane0 in range(0, 640, 128):
                wide[lane0 // 128, pl.ds(q, 256, stride=2), :] = dot(
                    m_o[...], ring[8960 + 1280 * p : 10240 + 1280 * p, pl.ds(640 * q + lane0, 128)]
                )

        def place(i, carry):
            src = pl.multiple_of(64 * i, 64)
            dst = pl.multiple_of(64 * (1 + 2 * i + p), 64)
            for lane0 in range(0, 640, 128):
                put3(x_u, dst, lane0, 640, wide[lane0 // 128, pl.ds(src, 64), :], 64)
            return carry

        lax.fori_loop(0, 8, place, 0)
    start(ex_u)
    start(copies_d2b)
    finish(ex_s)
    halo(x_s, 64, 640, 16)
    finish(copies_d2a)

    def dec2a(i, carry):
        block = i + 1 - 2 * (i % 2)
        row0 = pl.multiple_of(block * 256, 256)

        @pl.when(i == 1)
        def _():
            finish(ex_u)
            halo(x_u, 64, 640, 16)

        @pl.when(i == 3)
        def _():
            start(ex_b)

        for lane0, lanes in tiles:
            acc = None
            for tap in range(9):
                rows = pl.ds(row0 + 64 * (tap // 3), 256)
                cols = pl.ds(640 * (tap % 3), 640)
                lhs = jnp.concatenate([x_u[rows, cols], x_s[rows, cols]], axis=1)
                base = 1280 * (tap // 2)
                part = dot(lhs, ring[base : base + 1280, pl.ds(640 * (tap % 2) + lane0, lanes)])
                acc = part if acc is None else acc + part
            value = jnp.maximum(acc + b_d2a[:, pl.ds(lane0, lanes)], 0.0)
            put3(x_a, row0 + 64, lane0, 640, value, 64)
        return carry

    lax.fori_loop(0, 4, dec2a, 0)
    finish(copies_d2b)

    def dec2b(i, carry):
        block = i + 1 - 2 * (i % 2)
        row0 = pl.multiple_of(block * 256, 256)

        @pl.when(i == 1)
        def _():
            finish(ex_b)
            halo(x_a, 64, 640, 16)

        @pl.when(i == 3)
        def _():
            start(ex_d)

        for lane0, lanes in tiles:
            value = jnp.maximum(conv640(x_a, row0, 6400, lane0, lanes) + b_d2b[:, pl.ds(lane0, lanes)], 0.0)
            d_2[pl.ds(row0 + 64, 256), pl.ds(lane0, lanes)] = value.astype(BF16)
        return carry

    lax.fori_loop(0, 4, dec2b, 0)
    finish(ex_d)
    halo(d_2, 64, 640, 16, plain=True)
    result = pltpu.make_async_copy(d_2, out, sem_out)
    result.start()
    result.wait()


def dec1_kernel(
    d_2, s1, w_u1, w_d1a, w_d1b, b_d1a, b_d1b, w_head, b_head, out,
    x_u, x_s, x_d, y_rest, st_u, st_a, st_b, wu_rest, wa_main, wa_rest, wb_main, wb_rest, wide, sem,
):
    strip = strip_index()
    copy_u = pltpu.make_async_copy(w_u1, st_u, sem.at[0])
    copy_a = pltpu.make_async_copy(w_d1a, st_a, sem.at[1])
    copy_s = pltpu.make_async_copy(s1, x_s, sem.at[2])
    copy_b = pltpu.make_async_copy(w_d1b, st_b, sem.at[3])
    for copy in (copy_u, copy_a, copy_s, copy_b):
        copy.start()

    copy_u.wait()
    for start in range(0, 640, 128):
        wu_rest[start : start + 128, :] = jnp.concatenate(
            [st_u[640 * tap + start : 640 * tap + start + 128, 256:320] for tap in range(4)], axis=1
        )

    def up1(i, carry):
        row0 = pl.multiple_of(i * 384, 128)
        lhs = d_2[pl.ds(row0, 384), :]
        rest = dot(lhs, wu_rest[...])
        for p in range(2):
            part = rest[:, 128 * p : 128 * p + 128]
            wide[2, pl.ds(0, 384, stride=2), :] = low_lanes(part)
            wide[2, pl.ds(1, 384, stride=2), :] = low_lanes(pltpu.roll(part, 64, axis=1))
            for q in range(2):
                tap = 2 * p + q
                main = dot(lhs, st_u[640 * tap : 640 * tap + 640, 0:256])
                wide[0, pl.ds(q, 384, stride=2), :] = main[:, 0:128]
                wide[1, pl.ds(q, 384, stride=2), :] = main[:, 128:256]
            for r in range(6):
                main = jnp.concatenate([wide[0, 128 * r : 128 * r + 128, :], wide[1, 128 * r : 128 * r + 128, :]], axis=1)
                put3_320(
                    x_u, pl.multiple_of((12 * i + 2 * r + p) * 128, 128), main, wide[2, 128 * r : 128 * r + 128, :], 128
                )
        return carry

    lax.fori_loop(0, 3, up1, 0)

    copy_a.wait()
    for src in range(2):
        pack_weights(st_a, 640, 320 * src, wa_main, 3072 * src, wa_rest, 1024 * src)
    copy_s.wait()

    def rest_a(i, carry):
        row0 = pl.multiple_of(i * 256, 256)
        rows = pl.ds(row0, 256)
        y_rest[rows, :] = dot(x_u[rows, :], wa_rest[0:1024, :]) + dot(x_s[rows, :], wa_rest[1024:2048, :])
        return carry

    lax.fori_loop(0, 18, rest_a, 0)

    def dec1a(i, carry):
        row0 = pl.multiple_of(i * 256, 256)
        acc = None
        for di in range(3):
            rows = pl.ds(row0 + 128 * di, 256)
            for src, ref in enumerate((x_u, x_s)):
                base = 3072 * src + 1024 * di
                part = dot(ref[rows, :], wa_main[base : base + 1024, :])
                acc = part if acc is None else acc + part
        first_row = 32 * strip - 1 + 2 * i
        main = valid_rows(jnp.maximum(acc + b_d1a[:, 0:256], 0.0), first_row, 128)
        tail = valid_rows(jnp.maximum(rest_sum(y_rest, row0, 256) + b_d1a[:, 256:384], 0.0), first_row, 128)
        put3_320(x_d, row0, main, low_lanes(tail), 128)
        return carry

    lax.fori_loop(0, 17, dec1a, 0)

    copy_b.wait()
    pack_weights(st_b, 320, 0, wb_main, 0, wb_rest, 0)

    def rest_b(i, carry):
        rows = pl.ds(pl.multiple_of(i * 256, 256), 256)
        y_rest[rows, :] = dot(x_d[rows, :], wb_rest[...])
        return carry

    lax.fori_loop(0, 17, rest_b, 0)

    def dec1b(i, carry):
        row0 = pl.multiple_of(i * 512, 512)
        acc = dot(x_d[pl.ds(row0, 512), :], wb_main[0:1024, :])
        acc = acc + dot(x_d[pl.ds(row0 + 128, 512), :], wb_main[1024:2048, :])
        acc = acc + dot(x_d[pl.ds(row0 + 256, 512), :], wb_main[2048:3072, :])
        main = jnp.maximum(acc + b_d1b[:, 0:256], 0.0).astype(BF16)
        tail = low_lanes(jnp.maximum(rest_sum(y_rest, row0, 512) + b_d1b[:, 256:384], 0.0)).astype(BF16)
        hidden = jnp.concatenate([main, tail], axis=1)
        head = lax.dot_general(w_head[...], hidden, (((1,), (1,)), ((), ())), preferred_element_type=F32)
        out[:, pl.ds(row0, 512)] = head[0:8, :] + b_head[...]
        return carry

    lax.fori_loop(0, 8, dec1b, 0)


def solution(mesh):
    tile_spec = P(("data", "row"), "col", None)

    def body(image_tile, *params):
        (w_enc1a, b_enc1a, w_enc1b, b_enc1b, w_enc2a, b_enc2a, w_enc2b, b_enc2b,
         w_mid_a, b_mid_a, w_mid_b, b_mid_b, w_up2, w_dec2a, b_dec2a, w_dec2b, b_dec2b,
         w_up1, w_dec1a, b_dec1a, w_dec1b, b_dec1b, w_head, b_head) = params
        strip = strip_index()
        row = lax.axis_index("row")
        col = lax.axis_index("col")

        planes = lax.all_gather(image_tile.transpose(2, 0, 1), ("col", "row"), axis=0)
        planes = planes.reshape(2, 4, 4, 64, 64).transpose(2, 1, 3, 0, 4).reshape(4, 256, 128)
        planes = jnp.pad(planes, ((0, 0), (4, 4), (1, 1)))
        planes = lax.dynamic_slice_in_dim(planes, 32 * strip, 40, axis=1)
        patch = jnp.stack([planes[:, di : di + 38, dj : dj + 128] for di in range(3) for dj in range(3)])
        patch = jnp.pad(patch.reshape(36, 38 * 128), ((0, 12), (0, 0)))

        def flat(weight):
            return weight.reshape(-1, weight.shape[-1])

        def wide_bias(bias):
            return jnp.pad(bias, (0, 384 - bias.shape[0]))[None]

        vmem = pl.BlockSpec(memory_space=pltpu.VMEM)
        hbm = pl.BlockSpec(memory_space=pl.ANY)
        whole = lambda i: (0, 0)
        s1, p1 = pl.pallas_call(
            enc1_kernel,
            grid=(9,),
            out_shape=(jax.ShapeDtypeStruct((4608, 1024), BF16), jax.ShapeDtypeStruct((1152, 1024), BF16)),
            in_specs=[
                pl.BlockSpec((48, 4864), whole),
                pl.BlockSpec((48, 384), whole),
                pl.BlockSpec((1, 384), whole),
                pl.BlockSpec((2880, 320), whole),
                pl.BlockSpec((1, 384), whole),
            ],
            out_specs=(pl.BlockSpec((512, 1024), lambda i: (i, 0)), pl.BlockSpec((128, 1024), lambda i: (i, 0))),
            scratch_shapes=[
                pltpu.VMEM((4864, 1024), BF16),
                pltpu.VMEM((4864, 256), F32),
                pltpu.VMEM((3072, 256), BF16),
                pltpu.VMEM((1024, 256), BF16),
                pltpu.VMEM((256, 128), F32),
            ],
            compiler_params=pltpu.CompilerParams(vmem_limit_bytes=VMEM_LIMIT, dimension_semantics=("arbitrary",)),
            name="enc1",
        )(
            patch,
            jnp.pad(w_enc1a.reshape(36, 320), ((0, 12), (0, 64))),
            wide_bias(b_enc1a),
            flat(w_enc1b),
            wide_bias(b_enc1b),
        )

        dma = pltpu.SemaphoreType.DMA
        d2 = pl.pallas_call(
            mid_kernel,
            out_shape=jax.ShapeDtypeStruct((1152, 640), BF16),
            in_specs=[vmem] + [hbm] * 7 + [vmem] * 6,
            out_specs=hbm,
            scratch_shapes=[
                pltpu.VMEM((3072, 640), BF16),
                pltpu.VMEM((RING_ROWS, 1280), BF16),
                pltpu.VMEM((1152, 1920), BF16),
                pltpu.VMEM((1152, 1920), BF16),
                pltpu.VMEM((1152, 1920), BF16),
                pltpu.VMEM((320, 1920), BF16),
                pltpu.VMEM((320, 3840), BF16),
                pltpu.VMEM((256, 1280), BF16),
                pltpu.VMEM((1152, 640), BF16),
                pltpu.VMEM((256, 1280), F32),
                pltpu.VMEM((5, 512, 128), F32),
                pltpu.VMEM((128, 128), F32),
                dma((18,)), dma((9,)), dma((3,)), dma((9,)), dma((4,)), dma((9,)), dma((9,)), dma,
                dma((7, 2)), dma((7, 2)),
            ],
            compiler_params=pltpu.CompilerParams(
                vmem_limit_bytes=VMEM_LIMIT, collective_id=0, has_side_effects=True
            ),
            name="mid",
        )(
            p1, flat(w_enc2a), flat(w_enc2b), flat(w_mid_a), flat(w_mid_b), flat(w_up2), flat(w_dec2a), flat(w_dec2b),
            b_enc2a[None], b_enc2b[None], b_mid_a[None], b_mid_b[None], b_dec2a[None], b_dec2b[None],
        )

        y = pl.pallas_call(
            dec1_kernel,
            out_shape=jax.ShapeDtypeStruct((8, 4096), F32),
            in_specs=[vmem] + [hbm] * 4 + [vmem] * 4,
            out_specs=vmem,
            scratch_shapes=[
                pltpu.VMEM((4608, 1024), BF16),
                pltpu.VMEM((4608, 1024), BF16),
                pltpu.VMEM((4352, 1024), BF16),
                pltpu.VMEM((4608, 256), F32),
                pltpu.VMEM((2560, 320), BF16),
                pltpu.VMEM((5760, 320), BF16),
                pltpu.VMEM((2880, 320), BF16),
                pltpu.VMEM((640, 256), BF16),
                pltpu.VMEM((6144, 256), BF16),
                pltpu.VMEM((2048, 256), BF16),
                pltpu.VMEM((3072, 256), BF16),
                pltpu.VMEM((1024, 256), BF16),
                pltpu.VMEM((3, 768, 128), F32),
                dma((4,)),
            ],
            compiler_params=pltpu.CompilerParams(vmem_limit_bytes=VMEM_LIMIT),
            name="dec1",
        )(
            d2, s1, flat(w_up1), flat(w_dec1a), flat(w_dec1b), wide_bias(b_dec1a), wide_bias(b_dec1b),
            jnp.pad(w_head.T, ((0, 12), (0, 64))),
            jnp.pad(b_head, (0, 4))[:, None],
        )

        strips = lax.all_gather(y[0:4].reshape(4, 32, 128), ("col", "row"), axis=0)
        strips = jnp.concatenate([strips[0:4], strips[4:8][::-1]], axis=0)
        pair = lax.dynamic_slice_in_dim(strips, 2 * row, 2, axis=0)
        pair = lax.dynamic_slice_in_dim(pair, 64 * col, 64, axis=3)
        return pair.transpose(0, 2, 3, 1).reshape(64, 64, 4)

    def program(image, *params):
        mapped = jax.shard_map(
            body, mesh=mesh, in_specs=(tile_spec,) + (P(),) * len(params), out_specs=tile_spec, check_vma=False
        )
        return mapped(image, *params)

    return program
```

```python
import functools

import jax
import jax.numpy as jnp
from jax import lax
from jax.experimental import pallas as pl
from jax.experimental.pallas import tpu as pltpu
from jax.sharding import PartitionSpec as P

IN_CH = 4
FIVE = 5
SIX = 6
LAST_STRIP = 7
STRIPS = 8
TAPS = 9
N12 = 12
N16 = 16
N18 = 18
N28 = 28
N31 = 31
STRIP_ROWS = 32
N36 = 36
N40 = 40
N42 = 42
N60 = 60
REST = 64
N96 = 96
N127 = 127
LANES = 128
TILE = 256
BASE = 320
BASE_PAD = 384
N512 = 512
MIDDLE = 640
REST_AT = 768
N896 = 896
PACK_USED = 960
PACK = 1024
N1152 = 1152
DEEP = 1280
N1536 = 1536
N1792 = 1792
MIDDLE3 = 1920
N2048 = 2048
N2560 = 2560
N2880 = 2880
N3072 = 3072
N3200 = 3200
N3840 = 3840
N4096 = 4096
N4352 = 4352
N4608 = 4608
N5120 = 5120
N6144 = 6144
N6400 = 6400
N8960 = 8960
N10240 = 10240
N11520 = 11520
BF16 = jnp.bfloat16
F32 = jnp.float32
MESH = pl.DeviceIdType.MESH
VMEM_LIMIT = 66_900_000
RING_ROWS = N11520


def strip_index():
    col = lax.axis_index("col")
    row = lax.axis_index("row")
    return row + col * (LAST_STRIP - 2 * row)


def strip_device(position):
    col = position // IN_CH
    rest = position % IN_CH
    return (lax.axis_index("data"), col, rest + col * (3 - 2 * rest))


def dot(a, b):
    return jnp.dot(a, b, preferred_element_type=F32)


def shifted(value, width, step):
    if step == 1:
        return value
    rows = value.shape[0]
    column = lax.broadcasted_iota(jnp.int32, value.shape, 0) % width
    if step == 0:
        return jnp.where(column == 0, 0.0, pltpu.roll(value, 1, axis=0))
    return jnp.where(column == width - 1, 0.0, pltpu.roll(value, rows - 1, axis=0))


def put3(dst, row0, lane0, channels, value, width):
    rows, lanes = value.shape
    for step in range(3):
        dst[pl.ds(row0, rows), pl.ds(step * channels + lane0, lanes)] = shifted(value, width, step).astype(BF16)


def put3_320(dst, row0, main, rest, width):
    rows = main.shape[0]
    for step in range(3):
        dst[pl.ds(row0, rows), pl.ds(step * TILE, TILE)] = shifted(main, width, step).astype(BF16)
    first = shifted(rest, width, 0) + pltpu.roll(rest, REST, axis=1)
    dst[pl.ds(row0, rows), pl.ds(REST_AT, LANES)] = first.astype(BF16)
    dst[pl.ds(row0, rows), pl.ds(N896, LANES)] = shifted(rest, width, 2).astype(BF16)


def low_lanes(value):
    return jnp.where(lax.broadcasted_iota(jnp.int32, value.shape, 1) < REST, value, 0.0)


def pack_weights(staged, main_ref, rest_ref):
    for dj in range(3):
        for start, size, row in ((0, TILE, TILE * dj), (TILE, REST, REST_AT + REST * dj)):
            parts = []
            for di in range(3):
                base = (3 * di + dj) * BASE + start
                main_ref[pl.ds(PACK * di + row, size), :] = staged[pl.ds(base, size), 0:TILE]
                parts.append(staged[pl.ds(base, size), TILE:BASE])
            parts.append(jnp.zeros((size, REST), BF16))
            rest_ref[pl.ds(row, size), :] = jnp.concatenate(parts, axis=1)
    clear_pad(main_ref, 3)
    clear_pad(rest_ref, 1)


def clear_pad(ref, groups):
    for group in range(groups):
        ref[pl.ds(PACK * group + PACK_USED, REST), :] = jnp.zeros((REST, ref.shape[1]), BF16)


def pack_transposed(staged, main_ref, rest_ref):
    for dj in range(3):

        def main_part(di, carry):
            turned = staged[pl.ds(pl.multiple_of(PACK_USED * di + BASE * dj, REST), TILE), :].T
            for src in range(2):
                base = N3072 * src + PACK * di
                main_ref[pl.ds(pl.multiple_of(base + TILE * dj, REST), TILE), :] = turned[BASE * src : BASE * src + TILE]
                main_ref[pl.ds(pl.multiple_of(base + REST_AT + REST * dj, REST), REST), :] = turned[BASE * src + TILE : BASE * src + BASE]
            return carry

        lax.fori_loop(0, 3, main_part, 0)
        parts = [staged[pl.ds(PACK_USED * di + BASE * dj + TILE, REST), :] for di in range(3)] + [jnp.zeros((REST, MIDDLE), BF16)]
        turned = jnp.concatenate(parts, axis=0).T
        for src in range(2):
            rest_ref[pl.ds(PACK * src + TILE * dj, TILE), :] = turned[BASE * src : BASE * src + TILE]
            rest_ref[pl.ds(PACK * src + REST_AT + REST * dj, REST), :] = turned[BASE * src + TILE : BASE * src + BASE]
    clear_pad(main_ref, SIX)
    clear_pad(rest_ref, 2)


def bias_row(ref, start, size):
    return ref[pl.ds(start, size)].reshape(1, size)


def bias_rest(ref):
    return jnp.concatenate([bias_row(ref, TILE, REST), jnp.zeros((1, REST), F32)], axis=1)


def enter_barrier():
    barrier = pltpu.get_barrier_semaphore()
    for position in range(STRIPS):
        pl.semaphore_signal(barrier, inc=1, device_id=strip_device(position), device_id_type=MESH)
    return barrier


class Push:
    def __init__(self, src, dst, send_sem, recv_sem, device, here):
        self.here = here
        self.local = pltpu.make_async_copy(src, dst, recv_sem)
        self.remote = pltpu.make_async_remote_copy(
            src_ref=src, dst_ref=dst, send_sem=send_sem, recv_sem=recv_sem, device_id=device, device_id_type=MESH
        )

    def start(self):
        @pl.when(self.here)
        def _():
            self.local.start()

        @pl.when(jnp.logical_not(self.here))
        def _():
            self.remote.start()

    def wait_send(self):
        @pl.when(jnp.logical_not(self.here))
        def _():
            self.remote.wait_send()

    def wait_recv(self):
        self.remote.wait_recv()


def rest_sum(y_ref, row0, rows):
    total = y_ref[pl.ds(row0, rows), 0:LANES] + y_ref[pl.ds(row0 + TILE, rows), LANES:TILE]
    return total + pltpu.roll(y_ref[pl.ds(row0 + LANES, rows), 0:LANES], REST, axis=1)


def valid_rows(value, first_row, width):
    row = first_row + lax.broadcasted_iota(jnp.int32, value.shape, 0) // width
    return jnp.where((row >= 0) & (row < TILE), value, 0.0)


def pooled(value, width, scratch):
    rows, lanes = value.shape
    tall = jnp.concatenate(
        [jnp.maximum(value[s : s + width], value[s + width : s + 2 * width]) for s in range(0, rows, 2 * width)], axis=0
    )
    halves = []
    for start in range(0, lanes, LANES):
        scratch[0 : rows // 2, :] = tall[:, start : start + LANES]
        halves.append(
            jnp.maximum(scratch[pl.ds(0, rows // IN_CH, stride=2), :], scratch[pl.ds(1, rows // IN_CH, stride=2), :])
        )
    return jnp.concatenate(halves, axis=1) if len(halves) > 1 else halves[0]


def enc1_kernel(
    image, w_a, b_a, w_b, b_b, s1_out, p1_out,
    halves, planes, w_stem, staged, x_a, y_rest, w_main, w_rest, pool_buf, w_sem, send_sem, recv_sem,
):
    step = pl.program_id(0)
    strip = strip_index()

    @pl.when(step == 0)
    def _():
        row = lax.axis_index("row")
        col = lax.axis_index("col")
        copy_w = pltpu.make_async_copy(w_b, staged, w_sem)
        copy_w.start()
        barrier = enter_barrier()

        for di in range(3):
            taps = []
            for dj in range(3):
                tap = jnp.concatenate([w_a[di, dj].astype(F32), jnp.zeros((IN_CH, BASE), F32)], axis=0)
                taps.append(jnp.concatenate([tap, jnp.zeros((STRIPS, REST), F32)], axis=1))
            taps.append(jnp.zeros((STRIPS, BASE_PAD), F32))
            w_stem[STRIP_ROWS * di : STRIP_ROWS * di + STRIP_ROWS, :] = jnp.concatenate(taps, axis=0).astype(BF16)
        planes[N40:N42, :, :] = jnp.zeros((2, STRIP_ROWS, LANES), BF16)

        pl.semaphore_wait(barrier, STRIPS)
        pushes = []
        for index, (target, src_row, dst_row, rows) in enumerate(
            ((2 * row, 0, IN_CH, N36), (2 * row + 1, N28, 0, N36), ((2 * row + 2) % STRIPS, N60, 0, IN_CH), ((2 * row + LAST_STRIP) % STRIPS, 0, N36, IN_CH))
        ):
            pushes.append(
                Push(
                    image.at[pl.ds(src_row, rows)],
                    halves.at[col, pl.ds(dst_row, rows)],
                    send_sem.at[index],
                    recv_sem.at[index // 2, col],
                    strip_device(target),
                    target == strip,
                )
            )
        for push in pushes:
            push.start()
        copy_w.wait()
        pack_weights(staged, w_main, w_rest)
        for push in pushes:
            push.wait_send()
        for kind, rows in ((0, N36), (1, IN_CH)):
            for side in range(2):
                Push(
                    image.at[pl.ds(0, rows)], halves.at[side, pl.ds(0, rows)],
                    send_sem.at[0], recv_sem.at[kind, side], strip_device(strip), strip < 0,
                ).wait_recv()

        def expand(i, carry):
            for j in range(STRIPS):
                r = STRIPS * i + j
                both = jnp.concatenate([halves[0, r].astype(F32), halves[1, r].astype(F32)], axis=1)
                image_row = STRIP_ROWS * strip - IN_CH + r
                both = jnp.where((image_row >= 0) & (image_row < TILE), both, 0.0)
                both = jnp.concatenate([both, jnp.zeros((IN_CH, LANES), F32)], axis=0)
                column = lax.broadcasted_iota(jnp.int32, (STRIPS, LANES), 1)
                before = jnp.where(column == 0, 0.0, pltpu.roll(both, 1, axis=1))
                after = jnp.where(column == N127, 0.0, pltpu.roll(both, N127, axis=1))
                planes[r] = jnp.concatenate([before, both, after, jnp.zeros((STRIPS, LANES), F32)], axis=0).astype(BF16)
            return carry

        lax.fori_loop(0, FIVE, expand, 0)

        def stem(i, carry):
            for j in range(IN_CH):
                r = STRIPS * i + 2 * j
                row0 = pl.multiple_of(r * LANES, TILE)
                patch = jnp.concatenate(
                    [jnp.concatenate([planes[r + k + di] for di in range(3)], axis=0) for k in range(2)], axis=1
                )
                acc = lax.dot_general(patch, w_stem[...], (((0,), (0,)), ((), ())), preferred_element_type=F32)
                main = jnp.maximum(acc[:, 0:TILE] + bias_row(b_a, 0, TILE), 0.0)
                tail = jnp.maximum(acc[:, TILE:BASE_PAD] + bias_rest(b_a), 0.0)
                first_row = STRIP_ROWS * strip - 3 + r
                put3_320(x_a, row0, valid_rows(main, first_row, LANES), valid_rows(tail, first_row, LANES), LANES)
            return carry

        lax.fori_loop(0, FIVE, stem, 0)

    base = pl.multiple_of(step * N1536, N512)

    def rest(j):
        y_rest[TILE * j : TILE * j + TILE, :] = dot(x_a[pl.ds(base + TILE * j, TILE), :], w_rest[...])

    rest(0)
    for j in range(SIX):
        rest(j + 1)
        acc = dot(x_a[pl.ds(base + TILE * j, TILE), :], w_main[0:PACK, :])
        acc = acc + dot(x_a[pl.ds(base + TILE * j + LANES, TILE), :], w_main[PACK:N2048, :])
        acc = acc + dot(x_a[pl.ds(base + TILE * j + TILE, TILE), :], w_main[N2048:N3072, :])
        first_row = STRIP_ROWS * strip - 2 + N12 * step + 2 * j
        main = valid_rows(jnp.maximum(acc + bias_row(b_b, 0, TILE), 0.0), first_row, LANES)
        tail = jnp.maximum(rest_sum(y_rest, TILE * j, TILE) + bias_rest(b_b), 0.0)
        tail = low_lanes(valid_rows(tail, first_row, LANES))
        put3_320(s1_out, TILE * j, main, tail, LANES)
        put3_320(p1_out, REST * j, pooled(main, LANES, pool_buf), pooled(tail, LANES, pool_buf), REST)


def mid_kernel(
    p1, w_2a, w_2b, w_ma, w_mb, w_u2, w_d2a, w_d2b, b_2a, b_2b, b_ma, b_mb, b_d2a, b_d2b, out,
    first_w, ring, x_a, x_s, x_u, m_1, m_2, m_o, d_2, acc_ref, wide, pool_buf,
    sem_2a, sem_2b, sem_ma, sem_mb, sem_u2, sem_d2a, sem_d2b, sem_out, send_sem, recv_sem,
):
    strip = strip_index()
    prev_dev = strip_device((strip + LAST_STRIP) % STRIPS)
    next_dev = strip_device((strip + 1) % STRIPS)

    def exchange(buf, width, lane0, lanes, rows, index):
        lane = pl.ds(lane0, lanes)
        copies = []
        for side, src_row, dst_row, device in ((0, 1, rows + 1, prev_dev), (1, rows, 0, next_dev)):
            copies.append(
                pltpu.make_async_remote_copy(
                    src_ref=buf.at[pl.ds(src_row * width, width), lane],
                    dst_ref=buf.at[pl.ds(dst_row * width, width), lane],
                    send_sem=send_sem.at[index, side],
                    recv_sem=recv_sem.at[index, side],
                    device_id=device,
                    device_id_type=MESH,
                )
            )
        return copies

    def start(copies):
        for copy in copies:
            copy.start()

    def finish(copies):
        for copy in copies:
            copy.wait()

    def halo(buf, width, channels, rows, plain=False):
        for row, inside in ((0, strip > 0), (rows + 1, strip < LAST_STRIP)):
            lanes = pl.ds(0 if plain else channels, channels)
            value = buf[pl.ds(row * width, width), lanes].astype(F32)
            value = jnp.where(inside, value, 0.0)
            if plain:
                buf[pl.ds(row * width, width), lanes] = value.astype(BF16)
            else:
                put3(buf, row * width, 0, channels, value, width)

    copies_2a = []
    for tap in range(TAPS):
        di, dj = tap // 3, tap % 3
        for part, (start_row, size, row) in enumerate(((0, TILE, TILE * dj), (TILE, REST, REST_AT + REST * dj))):
            copies_2a.append(
                pltpu.make_async_copy(
                    w_2a.at[pl.ds(BASE * tap + start_row, size), :],
                    first_w.at[pl.ds(PACK * di + row, size), :],
                    sem_2a.at[2 * tap + part],
                )
            )

    def tap_copies(src, rows, base, sem):
        return [
            pltpu.make_async_copy(
                src.at[pl.ds(rows * tap, rows), :],
                ring.at[pl.ds(base + rows * (tap // 2), rows), pl.ds(MIDDLE * (tap % 2), MIDDLE)],
                sem.at[tap],
            )
            for tap in range(src.shape[0] // rows)
        ]

    copies_2b = tap_copies(w_2b, MIDDLE, 0, sem_2b)
    copies_ma = [
        pltpu.make_async_copy(w_ma.at[pl.ds(MIDDLE3 * di, MIDDLE3), :], ring.at[pl.ds(N3200 + MIDDLE3 * t, MIDDLE3), :], sem_ma.at[t])
        for t, di in enumerate((1, 0, 2))
    ]

    def mb_row(k):
        return (N8960 + DEEP * k) % RING_ROWS

    copies_mb = [
        pltpu.make_async_copy(
            w_mb.at[pl.ds(DEEP * (3 * (1, 0, 2)[k // 3] + k % 3), DEEP), :], ring.at[pl.ds(mb_row(k), DEEP), :], sem_mb.at[k]
        )
        for k in range(TAPS)
    ]
    copies_u2 = tap_copies(w_u2, DEEP, N8960, sem_u2)
    copies_d2a = tap_copies(w_d2a, DEEP, 0, sem_d2a)
    copies_d2b = tap_copies(w_d2b, MIDDLE, N6400, sem_d2b)

    start(copies_2a)
    start(copies_2b)
    start(copies_ma)
    start(copies_mb[0:2])

    barrier = pltpu.get_barrier_semaphore()
    for device in (prev_dev, next_dev):
        pl.semaphore_signal(barrier, inc=1, device_id=device, device_id_type=MESH)
    pl.semaphore_wait(barrier, 2)

    for di in range(3):
        first_w[PACK * di + PACK_USED : PACK * di + PACK, :] = jnp.zeros((REST, MIDDLE), BF16)
    finish(copies_2a)

    ex_a = exchange(x_a, REST, MIDDLE, MIDDLE, N16, 0)
    ex_s = exchange(x_s, REST, MIDDLE, MIDDLE, N16, 1)
    ex_m1 = exchange(m_1, STRIP_ROWS, MIDDLE, MIDDLE, STRIPS, 2)
    ex_m2 = exchange(m_2, STRIP_ROWS, DEEP, DEEP, STRIPS, 3)
    ex_u = exchange(x_u, REST, MIDDLE, MIDDLE, N16, IN_CH)
    ex_b = exchange(x_a, REST, MIDDLE, MIDDLE, N16, FIVE)
    ex_d = exchange(d_2, REST, 0, MIDDLE, N16, SIX)
    tiles = ((0, TILE), (TILE, TILE), (N512, LANES))

    def enc2a(i, carry):
        block = i + 1 - 2 * (i % 2)
        row0 = pl.multiple_of(block * TILE, TILE)

        @pl.when(i == 3)
        def _():
            start(ex_a)

        for lane0, lanes in tiles:
            acc = dot(p1[pl.ds(row0, TILE), :], first_w[0:PACK, pl.ds(lane0, lanes)])
            for di in (1, 2):
                acc = acc + dot(
                    p1[pl.ds(row0 + REST * di, TILE), :], first_w[PACK * di : PACK * di + PACK, pl.ds(lane0, lanes)]
                )
            value = jnp.maximum(acc + bias_row(b_2a, lane0, lanes), 0.0)
            put3(x_a, row0 + REST, lane0, MIDDLE, value, REST)
        return carry

    lax.fori_loop(0, IN_CH, enc2a, 0)
    finish(copies_2b)

    def conv640(src, row0, base, lane0, lanes):
        acc = None
        for di in range(3):
            weights = jnp.concatenate(
                [
                    ring[base + MIDDLE * (t // 2) : base + MIDDLE * (t // 2) + MIDDLE, pl.ds(MIDDLE * (t % 2) + lane0, lanes)]
                    for t in range(3 * di, 3 * di + 3)
                ],
                axis=0,
            )
            part = dot(src[pl.ds(row0 + REST * di, TILE), :], weights)
            acc = part if acc is None else acc + part
        return acc

    def enc2b(i, carry):
        block = i + 1 - 2 * (i % 2)
        row0 = pl.multiple_of(block * TILE, TILE)

        @pl.when(i == 1)
        def _():
            finish(ex_a)
            halo(x_a, REST, MIDDLE, N16)

        @pl.when(i == 3)
        def _():
            start(ex_m1)
            start(ex_s)

        for lane0, lanes in tiles:
            value = jnp.maximum(conv640(x_a, row0, 0, lane0, lanes) + bias_row(b_2b, lane0, lanes), 0.0)
            put3(x_s, row0 + REST, lane0, MIDDLE, value, REST)
            put3(m_1, pl.multiple_of(block * REST + STRIP_ROWS, STRIP_ROWS), lane0, MIDDLE, pooled(value, REST, pool_buf), STRIP_ROWS)
        return carry

    lax.fori_loop(0, IN_CH, enc2b, 0)
    start(copies_mb[2:IN_CH])

    acc_ref[...] = jnp.zeros_like(acc_ref)
    finish(copies_ma)

    def mid_a(t, carry):
        di = (t + 1) % 2 + 2 * (t // 2) - t // 2

        @pl.when(t == 1)
        def _():
            finish(ex_m1)
            halo(m_1, STRIP_ROWS, MIDDLE, STRIPS)

        base = pl.multiple_of(N3200 + MIDDLE3 * t, LANES)
        lhs_row = pl.multiple_of(STRIP_ROWS * di, STRIP_ROWS)
        for lane0 in range(0, DEEP, TILE):
            acc_ref[:, pl.ds(lane0, TILE)] += dot(
                m_1[pl.ds(lhs_row, TILE), :], ring[pl.ds(base, MIDDLE3), pl.ds(lane0, TILE)]
            )
        return carry

    lax.fori_loop(0, 3, mid_a, 0)
    start(copies_mb[IN_CH:TAPS])
    for lane0 in range(0, DEEP, TILE):
        value = jnp.maximum(acc_ref[:, pl.ds(lane0, TILE)] + bias_row(b_ma, lane0, TILE), 0.0)
        put3(m_2, STRIP_ROWS, lane0, DEEP, value, STRIP_ROWS)
    start(ex_m2)
    acc_ref[...] = jnp.zeros_like(acc_ref)

    def mid_b(k, carry):
        t = k // 3
        di = (t + 1) % 2 + 2 * (t // 2) - t // 2

        for j in range(TAPS):
            @pl.when(k == j)
            def _(j=j):
                copies_mb[j].wait()

        @pl.when(k == 3)
        def _():
            start(copies_u2)
            finish(ex_m2)
            halo(m_2, STRIP_ROWS, DEEP, STRIPS)

        @pl.when(k == FIVE)
        def _():
            start(copies_d2a[0:IN_CH])

        @pl.when(k == STRIPS)
        def _():
            start(copies_d2a[IN_CH:TAPS])

        base = pl.multiple_of(mb_row(k), LANES)
        lhs_row = pl.multiple_of(STRIP_ROWS * di, STRIP_ROWS)
        lhs_lane = pl.multiple_of(DEEP * (k % 3), DEEP)
        for lane0 in range(0, DEEP, TILE):
            acc_ref[:, pl.ds(lane0, TILE)] += dot(
                m_2[pl.ds(lhs_row, TILE), pl.ds(lhs_lane, DEEP)], ring[pl.ds(base, DEEP), pl.ds(lane0, TILE)]
            )
        return carry

    lax.fori_loop(0, TAPS, mid_b, 0)
    for lane0 in range(0, DEEP, TILE):
        value = jnp.maximum(acc_ref[:, pl.ds(lane0, TILE)] + bias_row(b_mb, lane0, TILE), 0.0)
        m_o[:, pl.ds(lane0, TILE)] = value.astype(BF16)

    finish(copies_u2)
    for p in range(2):
        for q in range(2):
            for lane0, lanes in tiles:
                part = dot(m_o[...], ring[N8960 + DEEP * p : N10240 + DEEP * p, pl.ds(MIDDLE * q + lane0, lanes)])
                for lane in range(0, lanes, LANES):
                    wide[(lane0 + lane) // LANES, pl.ds(q, TILE, stride=2), :] = part[:, lane : lane + LANES]

        def place(i, carry):
            src = pl.multiple_of(REST * i, REST)
            dst = pl.multiple_of(REST * (1 + 2 * i + p), REST)
            for lane0 in range(0, MIDDLE, LANES):
                put3(x_u, dst, lane0, MIDDLE, wide[lane0 // LANES, pl.ds(src, REST), :], REST)
            return carry

        lax.fori_loop(0, STRIPS, place, 0)
    start(ex_u)
    start(copies_d2b)
    finish(ex_s)
    halo(x_s, REST, MIDDLE, N16)
    finish(copies_d2a)

    def dec2a(i, carry):
        block = i + 1 - 2 * (i % 2)
        row0 = pl.multiple_of(block * TILE, TILE)

        @pl.when(i == 1)
        def _():
            finish(ex_u)
            halo(x_u, REST, MIDDLE, N16)

        @pl.when(i == 3)
        def _():
            start(ex_b)

        for lane0, lanes in tiles:
            acc = None
            for tap in range(TAPS):
                rows = pl.ds(row0 + REST * (tap // 3), TILE)
                cols = pl.ds(MIDDLE * (tap % 3), MIDDLE)
                lhs = jnp.concatenate([x_u[rows, cols], x_s[rows, cols]], axis=1)
                base = DEEP * (tap // 2)
                part = dot(lhs, ring[base : base + DEEP, pl.ds(MIDDLE * (tap % 2) + lane0, lanes)])
                acc = part if acc is None else acc + part
            value = jnp.maximum(acc + bias_row(b_d2a, lane0, lanes), 0.0)
            put3(x_a, row0 + REST, lane0, MIDDLE, value, REST)
        return carry

    lax.fori_loop(0, IN_CH, dec2a, 0)
    finish(copies_d2b)

    def dec2b(i, carry):
        block = i + 1 - 2 * (i % 2)
        row0 = pl.multiple_of(block * TILE, TILE)

        @pl.when(i == 1)
        def _():
            finish(ex_b)
            halo(x_a, REST, MIDDLE, N16)

        @pl.when(i == 3)
        def _():
            start(ex_d)

        for lane0, lanes in tiles:
            value = jnp.maximum(conv640(x_a, row0, N6400, lane0, lanes) + bias_row(b_d2b, lane0, lanes), 0.0)
            d_2[pl.ds(row0 + REST, TILE), pl.ds(lane0, lanes)] = value.astype(BF16)
        return carry

    lax.fori_loop(0, IN_CH, dec2b, 0)
    finish(ex_d)
    halo(d_2, REST, MIDDLE, N16, plain=True)
    result = pltpu.make_async_copy(d_2, out, sem_out)
    result.start()
    result.wait()


def dec1_kernel(
    d_2, s1, w_u1, w_d1a, w_d1b, b_d1a, b_d1b, w_head, b_head, out,
    x_u, x_s, x_d, y_rest, st_u, st_a, st_b, wu_main, wu_rest, wa_main, wa_rest, wb_main, wb_rest, wide, result,
    sem, send_sem, recv_sem,
):
    strip = strip_index()
    row = lax.axis_index("row")
    col = lax.axis_index("col")
    copy_u = pltpu.make_async_copy(w_u1, st_u, sem.at[0])
    copy_a = pltpu.make_async_copy(w_d1a, st_a, sem.at[1])
    copy_s = pltpu.make_async_copy(s1, x_s, sem.at[2])
    copy_b = pltpu.make_async_copy(w_d1b, st_b, sem.at[3])
    for copy in (copy_u, copy_a, copy_s, copy_b):
        copy.start()
    barrier = enter_barrier()

    copy_u.wait()
    for tap in range(IN_CH):
        wu_main[MIDDLE * tap : MIDDLE * tap + MIDDLE, :] = st_u[BASE * tap : BASE * tap + TILE, :].T
    wu_rest[...] = jnp.concatenate([st_u[BASE * tap + TILE : BASE * tap + BASE, :] for tap in range(IN_CH)], axis=0).T

    def up1(i, carry):
        row0 = pl.multiple_of(i * BASE_PAD, LANES)
        lhs = d_2[pl.ds(row0, BASE_PAD), :]
        rest = dot(lhs, wu_rest[...])
        for p in range(2):
            part = rest[:, LANES * p : LANES * p + LANES]
            buf = wide.at[p]
            buf[2, pl.ds(0, BASE_PAD, stride=2), :] = low_lanes(part)
            buf[2, pl.ds(1, BASE_PAD, stride=2), :] = low_lanes(pltpu.roll(part, REST, axis=1))
            for q in range(2):
                tap = 2 * p + q
                main = dot(lhs, wu_main[MIDDLE * tap : MIDDLE * tap + MIDDLE, :])
                buf[0, pl.ds(q, BASE_PAD, stride=2), :] = main[:, 0:LANES]
                buf[1, pl.ds(q, BASE_PAD, stride=2), :] = main[:, LANES:TILE]
            for r in range(SIX):
                main = jnp.concatenate([buf[0, LANES * r : LANES * r + LANES, :], buf[1, LANES * r : LANES * r + LANES, :]], axis=1)
                put3_320(
                    x_u, pl.multiple_of((N12 * i + 2 * r + p) * LANES, LANES), main, buf[2, LANES * r : LANES * r + LANES, :], LANES
                )
        return carry

    lax.fori_loop(0, 3, up1, 0)

    copy_a.wait()
    pack_transposed(st_a, wa_main, wa_rest)
    copy_s.wait()

    def rest_a(i, carry):
        for j in range(SIX):
            rows = pl.ds(pl.multiple_of(i * N1536 + TILE * j, TILE), TILE)
            y_rest[rows, :] = dot(x_u[rows, :], wa_rest[0:PACK, :]) + dot(x_s[rows, :], wa_rest[PACK:N2048, :])
        return carry

    lax.fori_loop(0, 3, rest_a, 0)

    def conv_a(row0, first_row):
        acc = None
        for di in range(3):
            rows = pl.ds(row0 + LANES * di, TILE)
            for src, ref in enumerate((x_u, x_s)):
                base = N3072 * src + PACK * di
                part = dot(ref[rows, :], wa_main[base : base + PACK, :])
                acc = part if acc is None else acc + part
        main = valid_rows(jnp.maximum(acc + bias_row(b_d1a, 0, TILE), 0.0), first_row, LANES)
        tail = valid_rows(jnp.maximum(rest_sum(y_rest, row0, TILE) + bias_rest(b_d1a), 0.0), first_row, LANES)
        put3_320(x_d, row0, main, low_lanes(tail), LANES)

    def dec1a(i, carry):
        for j in range(IN_CH):
            conv_a(pl.multiple_of(i * PACK + TILE * j, TILE), STRIP_ROWS * strip - 1 + STRIPS * i + 2 * j)
        return carry

    lax.fori_loop(0, IN_CH, dec1a, 0)
    conv_a(N4096, STRIP_ROWS * strip + N31)

    copy_b.wait()
    pack_weights(st_b, wb_main, wb_rest)
    head_bias = jnp.zeros((IN_CH, LANES), F32)
    for channel in range(IN_CH):
        head_bias = jnp.where(lax.broadcasted_iota(jnp.int32, (IN_CH, LANES), 0) == channel, b_head[channel], head_bias)

    def dec1b(i, carry):
        base = pl.multiple_of(i * PACK, PACK)

        def rest(j):
            y_rest[TILE * j : TILE * j + TILE, :] = dot(x_d[pl.ds(base + TILE * j, TILE), :], wb_rest[...])

        rest(0)
        for j in range(IN_CH):
            rest(j + 1)
            acc = dot(x_d[pl.ds(base + TILE * j, TILE), :], wb_main[0:PACK, :])
            acc = acc + dot(x_d[pl.ds(base + TILE * j + LANES, TILE), :], wb_main[PACK:N2048, :])
            acc = acc + dot(x_d[pl.ds(base + TILE * j + TILE, TILE), :], wb_main[N2048:N3072, :])
            main = jnp.maximum(acc + bias_row(b_d1b, 0, TILE), 0.0).astype(BF16)
            tail = jnp.maximum(rest_sum(y_rest, TILE * j, TILE) + bias_rest(b_d1b), 0.0).astype(BF16)
            hidden = jnp.concatenate([main, tail[:, 0:REST]], axis=1)
            head = lax.dot_general(w_head[...], hidden, (((1,), (1,)), ((), ())), preferred_element_type=F32)
            for r in range(2):
                line = head[:, LANES * r : LANES * r + LANES] + head_bias
                result[0, STRIPS * i + 2 * j + r] = line[:, 0:REST]
                result[1, STRIPS * i + 2 * j + r] = line[:, REST:LANES]
        return carry

    lax.fori_loop(0, IN_CH, dec1b, 0)

    pl.semaphore_wait(barrier, STRIPS)
    pushes = []
    for side in range(2):
        tile_row = strip // 2
        pushes.append(
            Push(
                result.at[side],
                out.at[pl.ds(STRIP_ROWS * (strip % 2), STRIP_ROWS)],
                send_sem.at[side],
                recv_sem.at[strip % 2],
                (lax.axis_index("data"), side, tile_row),
                (tile_row == row) & (col == side),
            )
        )
    for push in pushes:
        push.start()
    for push in pushes:
        push.wait_send()
    for half in range(2):
        Push(
            result.at[0], out.at[pl.ds(STRIP_ROWS * half, STRIP_ROWS)], send_sem.at[0], recv_sem.at[half], strip_device(strip), strip < 0
        ).wait_recv()


def solution(mesh):
    tile_spec = P(("data", "row"), "col", None)

    def body(image_tile, *params):
        (w_enc1a, b_enc1a, w_enc1b, b_enc1b, w_enc2a, b_enc2a, w_enc2b, b_enc2b,
         w_mid_a, b_mid_a, w_mid_b, b_mid_b, w_up2, w_dec2a, b_dec2a, w_dec2b, b_dec2b,
         w_up1, w_dec1a, b_dec1a, w_dec1b, b_dec1b, w_head, b_head) = params
        def flat(weight):
            return weight.reshape(-1, weight.shape[-1])

        vmem = pl.BlockSpec(memory_space=pltpu.VMEM)
        hbm = pl.BlockSpec(memory_space=pl.ANY)
        dma = pltpu.SemaphoreType.DMA
        s1, p1 = pl.pallas_call(
            enc1_kernel,
            grid=(3,),
            out_shape=(jax.ShapeDtypeStruct((N4608, PACK), BF16), jax.ShapeDtypeStruct((N1152, PACK), BF16)),
            in_specs=[vmem, vmem, vmem, hbm, vmem],
            out_specs=(pl.BlockSpec((N1536, PACK), lambda i: (i, 0)), pl.BlockSpec((BASE_PAD, PACK), lambda i: (i, 0))),
            scratch_shapes=[
                pltpu.VMEM((2, N40, IN_CH, REST), BF16),
                pltpu.VMEM((N42, STRIP_ROWS, LANES), BF16),
                pltpu.VMEM((N96, BASE_PAD), BF16),
                pltpu.VMEM((N2880, BASE), BF16),
                pltpu.VMEM((N5120, PACK), BF16),
                pltpu.VMEM((N1792, TILE), F32),
                pltpu.VMEM((N3072, TILE), BF16),
                pltpu.VMEM((PACK, TILE), BF16),
                pltpu.VMEM((LANES, LANES), F32),
                dma, dma((IN_CH,)), dma((2, 2)),
            ],
            compiler_params=pltpu.CompilerParams(
                vmem_limit_bytes=VMEM_LIMIT, collective_id=1, has_side_effects=True, dimension_semantics=("arbitrary",)
            ),
            name="enc1",
        )(image_tile.transpose(0, 2, 1), w_enc1a, b_enc1a, flat(w_enc1b), b_enc1b)

        d2 = pl.pallas_call(
            mid_kernel,
            out_shape=jax.ShapeDtypeStruct((N1152, MIDDLE), BF16),
            in_specs=[vmem] + [hbm] * LAST_STRIP + [vmem] * SIX,
            out_specs=hbm,
            scratch_shapes=[
                pltpu.VMEM((N3072, MIDDLE), BF16),
                pltpu.VMEM((RING_ROWS, DEEP), BF16),
                pltpu.VMEM((N1152, MIDDLE3), BF16),
                pltpu.VMEM((N1152, MIDDLE3), BF16),
                pltpu.VMEM((N1152, MIDDLE3), BF16),
                pltpu.VMEM((BASE, MIDDLE3), BF16),
                pltpu.VMEM((BASE, N3840), BF16),
                pltpu.VMEM((TILE, DEEP), BF16),
                pltpu.VMEM((N1152, MIDDLE), BF16),
                pltpu.VMEM((TILE, DEEP), F32),
                pltpu.VMEM((FIVE, N512, LANES), F32),
                pltpu.VMEM((LANES, LANES), F32),
                dma((N18,)), dma((TAPS,)), dma((3,)), dma((TAPS,)), dma((IN_CH,)), dma((TAPS,)), dma((TAPS,)), dma,
                dma((LAST_STRIP, 2)), dma((LAST_STRIP, 2)),
            ],
            compiler_params=pltpu.CompilerParams(
                vmem_limit_bytes=VMEM_LIMIT, collective_id=0, has_side_effects=True
            ),
            name="mid",
        )(
            p1, flat(w_enc2a), flat(w_enc2b), flat(w_mid_a), flat(w_mid_b), flat(w_up2), flat(w_dec2a), flat(w_dec2b),
            b_enc2a, b_enc2b, b_mid_a, b_mid_b, b_dec2a, b_dec2b,
        )

        def turned(weight):
            return weight.transpose(0, 1, 3, 2).reshape(-1, weight.shape[2])

        y = pl.pallas_call(
            dec1_kernel,
            out_shape=jax.ShapeDtypeStruct((REST, IN_CH, REST), F32),
            in_specs=[vmem] + [hbm] * IN_CH + [vmem] * 3 + [pl.BlockSpec(memory_space=pltpu.SMEM)],
            out_specs=hbm,
            scratch_shapes=[
                pltpu.VMEM((N4608, PACK), BF16),
                pltpu.VMEM((N4608, PACK), BF16),
                pltpu.VMEM((N4352, PACK), BF16),
                pltpu.VMEM((N4608, TILE), F32),
                pltpu.VMEM((DEEP, MIDDLE), BF16),
                pltpu.VMEM((N2880, MIDDLE), BF16),
                pltpu.VMEM((N2880, BASE), BF16),
                pltpu.VMEM((N2560, TILE), BF16),
                pltpu.VMEM((MIDDLE, TILE), BF16),
                pltpu.VMEM((N6144, TILE), BF16),
                pltpu.VMEM((N2048, TILE), BF16),
                pltpu.VMEM((N3072, TILE), BF16),
                pltpu.VMEM((PACK, TILE), BF16),
                pltpu.VMEM((2, 3, REST_AT, LANES), F32),
                pltpu.VMEM((2, STRIP_ROWS, IN_CH, REST), F32),
                dma((IN_CH,)), dma((2,)), dma((2,)),
            ],
            compiler_params=pltpu.CompilerParams(vmem_limit_bytes=VMEM_LIMIT, collective_id=2, has_side_effects=True),
            name="dec1",
        )(d2, s1, turned(w_up1), turned(w_dec1a), flat(w_dec1b), b_dec1a, b_dec1b, w_head.T, b_head)
        return y.transpose(0, 2, 1)

    def program(image, *params):
        mapped = jax.shard_map(
            body, mesh=mesh, in_specs=(tile_spec,) + (P(),) * len(params), out_specs=tile_spec, check_vma=False
        )
        return mapped(image, *params)

    return program
```

```python
import functools

import jax
import jax.numpy as jnp
from jax import lax
from jax.experimental import pallas as pl
from jax.experimental.pallas import tpu as pltpu
from jax.sharding import PartitionSpec as P

IN_CH = 4
FIVE = 5
SIX = 6
LAST_STRIP = 7
STRIPS = 8
TAPS = 9
N12 = 12
N16 = 16
N18 = 18
N28 = 28
N31 = 31
STRIP_ROWS = 32
N36 = 36
N40 = 40
N42 = 42
N60 = 60
REST = 64
N96 = 96
N127 = 127
LANES = 128
TILE = 256
BASE = 320
BASE_PAD = 384
N512 = 512
MIDDLE = 640
REST_AT = 768
N896 = 896
PACK_USED = 960
PACK = 1024
N1152 = 1152
DEEP = 1280
N1536 = 1536
N1792 = 1792
MIDDLE3 = 1920
N2048 = 2048
N2560 = 2560
N2880 = 2880
N3072 = 3072
N3200 = 3200
N3840 = 3840
N4096 = 4096
N4352 = 4352
N4608 = 4608
N5120 = 5120
N6144 = 6144
N6400 = 6400
N8960 = 8960
N10240 = 10240
N11520 = 11520
BF16 = jnp.bfloat16
F32 = jnp.float32
MESH = pl.DeviceIdType.MESH
VMEM_LIMIT = 66_900_000
RING_ROWS = N11520


def strip_index():
    col = lax.axis_index("col")
    row = lax.axis_index("row")
    return row + col * (LAST_STRIP - 2 * row)


def strip_device(position):
    col = position // IN_CH
    rest = position % IN_CH
    return (lax.axis_index("data"), col, rest + col * (3 - 2 * rest))


def dot(a, b):
    return jnp.dot(a, b, preferred_element_type=F32)


def shifted(value, width, step):
    if step == 1:
        return value
    rows = value.shape[0]
    column = lax.broadcasted_iota(jnp.int32, value.shape, 0) % width
    if step == 0:
        return jnp.where(column == 0, 0.0, pltpu.roll(value, 1, axis=0))
    return jnp.where(column == width - 1, 0.0, pltpu.roll(value, rows - 1, axis=0))


def put3(dst, row0, lane0, channels, value, width):
    rows, lanes = value.shape
    for step in range(3):
        dst[pl.ds(row0, rows), pl.ds(step * channels + lane0, lanes)] = shifted(value, width, step).astype(BF16)


def put3_320(dst, row0, main, rest, width):
    rows = main.shape[0]
    for step in range(3):
        dst[pl.ds(row0, rows), pl.ds(step * TILE, TILE)] = shifted(main, width, step).astype(BF16)
    first = shifted(rest, width, 0) + pltpu.roll(rest, REST, axis=1)
    dst[pl.ds(row0, rows), pl.ds(REST_AT, LANES)] = first.astype(BF16)
    dst[pl.ds(row0, rows), pl.ds(N896, LANES)] = shifted(rest, width, 2).astype(BF16)


def low_lanes(value):
    return jnp.where(lax.broadcasted_iota(jnp.int32, value.shape, 1) < REST, value, 0.0)


def pack_weights(staged, main_ref, rest_ref):
    for dj in range(3):
        for start, size, row in ((0, TILE, TILE * dj), (TILE, REST, REST_AT + REST * dj)):
            parts = []
            for di in range(3):
                base = (3 * di + dj) * BASE + start
                main_ref[pl.ds(PACK * di + row, size), :] = staged[pl.ds(base, size), 0:TILE]
                parts.append(staged[pl.ds(base, size), TILE:BASE])
            parts.append(jnp.zeros((size, REST), BF16))
            rest_ref[pl.ds(row, size), :] = jnp.concatenate(parts, axis=1)
    clear_pad(main_ref, 3)
    clear_pad(rest_ref, 1)


def clear_pad(ref, groups):
    for group in range(groups):
        ref[pl.ds(PACK * group + PACK_USED, REST), :] = jnp.zeros((REST, ref.shape[1]), BF16)


def pack_transposed(staged, main_ref, rest_ref):
    for dj in range(3):

        def main_part(di, carry):
            turned = staged[pl.ds(pl.multiple_of(PACK_USED * di + BASE * dj, REST), TILE), :].T
            for src in range(2):
                base = N3072 * src + PACK * di
                main_ref[pl.ds(pl.multiple_of(base + TILE * dj, REST), TILE), :] = turned[BASE * src : BASE * src + TILE]
                main_ref[pl.ds(pl.multiple_of(base + REST_AT + REST * dj, REST), REST), :] = turned[BASE * src + TILE : BASE * src + BASE]
            return carry

        lax.fori_loop(0, 3, main_part, 0)
        parts = [staged[pl.ds(PACK_USED * di + BASE * dj + TILE, REST), :] for di in range(3)] + [jnp.zeros((REST, MIDDLE), BF16)]
        turned = jnp.concatenate(parts, axis=0).T
        for src in range(2):
            rest_ref[pl.ds(PACK * src + TILE * dj, TILE), :] = turned[BASE * src : BASE * src + TILE]
            rest_ref[pl.ds(PACK * src + REST_AT + REST * dj, REST), :] = turned[BASE * src + TILE : BASE * src + BASE]
    clear_pad(main_ref, SIX)
    clear_pad(rest_ref, 2)


def bias_row(ref, start, size):
    return ref[pl.ds(start, size)].reshape(1, size)


def bias_rest(ref):
    return jnp.concatenate([bias_row(ref, TILE, REST), jnp.zeros((1, REST), F32)], axis=1)


def enter_barrier():
    barrier = pltpu.get_barrier_semaphore()
    for position in range(STRIPS):
        pl.semaphore_signal(barrier, inc=1, device_id=strip_device(position), device_id_type=MESH)
    return barrier


class Push:
    def __init__(self, src, dst, send_sem, recv_sem, device, here):
        self.here = here
        self.local = pltpu.make_async_copy(src, dst, recv_sem)
        self.remote = pltpu.make_async_remote_copy(
            src_ref=src, dst_ref=dst, send_sem=send_sem, recv_sem=recv_sem, device_id=device, device_id_type=MESH
        )

    def start(self):
        @pl.when(self.here)
        def _():
            self.local.start()

        @pl.when(jnp.logical_not(self.here))
        def _():
            self.remote.start()

    def wait_send(self):
        @pl.when(jnp.logical_not(self.here))
        def _():
            self.remote.wait_send()

    def wait_recv(self):
        self.remote.wait_recv()


def rest_sum(y_ref, row0, rows):
    total = y_ref[pl.ds(row0, rows), 0:LANES] + y_ref[pl.ds(row0 + TILE, rows), LANES:TILE]
    return total + pltpu.roll(y_ref[pl.ds(row0 + LANES, rows), 0:LANES], REST, axis=1)


def valid_rows(value, first_row, width):
    row = first_row + lax.broadcasted_iota(jnp.int32, value.shape, 0) // width
    return jnp.where((row >= 0) & (row < TILE), value, 0.0)


def pooled(value, width, scratch):
    rows, lanes = value.shape
    tall = jnp.concatenate(
        [jnp.maximum(value[s : s + width], value[s + width : s + 2 * width]) for s in range(0, rows, 2 * width)], axis=0
    )
    halves = []
    for start in range(0, lanes, LANES):
        scratch[0 : rows // 2, :] = tall[:, start : start + LANES]
        halves.append(
            jnp.maximum(scratch[pl.ds(0, rows // IN_CH, stride=2), :], scratch[pl.ds(1, rows // IN_CH, stride=2), :])
        )
    return jnp.concatenate(halves, axis=1) if len(halves) > 1 else halves[0]


def enc1_kernel(
    image, w_a, b_a, w_b, b_b, s1_out, p1_out,
    halves, planes, w_stem, staged, x_a, y_rest, w_main, w_rest, pool_buf, w_sem, send_sem, recv_sem,
):
    step = pl.program_id(0)
    strip = strip_index()

    @pl.when(step == 0)
    def _():
        row = lax.axis_index("row")
        col = lax.axis_index("col")
        copy_w = pltpu.make_async_copy(w_b, staged, w_sem)
        copy_w.start()
        barrier = enter_barrier()

        for di in range(3):
            taps = []
            for dj in range(3):
                tap = jnp.concatenate([w_a[di, dj].astype(F32), jnp.zeros((IN_CH, BASE), F32)], axis=0)
                taps.append(jnp.concatenate([tap, jnp.zeros((STRIPS, REST), F32)], axis=1))
            taps.append(jnp.zeros((STRIPS, BASE_PAD), F32))
            w_stem[STRIP_ROWS * di : STRIP_ROWS * di + STRIP_ROWS, :] = jnp.concatenate(taps, axis=0).astype(BF16)
        planes[N40:N42, :, :] = jnp.zeros((2, STRIP_ROWS, LANES), BF16)

        pl.semaphore_wait(barrier, STRIPS)
        pushes = []
        for index, (target, src_row, dst_row, rows) in enumerate(
            ((2 * row, 0, IN_CH, N36), (2 * row + 1, N28, 0, N36), ((2 * row + 2) % STRIPS, N60, 0, IN_CH), ((2 * row + LAST_STRIP) % STRIPS, 0, N36, IN_CH))
        ):
            pushes.append(
                Push(
                    image.at[pl.ds(src_row, rows)],
                    halves.at[col, pl.ds(dst_row, rows)],
                    send_sem.at[index],
                    recv_sem.at[index // 2, col],
                    strip_device(target),
                    target == strip,
                )
            )
        for push in pushes:
            push.start()
        copy_w.wait()
        pack_weights(staged, w_main, w_rest)
        for push in pushes:
            push.wait_send()
        for kind, rows in ((0, N36), (1, IN_CH)):
            for side in range(2):
                Push(
                    image.at[pl.ds(0, rows)], halves.at[side, pl.ds(0, rows)],
                    send_sem.at[0], recv_sem.at[kind, side], strip_device(strip), strip < 0,
                ).wait_recv()

        def expand(i, carry):
            for j in range(STRIPS):
                r = STRIPS * i + j
                both = jnp.concatenate([halves[0, r].astype(F32), halves[1, r].astype(F32)], axis=1)
                image_row = STRIP_ROWS * strip - IN_CH + r
                both = jnp.where((image_row >= 0) & (image_row < TILE), both, 0.0)
                both = jnp.concatenate([both, jnp.zeros((IN_CH, LANES), F32)], axis=0)
                column = lax.broadcasted_iota(jnp.int32, (STRIPS, LANES), 1)
                before = jnp.where(column == 0, 0.0, pltpu.roll(both, 1, axis=1))
                after = jnp.where(column == N127, 0.0, pltpu.roll(both, N127, axis=1))
                planes[r] = jnp.concatenate([before, both, after, jnp.zeros((STRIPS, LANES), F32)], axis=0).astype(BF16)
            return carry

        lax.fori_loop(0, FIVE, expand, 0)

        def stem(i, carry):
            for j in range(IN_CH):
                r = STRIPS * i + 2 * j
                row0 = pl.multiple_of(r * LANES, TILE)
                patch = jnp.concatenate(
                    [jnp.concatenate([planes[r + k + di] for di in range(3)], axis=0) for k in range(2)], axis=1
                )
                acc = lax.dot_general(patch, w_stem[...], (((0,), (0,)), ((), ())), preferred_element_type=F32)
                main = jnp.maximum(acc[:, 0:TILE] + bias_row(b_a, 0, TILE), 0.0)
                tail = jnp.maximum(acc[:, TILE:BASE_PAD] + bias_rest(b_a), 0.0)
                first_row = STRIP_ROWS * strip - 3 + r
                put3_320(x_a, row0, valid_rows(main, first_row, LANES), valid_rows(tail, first_row, LANES), LANES)
            return carry

        lax.fori_loop(0, FIVE, stem, 0)

    base = pl.multiple_of(step * N1536, N512)

    def rest(j):
        y_rest[TILE * j : TILE * j + TILE, :] = dot(x_a[pl.ds(base + TILE * j, TILE), 0:PACK], w_rest[...])

    rest(0)
    for j in range(SIX):
        rest(j + 1)
        acc = dot(x_a[pl.ds(base + TILE * j, TILE), 0:PACK], w_main[0:PACK, :])
        acc = acc + dot(x_a[pl.ds(base + TILE * j + LANES, TILE), 0:PACK], w_main[PACK:N2048, :])
        acc = acc + dot(x_a[pl.ds(base + TILE * j + TILE, TILE), 0:PACK], w_main[N2048:N3072, :])
        first_row = STRIP_ROWS * strip - 2 + N12 * step + 2 * j
        main = valid_rows(jnp.maximum(acc + bias_row(b_b, 0, TILE), 0.0), first_row, LANES)
        tail = jnp.maximum(rest_sum(y_rest, TILE * j, TILE) + bias_rest(b_b), 0.0)
        tail = low_lanes(valid_rows(tail, first_row, LANES))
        put3_320(s1_out, TILE * j, main, tail, LANES)
        put3_320(p1_out, REST * j, pooled(main, LANES, pool_buf), pooled(tail, LANES, pool_buf), REST)


def mid_kernel(
    p1, w_2a, w_2b, w_ma, w_mb, w_u2, w_d2a, w_d2b, b_2a, b_2b, b_ma, b_mb, b_d2a, b_d2b, out,
    first_w, ring, x_a, x_s, x_u, m_1, m_2, m_o, d_2, acc_ref, wide, pool_buf,
    sem_2a, sem_2b, sem_ma, sem_mb, sem_u2, sem_d2a, sem_d2b, sem_out, send_sem, recv_sem,
):
    strip = strip_index()
    prev_dev = strip_device((strip + LAST_STRIP) % STRIPS)
    next_dev = strip_device((strip + 1) % STRIPS)

    def exchange(buf, width, lane0, lanes, rows, index):
        lane = pl.ds(lane0, lanes)
        copies = []
        for side, src_row, dst_row, device in ((0, 1, rows + 1, prev_dev), (1, rows, 0, next_dev)):
            copies.append(
                pltpu.make_async_remote_copy(
                    src_ref=buf.at[pl.ds(src_row * width, width), lane],
                    dst_ref=buf.at[pl.ds(dst_row * width, width), lane],
                    send_sem=send_sem.at[index, side],
                    recv_sem=recv_sem.at[index, side],
                    device_id=device,
                    device_id_type=MESH,
                )
            )
        return copies

    def start(copies):
        for copy in copies:
            copy.start()

    def finish(copies):
        for copy in copies:
            copy.wait()

    def halo(buf, width, channels, rows, plain=False):
        for row, inside in ((0, strip > 0), (rows + 1, strip < LAST_STRIP)):
            lanes = pl.ds(0 if plain else channels, channels)
            value = buf[pl.ds(row * width, width), lanes].astype(F32)
            value = jnp.where(inside, value, 0.0)
            if plain:
                buf[pl.ds(row * width, width), lanes] = value.astype(BF16)
            else:
                put3(buf, row * width, 0, channels, value, width)

    copies_2a = []
    for tap in range(TAPS):
        di, dj = tap // 3, tap % 3
        for part, (start_row, size, row) in enumerate(((0, TILE, TILE * dj), (TILE, REST, REST_AT + REST * dj))):
            copies_2a.append(
                pltpu.make_async_copy(
                    w_2a.at[pl.ds(BASE * tap + start_row, size), :],
                    first_w.at[pl.ds(PACK * di + row, size), :],
                    sem_2a.at[2 * tap + part],
                )
            )

    def tap_copies(src, rows, base, sem):
        return [
            pltpu.make_async_copy(
                src.at[pl.ds(rows * tap, rows), :],
                ring.at[pl.ds(base + rows * (tap // 2), rows), pl.ds(MIDDLE * (tap % 2), MIDDLE)],
                sem.at[tap],
            )
            for tap in range(src.shape[0] // rows)
        ]

    copies_2b = tap_copies(w_2b, MIDDLE, 0, sem_2b)
    copies_ma = [
        pltpu.make_async_copy(w_ma.at[pl.ds(MIDDLE3 * di, MIDDLE3), :], ring.at[pl.ds(N3200 + MIDDLE3 * t, MIDDLE3), :], sem_ma.at[t])
        for t, di in enumerate((1, 0, 2))
    ]

    def mb_row(k):
        return (N8960 + DEEP * k) % RING_ROWS

    copies_mb = [
        pltpu.make_async_copy(
            w_mb.at[pl.ds(DEEP * (3 * (1, 0, 2)[k // 3] + k % 3), DEEP), :], ring.at[pl.ds(mb_row(k), DEEP), :], sem_mb.at[k]
        )
        for k in range(TAPS)
    ]
    copies_u2 = tap_copies(w_u2, DEEP, N8960, sem_u2)
    copies_d2a = tap_copies(w_d2a, DEEP, 0, sem_d2a)
    copies_d2b = tap_copies(w_d2b, MIDDLE, N6400, sem_d2b)

    start(copies_2a)
    start(copies_2b)
    start(copies_ma)
    start(copies_mb[0:2])

    barrier = pltpu.get_barrier_semaphore()
    for device in (prev_dev, next_dev):
        pl.semaphore_signal(barrier, inc=1, device_id=device, device_id_type=MESH)
    pl.semaphore_wait(barrier, 2)

    for di in range(3):
        first_w[PACK * di + PACK_USED : PACK * di + PACK, :] = jnp.zeros((REST, MIDDLE), BF16)
    finish(copies_2a)

    ex_a = exchange(x_a, REST, MIDDLE, MIDDLE, N16, 0)
    ex_s = exchange(x_s, REST, MIDDLE, MIDDLE, N16, 1)
    ex_m1 = exchange(m_1, STRIP_ROWS, MIDDLE, MIDDLE, STRIPS, 2)
    ex_m2 = exchange(m_2, STRIP_ROWS, DEEP, DEEP, STRIPS, 3)
    ex_u = exchange(x_u, REST, MIDDLE, MIDDLE, N16, IN_CH)
    ex_b = exchange(x_a, REST, MIDDLE, MIDDLE, N16, FIVE)
    ex_d = exchange(d_2, REST, 0, MIDDLE, N16, SIX)
    tiles = ((0, TILE), (TILE, TILE), (N512, LANES))

    def enc2a(i, carry):
        block = i + 1 - 2 * (i % 2)
        row0 = pl.multiple_of(block * TILE, TILE)

        @pl.when(i == 3)
        def _():
            start(ex_a)

        for lane0, lanes in tiles:
            acc = dot(p1[pl.ds(row0, TILE), 0:PACK], first_w[0:PACK, pl.ds(lane0, lanes)])
            for di in (1, 2):
                acc = acc + dot(
                    p1[pl.ds(row0 + REST * di, TILE), 0:PACK], first_w[PACK * di : PACK * di + PACK, pl.ds(lane0, lanes)]
                )
            value = jnp.maximum(acc + bias_row(b_2a, lane0, lanes), 0.0)
            put3(x_a, row0 + REST, lane0, MIDDLE, value, REST)
        return carry

    lax.fori_loop(0, IN_CH, enc2a, 0)
    finish(copies_2b)

    def conv640(src, row0, base, lane0, lanes):
        acc = None
        for di in range(3):
            weights = jnp.concatenate(
                [
                    ring[base + MIDDLE * (t // 2) : base + MIDDLE * (t // 2) + MIDDLE, pl.ds(MIDDLE * (t % 2) + lane0, lanes)]
                    for t in range(3 * di, 3 * di + 3)
                ],
                axis=0,
            )
            part = dot(src[pl.ds(row0 + REST * di, TILE), :], weights)
            acc = part if acc is None else acc + part
        return acc

    def enc2b(i, carry):
        block = i + 1 - 2 * (i % 2)
        row0 = pl.multiple_of(block * TILE, TILE)

        @pl.when(i == 1)
        def _():
            finish(ex_a)
            halo(x_a, REST, MIDDLE, N16)

        @pl.when(i == 3)
        def _():
            start(ex_m1)
            start(ex_s)

        for lane0, lanes in tiles:
            value = jnp.maximum(conv640(x_a, row0, 0, lane0, lanes) + bias_row(b_2b, lane0, lanes), 0.0)
            put3(x_s, row0 + REST, lane0, MIDDLE, value, REST)
            put3(m_1, pl.multiple_of(block * REST + STRIP_ROWS, STRIP_ROWS), lane0, MIDDLE, pooled(value, REST, pool_buf), STRIP_ROWS)
        return carry

    lax.fori_loop(0, IN_CH, enc2b, 0)
    start(copies_mb[2:IN_CH])

    acc_ref[...] = jnp.zeros_like(acc_ref)
    finish(copies_ma)

    def mid_a(t, carry):
        di = (t + 1) % 2 + 2 * (t // 2) - t // 2

        @pl.when(t == 1)
        def _():
            finish(ex_m1)
            halo(m_1, STRIP_ROWS, MIDDLE, STRIPS)

        base = pl.multiple_of(N3200 + MIDDLE3 * t, LANES)
        lhs_row = pl.multiple_of(STRIP_ROWS * di, STRIP_ROWS)
        for lane0 in range(0, DEEP, TILE):
            acc_ref[:, pl.ds(lane0, TILE)] += dot(
                m_1[pl.ds(lhs_row, TILE), :], ring[pl.ds(base, MIDDLE3), pl.ds(lane0, TILE)]
            )
        return carry

    lax.fori_loop(0, 3, mid_a, 0)
    start(copies_mb[IN_CH:TAPS])
    for lane0 in range(0, DEEP, TILE):
        value = jnp.maximum(acc_ref[:, pl.ds(lane0, TILE)] + bias_row(b_ma, lane0, TILE), 0.0)
        put3(m_2, STRIP_ROWS, lane0, DEEP, value, STRIP_ROWS)
    start(ex_m2)
    acc_ref[...] = jnp.zeros_like(acc_ref)

    def mid_b(k, carry):
        t = k // 3
        di = (t + 1) % 2 + 2 * (t // 2) - t // 2

        for j in range(TAPS):
            @pl.when(k == j)
            def _(j=j):
                copies_mb[j].wait()

        @pl.when(k == 3)
        def _():
            start(copies_u2)
            finish(ex_m2)
            halo(m_2, STRIP_ROWS, DEEP, STRIPS)

        @pl.when(k == FIVE)
        def _():
            start(copies_d2a[0:IN_CH])

        @pl.when(k == STRIPS)
        def _():
            start(copies_d2a[IN_CH:TAPS])

        base = pl.multiple_of(mb_row(k), LANES)
        lhs_row = pl.multiple_of(STRIP_ROWS * di, STRIP_ROWS)
        lhs_lane = pl.multiple_of(DEEP * (k % 3), DEEP)
        for lane0 in range(0, DEEP, TILE):
            acc_ref[:, pl.ds(lane0, TILE)] += dot(
                m_2[pl.ds(lhs_row, TILE), pl.ds(lhs_lane, DEEP)], ring[pl.ds(base, DEEP), pl.ds(lane0, TILE)]
            )
        return carry

    lax.fori_loop(0, TAPS, mid_b, 0)
    for lane0 in range(0, DEEP, TILE):
        value = jnp.maximum(acc_ref[:, pl.ds(lane0, TILE)] + bias_row(b_mb, lane0, TILE), 0.0)
        m_o[:, pl.ds(lane0, TILE)] = value.astype(BF16)

    finish(copies_u2)
    for p in range(2):
        for q in range(2):
            for lane0, lanes in tiles:
                part = dot(m_o[...], ring[N8960 + DEEP * p : N10240 + DEEP * p, pl.ds(MIDDLE * q + lane0, lanes)])
                for lane in range(0, lanes, LANES):
                    wide[(lane0 + lane) // LANES, pl.ds(q, TILE, stride=2), :] = part[:, lane : lane + LANES]

        def place(i, carry):
            src = pl.multiple_of(REST * i, REST)
            dst = pl.multiple_of(REST * (1 + 2 * i + p), REST)
            for lane0 in range(0, MIDDLE, LANES):
                put3(x_u, dst, lane0, MIDDLE, wide[lane0 // LANES, pl.ds(src, REST), :], REST)
            return carry

        lax.fori_loop(0, STRIPS, place, 0)
    start(ex_u)
    start(copies_d2b)
    finish(ex_s)
    halo(x_s, REST, MIDDLE, N16)
    finish(copies_d2a)

    def dec2a(i, carry):
        block = i + 1 - 2 * (i % 2)
        row0 = pl.multiple_of(block * TILE, TILE)

        @pl.when(i == 1)
        def _():
            finish(ex_u)
            halo(x_u, REST, MIDDLE, N16)

        @pl.when(i == 3)
        def _():
            start(ex_b)

        for lane0, lanes in tiles:
            acc = None
            for tap in range(TAPS):
                rows = pl.ds(row0 + REST * (tap // 3), TILE)
                cols = pl.ds(MIDDLE * (tap % 3), MIDDLE)
                lhs = jnp.concatenate([x_u[rows, cols], x_s[rows, cols]], axis=1)
                base = DEEP * (tap // 2)
                part = dot(lhs, ring[base : base + DEEP, pl.ds(MIDDLE * (tap % 2) + lane0, lanes)])
                acc = part if acc is None else acc + part
            value = jnp.maximum(acc + bias_row(b_d2a, lane0, lanes), 0.0)
            put3(x_a, row0 + REST, lane0, MIDDLE, value, REST)
        return carry

    lax.fori_loop(0, IN_CH, dec2a, 0)
    finish(copies_d2b)

    def dec2b(i, carry):
        block = i + 1 - 2 * (i % 2)
        row0 = pl.multiple_of(block * TILE, TILE)

        @pl.when(i == 1)
        def _():
            finish(ex_b)
            halo(x_a, REST, MIDDLE, N16)

        @pl.when(i == 3)
        def _():
            start(ex_d)

        for lane0, lanes in tiles:
            value = jnp.maximum(conv640(x_a, row0, N6400, lane0, lanes) + bias_row(b_d2b, lane0, lanes), 0.0)
            d_2[pl.ds(row0 + REST, TILE), pl.ds(lane0, lanes)] = value.astype(BF16)
        return carry

    lax.fori_loop(0, IN_CH, dec2b, 0)
    finish(ex_d)
    halo(d_2, REST, MIDDLE, N16, plain=True)
    result = pltpu.make_async_copy(d_2, out, sem_out)
    result.start()
    result.wait()


def dec1_kernel(
    d_2, s1, w_u1, w_d1a, w_d1b, b_d1a, b_d1b, w_head, b_head, out,
    x_u, x_s, x_d, y_rest, st_u, st_a, st_b, wu_main, wu_rest, wa_main, wa_rest, wb_main, wb_rest, wide, result,
    sem, send_sem, recv_sem,
):
    strip = strip_index()
    row = lax.axis_index("row")
    col = lax.axis_index("col")
    copy_u = pltpu.make_async_copy(w_u1, st_u, sem.at[0])
    copy_a = pltpu.make_async_copy(w_d1a, st_a, sem.at[1])
    copy_s = pltpu.make_async_copy(s1, x_s, sem.at[2])
    copy_b = pltpu.make_async_copy(w_d1b, st_b, sem.at[3])
    for copy in (copy_u, copy_a, copy_s, copy_b):
        copy.start()
    barrier = enter_barrier()

    copy_u.wait()
    for tap in range(IN_CH):
        wu_main[MIDDLE * tap : MIDDLE * tap + MIDDLE, :] = st_u[BASE * tap : BASE * tap + TILE, :].T
    wu_rest[...] = jnp.concatenate([st_u[BASE * tap + TILE : BASE * tap + BASE, :] for tap in range(IN_CH)], axis=0).T

    def up1(i, carry):
        row0 = pl.multiple_of(i * BASE_PAD, LANES)
        lhs = d_2[pl.ds(row0, BASE_PAD), :]
        rest = dot(lhs, wu_rest[...])
        for p in range(2):
            part = rest[:, LANES * p : LANES * p + LANES]
            buf = wide.at[p]
            buf[2, pl.ds(0, BASE_PAD, stride=2), :] = low_lanes(part)
            buf[2, pl.ds(1, BASE_PAD, stride=2), :] = low_lanes(pltpu.roll(part, REST, axis=1))
            for q in range(2):
                tap = 2 * p + q
                main = dot(lhs, wu_main[MIDDLE * tap : MIDDLE * tap + MIDDLE, :])
                buf[0, pl.ds(q, BASE_PAD, stride=2), :] = main[:, 0:LANES]
                buf[1, pl.ds(q, BASE_PAD, stride=2), :] = main[:, LANES:TILE]
            for r in range(SIX):
                main = jnp.concatenate([buf[0, LANES * r : LANES * r + LANES, :], buf[1, LANES * r : LANES * r + LANES, :]], axis=1)
                put3_320(
                    x_u, pl.multiple_of((N12 * i + 2 * r + p) * LANES, LANES), main, buf[2, LANES * r : LANES * r + LANES, :], LANES
                )
        return carry

    lax.fori_loop(0, 3, up1, 0)

    copy_a.wait()
    pack_transposed(st_a, wa_main, wa_rest)
    copy_s.wait()

    def rest_a(i, carry):
        for j in range(SIX):
            rows = pl.ds(pl.multiple_of(i * N1536 + TILE * j, TILE), TILE)
            y_rest[rows, :] = dot(x_u[rows, 0:PACK], wa_rest[0:PACK, :]) + dot(
                x_s[rows, 0:PACK], wa_rest[PACK:N2048, :]
            )
        return carry

    lax.fori_loop(0, 3, rest_a, 0)

    def conv_a(row0, first_row):
        acc = None
        for di in range(3):
            rows = pl.ds(row0 + LANES * di, TILE)
            for src, ref in enumerate((x_u, x_s)):
                base = N3072 * src + PACK * di
                part = dot(ref[rows, 0:PACK], wa_main[base : base + PACK, :])
                acc = part if acc is None else acc + part
        main = valid_rows(jnp.maximum(acc + bias_row(b_d1a, 0, TILE), 0.0), first_row, LANES)
        tail = valid_rows(jnp.maximum(rest_sum(y_rest, row0, TILE) + bias_rest(b_d1a), 0.0), first_row, LANES)
        put3_320(x_d, row0, main, low_lanes(tail), LANES)

    def dec1a(i, carry):
        for j in range(IN_CH):
            conv_a(pl.multiple_of(i * PACK + TILE * j, TILE), STRIP_ROWS * strip - 1 + STRIPS * i + 2 * j)
        return carry

    lax.fori_loop(0, IN_CH, dec1a, 0)
    conv_a(N4096, STRIP_ROWS * strip + N31)

    copy_b.wait()
    pack_weights(st_b, wb_main, wb_rest)
    head_bias = jnp.zeros((IN_CH, LANES), F32)
    for channel in range(IN_CH):
        head_bias = jnp.where(lax.broadcasted_iota(jnp.int32, (IN_CH, LANES), 0) == channel, b_head[channel], head_bias)

    def dec1b(i, carry):
        base = pl.multiple_of(i * PACK, PACK)

        def rest(j):
            y_rest[TILE * j : TILE * j + TILE, :] = dot(x_d[pl.ds(base + TILE * j, TILE), 0:PACK], wb_rest[...])

        rest(0)
        for j in range(IN_CH):
            rest(j + 1)
            acc = dot(x_d[pl.ds(base + TILE * j, TILE), 0:PACK], wb_main[0:PACK, :])
            acc = acc + dot(x_d[pl.ds(base + TILE * j + LANES, TILE), 0:PACK], wb_main[PACK:N2048, :])
            acc = acc + dot(x_d[pl.ds(base + TILE * j + TILE, TILE), 0:PACK], wb_main[N2048:N3072, :])
            main = jnp.maximum(acc + bias_row(b_d1b, 0, TILE), 0.0).astype(BF16)
            tail = jnp.maximum(rest_sum(y_rest, TILE * j, TILE) + bias_rest(b_d1b), 0.0).astype(BF16)
            hidden = jnp.concatenate([main, tail[:, 0:REST]], axis=1)
            head = lax.dot_general(w_head[...], hidden, (((1,), (1,)), ((), ())), preferred_element_type=F32)
            for r in range(2):
                line = head[:, LANES * r : LANES * r + LANES] + head_bias
                result[0, STRIPS * i + 2 * j + r] = line[:, 0:REST]
                result[1, STRIPS * i + 2 * j + r] = line[:, REST:LANES]
        return carry

    lax.fori_loop(0, IN_CH, dec1b, 0)

    pl.semaphore_wait(barrier, STRIPS)
    pushes = []
    for side in range(2):
        tile_row = strip // 2
        pushes.append(
            Push(
                result.at[side],
                out.at[pl.ds(STRIP_ROWS * (strip % 2), STRIP_ROWS)],
                send_sem.at[side],
                recv_sem.at[strip % 2],
                (lax.axis_index("data"), side, tile_row),
                (tile_row == row) & (col == side),
            )
        )
    for push in pushes:
        push.start()
    for push in pushes:
        push.wait_send()
    for half in range(2):
        Push(
            result.at[0], out.at[pl.ds(STRIP_ROWS * half, STRIP_ROWS)], send_sem.at[0], recv_sem.at[half], strip_device(strip), strip < 0
        ).wait_recv()


def solution(mesh):
    tile_spec = P(("data", "row"), "col", None)

    def body(image_tile, *params):
        (w_enc1a, b_enc1a, w_enc1b, b_enc1b, w_enc2a, b_enc2a, w_enc2b, b_enc2b,
         w_mid_a, b_mid_a, w_mid_b, b_mid_b, w_up2, w_dec2a, b_dec2a, w_dec2b, b_dec2b,
         w_up1, w_dec1a, b_dec1a, w_dec1b, b_dec1b, w_head, b_head) = params
        def flat(weight):
            return weight.reshape(-1, weight.shape[-1])

        vmem = pl.BlockSpec(memory_space=pltpu.VMEM)
        hbm = pl.BlockSpec(memory_space=pl.ANY)
        dma = pltpu.SemaphoreType.DMA
        s1, p1 = pl.pallas_call(
            enc1_kernel,
            grid=(3,),
            out_shape=(jax.ShapeDtypeStruct((N4608, N1152), BF16), jax.ShapeDtypeStruct((N1152, N1152), BF16)),
            in_specs=[vmem, vmem, vmem, hbm, vmem],
            out_specs=(pl.BlockSpec((N1536, N1152), lambda i: (i, 0)), pl.BlockSpec((BASE_PAD, N1152), lambda i: (i, 0))),
            scratch_shapes=[
                pltpu.VMEM((2, N40, IN_CH, REST), BF16),
                pltpu.VMEM((N42, STRIP_ROWS, LANES), BF16),
                pltpu.VMEM((N96, BASE_PAD), BF16),
                pltpu.VMEM((N2880, BASE), BF16),
                pltpu.VMEM((N5120, N1152), BF16),
                pltpu.VMEM((N1792, TILE), F32),
                pltpu.VMEM((N3072, TILE), BF16),
                pltpu.VMEM((PACK, TILE), BF16),
                pltpu.VMEM((LANES, LANES), F32),
                dma, dma((IN_CH,)), dma((2, 2)),
            ],
            compiler_params=pltpu.CompilerParams(
                vmem_limit_bytes=VMEM_LIMIT, collective_id=1, has_side_effects=True, dimension_semantics=("arbitrary",)
            ),
            name="enc1",
        )(image_tile.transpose(0, 2, 1), w_enc1a, b_enc1a, flat(w_enc1b), b_enc1b)

        d2 = pl.pallas_call(
            mid_kernel,
            out_shape=jax.ShapeDtypeStruct((N1152, MIDDLE), BF16),
            in_specs=[vmem] + [hbm] * LAST_STRIP + [vmem] * SIX,
            out_specs=hbm,
            scratch_shapes=[
                pltpu.VMEM((N3072, MIDDLE), BF16),
                pltpu.VMEM((RING_ROWS, DEEP), BF16),
                pltpu.VMEM((N1152, MIDDLE3), BF16),
                pltpu.VMEM((N1152, MIDDLE3), BF16),
                pltpu.VMEM((N1152, MIDDLE3), BF16),
                pltpu.VMEM((BASE, MIDDLE3), BF16),
                pltpu.VMEM((BASE, N3840), BF16),
                pltpu.VMEM((TILE, DEEP), BF16),
                pltpu.VMEM((N1152, MIDDLE), BF16),
                pltpu.VMEM((TILE, DEEP), F32),
                pltpu.VMEM((FIVE, N512, LANES), F32),
                pltpu.VMEM((LANES, LANES), F32),
                dma((N18,)), dma((TAPS,)), dma((3,)), dma((TAPS,)), dma((IN_CH,)), dma((TAPS,)), dma((TAPS,)), dma,
                dma((LAST_STRIP, 2)), dma((LAST_STRIP, 2)),
            ],
            compiler_params=pltpu.CompilerParams(
                vmem_limit_bytes=VMEM_LIMIT, collective_id=0, has_side_effects=True
            ),
            name="mid",
        )(
            p1, flat(w_enc2a), flat(w_enc2b), flat(w_mid_a), flat(w_mid_b), flat(w_up2), flat(w_dec2a), flat(w_dec2b),
            b_enc2a, b_enc2b, b_mid_a, b_mid_b, b_dec2a, b_dec2b,
        )

        def turned(weight):
            return weight.transpose(0, 1, 3, 2).reshape(-1, weight.shape[2])

        y = pl.pallas_call(
            dec1_kernel,
            out_shape=jax.ShapeDtypeStruct((REST, IN_CH, REST), F32),
            in_specs=[vmem] + [hbm] * IN_CH + [vmem] * 3 + [pl.BlockSpec(memory_space=pltpu.SMEM)],
            out_specs=hbm,
            scratch_shapes=[
                pltpu.VMEM((N4608, N1152), BF16),
                pltpu.VMEM((N4608, N1152), BF16),
                pltpu.VMEM((N4352, N1152), BF16),
                pltpu.VMEM((N4608, TILE), F32),
                pltpu.VMEM((DEEP, MIDDLE), BF16),
                pltpu.VMEM((N2880, MIDDLE), BF16),
                pltpu.VMEM((N2880, BASE), BF16),
                pltpu.VMEM((N2560, TILE), BF16),
                pltpu.VMEM((MIDDLE, TILE), BF16),
                pltpu.VMEM((N6144, TILE), BF16),
                pltpu.VMEM((N2048, TILE), BF16),
                pltpu.VMEM((N3072, TILE), BF16),
                pltpu.VMEM((PACK, TILE), BF16),
                pltpu.VMEM((2, 3, REST_AT, LANES), F32),
                pltpu.VMEM((2, STRIP_ROWS, IN_CH, REST), F32),
                dma((IN_CH,)), dma((2,)), dma((2,)),
            ],
            compiler_params=pltpu.CompilerParams(vmem_limit_bytes=VMEM_LIMIT, collective_id=2, has_side_effects=True),
            name="dec1",
        )(d2, s1, turned(w_up1), turned(w_dec1a), flat(w_dec1b), b_dec1a, b_dec1b, w_head.T, b_head)
        return y.transpose(0, 2, 1)

    def program(image, *params):
        mapped = jax.shard_map(
            body, mesh=mesh, in_specs=(tile_spec,) + (P(),) * len(params), out_specs=tile_spec, check_vma=False
        )
        return mapped(image, *params)

    return program
```

```python
import functools

import jax
import jax.numpy as jnp
from jax import lax
from jax.experimental import pallas as pl
from jax.experimental.pallas import tpu as pltpu
from jax.sharding import PartitionSpec as P

IN_CH = 4
FIVE = 5
SIX = 6
LAST_STRIP = 7
STRIPS = 8
TAPS = 9
N12 = 12
N16 = 16
N18 = 18
N28 = 28
N30 = 30
N31 = 31
STRIP_ROWS = 32
N36 = 36
N40 = 40
N42 = 42
N60 = 60
REST = 64
N96 = 96
N127 = 127
LANES = 128
TILE = 256
BASE = 320
BASE_PAD = 384
N512 = 512
MIDDLE = 640
REST_AT = 768
N896 = 896
PACK_USED = 960
PACK = 1024
N1152 = 1152
DEEP = 1280
N1536 = 1536
N1792 = 1792
MIDDLE3 = 1920
N2048 = 2048
N2560 = 2560
N2880 = 2880
N3072 = 3072
N3200 = 3200
N3840 = 3840
N4096 = 4096
N4352 = 4352
N4608 = 4608
N5120 = 5120
N6144 = 6144
N6400 = 6400
N8960 = 8960
N10240 = 10240
N11520 = 11520
BF16 = jnp.bfloat16
F32 = jnp.float32
MESH = pl.DeviceIdType.MESH
VMEM_LIMIT = 66_900_000
RING_ROWS = N11520


def strip_index():
    col = lax.axis_index("col")
    row = lax.axis_index("row")
    return row + col * (LAST_STRIP - 2 * row)


def strip_device(position):
    col = position // IN_CH
    rest = position % IN_CH
    return (lax.axis_index("data"), col, rest + col * (3 - 2 * rest))


def dot(a, b):
    return jnp.dot(a, b, preferred_element_type=F32)


def shifted(value, width, step):
    if step == 1:
        return value
    rows = value.shape[0]
    column = lax.broadcasted_iota(jnp.int32, value.shape, 0) % width
    if step == 0:
        return jnp.where(column == 0, 0.0, pltpu.roll(value, 1, axis=0))
    return jnp.where(column == width - 1, 0.0, pltpu.roll(value, rows - 1, axis=0))


def put3(dst, row0, lane0, channels, value, width):
    rows, lanes = value.shape
    for step in range(3):
        dst[pl.ds(row0, rows), pl.ds(step * channels + lane0, lanes)] = shifted(value, width, step).astype(BF16)


def put3_320(dst, row0, main, rest, width):
    rows = main.shape[0]
    for step in range(3):
        dst[pl.ds(row0, rows), pl.ds(step * TILE, TILE)] = shifted(main, width, step).astype(BF16)
    first = shifted(rest, width, 0) + pltpu.roll(rest, REST, axis=1)
    dst[pl.ds(row0, rows), pl.ds(REST_AT, LANES)] = first.astype(BF16)
    dst[pl.ds(row0, rows), pl.ds(N896, LANES)] = shifted(rest, width, 2).astype(BF16)


def low_lanes(value):
    return jnp.where(lax.broadcasted_iota(jnp.int32, value.shape, 1) < REST, value, 0.0)


def pack_weights(staged, main_ref, rest_ref):
    for dj in range(3):
        for start, size, row in ((0, TILE, TILE * dj), (TILE, REST, REST_AT + REST * dj)):
            parts = []
            for di in range(3):
                base = (3 * di + dj) * BASE + start
                main_ref[pl.ds(PACK * di + row, size), :] = staged[pl.ds(base, size), 0:TILE]
                parts.append(staged[pl.ds(base, size), TILE:BASE])
            parts.append(jnp.zeros((size, REST), BF16))
            rest_ref[pl.ds(row, size), :] = jnp.concatenate(parts, axis=1)
    clear_pad(main_ref, 3)
    clear_pad(rest_ref, 1)


def clear_pad(ref, groups):
    for group in range(groups):
        ref[pl.ds(PACK * group + PACK_USED, REST), :] = jnp.zeros((REST, ref.shape[1]), BF16)


def pack_transposed(staged, main_ref, rest_ref):
    for dj in range(3):

        def main_part(di, carry):
            turned = staged[pl.ds(pl.multiple_of(PACK_USED * di + BASE * dj, REST), TILE), :].T
            for src in range(2):
                base = N3072 * src + PACK * di
                main_ref[pl.ds(pl.multiple_of(base + TILE * dj, REST), TILE), :] = turned[BASE * src : BASE * src + TILE]
                main_ref[pl.ds(pl.multiple_of(base + REST_AT + REST * dj, REST), REST), :] = turned[BASE * src + TILE : BASE * src + BASE]
            return carry

        lax.fori_loop(0, 3, main_part, 0)
        parts = [staged[pl.ds(PACK_USED * di + BASE * dj + TILE, REST), :] for di in range(3)] + [jnp.zeros((REST, MIDDLE), BF16)]
        turned = jnp.concatenate(parts, axis=0).T
        for src in range(2):
            rest_ref[pl.ds(PACK * src + TILE * dj, TILE), :] = turned[BASE * src : BASE * src + TILE]
            rest_ref[pl.ds(PACK * src + REST_AT + REST * dj, REST), :] = turned[BASE * src + TILE : BASE * src + BASE]
    clear_pad(main_ref, SIX)
    clear_pad(rest_ref, 2)


def bias_row(ref, start, size):
    return ref[pl.ds(start, size)].reshape(1, size)


def bias_rest(ref):
    return jnp.concatenate([bias_row(ref, TILE, REST), jnp.zeros((1, REST), F32)], axis=1)


def enter_barrier():
    barrier = pltpu.get_barrier_semaphore()
    for position in range(STRIPS):
        pl.semaphore_signal(barrier, inc=1, device_id=strip_device(position), device_id_type=MESH)
    return barrier


class Push:
    def __init__(self, src, dst, send_sem, recv_sem, device, here):
        self.here = here
        self.local = pltpu.make_async_copy(src, dst, recv_sem)
        self.remote = pltpu.make_async_remote_copy(
            src_ref=src, dst_ref=dst, send_sem=send_sem, recv_sem=recv_sem, device_id=device, device_id_type=MESH
        )

    def start(self):
        @pl.when(self.here)
        def _():
            self.local.start()

        @pl.when(jnp.logical_not(self.here))
        def _():
            self.remote.start()

    def wait_send(self):
        @pl.when(jnp.logical_not(self.here))
        def _():
            self.remote.wait_send()

    def wait_recv(self):
        self.remote.wait_recv()


def rest_sum(y_ref, row0, rows):
    total = y_ref[pl.ds(row0, rows), 0:LANES] + y_ref[pl.ds(row0 + TILE, rows), LANES:TILE]
    return total + pltpu.roll(y_ref[pl.ds(row0 + LANES, rows), 0:LANES], REST, axis=1)


def valid_rows(value, first_row, width):
    row = first_row + lax.broadcasted_iota(jnp.int32, value.shape, 0) // width
    return jnp.where((row >= 0) & (row < TILE), value, 0.0)


def pooled(value, width, scratch):
    rows, lanes = value.shape
    tall = jnp.concatenate(
        [jnp.maximum(value[s : s + width], value[s + width : s + 2 * width]) for s in range(0, rows, 2 * width)], axis=0
    )
    halves = []
    for start in range(0, lanes, LANES):
        scratch[0 : rows // 2, :] = tall[:, start : start + LANES]
        halves.append(
            jnp.maximum(scratch[pl.ds(0, rows // IN_CH, stride=2), :], scratch[pl.ds(1, rows // IN_CH, stride=2), :])
        )
    return jnp.concatenate(halves, axis=1) if len(halves) > 1 else halves[0]


def enc1_kernel(
    image, w_a, b_a, w_b, b_b, s1_out, p1_out,
    halves, planes, w_stem, staged, x_a, y_rest, w_main, w_rest, pool_buf, w_sem, send_sem, recv_sem,
):
    step = pl.program_id(0)
    strip = strip_index()

    @pl.when(step == 0)
    def _():
        row = lax.axis_index("row")
        col = lax.axis_index("col")
        copy_w = pltpu.make_async_copy(w_b, staged, w_sem)
        copy_w.start()
        barrier = enter_barrier()

        for di in range(3):
            taps = []
            for dj in range(3):
                tap = jnp.concatenate([w_a[di, dj].astype(F32), jnp.zeros((IN_CH, BASE), F32)], axis=0)
                taps.append(jnp.concatenate([tap, jnp.zeros((STRIPS, REST), F32)], axis=1))
            taps.append(jnp.zeros((STRIPS, BASE_PAD), F32))
            w_stem[STRIP_ROWS * di : STRIP_ROWS * di + STRIP_ROWS, :] = jnp.concatenate(taps, axis=0).astype(BF16)
        planes[N40:N42, :, :] = jnp.zeros((2, STRIP_ROWS, LANES), BF16)

        pl.semaphore_wait(barrier, STRIPS)
        pushes = []
        for index, (target, src_row, dst_row, rows) in enumerate(
            ((2 * row, 0, IN_CH, N36), (2 * row + 1, N28, 0, N36), ((2 * row + 2) % STRIPS, N60, 0, IN_CH), ((2 * row + LAST_STRIP) % STRIPS, 0, N36, IN_CH))
        ):
            pushes.append(
                Push(
                    image.at[pl.ds(src_row, rows)],
                    halves.at[col, pl.ds(dst_row, rows)],
                    send_sem.at[index],
                    recv_sem.at[index // 2, col],
                    strip_device(target),
                    target == strip,
                )
            )
        for push in pushes:
            push.start()
        copy_w.wait()
        pack_weights(staged, w_main, w_rest)
        for push in pushes:
            push.wait_send()
        for kind, rows in ((0, N36), (1, IN_CH)):
            for side in range(2):
                Push(
                    image.at[pl.ds(0, rows)], halves.at[side, pl.ds(0, rows)],
                    send_sem.at[0], recv_sem.at[kind, side], strip_device(strip), strip < 0,
                ).wait_recv()

        def expand(i, carry):
            for j in range(STRIPS):
                r = STRIPS * i + j
                both = jnp.concatenate([halves[0, r].astype(F32), halves[1, r].astype(F32)], axis=1)
                image_row = STRIP_ROWS * strip - IN_CH + r
                both = jnp.where((image_row >= 0) & (image_row < TILE), both, 0.0)
                both = jnp.concatenate([both, jnp.zeros((IN_CH, LANES), F32)], axis=0)
                column = lax.broadcasted_iota(jnp.int32, (STRIPS, LANES), 1)
                before = jnp.where(column == 0, 0.0, pltpu.roll(both, 1, axis=1))
                after = jnp.where(column == N127, 0.0, pltpu.roll(both, N127, axis=1))
                planes[r] = jnp.concatenate([before, both, after, jnp.zeros((STRIPS, LANES), F32)], axis=0).astype(BF16)
            return carry

        lax.fori_loop(0, FIVE, expand, 0)

        def stem(i, carry):
            for j in range(IN_CH):
                r = STRIPS * i + 2 * j
                row0 = pl.multiple_of(r * LANES, TILE)
                patch = jnp.concatenate(
                    [jnp.concatenate([planes[r + k + di] for di in range(3)], axis=0) for k in range(2)], axis=1
                )
                acc = lax.dot_general(patch, w_stem[...], (((0,), (0,)), ((), ())), preferred_element_type=F32)
                main = jnp.maximum(acc[:, 0:TILE] + bias_row(b_a, 0, TILE), 0.0)
                tail = jnp.maximum(acc[:, TILE:BASE_PAD] + bias_rest(b_a), 0.0)
                first_row = STRIP_ROWS * strip - 3 + r
                put3_320(x_a, row0, valid_rows(main, first_row, LANES), valid_rows(tail, first_row, LANES), LANES)
            return carry

        lax.fori_loop(0, FIVE, stem, 0)

    base = pl.multiple_of(step * N1536, N512)

    def rest(j):
        y_rest[TILE * j : TILE * j + TILE, :] = dot(x_a[pl.ds(base + TILE * j, TILE), 0:PACK], w_rest[...])

    rest(0)
    for j in range(SIX):
        rest(j + 1)
        acc = dot(x_a[pl.ds(base + TILE * j, TILE), 0:PACK], w_main[0:PACK, :])
        acc = acc + dot(x_a[pl.ds(base + TILE * j + LANES, TILE), 0:PACK], w_main[PACK:N2048, :])
        acc = acc + dot(x_a[pl.ds(base + TILE * j + TILE, TILE), 0:PACK], w_main[N2048:N3072, :])
        first_row = STRIP_ROWS * strip - 2 + N12 * step + 2 * j
        main = valid_rows(jnp.maximum(acc + bias_row(b_b, 0, TILE), 0.0), first_row, LANES)
        tail = jnp.maximum(rest_sum(y_rest, TILE * j, TILE) + bias_rest(b_b), 0.0)
        tail = low_lanes(valid_rows(tail, first_row, LANES))
        put3_320(s1_out, TILE * j, main, tail, LANES)
        put3_320(p1_out, REST * j, pooled(main, LANES, pool_buf), pooled(tail, LANES, pool_buf), REST)


def mid_kernel(
    p1, w_2a, w_2b, w_ma, w_mb, w_u2, w_d2a, w_d2b, b_2a, b_2b, b_ma, b_mb, b_d2a, b_d2b, out,
    first_w, ring, x_a, x_s, x_u, m_1, m_2, m_o, d_2, acc_ref, wide, pool_buf,
    sem_2a, sem_2b, sem_ma, sem_mb, sem_u2, sem_d2a, sem_d2b, sem_out, send_sem, recv_sem,
):
    strip = strip_index()
    prev_dev = strip_device((strip + LAST_STRIP) % STRIPS)
    next_dev = strip_device((strip + 1) % STRIPS)

    def exchange(buf, width, lane0, lanes, rows, index):
        lane = pl.ds(lane0, lanes)
        copies = []
        for side, src_row, dst_row, device in ((0, 1, rows + 1, prev_dev), (1, rows, 0, next_dev)):
            copies.append(
                pltpu.make_async_remote_copy(
                    src_ref=buf.at[pl.ds(src_row * width, width), lane],
                    dst_ref=buf.at[pl.ds(dst_row * width, width), lane],
                    send_sem=send_sem.at[index, side],
                    recv_sem=recv_sem.at[index, side],
                    device_id=device,
                    device_id_type=MESH,
                )
            )
        return copies

    def start(copies):
        for copy in copies:
            copy.start()

    def finish(copies):
        for copy in copies:
            copy.wait()

    def halo(buf, width, channels, rows, plain=False):
        for row, inside in ((0, strip > 0), (rows + 1, strip < LAST_STRIP)):
            lanes = pl.ds(0 if plain else channels, channels)
            value = buf[pl.ds(row * width, width), lanes].astype(F32)
            value = jnp.where(inside, value, 0.0)
            if plain:
                buf[pl.ds(row * width, width), lanes] = value.astype(BF16)
            else:
                put3(buf, row * width, 0, channels, value, width)

    copies_2a = []
    for tap in range(TAPS):
        di, dj = tap // 3, tap % 3
        for part, (start_row, size, row) in enumerate(((0, TILE, TILE * dj), (TILE, REST, REST_AT + REST * dj))):
            copies_2a.append(
                pltpu.make_async_copy(
                    w_2a.at[pl.ds(BASE * tap + start_row, size), :],
                    first_w.at[pl.ds(PACK * di + row, size), :],
                    sem_2a.at[2 * tap + part],
                )
            )

    def tap_copies(src, rows, base, sem):
        return [
            pltpu.make_async_copy(
                src.at[pl.ds(rows * tap, rows), :],
                ring.at[pl.ds(base + rows * (tap // 2), rows), pl.ds(MIDDLE * (tap % 2), MIDDLE)],
                sem.at[tap],
            )
            for tap in range(src.shape[0] // rows)
        ]

    copies_2b = tap_copies(w_2b, MIDDLE, 0, sem_2b)
    copies_ma = [
        pltpu.make_async_copy(w_ma.at[pl.ds(MIDDLE3 * di, MIDDLE3), :], ring.at[pl.ds(N3200 + MIDDLE3 * t, MIDDLE3), :], sem_ma.at[t])
        for t, di in enumerate((1, 0, 2))
    ]

    def mb_row(k):
        return (N8960 + DEEP * k) % RING_ROWS

    copies_mb = [
        pltpu.make_async_copy(
            w_mb.at[pl.ds(DEEP * (3 * (1, 0, 2)[k // 3] + k % 3), DEEP), :], ring.at[pl.ds(mb_row(k), DEEP), :], sem_mb.at[k]
        )
        for k in range(TAPS)
    ]
    copies_u2 = [
        pltpu.make_async_copy(
            w_u2.at[pl.ds(DEEP * tap, DEEP), :],
            first_w.at[pl.ds(DEEP * tap, DEEP), :] if tap < 2 else ring.at[pl.ds(N8960, DEEP), pl.ds(MIDDLE * (tap - 2), MIDDLE)],
            sem_u2.at[tap],
        )
        for tap in range(IN_CH)
    ]
    copies_d2a = tap_copies(w_d2a, DEEP, 0, sem_d2a)
    copies_d2b = tap_copies(w_d2b, MIDDLE, N6400, sem_d2b)

    start(copies_2a)

    barrier = pltpu.get_barrier_semaphore()
    for device in (prev_dev, next_dev):
        pl.semaphore_signal(barrier, inc=1, device_id=device, device_id_type=MESH)
    pl.semaphore_wait(barrier, 2)

    for di in range(3):
        first_w[PACK * di + PACK_USED : PACK * di + PACK, :] = jnp.zeros((REST, MIDDLE), BF16)
    finish(copies_2a)
    start(copies_2b)
    start(copies_ma)

    ex_a = exchange(x_a, REST, MIDDLE, MIDDLE, N16, 0)
    ex_s = exchange(x_s, REST, MIDDLE, MIDDLE, N16, 1)
    ex_m1 = exchange(m_1, STRIP_ROWS, MIDDLE, MIDDLE, STRIPS, 2)
    ex_m2 = exchange(m_2, STRIP_ROWS, DEEP, DEEP, STRIPS, 3)
    ex_u = exchange(x_u, REST, MIDDLE, MIDDLE, N16, IN_CH)
    ex_b = exchange(x_a, REST, MIDDLE, MIDDLE, N16, FIVE)
    ex_d = exchange(d_2, REST, 0, MIDDLE, N16, SIX)
    tiles = ((0, TILE), (TILE, TILE), (N512, LANES))

    def enc2a(i, carry):
        block = i + 1 - 2 * (i % 2)
        row0 = pl.multiple_of(block * TILE, TILE)

        @pl.when(i == 3)
        def _():
            start(ex_a)

        for lane0, lanes in tiles:
            acc = dot(p1[pl.ds(row0, TILE), 0:PACK], first_w[0:PACK, pl.ds(lane0, lanes)])
            for di in (1, 2):
                acc = acc + dot(
                    p1[pl.ds(row0 + REST * di, TILE), 0:PACK], first_w[PACK * di : PACK * di + PACK, pl.ds(lane0, lanes)]
                )
            value = jnp.maximum(acc + bias_row(b_2a, lane0, lanes), 0.0)
            put3(x_a, row0 + REST, lane0, MIDDLE, value, REST)
        return carry

    lax.fori_loop(0, IN_CH, enc2a, 0)
    finish(copies_2b)
    start(copies_mb[0:2])
    start(copies_u2[0:2])

    def conv640(src, row0, base, lane0, lanes):
        acc = None
        for di in range(3):
            weights = jnp.concatenate(
                [
                    ring[base + MIDDLE * (t // 2) : base + MIDDLE * (t // 2) + MIDDLE, pl.ds(MIDDLE * (t % 2) + lane0, lanes)]
                    for t in range(3 * di, 3 * di + 3)
                ],
                axis=0,
            )
            part = dot(src[pl.ds(row0 + REST * di, TILE), :], weights)
            acc = part if acc is None else acc + part
        return acc

    def enc2b(i, carry):
        block = i + 1 - 2 * (i % 2)
        row0 = pl.multiple_of(block * TILE, TILE)

        @pl.when(i == 1)
        def _():
            finish(ex_a)
            halo(x_a, REST, MIDDLE, N16)

        @pl.when(i == 3)
        def _():
            start(ex_m1)
            start(ex_s)

        for lane0, lanes in tiles:
            value = jnp.maximum(conv640(x_a, row0, 0, lane0, lanes) + bias_row(b_2b, lane0, lanes), 0.0)
            put3(x_s, row0 + REST, lane0, MIDDLE, value, REST)
            put3(m_1, pl.multiple_of(block * REST + STRIP_ROWS, STRIP_ROWS), lane0, MIDDLE, pooled(value, REST, pool_buf), STRIP_ROWS)
        return carry

    lax.fori_loop(0, IN_CH, enc2b, 0)
    start(copies_mb[2:IN_CH])

    acc_ref[...] = jnp.zeros_like(acc_ref)
    finish(copies_ma)

    def mid_a(t, carry):
        di = (t + 1) % 2 + 2 * (t // 2) - t // 2

        @pl.when(t == 1)
        def _():
            start(copies_mb[IN_CH:SIX])
            finish(ex_m1)
            halo(m_1, STRIP_ROWS, MIDDLE, STRIPS)

        @pl.when(t == 2)
        def _():
            start(copies_mb[SIX:LAST_STRIP])

        base = pl.multiple_of(N3200 + MIDDLE3 * t, LANES)
        lhs_row = pl.multiple_of(STRIP_ROWS * di, STRIP_ROWS)
        for lane0 in range(0, DEEP, TILE):
            acc_ref[:, pl.ds(lane0, TILE)] += dot(
                m_1[pl.ds(lhs_row, TILE), :], ring[pl.ds(base, MIDDLE3), pl.ds(lane0, TILE)]
            )
        return carry

    lax.fori_loop(0, 3, mid_a, 0)
    start(copies_mb[LAST_STRIP:TAPS])
    for lane0 in range(0, DEEP, TILE):
        value = jnp.maximum(acc_ref[:, pl.ds(lane0, TILE)] + bias_row(b_ma, lane0, TILE), 0.0)
        put3(m_2, STRIP_ROWS, lane0, DEEP, value, STRIP_ROWS)
    start(ex_m2)
    acc_ref[...] = jnp.zeros_like(acc_ref)

    def mid_b(k, carry):
        t = k // 3
        di = (t + 1) % 2 + 2 * (t // 2) - t // 2

        for j in range(TAPS):
            @pl.when(k == j)
            def _(j=j):
                copies_mb[j].wait()

        @pl.when(k == 3)
        def _():
            start(copies_u2[2:IN_CH])
            finish(ex_m2)
            halo(m_2, STRIP_ROWS, DEEP, STRIPS)

        @pl.when(k == FIVE)
        def _():
            start(copies_d2a[0:IN_CH])

        @pl.when(k == LAST_STRIP)
        def _():
            start(copies_d2a[IN_CH:TAPS])

        base = pl.multiple_of(mb_row(k), LANES)
        lhs_row = pl.multiple_of(STRIP_ROWS * di, STRIP_ROWS)
        lhs_lane = pl.multiple_of(DEEP * (k % 3), DEEP)
        for lane0 in range(0, DEEP, TILE):
            acc_ref[:, pl.ds(lane0, TILE)] += dot(
                m_2[pl.ds(lhs_row, TILE), pl.ds(lhs_lane, DEEP)], ring[pl.ds(base, DEEP), pl.ds(lane0, TILE)]
            )
        return carry

    lax.fori_loop(0, TAPS, mid_b, 0)
    for lane0 in range(0, DEEP, TILE):
        value = jnp.maximum(acc_ref[:, pl.ds(lane0, TILE)] + bias_row(b_mb, lane0, TILE), 0.0)
        m_o[:, pl.ds(lane0, TILE)] = value.astype(BF16)

    finish(copies_u2)
    for p in range(2):
        for q in range(2):
            for lane0, lanes in tiles:
                if p == 0:
                    weights = first_w[DEEP * q : DEEP * q + DEEP, pl.ds(lane0, lanes)]
                else:
                    weights = ring[N8960:N10240, pl.ds(MIDDLE * q + lane0, lanes)]
                part = dot(m_o[...], weights)
                for lane in range(0, lanes, LANES):
                    wide[(lane0 + lane) // LANES, pl.ds(q, TILE, stride=2), :] = part[:, lane : lane + LANES]

        def place(i, carry):
            src = pl.multiple_of(REST * i, REST)
            dst = pl.multiple_of(REST * (1 + 2 * i + p), REST)
            for lane0 in range(0, MIDDLE, LANES):
                put3(x_u, dst, lane0, MIDDLE, wide[lane0 // LANES, pl.ds(src, REST), :], REST)
            return carry

        lax.fori_loop(0, STRIPS, place, 0)
    start(ex_u)
    start(copies_d2b)
    finish(ex_s)
    halo(x_s, REST, MIDDLE, N16)
    finish(copies_d2a)

    def dec2a(i, carry):
        block = i + 1 - 2 * (i % 2)
        row0 = pl.multiple_of(block * TILE, TILE)

        @pl.when(i == 1)
        def _():
            finish(ex_u)
            halo(x_u, REST, MIDDLE, N16)

        @pl.when(i == 3)
        def _():
            start(ex_b)

        for lane0, lanes in tiles:
            acc = None
            for tap in range(TAPS):
                rows = pl.ds(row0 + REST * (tap // 3), TILE)
                cols = pl.ds(MIDDLE * (tap % 3), MIDDLE)
                lhs = jnp.concatenate([x_u[rows, cols], x_s[rows, cols]], axis=1)
                base = DEEP * (tap // 2)
                part = dot(lhs, ring[base : base + DEEP, pl.ds(MIDDLE * (tap % 2) + lane0, lanes)])
                acc = part if acc is None else acc + part
            value = jnp.maximum(acc + bias_row(b_d2a, lane0, lanes), 0.0)
            put3(x_a, row0 + REST, lane0, MIDDLE, value, REST)
        return carry

    lax.fori_loop(0, IN_CH, dec2a, 0)
    finish(copies_d2b)

    def dec2b(i, carry):
        block = i + 1 - 2 * (i % 2)
        row0 = pl.multiple_of(block * TILE, TILE)

        @pl.when(i == 1)
        def _():
            finish(ex_b)
            halo(x_a, REST, MIDDLE, N16)

        @pl.when(i == 3)
        def _():
            start(ex_d)

        for lane0, lanes in tiles:
            value = jnp.maximum(conv640(x_a, row0, N6400, lane0, lanes) + bias_row(b_d2b, lane0, lanes), 0.0)
            d_2[pl.ds(row0 + REST, TILE), pl.ds(lane0, lanes)] = value.astype(BF16)
        return carry

    lax.fori_loop(0, IN_CH, dec2b, 0)
    finish(ex_d)
    halo(d_2, REST, MIDDLE, N16, plain=True)
    result = pltpu.make_async_copy(d_2, out, sem_out)
    result.start()
    result.wait()


def dec1_kernel(
    d_2, s1, w_u1, w_d1a, w_d1b, b_d1a, b_d1b, w_head, b_head, out,
    x_u, x_s, x_d, y_rest, st_u, st_a, st_b, wu_main, wu_rest, wa_main, wa_rest, wb_main, wb_rest, wide, result, pending,
    sem, send_sem, recv_sem,
):
    strip = strip_index()
    row = lax.axis_index("row")
    col = lax.axis_index("col")
    copy_u = pltpu.make_async_copy(w_u1, st_u, sem.at[0])
    copy_a = pltpu.make_async_copy(w_d1a, st_a, sem.at[1])
    copy_s = pltpu.make_async_copy(s1, x_s, sem.at[2])
    copy_b = pltpu.make_async_copy(w_d1b, st_b, sem.at[3])
    for copy in (copy_u, copy_a, copy_s, copy_b):
        copy.start()
    barrier = enter_barrier()

    copy_u.wait()
    for tap in range(IN_CH):
        wu_main[MIDDLE * tap : MIDDLE * tap + MIDDLE, :] = st_u[BASE * tap : BASE * tap + TILE, :].T
    wu_rest[...] = jnp.concatenate([st_u[BASE * tap + TILE : BASE * tap + BASE, :] for tap in range(IN_CH)], axis=0).T

    def up1(i, carry):
        row0 = pl.multiple_of(i * BASE_PAD, LANES)
        lhs = d_2[pl.ds(row0, BASE_PAD), :]
        rest = dot(lhs, wu_rest[...])
        for p in range(2):
            part = rest[:, LANES * p : LANES * p + LANES]
            buf = wide.at[p]
            buf[2, pl.ds(0, BASE_PAD, stride=2), :] = low_lanes(part)
            buf[2, pl.ds(1, BASE_PAD, stride=2), :] = low_lanes(pltpu.roll(part, REST, axis=1))
            for q in range(2):
                tap = 2 * p + q
                main = dot(lhs, wu_main[MIDDLE * tap : MIDDLE * tap + MIDDLE, :])
                buf[0, pl.ds(q, BASE_PAD, stride=2), :] = main[:, 0:LANES]
                buf[1, pl.ds(q, BASE_PAD, stride=2), :] = main[:, LANES:TILE]
            for r in range(SIX):
                main = jnp.concatenate([buf[0, LANES * r : LANES * r + LANES, :], buf[1, LANES * r : LANES * r + LANES, :]], axis=1)
                put3_320(
                    x_u, pl.multiple_of((N12 * i + 2 * r + p) * LANES, LANES), main, buf[2, LANES * r : LANES * r + LANES, :], LANES
                )
        return carry

    lax.fori_loop(0, 3, up1, 0)

    copy_a.wait()
    pack_transposed(st_a, wa_main, wa_rest)
    copy_s.wait()

    def rest_a(i, carry):
        for j in range(SIX):
            rows = pl.ds(pl.multiple_of(i * N1536 + TILE * j, TILE), TILE)
            y_rest[rows, :] = dot(x_u[rows, 0:PACK], wa_rest[0:PACK, :]) + dot(
                x_s[rows, 0:PACK], wa_rest[PACK:N2048, :]
            )
        return carry

    lax.fori_loop(0, 3, rest_a, 0)

    def conv_a(row0, first_row):
        acc = None
        for di in range(3):
            rows = pl.ds(row0 + LANES * di, TILE)
            for src, ref in enumerate((x_u, x_s)):
                base = N3072 * src + PACK * di
                part = dot(ref[rows, 0:PACK], wa_main[base : base + PACK, :])
                acc = part if acc is None else acc + part
        main = valid_rows(jnp.maximum(acc + bias_row(b_d1a, 0, TILE), 0.0), first_row, LANES)
        tail = valid_rows(jnp.maximum(rest_sum(y_rest, row0, TILE) + bias_rest(b_d1a), 0.0), first_row, LANES)
        put3_320(x_d, row0, main, low_lanes(tail), LANES)

    def dec1a(i, carry):
        for j in range(IN_CH):
            conv_a(pl.multiple_of(i * PACK + TILE * j, TILE), STRIP_ROWS * strip - 1 + STRIPS * i + 2 * j)
        return carry

    lax.fori_loop(0, IN_CH, dec1a, 0)
    conv_a(N4096, STRIP_ROWS * strip + N31)

    copy_b.wait()
    pack_weights(st_b, wb_main, wb_rest)
    head_bias = jnp.zeros((IN_CH, LANES), F32)
    for channel in range(IN_CH):
        head_bias = jnp.where(lax.broadcasted_iota(jnp.int32, (IN_CH, LANES), 0) == channel, b_head[channel], head_bias)

    pending[...] = jnp.zeros_like(pending)

    def head(hidden, row0):
        line = lax.dot_general(w_head[...], hidden, (((1,), (1,)), ((), ())), preferred_element_type=F32)
        for r in range(2):
            part = line[:, LANES * r : LANES * r + LANES] + head_bias
            result[0, row0 + r] = part[:, 0:REST]
            result[1, row0 + r] = part[:, REST:LANES]

    def dec1b(i, carry):
        base = pl.multiple_of(i * PACK, PACK)

        def rest(j):
            y_rest[TILE * j : TILE * j + TILE, :] = dot(x_d[pl.ds(base + TILE * j, TILE), 0:PACK], wb_rest[...])

        rest(0)
        waiting = pending[...]
        for j in range(IN_CH):
            rest(j + 1)
            acc = dot(x_d[pl.ds(base + TILE * j, TILE), 0:PACK], wb_main[0:PACK, :])
            acc = acc + dot(x_d[pl.ds(base + TILE * j + LANES, TILE), 0:PACK], wb_main[PACK:N2048, :])
            acc = acc + dot(x_d[pl.ds(base + TILE * j + TILE, TILE), 0:PACK], wb_main[N2048:N3072, :])
            head(waiting, jnp.maximum(STRIPS * i + 2 * j - 2, 0))
            main = jnp.maximum(acc + bias_row(b_d1b, 0, TILE), 0.0).astype(BF16)
            tail = jnp.maximum(rest_sum(y_rest, TILE * j, TILE) + bias_rest(b_d1b), 0.0).astype(BF16)
            waiting = jnp.concatenate([main, tail[:, 0:REST]], axis=1)
        pending[...] = waiting
        return carry

    lax.fori_loop(0, IN_CH, dec1b, 0)
    head(pending[...], N30)

    pl.semaphore_wait(barrier, STRIPS)
    pushes = []
    for side in range(2):
        tile_row = strip // 2
        pushes.append(
            Push(
                result.at[side],
                out.at[pl.ds(STRIP_ROWS * (strip % 2), STRIP_ROWS)],
                send_sem.at[side],
                recv_sem.at[strip % 2],
                (lax.axis_index("data"), side, tile_row),
                (tile_row == row) & (col == side),
            )
        )
    for push in pushes:
        push.start()
    for push in pushes:
        push.wait_send()
    for half in range(2):
        Push(
            result.at[0], out.at[pl.ds(STRIP_ROWS * half, STRIP_ROWS)], send_sem.at[0], recv_sem.at[half], strip_device(strip), strip < 0
        ).wait_recv()


def solution(mesh):
    tile_spec = P(("data", "row"), "col", None)

    def body(image_tile, *params):
        (w_enc1a, b_enc1a, w_enc1b, b_enc1b, w_enc2a, b_enc2a, w_enc2b, b_enc2b,
         w_mid_a, b_mid_a, w_mid_b, b_mid_b, w_up2, w_dec2a, b_dec2a, w_dec2b, b_dec2b,
         w_up1, w_dec1a, b_dec1a, w_dec1b, b_dec1b, w_head, b_head) = params
        def flat(weight):
            return weight.reshape(-1, weight.shape[-1])

        vmem = pl.BlockSpec(memory_space=pltpu.VMEM)
        hbm = pl.BlockSpec(memory_space=pl.ANY)
        dma = pltpu.SemaphoreType.DMA
        s1, p1 = pl.pallas_call(
            enc1_kernel,
            grid=(3,),
            out_shape=(jax.ShapeDtypeStruct((N4608, N1152), BF16), jax.ShapeDtypeStruct((N1152, N1152), BF16)),
            in_specs=[vmem, vmem, vmem, hbm, vmem],
            out_specs=(pl.BlockSpec((N1536, N1152), lambda i: (i, 0)), pl.BlockSpec((BASE_PAD, N1152), lambda i: (i, 0))),
            scratch_shapes=[
                pltpu.VMEM((2, N40, IN_CH, REST), BF16),
                pltpu.VMEM((N42, STRIP_ROWS, LANES), BF16),
                pltpu.VMEM((N96, BASE_PAD), BF16),
                pltpu.VMEM((N2880, BASE), BF16),
                pltpu.VMEM((N5120, N1152), BF16),
                pltpu.VMEM((N1792, TILE), F32),
                pltpu.VMEM((N3072, TILE), BF16),
                pltpu.VMEM((PACK, TILE), BF16),
                pltpu.VMEM((LANES, LANES), F32),
                dma, dma((IN_CH,)), dma((2, 2)),
            ],
            compiler_params=pltpu.CompilerParams(
                vmem_limit_bytes=VMEM_LIMIT, collective_id=1, has_side_effects=True, dimension_semantics=("arbitrary",)
            ),
            name="enc1",
        )(image_tile.transpose(0, 2, 1), w_enc1a, b_enc1a, flat(w_enc1b), b_enc1b)

        d2 = pl.pallas_call(
            mid_kernel,
            out_shape=jax.ShapeDtypeStruct((N1152, MIDDLE), BF16),
            in_specs=[vmem] + [hbm] * LAST_STRIP + [vmem] * SIX,
            out_specs=hbm,
            scratch_shapes=[
                pltpu.VMEM((N3072, MIDDLE), BF16),
                pltpu.VMEM((RING_ROWS, DEEP), BF16),
                pltpu.VMEM((N1152, MIDDLE3), BF16),
                pltpu.VMEM((N1152, MIDDLE3), BF16),
                pltpu.VMEM((N1152, MIDDLE3), BF16),
                pltpu.VMEM((BASE, MIDDLE3), BF16),
                pltpu.VMEM((BASE, N3840), BF16),
                pltpu.VMEM((TILE, DEEP), BF16),
                pltpu.VMEM((N1152, MIDDLE), BF16),
                pltpu.VMEM((TILE, DEEP), F32),
                pltpu.VMEM((FIVE, N512, LANES), F32),
                pltpu.VMEM((LANES, LANES), F32),
                dma((N18,)), dma((TAPS,)), dma((3,)), dma((TAPS,)), dma((IN_CH,)), dma((TAPS,)), dma((TAPS,)), dma,
                dma((LAST_STRIP, 2)), dma((LAST_STRIP, 2)),
            ],
            compiler_params=pltpu.CompilerParams(
                vmem_limit_bytes=VMEM_LIMIT, collective_id=0, has_side_effects=True
            ),
            name="mid",
        )(
            p1, flat(w_enc2a), flat(w_enc2b), flat(w_mid_a), flat(w_mid_b), flat(w_up2), flat(w_dec2a), flat(w_dec2b),
            b_enc2a, b_enc2b, b_mid_a, b_mid_b, b_dec2a, b_dec2b,
        )

        def turned(weight):
            return weight.transpose(0, 1, 3, 2).reshape(-1, weight.shape[2])

        y = pl.pallas_call(
            dec1_kernel,
            out_shape=jax.ShapeDtypeStruct((REST, IN_CH, REST), F32),
            in_specs=[vmem] + [hbm] * IN_CH + [vmem] * 3 + [pl.BlockSpec(memory_space=pltpu.SMEM)],
            out_specs=hbm,
            scratch_shapes=[
                pltpu.VMEM((N4608, N1152), BF16),
                pltpu.VMEM((N4608, N1152), BF16),
                pltpu.VMEM((N4352, N1152), BF16),
                pltpu.VMEM((N4608, TILE), F32),
                pltpu.VMEM((DEEP, MIDDLE), BF16),
                pltpu.VMEM((N2880, MIDDLE), BF16),
                pltpu.VMEM((N2880, BASE), BF16),
                pltpu.VMEM((N2560, TILE), BF16),
                pltpu.VMEM((MIDDLE, TILE), BF16),
                pltpu.VMEM((N6144, TILE), BF16),
                pltpu.VMEM((N2048, TILE), BF16),
                pltpu.VMEM((N3072, TILE), BF16),
                pltpu.VMEM((PACK, TILE), BF16),
                pltpu.VMEM((2, 3, REST_AT, LANES), F32),
                pltpu.VMEM((2, STRIP_ROWS, IN_CH, REST), F32),
                pltpu.VMEM((TILE, BASE), BF16),
                dma((IN_CH,)), dma((2,)), dma((2,)),
            ],
            compiler_params=pltpu.CompilerParams(vmem_limit_bytes=VMEM_LIMIT, collective_id=2, has_side_effects=True),
            name="dec1",
        )(d2, s1, turned(w_up1), turned(w_dec1a), flat(w_dec1b), b_dec1a, b_dec1b, w_head.T, b_head)
        return y.transpose(0, 2, 1)

    def program(image, *params):
        mapped = jax.shard_map(
            body, mesh=mesh, in_specs=(tile_spec,) + (P(),) * len(params), out_specs=tile_spec, check_vma=False
        )
        return mapped(image, *params)

    return program
```

```python
import functools

import jax
import jax.numpy as jnp
from jax import lax
from jax.experimental import pallas as pl
from jax.experimental.pallas import tpu as pltpu
from jax.sharding import PartitionSpec as P

IN_CH = 4
FIVE = 5
SIX = 6
LAST_STRIP = 7
STRIPS = 8
TAPS = 9
N12 = 12
N16 = 16
N18 = 18
N28 = 28
N30 = 30
N31 = 31
STRIP_ROWS = 32
N36 = 36
N40 = 40
N42 = 42
N60 = 60
REST = 64
N80 = 80
N96 = 96
N127 = 127
LANES = 128
N192 = 192
N224 = 224
TILE = 256
N288 = 288
BASE = 320
BASE_PAD = 384
N512 = 512
MIDDLE = 640
REST_AT = 768
N896 = 896
PACK_USED = 960
PACK = 1024
N1152 = 1152
DEEP = 1280
N1536 = 1536
N1792 = 1792
MIDDLE3 = 1920
N2048 = 2048
N2560 = 2560
N2880 = 2880
N3072 = 3072
N3200 = 3200
N3840 = 3840
N4096 = 4096
N4352 = 4352
N4608 = 4608
N5120 = 5120
N6144 = 6144
N6400 = 6400
N8960 = 8960
N10240 = 10240
N11520 = 11520
BF16 = jnp.bfloat16
F32 = jnp.float32
MESH = pl.DeviceIdType.MESH
VMEM_LIMIT = 66_900_000
RING_ROWS = N11520


def strip_index():
    col = lax.axis_index("col")
    row = lax.axis_index("row")
    return row + col * (LAST_STRIP - 2 * row)


def strip_device(position):
    col = position // IN_CH
    rest = position % IN_CH
    return (lax.axis_index("data"), col, rest + col * (3 - 2 * rest))


def dot(a, b):
    return jnp.dot(a, b, preferred_element_type=F32)


def shifted(value, width, step):
    if step == 1:
        return value
    rows = value.shape[0]
    column = lax.broadcasted_iota(jnp.int32, value.shape, 0) % width
    if step == 0:
        return jnp.where(column == 0, 0.0, pltpu.roll(value, 1, axis=0))
    return jnp.where(column == width - 1, 0.0, pltpu.roll(value, rows - 1, axis=0))


def put3(dst, row0, lane0, channels, value, width):
    rows, lanes = value.shape
    for step in range(3):
        dst[pl.ds(row0, rows), pl.ds(step * channels + lane0, lanes)] = shifted(value, width, step).astype(BF16)


def put3_320(dst, row0, main, rest, width, stage=None):
    rows = main.shape[0]
    pitch = width + N16
    planes = [main[:, 0:LANES], main[:, LANES:TILE], rest]
    for t, plane in enumerate(planes if stage is not None else []):
        for r in range(rows // width):
            stage[t, pitch * r + STRIPS : pitch * r + STRIPS + width, :] = plane[width * r : width * r + width]

    def moved(t, step):
        if step == 1 or stage is None:
            return shifted(planes[t], width, step)
        first = LAST_STRIP + step
        parts = [stage[t, pitch * r + first : pitch * r + first + width, :] for r in range(rows // width)]
        return jnp.concatenate(parts, axis=0) if len(parts) > 1 else parts[0]

    for step in range(3):
        for t in range(2):
            dst[pl.ds(row0, rows), pl.ds(step * TILE + LANES * t, LANES)] = moved(t, step).astype(BF16)
    first = moved(2, 0) + pltpu.roll(rest, REST, axis=1)
    dst[pl.ds(row0, rows), pl.ds(REST_AT, LANES)] = first.astype(BF16)
    dst[pl.ds(row0, rows), pl.ds(N896, LANES)] = moved(2, 2).astype(BF16)


def low_lanes(value):
    return jnp.where(lax.broadcasted_iota(jnp.int32, value.shape, 1) < REST, value, 0.0)


def pack_weights(staged, main_ref, rest_ref):
    for dj in range(3):
        for start, size, row in ((0, TILE, TILE * dj), (TILE, REST, REST_AT + REST * dj)):
            parts = []
            for di in range(3):
                base = (3 * di + dj) * BASE + start
                main_ref[pl.ds(PACK * di + row, size), :] = staged[pl.ds(base, size), 0:TILE]
                parts.append(staged[pl.ds(base, size), TILE:BASE])
            parts.append(jnp.zeros((size, REST), BF16))
            rest_ref[pl.ds(row, size), :] = jnp.concatenate(parts, axis=1)
    clear_pad(main_ref, 3)
    clear_pad(rest_ref, 1)


def clear_pad(ref, groups):
    for group in range(groups):
        ref[pl.ds(PACK * group + PACK_USED, REST), :] = jnp.zeros((REST, ref.shape[1]), BF16)


def turn_main(staged, main_ref, di, dj):
    turned = staged[pl.ds(pl.multiple_of(PACK_USED * di + BASE * dj, REST), TILE), :].T
    for src in range(2):
        base = N3072 * src + PACK * di
        main_ref[pl.ds(pl.multiple_of(base + TILE * dj, REST), TILE), :] = turned[BASE * src : BASE * src + TILE]
        main_ref[pl.ds(pl.multiple_of(base + REST_AT + REST * dj, REST), REST), :] = turned[BASE * src + TILE : BASE * src + BASE]


def turn_rest(staged, main_ref, rest_ref):
    for dj in range(3):
        parts = [staged[pl.ds(PACK_USED * di + BASE * dj + TILE, REST), :] for di in range(3)] + [jnp.zeros((REST, MIDDLE), BF16)]
        turned = jnp.concatenate(parts, axis=0).T
        for src in range(2):
            rest_ref[pl.ds(PACK * src + TILE * dj, TILE), :] = turned[BASE * src : BASE * src + TILE]
            rest_ref[pl.ds(PACK * src + REST_AT + REST * dj, REST), :] = turned[BASE * src + TILE : BASE * src + BASE]
    clear_pad(main_ref, SIX)
    clear_pad(rest_ref, 2)


def bias_row(ref, start, size):
    return ref[pl.ds(start, size)].reshape(1, size)


def bias_rest(ref):
    return jnp.concatenate([bias_row(ref, TILE, REST), jnp.zeros((1, REST), F32)], axis=1)


def enter_barrier():
    barrier = pltpu.get_barrier_semaphore()
    for position in range(STRIPS):
        pl.semaphore_signal(barrier, inc=1, device_id=strip_device(position), device_id_type=MESH)
    return barrier


class Push:
    def __init__(self, src, dst, send_sem, recv_sem, device, here):
        self.here = here
        self.local = pltpu.make_async_copy(src, dst, recv_sem)
        self.remote = pltpu.make_async_remote_copy(
            src_ref=src, dst_ref=dst, send_sem=send_sem, recv_sem=recv_sem, device_id=device, device_id_type=MESH
        )

    def start(self):
        @pl.when(self.here)
        def _():
            self.local.start()

        @pl.when(jnp.logical_not(self.here))
        def _():
            self.remote.start()

    def wait_send(self):
        @pl.when(jnp.logical_not(self.here))
        def _():
            self.remote.wait_send()

    def wait_recv(self):
        self.remote.wait_recv()


def rest_sum(y_ref, row0, rows):
    total = y_ref[pl.ds(row0, rows), 0:LANES] + y_ref[pl.ds(row0 + TILE, rows), LANES:TILE]
    return total + pltpu.roll(y_ref[pl.ds(row0 + LANES, rows), 0:LANES], REST, axis=1)


def valid_rows(value, first_row, width):
    row = first_row + lax.broadcasted_iota(jnp.int32, value.shape, 0) // width
    return jnp.where((row >= 0) & (row < TILE), value, 0.0)


def pooled(value, width, scratch):
    rows, lanes = value.shape
    tall = jnp.concatenate(
        [jnp.maximum(value[s : s + width], value[s + width : s + 2 * width]) for s in range(0, rows, 2 * width)], axis=0
    )
    halves = []
    for start in range(0, lanes, LANES):
        scratch[0 : rows // 2, :] = tall[:, start : start + LANES]
        halves.append(
            jnp.maximum(scratch[pl.ds(0, rows // IN_CH, stride=2), :], scratch[pl.ds(1, rows // IN_CH, stride=2), :])
        )
    return jnp.concatenate(halves, axis=1) if len(halves) > 1 else halves[0]


def enc1_kernel(
    image, w_a, b_a, w_b, b_b, s1_out, p1_out,
    halves, planes, w_stem, staged, x_a, y_rest, w_main, w_rest, pool_buf, stage, stage_p, w_sem, send_sem, recv_sem,
):
    step = pl.program_id(0)
    strip = strip_index()

    @pl.when(step == 0)
    def _():
        row = lax.axis_index("row")
        col = lax.axis_index("col")
        copy_w = pltpu.make_async_copy(w_b, staged, w_sem)
        copy_w.start()
        barrier = enter_barrier()
        stage[...] = jnp.zeros_like(stage)
        stage_p[...] = jnp.zeros_like(stage_p)

        for di in range(3):
            taps = []
            for dj in range(3):
                tap = jnp.concatenate([w_a[di, dj].astype(F32), jnp.zeros((IN_CH, BASE), F32)], axis=0)
                taps.append(jnp.concatenate([tap, jnp.zeros((STRIPS, REST), F32)], axis=1))
            taps.append(jnp.zeros((STRIPS, BASE_PAD), F32))
            w_stem[STRIP_ROWS * di : STRIP_ROWS * di + STRIP_ROWS, :] = jnp.concatenate(taps, axis=0).astype(BF16)
        planes[N40:N42, :, :] = jnp.zeros((2, STRIP_ROWS, LANES), BF16)

        pl.semaphore_wait(barrier, STRIPS)
        pushes = []
        for index, (target, src_row, dst_row, rows) in enumerate(
            ((2 * row, 0, IN_CH, N36), (2 * row + 1, N28, 0, N36), ((2 * row + 2) % STRIPS, N60, 0, IN_CH), ((2 * row + LAST_STRIP) % STRIPS, 0, N36, IN_CH))
        ):
            pushes.append(
                Push(
                    image.at[pl.ds(src_row, rows)],
                    halves.at[col, pl.ds(dst_row, rows)],
                    send_sem.at[index],
                    recv_sem.at[index // 2, col],
                    strip_device(target),
                    target == strip,
                )
            )
        for push in pushes:
            push.start()
        copy_w.wait()
        pack_weights(staged, w_main, w_rest)
        for push in pushes:
            push.wait_send()
        for kind, rows in ((0, N36), (1, IN_CH)):
            for side in range(2):
                Push(
                    image.at[pl.ds(0, rows)], halves.at[side, pl.ds(0, rows)],
                    send_sem.at[0], recv_sem.at[kind, side], strip_device(strip), strip < 0,
                ).wait_recv()

        def expand(i, carry):
            for j in range(STRIPS):
                r = STRIPS * i + j
                both = jnp.concatenate([halves[0, r].astype(F32), halves[1, r].astype(F32)], axis=1)
                image_row = STRIP_ROWS * strip - IN_CH + r
                both = jnp.where((image_row >= 0) & (image_row < TILE), both, 0.0)
                both = jnp.concatenate([both, jnp.zeros((IN_CH, LANES), F32)], axis=0)
                column = lax.broadcasted_iota(jnp.int32, (STRIPS, LANES), 1)
                before = jnp.where(column == 0, 0.0, pltpu.roll(both, 1, axis=1))
                after = jnp.where(column == N127, 0.0, pltpu.roll(both, N127, axis=1))
                planes[r] = jnp.concatenate([before, both, after, jnp.zeros((STRIPS, LANES), F32)], axis=0).astype(BF16)
            return carry

        lax.fori_loop(0, FIVE, expand, 0)

        def stem(i, carry):
            for j in range(IN_CH):
                r = STRIPS * i + 2 * j
                row0 = pl.multiple_of(r * LANES, TILE)
                patch = jnp.concatenate(
                    [jnp.concatenate([planes[r + k + di] for di in range(3)], axis=0) for k in range(2)], axis=1
                )
                acc = lax.dot_general(patch, w_stem[...], (((0,), (0,)), ((), ())), preferred_element_type=F32)
                main = jnp.maximum(acc[:, 0:TILE] + bias_row(b_a, 0, TILE), 0.0)
                tail = jnp.maximum(acc[:, TILE:BASE_PAD] + bias_rest(b_a), 0.0)
                first_row = STRIP_ROWS * strip - 3 + r
                put3_320(
                    x_a, row0, valid_rows(main, first_row, LANES), valid_rows(tail, first_row, LANES), LANES, stage.at[j % 2]
                )
            return carry

        lax.fori_loop(0, FIVE, stem, 0)

    base = pl.multiple_of(step * N1536, N512)

    def rest(j):
        y_rest[TILE * j : TILE * j + TILE, :] = dot(x_a[pl.ds(base + TILE * j, TILE), 0:PACK], w_rest[...])

    rest(0)
    for j in range(SIX):
        rest(j + 1)
        acc = dot(x_a[pl.ds(base + TILE * j, TILE), 0:PACK], w_main[0:PACK, :])
        acc = acc + dot(x_a[pl.ds(base + TILE * j + LANES, TILE), 0:PACK], w_main[PACK:N2048, :])
        acc = acc + dot(x_a[pl.ds(base + TILE * j + TILE, TILE), 0:PACK], w_main[N2048:N3072, :])
        first_row = STRIP_ROWS * strip - 2 + N12 * step + 2 * j
        main = valid_rows(jnp.maximum(acc + bias_row(b_b, 0, TILE), 0.0), first_row, LANES)
        tail = jnp.maximum(rest_sum(y_rest, TILE * j, TILE) + bias_rest(b_b), 0.0)
        tail = low_lanes(valid_rows(tail, first_row, LANES))
        s1_out[TILE * j : TILE * j + TILE, 0:TILE] = main.astype(BF16)
        s1_out[TILE * j : TILE * j + TILE, TILE:BASE_PAD] = tail.astype(BF16)
        put3_320(p1_out, REST * j, pooled(main, LANES, pool_buf.at[j % 2]), pooled(tail, LANES, pool_buf.at[j % 2]), REST, stage_p.at[j % 2])


def mid_kernel(
    p1_hbm, w_2a, w_2b, w_ma, w_mb, w_u2, w_d2a, w_d2b, b_2a, b_2b, b_ma, b_mb, b_d2a, b_d2b, out,
    p1, first_w, ring, x_a, x_s, x_u, m_1, m_2, m_o, d_2, acc_ref, wide, pool_buf,
    sem_2a, sem_2b, sem_ma, sem_mb, sem_u2, sem_d2a, sem_d2b, sem_p1, sem_out, send_sem, recv_sem,
):
    strip = strip_index()
    prev_dev = strip_device((strip + LAST_STRIP) % STRIPS)
    next_dev = strip_device((strip + 1) % STRIPS)

    def exchange(buf, width, lane0, lanes, rows, index, target=None):
        target = buf if target is None else target
        lane = pl.ds(lane0, lanes)
        copies = []
        for side, src_row, dst_row, device in ((0, 1, rows + 1, prev_dev), (1, rows, 0, next_dev)):
            copies.append(
                pltpu.make_async_remote_copy(
                    src_ref=buf.at[pl.ds(src_row * width, width), lane],
                    dst_ref=target.at[pl.ds(dst_row * width, width), lane],
                    send_sem=send_sem.at[index, side],
                    recv_sem=recv_sem.at[index, side],
                    device_id=device,
                    device_id_type=MESH,
                )
            )
        return copies

    def start(copies):
        for copy in copies:
            copy.start()

    def finish(copies):
        for copy in copies:
            copy.wait()

    def halo(buf, width, channels, rows):
        for row, inside in ((0, strip > 0), (rows + 1, strip < LAST_STRIP)):
            value = buf[pl.ds(row * width, width), pl.ds(channels, channels)].astype(F32)
            put3(buf, row * width, 0, channels, jnp.where(inside, value, 0.0), width)

    copies_2a = []
    for tap in range(TAPS):
        di, dj = tap // 3, tap % 3
        for part, (start_row, size, row) in enumerate(((0, TILE, TILE * dj), (TILE, REST, REST_AT + REST * dj))):
            copies_2a.append(
                pltpu.make_async_copy(
                    w_2a.at[pl.ds(BASE * tap + start_row, size), :],
                    first_w.at[pl.ds(PACK * di + row, size), :],
                    sem_2a.at[2 * tap + part],
                )
            )

    def tap_copies(src, rows, base, sem):
        return [
            pltpu.make_async_copy(
                src.at[pl.ds(rows * tap, rows), :],
                ring.at[pl.ds(base + rows * (tap // 2), rows), pl.ds(MIDDLE * (tap % 2), MIDDLE)],
                sem.at[tap],
            )
            for tap in range(src.shape[0] // rows)
        ]

    copies_2b = tap_copies(w_2b, MIDDLE, 0, sem_2b)
    copies_ma = [
        pltpu.make_async_copy(w_ma.at[pl.ds(MIDDLE3 * di, MIDDLE3), :], ring.at[pl.ds(N3200 + MIDDLE3 * t, MIDDLE3), :], sem_ma.at[t])
        for t, di in enumerate((1, 0, 2))
    ]

    def mb_row(k):
        return (N8960 + DEEP * k) % RING_ROWS

    copies_mb = [
        pltpu.make_async_copy(
            w_mb.at[pl.ds(DEEP * (3 * (1, 0, 2)[k // 3] + k % 3), DEEP), :], ring.at[pl.ds(mb_row(k), DEEP), :], sem_mb.at[k]
        )
        for k in range(TAPS)
    ]
    copies_u2 = [
        pltpu.make_async_copy(
            w_u2.at[pl.ds(DEEP * tap, DEEP), :],
            first_w.at[pl.ds(DEEP * tap, DEEP), :] if tap < 2 else ring.at[pl.ds(N8960, DEEP), pl.ds(MIDDLE * (tap - 2), MIDDLE)],
            sem_u2.at[tap],
        )
        for tap in range(IN_CH)
    ]
    copies_d2a = tap_copies(w_d2a, DEEP, 0, sem_d2a)
    copies_d2b = tap_copies(w_d2b, MIDDLE, N6400, sem_d2b)

    copy_p1 = pltpu.make_async_copy(p1_hbm, p1, sem_p1)
    copy_p1.start()
    start(copies_2a)

    barrier = pltpu.get_barrier_semaphore()
    for device in (prev_dev, next_dev):
        pl.semaphore_signal(barrier, inc=1, device_id=device, device_id_type=MESH)
    pl.semaphore_wait(barrier, 2)

    for di in range(3):
        first_w[PACK * di + PACK_USED : PACK * di + PACK, :] = jnp.zeros((REST, MIDDLE), BF16)
    copy_p1.wait()
    finish(copies_2a)
    start(copies_2b)
    start(copies_ma)

    ex_a = exchange(x_a, REST, MIDDLE, MIDDLE, N16, 0)
    ex_s = exchange(x_s, REST, MIDDLE, MIDDLE, N16, 1)
    ex_m1 = exchange(m_1, STRIP_ROWS, MIDDLE, MIDDLE, STRIPS, 2)
    ex_m2 = exchange(m_2, STRIP_ROWS, DEEP, DEEP, STRIPS, 3)
    ex_u = exchange(x_u, REST, MIDDLE, MIDDLE, N16, IN_CH)
    ex_b = exchange(x_a, REST, MIDDLE, MIDDLE, N16, FIVE)
    ex_d = exchange(d_2, REST, 0, MIDDLE, N16, SIX, out)
    tiles = ((0, TILE), (TILE, TILE), (N512, LANES))

    def enc2a(i, carry):
        @pl.when(i == 1)
        def _():
            start(ex_a)

        for block in (i, 3 - i):
            row0 = pl.multiple_of(block * TILE, TILE)
            for lane0, lanes in tiles:
                acc = dot(p1[pl.ds(row0, TILE), 0:PACK], first_w[0:PACK, pl.ds(lane0, lanes)])
                for di in (1, 2):
                    acc = acc + dot(
                        p1[pl.ds(row0 + REST * di, TILE), 0:PACK],
                        first_w[PACK * di : PACK * di + PACK, pl.ds(lane0, lanes)],
                    )
                value = jnp.maximum(acc + bias_row(b_2a, lane0, lanes), 0.0)
                put3(x_a, row0 + REST, lane0, MIDDLE, value, REST)
        return carry

    lax.fori_loop(0, 2, enc2a, 0)
    finish(copies_2b)
    start(copies_mb[0:2])
    start(copies_u2[0:2])

    def conv640(src, row0, base, lane0, lanes):
        acc = None
        for di in range(3):
            weights = jnp.concatenate(
                [
                    ring[base + MIDDLE * (t // 2) : base + MIDDLE * (t // 2) + MIDDLE, pl.ds(MIDDLE * (t % 2) + lane0, lanes)]
                    for t in range(3 * di, 3 * di + 3)
                ],
                axis=0,
            )
            part = dot(src[pl.ds(row0 + REST * di, TILE), :], weights)
            acc = part if acc is None else acc + part
        return acc

    def enc2b(i, carry):
        block = i + 1 - 2 * (i % 2)
        row0 = pl.multiple_of(block * TILE, TILE)

        @pl.when(i == 1)
        def _():
            finish(ex_a)
            halo(x_a, REST, MIDDLE, N16)

        @pl.when(i == 3)
        def _():
            start(ex_m1)
            start(ex_s)

        for lane0, lanes in tiles:
            value = jnp.maximum(conv640(x_a, row0, 0, lane0, lanes) + bias_row(b_2b, lane0, lanes), 0.0)
            put3(x_s, row0 + REST, lane0, MIDDLE, value, REST)
            put3(m_1, pl.multiple_of(block * REST + STRIP_ROWS, STRIP_ROWS), lane0, MIDDLE, pooled(value, REST, pool_buf), STRIP_ROWS)
        return carry

    lax.fori_loop(0, IN_CH, enc2b, 0)
    start(copies_mb[2:IN_CH])

    acc_ref[...] = jnp.zeros_like(acc_ref)
    finish(copies_ma)

    def mid_a(t, carry):
        di = (t + 1) % 2 + 2 * (t // 2) - t // 2

        @pl.when(t == 1)
        def _():
            start(copies_mb[IN_CH:SIX])
            finish(ex_m1)
            halo(m_1, STRIP_ROWS, MIDDLE, STRIPS)

        @pl.when(t == 2)
        def _():
            start(copies_mb[SIX:LAST_STRIP])

        base = pl.multiple_of(N3200 + MIDDLE3 * t, LANES)
        lhs_row = pl.multiple_of(STRIP_ROWS * di, STRIP_ROWS)
        for lane0 in range(0, DEEP, TILE):
            acc_ref[:, pl.ds(lane0, TILE)] += dot(
                m_1[pl.ds(lhs_row, TILE), :], ring[pl.ds(base, MIDDLE3), pl.ds(lane0, TILE)]
            )
        return carry

    lax.fori_loop(0, 3, mid_a, 0)
    start(copies_mb[LAST_STRIP:TAPS])

    def mid_a_rows(first, rows):
        for lane0 in range(0, DEEP, TILE):
            value = jnp.maximum(acc_ref[pl.ds(first, rows), pl.ds(lane0, TILE)] + bias_row(b_ma, lane0, TILE), 0.0)
            put3(m_2, STRIP_ROWS + first, lane0, DEEP, value, STRIP_ROWS)

    mid_a_rows(0, STRIP_ROWS)
    mid_a_rows(N224, STRIP_ROWS)
    start(ex_m2)
    mid_a_rows(STRIP_ROWS, N192)
    acc_ref[...] = jnp.zeros_like(acc_ref)

    def mid_b(k, carry):
        t = k // 3
        di = (t + 1) % 2 + 2 * (t // 2) - t // 2

        for j in range(TAPS):
            @pl.when(k == j)
            def _(j=j):
                copies_mb[j].wait()

        @pl.when(k == 3)
        def _():
            start(copies_u2[2:IN_CH])
            finish(ex_m2)
            halo(m_2, STRIP_ROWS, DEEP, STRIPS)

        @pl.when(k == FIVE)
        def _():
            start(copies_d2a[0:IN_CH])

        @pl.when(k == LAST_STRIP)
        def _():
            start(copies_d2a[IN_CH:TAPS])

        base = pl.multiple_of(mb_row(k), LANES)
        lhs_row = pl.multiple_of(STRIP_ROWS * di, STRIP_ROWS)
        lhs_lane = pl.multiple_of(DEEP * (k % 3), DEEP)
        for lane0 in range(0, DEEP, TILE):
            acc_ref[:, pl.ds(lane0, TILE)] += dot(
                m_2[pl.ds(lhs_row, TILE), pl.ds(lhs_lane, DEEP)], ring[pl.ds(base, DEEP), pl.ds(lane0, TILE)]
            )
        return carry

    lax.fori_loop(0, TAPS, mid_b, 0)
    for lane0 in range(0, DEEP, TILE):
        value = jnp.maximum(acc_ref[:, pl.ds(lane0, TILE)] + bias_row(b_mb, lane0, TILE), 0.0)
        m_o[:, pl.ds(lane0, TILE)] = value.astype(BF16)

    finish(copies_u2)
    for p in range(2):
        for q in range(2):
            for lane0, lanes in tiles:
                if p == 0:
                    weights = first_w[DEEP * q : DEEP * q + DEEP, pl.ds(lane0, lanes)]
                else:
                    weights = ring[N8960:N10240, pl.ds(MIDDLE * q + lane0, lanes)]
                part = dot(m_o[...], weights)
                for lane in range(0, lanes, LANES):
                    wide[(lane0 + lane) // LANES, pl.ds(q, TILE, stride=2), :] = part[:, lane : lane + LANES]

        def place(i, carry):
            src = pl.multiple_of(REST * i, REST)
            dst = pl.multiple_of(REST * (1 + 2 * i + p), REST)
            for lane0 in range(0, MIDDLE, LANES):
                put3(x_u, dst, lane0, MIDDLE, wide[lane0 // LANES, pl.ds(src, REST), :], REST)
            return carry

        lax.fori_loop(0, STRIPS, place, 0)
    start(ex_u)
    start(copies_d2b)
    finish(ex_s)
    halo(x_s, REST, MIDDLE, N16)
    finish(copies_d2a)

    def dec2a(i, carry):
        block = i + 1 - 2 * (i % 2)
        row0 = pl.multiple_of(block * TILE, TILE)

        @pl.when(i == 1)
        def _():
            finish(ex_u)
            halo(x_u, REST, MIDDLE, N16)

        @pl.when(i == 3)
        def _():
            start(ex_b)

        for lane0, lanes in tiles:
            acc = None
            for tap in range(TAPS):
                rows = pl.ds(row0 + REST * (tap // 3), TILE)
                cols = pl.ds(MIDDLE * (tap % 3), MIDDLE)
                lhs = jnp.concatenate([x_u[rows, cols], x_s[rows, cols]], axis=1)
                base = DEEP * (tap // 2)
                part = dot(lhs, ring[base : base + DEEP, pl.ds(MIDDLE * (tap % 2) + lane0, lanes)])
                acc = part if acc is None else acc + part
            value = jnp.maximum(acc + bias_row(b_d2a, lane0, lanes), 0.0)
            put3(x_a, row0 + REST, lane0, MIDDLE, value, REST)
        return carry

    lax.fori_loop(0, IN_CH, dec2a, 0)
    finish(copies_d2b)

    def dec2b(i, carry):
        block = i + 1 - 2 * (i % 2)
        row0 = pl.multiple_of(block * TILE, TILE)

        @pl.when(i == 1)
        def _():
            finish(ex_b)
            halo(x_a, REST, MIDDLE, N16)

        @pl.when(i == 3)
        def _():
            start(ex_d)

        for lane0, lanes in tiles:
            value = jnp.maximum(conv640(x_a, row0, N6400, lane0, lanes) + bias_row(b_d2b, lane0, lanes), 0.0)
            d_2[pl.ds(row0 + REST, TILE), pl.ds(lane0, lanes)] = value.astype(BF16)
        return carry

    lax.fori_loop(0, IN_CH, dec2b, 0)
    result = pltpu.make_async_copy(d_2.at[pl.ds(REST, PACK), :], out.at[pl.ds(REST, PACK), :], sem_out)
    result.start()
    finish(ex_d)
    result.wait()


def dec1_kernel(
    d_2, s1, w_u1, w_d1a, w_d1b, b_d1a, b_d1b, w_head, b_head, out,
    x_u, x_s, x_d, y_rest, st_u, st_a, st_b, wu_main, wu_rest, wa_main, wa_rest, wb_main, wb_rest, wide, result, pending, stage, skip, low,
    sem, send_sem, recv_sem,
):
    strip = strip_index()
    row = lax.axis_index("row")
    col = lax.axis_index("col")
    copy_u = pltpu.make_async_copy(w_u1, st_u, sem.at[0])
    copy_a = pltpu.make_async_copy(w_d1a, st_a, sem.at[1])
    copy_s = pltpu.make_async_copy(s1, skip, sem.at[2])
    copy_b = pltpu.make_async_copy(w_d1b, st_b, sem.at[3])
    copy_d = pltpu.make_async_copy(d_2, low, sem.at[IN_CH])
    copy_u.start()
    copy_d.start()
    barrier = enter_barrier()

    stage[...] = jnp.zeros_like(stage)
    copy_u.wait()
    copy_a.start()
    copy_s.start()
    copy_b.start()
    for tap in range(IN_CH):
        wu_main[MIDDLE * tap : MIDDLE * tap + MIDDLE, :] = st_u[BASE * tap : BASE * tap + TILE, :].T
    wu_rest[...] = jnp.concatenate([st_u[BASE * tap + TILE : BASE * tap + BASE, :] for tap in range(IN_CH)], axis=0).T
    copy_d.wait()

    def up1(i, carry):
        row0 = pl.multiple_of(i * BASE_PAD, LANES)
        lhs = low[pl.ds(row0, BASE_PAD), :]
        rest = dot(lhs, wu_rest[...])
        for p in range(2):
            part = rest[:, LANES * p : LANES * p + LANES]
            buf = wide.at[p]
            buf[2, pl.ds(0, BASE_PAD, stride=2), :] = low_lanes(part)
            buf[2, pl.ds(1, BASE_PAD, stride=2), :] = low_lanes(pltpu.roll(part, REST, axis=1))
            for q in range(2):
                tap = 2 * p + q
                main = dot(lhs, wu_main[MIDDLE * tap : MIDDLE * tap + MIDDLE, :])
                buf[0, pl.ds(q, BASE_PAD, stride=2), :] = main[:, 0:LANES]
                buf[1, pl.ds(q, BASE_PAD, stride=2), :] = main[:, LANES:TILE]
            for r in range(SIX):
                main = jnp.concatenate([buf[0, LANES * r : LANES * r + LANES, :], buf[1, LANES * r : LANES * r + LANES, :]], axis=1)
                put3_320(
                    x_u, pl.multiple_of((N12 * i + 2 * r + p) * LANES, LANES), main, buf[2, LANES * r : LANES * r + LANES, :], LANES
                )
        return carry

    lax.fori_loop(0, 3, up1, 0)

    @pl.when(strip == 0)
    def _():
        x_u[0:TILE, :] = jnp.zeros((TILE, N1152), BF16)

    @pl.when(strip == LAST_STRIP)
    def _():
        x_u[N4352:N4608, :] = jnp.zeros((TILE, N1152), BF16)

    copy_a.wait()
    turn_rest(st_a, wa_main, wa_rest)
    copy_s.wait()

    def rest_a(i, carry):
        base = pl.multiple_of(i * N1536, N512)

        def spread(j):
            rows = pl.ds(base + TILE * j, TILE)
            put3_320(
                x_s, base + TILE * j, skip[rows, 0:TILE].astype(F32), skip[rows, TILE:BASE_PAD].astype(F32), LANES, stage.at[j % 2]
            )

        spread(0)
        for j in range(SIX):
            rows = pl.ds(base + TILE * j, TILE)
            y_rest[rows, :] = dot(x_u[rows, 0:PACK], wa_rest[0:PACK, :]) + dot(
                x_s[rows, 0:PACK], wa_rest[PACK:N2048, :]
            )
            if j < FIVE:
                spread(j + 1)
            if j < 3:
                turn_main(st_a, wa_main, i, j)
        return carry

    lax.fori_loop(0, 3, rest_a, 0)

    def conv_a(row0, first_row, slot):
        acc = None
        for di in range(3):
            rows = pl.ds(row0 + LANES * di, TILE)
            for src, ref in enumerate((x_u, x_s)):
                base = N3072 * src + PACK * di
                part = dot(ref[rows, 0:PACK], wa_main[base : base + PACK, :])
                acc = part if acc is None else acc + part
        main = valid_rows(jnp.maximum(acc + bias_row(b_d1a, 0, TILE), 0.0), first_row, LANES)
        tail = valid_rows(jnp.maximum(rest_sum(y_rest, row0, TILE) + bias_rest(b_d1a), 0.0), first_row, LANES)
        put3_320(x_d, row0, main, low_lanes(tail), LANES, stage.at[slot])

    def dec1a(i, carry):
        for j in range(IN_CH):
            conv_a(pl.multiple_of(i * PACK + TILE * j, TILE), STRIP_ROWS * strip - 1 + STRIPS * i + 2 * j, j % 2)
        return carry

    lax.fori_loop(0, IN_CH, dec1a, 0)
    conv_a(N4096, STRIP_ROWS * strip + N31, 0)

    copy_b.wait()
    pack_weights(st_b, wb_main, wb_rest)
    head_bias = jnp.zeros((IN_CH, LANES), F32)
    for channel in range(IN_CH):
        head_bias = jnp.where(lax.broadcasted_iota(jnp.int32, (IN_CH, LANES), 0) == channel, b_head[channel], head_bias)

    pending[...] = jnp.zeros_like(pending)

    def head(hidden, row0):
        line = lax.dot_general(w_head[...], hidden, (((1,), (1,)), ((), ())), preferred_element_type=F32)
        for r in range(2):
            part = line[:, LANES * r : LANES * r + LANES] + head_bias
            result[0, row0 + r] = part[:, 0:REST]
            result[1, row0 + r] = part[:, REST:LANES]

    def dec1b(i, carry):
        base = pl.multiple_of(i * PACK, PACK)

        def rest(j):
            y_rest[TILE * j : TILE * j + TILE, :] = dot(x_d[pl.ds(base + TILE * j, TILE), 0:PACK], wb_rest[...])

        rest(0)
        waiting = pending[...]
        for j in range(IN_CH):
            rest(j + 1)
            acc = dot(x_d[pl.ds(base + TILE * j, TILE), 0:PACK], wb_main[0:PACK, :])
            acc = acc + dot(x_d[pl.ds(base + TILE * j + LANES, TILE), 0:PACK], wb_main[PACK:N2048, :])
            acc = acc + dot(x_d[pl.ds(base + TILE * j + TILE, TILE), 0:PACK], wb_main[N2048:N3072, :])
            head(waiting, jnp.maximum(STRIPS * i + 2 * j - 2, 0))
            main = jnp.maximum(acc + bias_row(b_d1b, 0, TILE), 0.0).astype(BF16)
            tail = jnp.maximum(rest_sum(y_rest, TILE * j, TILE) + bias_rest(b_d1b), 0.0).astype(BF16)
            waiting = jnp.concatenate([main, tail[:, 0:REST]], axis=1)
        pending[...] = waiting
        return carry

    lax.fori_loop(0, IN_CH, dec1b, 0)
    head(pending[...], N30)

    pl.semaphore_wait(barrier, STRIPS)
    pushes = []
    for side in range(2):
        tile_row = strip // 2
        pushes.append(
            Push(
                result.at[side],
                out.at[pl.ds(STRIP_ROWS * (strip % 2), STRIP_ROWS)],
                send_sem.at[side],
                recv_sem.at[strip % 2],
                (lax.axis_index("data"), side, tile_row),
                (tile_row == row) & (col == side),
            )
        )
    for push in pushes:
        push.start()
    for push in pushes:
        push.wait_send()
    for half in range(2):
        Push(
            result.at[0], out.at[pl.ds(STRIP_ROWS * half, STRIP_ROWS)], send_sem.at[0], recv_sem.at[half], strip_device(strip), strip < 0
        ).wait_recv()


def solution(mesh):
    tile_spec = P(("data", "row"), "col", None)

    def body(image_tile, *params):
        (w_enc1a, b_enc1a, w_enc1b, b_enc1b, w_enc2a, b_enc2a, w_enc2b, b_enc2b,
         w_mid_a, b_mid_a, w_mid_b, b_mid_b, w_up2, w_dec2a, b_dec2a, w_dec2b, b_dec2b,
         w_up1, w_dec1a, b_dec1a, w_dec1b, b_dec1b, w_head, b_head) = params
        def flat(weight):
            return weight.reshape(-1, weight.shape[-1])

        vmem = pl.BlockSpec(memory_space=pltpu.VMEM)
        hbm = pl.BlockSpec(memory_space=pl.ANY)
        dma = pltpu.SemaphoreType.DMA
        s1, p1 = pl.pallas_call(
            enc1_kernel,
            grid=(3,),
            out_shape=(jax.ShapeDtypeStruct((N4608, BASE_PAD), BF16), jax.ShapeDtypeStruct((N1152, N1152), BF16)),
            in_specs=[vmem, vmem, vmem, hbm, vmem],
            out_specs=(pl.BlockSpec((N1536, BASE_PAD), lambda i: (i, 0)), pl.BlockSpec((BASE_PAD, N1152), lambda i: (i, 0))),
            scratch_shapes=[
                pltpu.VMEM((2, N40, IN_CH, REST), BF16),
                pltpu.VMEM((N42, STRIP_ROWS, LANES), BF16),
                pltpu.VMEM((N96, BASE_PAD), BF16),
                pltpu.VMEM((N2880, BASE), BF16),
                pltpu.VMEM((N5120, N1152), BF16),
                pltpu.VMEM((N1792, TILE), F32),
                pltpu.VMEM((N3072, TILE), BF16),
                pltpu.VMEM((PACK, TILE), BF16),
                pltpu.VMEM((2, LANES, LANES), F32),
                pltpu.VMEM((2, 3, N288, LANES), F32),
                pltpu.VMEM((2, 3, N80, LANES), F32),
                dma, dma((IN_CH,)), dma((2, 2)),
            ],
            compiler_params=pltpu.CompilerParams(
                vmem_limit_bytes=VMEM_LIMIT, collective_id=1, has_side_effects=True, dimension_semantics=("arbitrary",)
            ),
            name="enc1",
        )(image_tile.transpose(0, 2, 1), w_enc1a, b_enc1a, flat(w_enc1b), b_enc1b)

        d2 = pl.pallas_call(
            mid_kernel,
            out_shape=jax.ShapeDtypeStruct((N1152, MIDDLE), BF16),
            in_specs=[hbm] * STRIPS + [vmem] * SIX,
            out_specs=hbm,
            scratch_shapes=[
                pltpu.VMEM((N1152, N1152), BF16),
                pltpu.VMEM((N3072, MIDDLE), BF16),
                pltpu.VMEM((RING_ROWS, DEEP), BF16),
                pltpu.VMEM((N1152, MIDDLE3), BF16),
                pltpu.VMEM((N1152, MIDDLE3), BF16),
                pltpu.VMEM((N1152, MIDDLE3), BF16),
                pltpu.VMEM((BASE, MIDDLE3), BF16),
                pltpu.VMEM((BASE, N3840), BF16),
                pltpu.VMEM((TILE, DEEP), BF16),
                pltpu.VMEM((N1152, MIDDLE), BF16),
                pltpu.VMEM((TILE, DEEP), F32),
                pltpu.VMEM((FIVE, N512, LANES), F32),
                pltpu.VMEM((LANES, LANES), F32),
                dma((N18,)), dma((TAPS,)), dma((3,)), dma((TAPS,)), dma((IN_CH,)), dma((TAPS,)), dma((TAPS,)), dma, dma,
                dma((LAST_STRIP, 2)), dma((LAST_STRIP, 2)),
            ],
            compiler_params=pltpu.CompilerParams(
                vmem_limit_bytes=VMEM_LIMIT, collective_id=0, has_side_effects=True
            ),
            name="mid",
        )(
            p1, flat(w_enc2a), flat(w_enc2b), flat(w_mid_a), flat(w_mid_b), flat(w_up2), flat(w_dec2a), flat(w_dec2b),
            b_enc2a, b_enc2b, b_mid_a, b_mid_b, b_dec2a, b_dec2b,
        )

        def turned(weight):
            return weight.transpose(0, 1, 3, 2).reshape(-1, weight.shape[2])

        y = pl.pallas_call(
            dec1_kernel,
            out_shape=jax.ShapeDtypeStruct((REST, IN_CH, REST), F32),
            in_specs=[hbm] * FIVE + [vmem] * 3 + [pl.BlockSpec(memory_space=pltpu.SMEM)],
            out_specs=hbm,
            scratch_shapes=[
                pltpu.VMEM((N4608, N1152), BF16),
                pltpu.VMEM((N4608, N1152), BF16),
                pltpu.VMEM((N4352, N1152), BF16),
                pltpu.VMEM((N4608, TILE), F32),
                pltpu.VMEM((DEEP, MIDDLE), BF16),
                pltpu.VMEM((N2880, MIDDLE), BF16),
                pltpu.VMEM((N2880, BASE), BF16),
                pltpu.VMEM((N2560, TILE), BF16),
                pltpu.VMEM((MIDDLE, TILE), BF16),
                pltpu.VMEM((N6144, TILE), BF16),
                pltpu.VMEM((N2048, TILE), BF16),
                pltpu.VMEM((N3072, TILE), BF16),
                pltpu.VMEM((PACK, TILE), BF16),
                pltpu.VMEM((2, 3, REST_AT, LANES), F32),
                pltpu.VMEM((2, STRIP_ROWS, IN_CH, REST), F32),
                pltpu.VMEM((TILE, BASE), BF16),
                pltpu.VMEM((2, 3, N288, LANES), F32),
                pltpu.VMEM((N4608, BASE_PAD), BF16),
                pltpu.VMEM((N1152, MIDDLE), BF16),
                dma((FIVE,)), dma((2,)), dma((2,)),
            ],
            compiler_params=pltpu.CompilerParams(vmem_limit_bytes=VMEM_LIMIT, collective_id=2, has_side_effects=True),
            name="dec1",
        )(d2, s1, turned(w_up1), turned(w_dec1a), flat(w_dec1b), b_dec1a, b_dec1b, w_head.T, b_head)
        return y.transpose(0, 2, 1)

    def program(image, *params):
        mapped = jax.shard_map(
            body, mesh=mesh, in_specs=(tile_spec,) + (P(),) * len(params), out_specs=tile_spec, check_vma=False
        )
        return mapped(image, *params)

    return program
```

```python
import functools

import jax
import jax.numpy as jnp
from jax import lax
from jax.experimental import pallas as pl
from jax.experimental.pallas import tpu as pltpu
from jax.sharding import PartitionSpec as P

KERNEL = 3
IN_CH = 4
FIVE = 5
SIX = 6
LAST_STRIP = 7
STRIPS = 8
TAPS = 9
N10 = 10
N12 = 12
N16 = 16
N18 = 18
N22 = 22
N28 = 28
N29 = 29
N30 = 30
N31 = 31
STRIP_ROWS = 32
N36 = 36
N40 = 40
N42 = 42
N60 = 60
REST = 64
N80 = 80
N96 = 96
N127 = 127
LANES = 128
N192 = 192
N224 = 224
TILE = 256
N288 = 288
BASE = 320
BASE_PAD = 384
N512 = 512
MIDDLE = 640
REST_AT = 768
N896 = 896
PACK_USED = 960
PACK = 1024
N1152 = 1152
DEEP = 1280
N1536 = 1536
N1792 = 1792
MIDDLE3 = 1920
N2048 = 2048
N2560 = 2560
N2880 = 2880
N3072 = 3072
N3200 = 3200
N3840 = 3840
N4096 = 4096
N4352 = 4352
N4608 = 4608
N5120 = 5120
N6144 = 6144
N6400 = 6400
N8960 = 8960
N10240 = 10240
N11520 = 11520
BF16 = jnp.bfloat16
F32 = jnp.float32
MESH = pl.DeviceIdType.MESH
VMEM_LIMIT = 66_900_000
RING_ROWS = N11520


def strip_index():
    col = lax.axis_index("col")
    row = lax.axis_index("row")
    return row + col * (LAST_STRIP - 2 * row)


def strip_device(position):
    col = position // IN_CH
    rest = position % IN_CH
    return (lax.axis_index("data"), col, rest + col * (KERNEL - 2 * rest))


def dot(a, b):
    return jnp.dot(a, b, preferred_element_type=F32)


def shifted(value, width, step):
    if step == 1:
        return value
    rows = value.shape[0]
    column = lax.broadcasted_iota(jnp.int32, value.shape, 0) % width
    if step == 0:
        return jnp.where(column == 0, 0.0, pltpu.roll(value, 1, axis=0))
    return jnp.where(column == width - 1, 0.0, pltpu.roll(value, rows - 1, axis=0))


def put3(dst, row0, lane0, channels, value, width):
    rows, lanes = value.shape
    for step in range(KERNEL):
        dst[pl.ds(row0, rows), pl.ds(step * channels + lane0, lanes)] = shifted(value, width, step).astype(BF16)


def put3_320(dst, row0, main, rest, width, stage=None):
    rows = main.shape[0]
    pitch = width + N16
    planes = [main[:, 0:LANES], main[:, LANES:TILE], rest]
    for t, plane in enumerate(planes if stage is not None else []):
        for r in range(rows // width):
            stage[t, pitch * r + STRIPS : pitch * r + STRIPS + width, :] = plane[width * r : width * r + width]

    def moved(t, step):
        if stage is None:
            return shifted(planes[t], width, step)
        first = LAST_STRIP + step
        parts = [stage[t, pitch * r + first : pitch * r + first + width, :] for r in range(rows // width)]
        return jnp.concatenate(parts, axis=0) if len(parts) > 1 else parts[0]

    for step in range(KERNEL):
        for t in range(2):
            dst[pl.ds(row0, rows), pl.ds(step * TILE + LANES * t, LANES)] = moved(t, step).astype(BF16)
    first = moved(2, 0) + pltpu.roll(moved(2, 1), REST, axis=1)
    dst[pl.ds(row0, rows), pl.ds(REST_AT, LANES)] = first.astype(BF16)
    dst[pl.ds(row0, rows), pl.ds(N896, LANES)] = moved(2, 2).astype(BF16)


def low_lanes(value):
    return jnp.where(lax.broadcasted_iota(jnp.int32, value.shape, 1) < REST, value, 0.0)


def pack_weights(staged, main_ref, rest_ref):
    for dj in range(KERNEL):
        for start, size, row in ((0, TILE, TILE * dj), (TILE, REST, REST_AT + REST * dj)):
            parts = []
            for di in range(KERNEL):
                base = (KERNEL * di + dj) * BASE + start
                main_ref[pl.ds(PACK * di + row, size), :] = staged[pl.ds(base, size), 0:TILE]
                parts.append(staged[pl.ds(base, size), TILE:BASE])
            parts.append(jnp.zeros((size, REST), BF16))
            rest_ref[pl.ds(row, size), :] = jnp.concatenate(parts, axis=1)
    clear_pad(main_ref, KERNEL)
    clear_pad(rest_ref, 1)


def clear_pad(ref, groups):
    for group in range(groups):
        ref[pl.ds(PACK * group + PACK_USED, REST), :] = jnp.zeros((REST, ref.shape[1]), BF16)


def turn_main(staged, main_ref, di, dj):
    turned = staged[pl.ds(pl.multiple_of(PACK_USED * di + BASE * dj, REST), TILE), :].T
    for src in range(2):
        base = N3072 * src + PACK * di
        main_ref[pl.ds(pl.multiple_of(base + TILE * dj, REST), TILE), :] = turned[BASE * src : BASE * src + TILE]
        main_ref[pl.ds(pl.multiple_of(base + REST_AT + REST * dj, REST), REST), :] = turned[BASE * src + TILE : BASE * src + BASE]


def turn_rest(staged, main_ref, rest_ref):
    for dj in range(KERNEL):
        parts = [staged[pl.ds(PACK_USED * di + BASE * dj + TILE, REST), :] for di in range(KERNEL)] + [jnp.zeros((REST, MIDDLE), BF16)]
        turned = jnp.concatenate(parts, axis=0).T
        for src in range(2):
            rest_ref[pl.ds(PACK * src + TILE * dj, TILE), :] = turned[BASE * src : BASE * src + TILE]
            rest_ref[pl.ds(PACK * src + REST_AT + REST * dj, REST), :] = turned[BASE * src + TILE : BASE * src + BASE]
    clear_pad(main_ref, SIX)
    clear_pad(rest_ref, 2)


def bias_row(ref, start, size):
    return ref[pl.ds(start, size)].reshape(1, size)


def bias_rest(ref):
    return jnp.concatenate([bias_row(ref, TILE, REST), jnp.zeros((1, REST), F32)], axis=1)


def enter_barrier():
    barrier = pltpu.get_barrier_semaphore()
    for position in range(STRIPS):
        pl.semaphore_signal(barrier, inc=1, device_id=strip_device(position), device_id_type=MESH)
    return barrier


class Push:
    def __init__(self, src, dst, send_sem, recv_sem, device, here):
        self.here = here
        self.local = pltpu.make_async_copy(src, dst, recv_sem)
        self.remote = pltpu.make_async_remote_copy(
            src_ref=src, dst_ref=dst, send_sem=send_sem, recv_sem=recv_sem, device_id=device, device_id_type=MESH
        )

    def start(self):
        @pl.when(self.here)
        def _():
            self.local.start()

        @pl.when(jnp.logical_not(self.here))
        def _():
            self.remote.start()

    def wait_send(self):
        @pl.when(jnp.logical_not(self.here))
        def _():
            self.remote.wait_send()

    def wait_recv(self):
        self.remote.wait_recv()


def rest_sum(y_ref, row0, rows):
    total = y_ref[pl.ds(row0, rows), 0:LANES] + y_ref[pl.ds(row0 + TILE, rows), LANES:TILE]
    return total + pltpu.roll(y_ref[pl.ds(row0 + LANES, rows), 0:LANES], REST, axis=1)


def valid_rows(value, first_row, width):
    row = first_row + lax.broadcasted_iota(jnp.int32, value.shape, 0) // width
    return jnp.where((row >= 0) & (row < TILE), value, 0.0)


def pooled(value, width, scratch):
    rows, lanes = value.shape
    tall = jnp.concatenate(
        [jnp.maximum(value[s : s + width], value[s + width : s + 2 * width]) for s in range(0, rows, 2 * width)], axis=0
    )
    halves = []
    for start in range(0, lanes, LANES):
        scratch[0 : rows // 2, :] = tall[:, start : start + LANES]
        halves.append(
            jnp.maximum(scratch[pl.ds(0, rows // IN_CH, stride=2), :], scratch[pl.ds(1, rows // IN_CH, stride=2), :])
        )
    return jnp.concatenate(halves, axis=1) if len(halves) > 1 else halves[0]


def enc1_kernel(
    image, w_a, b_a, w_b, b_b, s1_out, p1_out,
    halves, planes, w_stem, staged, x_a, y_rest, w_main, w_rest, pool_buf, stage, stage_p, w_sem, send_sem, recv_sem,
):
    step = pl.program_id(0)
    strip = strip_index()

    @pl.when(step == 0)
    def _():
        row = lax.axis_index("row")
        col = lax.axis_index("col")
        copy_w = pltpu.make_async_copy(w_b, staged, w_sem)
        copy_w.start()
        barrier = enter_barrier()
        stage[...] = jnp.zeros_like(stage)
        stage_p[...] = jnp.zeros_like(stage_p)

        for di in range(KERNEL):
            taps = []
            for dj in range(KERNEL):
                tap = jnp.concatenate([w_a[di, dj].astype(F32), jnp.zeros((IN_CH, BASE), F32)], axis=0)
                taps.append(jnp.concatenate([tap, jnp.zeros((STRIPS, REST), F32)], axis=1))
            taps.append(jnp.zeros((STRIPS, BASE_PAD), F32))
            w_stem[STRIP_ROWS * di : STRIP_ROWS * di + STRIP_ROWS, :] = jnp.concatenate(taps, axis=0).astype(BF16)
        planes[N40:N42, :, :] = jnp.zeros((2, STRIP_ROWS, LANES), BF16)

        pl.semaphore_wait(barrier, STRIPS)
        pushes = []
        for index, (target, src_row, dst_row, rows) in enumerate(
            ((2 * row, 0, IN_CH, N36), (2 * row + 1, N28, 0, N36), ((2 * row + 2) % STRIPS, N60, 0, IN_CH), ((2 * row + LAST_STRIP) % STRIPS, 0, N36, IN_CH))
        ):
            pushes.append(
                Push(
                    image.at[pl.ds(src_row, rows)],
                    halves.at[col, pl.ds(dst_row, rows)],
                    send_sem.at[index],
                    recv_sem.at[index // 2, col],
                    strip_device(target),
                    target == strip,
                )
            )
        for push in pushes:
            push.start()
        copy_w.wait()
        pack_weights(staged, w_main, w_rest)
        for push in pushes:
            push.wait_send()
        for kind, rows in ((0, N36), (1, IN_CH)):
            for side in range(2):
                Push(
                    image.at[pl.ds(0, rows)], halves.at[side, pl.ds(0, rows)],
                    send_sem.at[0], recv_sem.at[kind, side], strip_device(strip), strip < 0,
                ).wait_recv()

        def expand(i, carry):
            for j in range(STRIPS):
                r = STRIPS * i + j
                both = jnp.concatenate([halves[0, r].astype(F32), halves[1, r].astype(F32)], axis=1)
                image_row = STRIP_ROWS * strip - IN_CH + r
                both = jnp.where((image_row >= 0) & (image_row < TILE), both, 0.0)
                both = jnp.concatenate([both, jnp.zeros((IN_CH, LANES), F32)], axis=0)
                column = lax.broadcasted_iota(jnp.int32, (STRIPS, LANES), 1)
                before = jnp.where(column == 0, 0.0, pltpu.roll(both, 1, axis=1))
                after = jnp.where(column == N127, 0.0, pltpu.roll(both, N127, axis=1))
                planes[r] = jnp.concatenate([before, both, after, jnp.zeros((STRIPS, LANES), F32)], axis=0).astype(BF16)
            return carry

        lax.fori_loop(0, FIVE, expand, 0)

        def stem(i, carry):
            for j in range(STRIPS):
                r = STRIPS * i + j
                patch = jnp.concatenate([planes[r + di] for di in range(KERNEL)], axis=0)
                acc = lax.dot_general(patch, w_stem[...], (((0,), (0,)), ((), ())), preferred_element_type=F32)
                image_row = STRIP_ROWS * strip - KERNEL + r
                inside = (image_row >= 0) & (image_row < TILE)
                main = jnp.where(inside, jnp.maximum(acc[:, 0:TILE] + bias_row(b_a, 0, TILE), 0.0), 0.0)
                tail = jnp.where(inside, jnp.maximum(acc[:, TILE:BASE_PAD] + bias_rest(b_a), 0.0), 0.0)
                put3_320(x_a, pl.multiple_of(r * LANES, LANES), main, tail, LANES, stage.at[j % 2])
            return carry

        lax.fori_loop(0, FIVE, stem, 0)

    base = pl.multiple_of(step * N1536, N512)

    def rest(j):
        y_rest[TILE * j : TILE * j + TILE, :] = dot(x_a[pl.ds(base + TILE * j, TILE), 0:PACK], w_rest[...])

    rest(0)
    for j in range(SIX):
        rest(j + 1)
        acc = dot(x_a[pl.ds(base + TILE * j, TILE), 0:PACK], w_main[0:PACK, :])
        acc = acc + dot(x_a[pl.ds(base + TILE * j + LANES, TILE), 0:PACK], w_main[PACK:N2048, :])
        acc = acc + dot(x_a[pl.ds(base + TILE * j + TILE, TILE), 0:PACK], w_main[N2048:N3072, :])
        first_row = STRIP_ROWS * strip - 2 + N12 * step + 2 * j
        main = valid_rows(jnp.maximum(acc + bias_row(b_b, 0, TILE), 0.0), first_row, LANES)
        tail = jnp.maximum(rest_sum(y_rest, TILE * j, TILE) + bias_rest(b_b), 0.0)
        tail = low_lanes(valid_rows(tail, first_row, LANES))
        s1_out[TILE * j : TILE * j + TILE, 0:TILE] = main.astype(BF16)
        s1_out[TILE * j : TILE * j + TILE, TILE:BASE_PAD] = tail.astype(BF16)
        put3_320(p1_out, REST * j, pooled(main, LANES, pool_buf.at[j % 2]), pooled(tail, LANES, pool_buf.at[j % 2]), REST, stage_p.at[j % 2])


def mid_kernel(
    p1_hbm, w_2a, w_2b, w_ma, w_mb, w_u2, w_d2a, w_d2b, b_2a, b_2b, b_ma, b_mb, b_d2a, b_d2b, out,
    p1, first_w, ring, x_a, x_s, x_u, m_1, m_2, m_o, d_2, acc_ref, wide, pool_buf,
    sem_2a, sem_2b, sem_ma, sem_mb, sem_u2, sem_d2a, sem_d2b, sem_p1, sem_out, send_sem, recv_sem,
):
    strip = strip_index()
    prev_dev = strip_device((strip + LAST_STRIP) % STRIPS)
    next_dev = strip_device((strip + 1) % STRIPS)

    def exchange(buf, width, lane0, lanes, rows, index, target=None):
        target = buf if target is None else target
        lane = pl.ds(lane0, lanes)
        copies = []
        for side, src_row, dst_row, device in ((0, 1, rows + 1, prev_dev), (1, rows, 0, next_dev)):
            copies.append(
                pltpu.make_async_remote_copy(
                    src_ref=buf.at[pl.ds(src_row * width, width), lane],
                    dst_ref=target.at[pl.ds(dst_row * width, width), lane],
                    send_sem=send_sem.at[index, side],
                    recv_sem=recv_sem.at[index, side],
                    device_id=device,
                    device_id_type=MESH,
                )
            )
        return copies

    def start(copies):
        for copy in copies:
            copy.start()

    def finish(copies):
        for copy in copies:
            copy.wait()

    def halo(buf, width, channels, rows):
        for row, inside in ((0, strip > 0), (rows + 1, strip < LAST_STRIP)):
            value = buf[pl.ds(row * width, width), pl.ds(channels, channels)].astype(F32)
            put3(buf, row * width, 0, channels, jnp.where(inside, value, 0.0), width)

    copies_2a = []
    for tap in range(TAPS):
        di, dj = tap // KERNEL, tap % KERNEL
        for part, (start_row, size, row) in enumerate(((0, TILE, TILE * dj), (TILE, REST, REST_AT + REST * dj))):
            copies_2a.append(
                pltpu.make_async_copy(
                    w_2a.at[pl.ds(BASE * tap + start_row, size), :],
                    first_w.at[pl.ds(PACK * di + row, size), :],
                    sem_2a.at[2 * tap + part],
                )
            )

    def tap_copies(src, rows, base, sem):
        return [
            pltpu.make_async_copy(
                src.at[pl.ds(rows * tap, rows), :],
                ring.at[pl.ds(base + rows * (tap // 2), rows), pl.ds(MIDDLE * (tap % 2), MIDDLE)],
                sem.at[tap],
            )
            for tap in range(src.shape[0] // rows)
        ]

    copies_2b = tap_copies(w_2b, MIDDLE, 0, sem_2b)
    copies_ma = [
        pltpu.make_async_copy(w_ma.at[pl.ds(MIDDLE3 * di, MIDDLE3), :], ring.at[pl.ds(N3200 + MIDDLE3 * t, MIDDLE3), :], sem_ma.at[t])
        for t, di in enumerate((1, 0, 2))
    ]

    def mb_row(k):
        return (N8960 + DEEP * k) % RING_ROWS

    copies_mb = [
        pltpu.make_async_copy(
            w_mb.at[pl.ds(DEEP * (KERNEL * (1, 0, 2)[k // KERNEL] + k % KERNEL), DEEP), :], ring.at[pl.ds(mb_row(k), DEEP), :], sem_mb.at[k]
        )
        for k in range(TAPS)
    ]
    copies_u2 = [
        pltpu.make_async_copy(
            w_u2.at[pl.ds(DEEP * tap, DEEP), :],
            first_w.at[pl.ds(DEEP * tap, DEEP), :] if tap < 2 else ring.at[pl.ds(N8960, DEEP), pl.ds(MIDDLE * (tap - 2), MIDDLE)],
            sem_u2.at[tap],
        )
        for tap in range(IN_CH)
    ]
    copies_d2a = tap_copies(w_d2a, DEEP, 0, sem_d2a)
    copies_d2b = tap_copies(w_d2b, MIDDLE, N6400, sem_d2b)

    copy_p1 = pltpu.make_async_copy(p1_hbm, p1, sem_p1)
    copy_p1.start()
    start(copies_2a)

    barrier = pltpu.get_barrier_semaphore()
    for device in (prev_dev, next_dev):
        pl.semaphore_signal(barrier, inc=1, device_id=device, device_id_type=MESH)
    pl.semaphore_wait(barrier, 2)

    for di in range(KERNEL):
        first_w[PACK * di + PACK_USED : PACK * di + PACK, :] = jnp.zeros((REST, MIDDLE), BF16)
    copy_p1.wait()
    finish(copies_2a)
    start(copies_2b)
    start(copies_ma)

    ex_a = exchange(x_a, REST, MIDDLE, MIDDLE, N16, 0)
    ex_s = exchange(x_s, REST, MIDDLE, MIDDLE, N16, 1)
    ex_m1 = exchange(m_1, STRIP_ROWS, MIDDLE, MIDDLE, STRIPS, 2)
    ex_m2 = exchange(m_2, STRIP_ROWS, DEEP, DEEP, STRIPS, KERNEL)
    ex_u = exchange(x_u, REST, MIDDLE, MIDDLE, N16, IN_CH)
    ex_b = exchange(x_a, REST, MIDDLE, MIDDLE, N16, FIVE)
    ex_d = exchange(d_2, REST, 0, MIDDLE, N16, SIX, out)
    tiles = ((0, TILE), (TILE, TILE), (N512, LANES))

    def enc2a(i, carry):
        @pl.when(i == 1)
        def _():
            start(ex_a)

        for block in (i, KERNEL - i):
            row0 = pl.multiple_of(block * TILE, TILE)
            for lane0, lanes in tiles:
                acc = dot(p1[pl.ds(row0, TILE), 0:PACK], first_w[0:PACK, pl.ds(lane0, lanes)])
                for di in (1, 2):
                    acc = acc + dot(
                        p1[pl.ds(row0 + REST * di, TILE), 0:PACK],
                        first_w[PACK * di : PACK * di + PACK, pl.ds(lane0, lanes)],
                    )
                value = jnp.maximum(acc + bias_row(b_2a, lane0, lanes), 0.0)
                put3(x_a, row0 + REST, lane0, MIDDLE, value, REST)
        return carry

    lax.fori_loop(0, 2, enc2a, 0)
    finish(copies_2b)
    start(copies_mb[0:2])
    start(copies_u2[0:2])

    def conv640(src, row0, base, lane0, lanes):
        acc = None
        for di in range(KERNEL):
            weights = jnp.concatenate(
                [
                    ring[base + MIDDLE * (t // 2) : base + MIDDLE * (t // 2) + MIDDLE, pl.ds(MIDDLE * (t % 2) + lane0, lanes)]
                    for t in range(KERNEL * di, KERNEL * di + KERNEL)
                ],
                axis=0,
            )
            part = dot(src[pl.ds(row0 + REST * di, TILE), :], weights)
            acc = part if acc is None else acc + part
        return acc

    def enc2b(i, carry):
        block = i + 1 - 2 * (i % 2)
        row0 = pl.multiple_of(block * TILE, TILE)

        @pl.when(i == 1)
        def _():
            finish(ex_a)
            halo(x_a, REST, MIDDLE, N16)

        @pl.when(i == KERNEL)
        def _():
            start(ex_m1)
            start(ex_s)

        for lane0, lanes in tiles:
            value = jnp.maximum(conv640(x_a, row0, 0, lane0, lanes) + bias_row(b_2b, lane0, lanes), 0.0)
            put3(x_s, row0 + REST, lane0, MIDDLE, value, REST)
            put3(m_1, pl.multiple_of(block * REST + STRIP_ROWS, STRIP_ROWS), lane0, MIDDLE, pooled(value, REST, pool_buf), STRIP_ROWS)
        return carry

    lax.fori_loop(0, IN_CH, enc2b, 0)
    start(copies_mb[2:IN_CH])

    acc_ref[...] = jnp.zeros_like(acc_ref)
    finish(copies_ma)

    def mid_a(t, carry):
        di = (t + 1) % 2 + 2 * (t // 2) - t // 2

        @pl.when(t == 1)
        def _():
            start(copies_mb[IN_CH:SIX])
            finish(ex_m1)
            halo(m_1, STRIP_ROWS, MIDDLE, STRIPS)

        @pl.when(t == 2)
        def _():
            start(copies_mb[SIX:LAST_STRIP])

        base = pl.multiple_of(N3200 + MIDDLE3 * t, LANES)
        lhs_row = pl.multiple_of(STRIP_ROWS * di, STRIP_ROWS)
        for lane0 in range(0, DEEP, TILE):
            acc_ref[:, pl.ds(lane0, TILE)] += dot(
                m_1[pl.ds(lhs_row, TILE), :], ring[pl.ds(base, MIDDLE3), pl.ds(lane0, TILE)]
            )
        return carry

    lax.fori_loop(0, KERNEL, mid_a, 0)
    start(copies_mb[LAST_STRIP:TAPS])

    def mid_a_rows(first, rows):
        for lane0 in range(0, DEEP, TILE):
            value = jnp.maximum(acc_ref[pl.ds(first, rows), pl.ds(lane0, TILE)] + bias_row(b_ma, lane0, TILE), 0.0)
            put3(m_2, STRIP_ROWS + first, lane0, DEEP, value, STRIP_ROWS)

    mid_a_rows(0, STRIP_ROWS)
    mid_a_rows(N224, STRIP_ROWS)
    start(ex_m2)
    mid_a_rows(STRIP_ROWS, N192)
    acc_ref[...] = jnp.zeros_like(acc_ref)

    def mid_b(t, carry):
        di = (t + 1) % 2 + 2 * (t // 2) - t // 2

        for j in range(KERNEL):
            @pl.when(t == j)
            def _(j=j):
                finish(copies_mb[KERNEL * j : KERNEL * j + KERNEL])

        @pl.when(t == 1)
        def _():
            start(copies_u2[2:IN_CH])
            start(copies_d2a[0:2])
            finish(ex_m2)
            halo(m_2, STRIP_ROWS, DEEP, STRIPS)

        @pl.when(t == 2)
        def _():
            start(copies_d2a[2:STRIPS])

        lhs_row = pl.multiple_of(STRIP_ROWS * di, STRIP_ROWS)
        for lane0 in range(0, DEEP, TILE):
            acc = None
            for dj in range(KERNEL):
                base = pl.multiple_of(mb_row(KERNEL * t + dj), LANES)
                part = dot(
                    m_2[pl.ds(lhs_row, TILE), DEEP * dj : DEEP * dj + DEEP], ring[pl.ds(base, DEEP), pl.ds(lane0, TILE)]
                )
                acc = part if acc is None else acc + part
            acc_ref[:, pl.ds(lane0, TILE)] += acc
        return carry

    lax.fori_loop(0, KERNEL, mid_b, 0)
    start(copies_d2a[STRIPS:TAPS])
    for lane0 in range(0, DEEP, TILE):
        value = jnp.maximum(acc_ref[:, pl.ds(lane0, TILE)] + bias_row(b_mb, lane0, TILE), 0.0)
        m_o[:, pl.ds(lane0, TILE)] = value.astype(BF16)

    finish(copies_u2)
    for p in range(2):
        for q in range(2):
            for lane0, lanes in tiles:
                if p == 0:
                    weights = first_w[DEEP * q : DEEP * q + DEEP, pl.ds(lane0, lanes)]
                else:
                    weights = ring[N8960:N10240, pl.ds(MIDDLE * q + lane0, lanes)]
                part = dot(m_o[...], weights)
                for lane in range(0, lanes, LANES):
                    wide[(lane0 + lane) // LANES, pl.ds(q, TILE, stride=2), :] = part[:, lane : lane + LANES]

        def place(i, carry):
            src = pl.multiple_of(REST * i, REST)
            dst = pl.multiple_of(REST * (1 + 2 * i + p), REST)
            for lane0 in range(0, MIDDLE, LANES):
                put3(x_u, dst, lane0, MIDDLE, wide[lane0 // LANES, pl.ds(src, REST), :], REST)
            return carry

        lax.fori_loop(0, STRIPS, place, 0)
    start(ex_u)
    start(copies_d2b)
    finish(ex_s)
    halo(x_s, REST, MIDDLE, N16)
    finish(copies_d2a)

    def dec2a(i, carry):
        block = i + 1 - 2 * (i % 2)
        row0 = pl.multiple_of(block * TILE, TILE)

        @pl.when(i == 1)
        def _():
            finish(ex_u)
            halo(x_u, REST, MIDDLE, N16)

        @pl.when(i == KERNEL)
        def _():
            start(ex_b)

        for lane0, lanes in tiles:
            acc = None
            for tap in range(TAPS):
                rows = pl.ds(row0 + REST * (tap // KERNEL), TILE)
                cols = pl.ds(MIDDLE * (tap % KERNEL), MIDDLE)
                lhs = jnp.concatenate([x_u[rows, cols], x_s[rows, cols]], axis=1)
                base = DEEP * (tap // 2)
                part = dot(lhs, ring[base : base + DEEP, pl.ds(MIDDLE * (tap % 2) + lane0, lanes)])
                acc = part if acc is None else acc + part
            value = jnp.maximum(acc + bias_row(b_d2a, lane0, lanes), 0.0)
            put3(x_a, row0 + REST, lane0, MIDDLE, value, REST)
        return carry

    lax.fori_loop(0, IN_CH, dec2a, 0)
    finish(copies_d2b)

    def dec2b(i, carry):
        block = i + 1 - 2 * (i % 2)
        row0 = pl.multiple_of(block * TILE, TILE)

        @pl.when(i == 1)
        def _():
            finish(ex_b)
            halo(x_a, REST, MIDDLE, N16)

        @pl.when(i == KERNEL)
        def _():
            start(ex_d)

        for lane0, lanes in tiles:
            value = jnp.maximum(conv640(x_a, row0, N6400, lane0, lanes) + bias_row(b_d2b, lane0, lanes), 0.0)
            d_2[pl.ds(row0 + REST, TILE), pl.ds(lane0, lanes)] = value.astype(BF16)
        return carry

    lax.fori_loop(0, IN_CH, dec2b, 0)
    result = pltpu.make_async_copy(d_2.at[pl.ds(REST, PACK), :], out.at[pl.ds(REST, PACK), :], sem_out)
    result.start()
    finish(ex_d)
    result.wait()


def dec1_kernel(
    d_2, s1, w_u1, w_d1a, w_d1b, b_d1a, b_d1b, w_head, b_head, out,
    x_u, x_s, x_d, y_rest, st_u, st_a, st_b, wu_main, wu_rest, wa_main, wa_rest, wb_main, wb_rest, wide, result, pending, stage, skip, low, late,
    sem, send_sem, recv_sem,
):
    strip = strip_index()
    row = lax.axis_index("row")
    col = lax.axis_index("col")
    copy_u = pltpu.make_async_copy(w_u1, st_u, sem.at[0])
    copy_a = pltpu.make_async_copy(w_d1a, st_a, sem.at[1])
    copy_s = pltpu.make_async_copy(s1, skip, sem.at[2])
    copy_b = pltpu.make_async_copy(w_d1b, st_b, sem.at[KERNEL])
    copy_d = pltpu.make_async_copy(d_2, low, sem.at[IN_CH])
    copy_u.start()
    copy_d.start()
    barrier = enter_barrier()

    stage[...] = jnp.zeros_like(stage)
    copy_u.wait()
    copy_a.start()
    copy_s.start()
    copy_b.start()
    for tap in range(IN_CH):
        wu_main[MIDDLE * tap : MIDDLE * tap + MIDDLE, :] = st_u[BASE * tap : BASE * tap + TILE, :].T
    wu_rest[...] = jnp.concatenate([st_u[BASE * tap + TILE : BASE * tap + BASE, :] for tap in range(IN_CH)], axis=0).T
    copy_d.wait()

    def up1(i, carry):
        row0 = pl.multiple_of(i * BASE_PAD, LANES)
        lhs = low[pl.ds(row0, BASE_PAD), :]
        rest = dot(lhs, wu_rest[...])
        for p in range(2):
            part = rest[:, LANES * p : LANES * p + LANES]
            buf = wide.at[p]
            buf[2, pl.ds(0, BASE_PAD, stride=2), :] = low_lanes(part)
            buf[2, pl.ds(1, BASE_PAD, stride=2), :] = low_lanes(pltpu.roll(part, REST, axis=1))
            for q in range(2):
                tap = 2 * p + q
                main = dot(lhs, wu_main[MIDDLE * tap : MIDDLE * tap + MIDDLE, :])
                buf[0, pl.ds(q, BASE_PAD, stride=2), :] = main[:, 0:LANES]
                buf[1, pl.ds(q, BASE_PAD, stride=2), :] = main[:, LANES:TILE]
            for r in range(SIX):
                main = jnp.concatenate([buf[0, LANES * r : LANES * r + LANES, :], buf[1, LANES * r : LANES * r + LANES, :]], axis=1)
                put3_320(
                    x_u, pl.multiple_of((N12 * i + 2 * r + p) * LANES, LANES), main, buf[2, LANES * r : LANES * r + LANES, :], LANES
                )
        return carry

    lax.fori_loop(0, KERNEL, up1, 0)

    @pl.when(strip == 0)
    def _():
        x_u[0:TILE, :] = jnp.zeros((TILE, N1152), BF16)

    @pl.when(strip == LAST_STRIP)
    def _():
        x_u[N4352:N4608, :] = jnp.zeros((TILE, N1152), BF16)

    copy_a.wait()
    turn_rest(st_a, wa_main, wa_rest)
    copy_s.wait()

    def rest_a(i, carry):
        base = pl.multiple_of(i * N1536, N512)

        def spread(j):
            rows = pl.ds(base + TILE * j, TILE)
            put3_320(
                x_s, base + TILE * j, skip[rows, 0:TILE].astype(F32), skip[rows, TILE:BASE_PAD].astype(F32), LANES, stage.at[j % 2]
            )

        spread(0)
        for j in range(SIX):
            rows = pl.ds(base + TILE * j, TILE)
            y_rest[rows, :] = dot(x_u[rows, 0:PACK], wa_rest[0:PACK, :]) + dot(
                x_s[rows, 0:PACK], wa_rest[PACK:N2048, :]
            )
            if j < FIVE:
                spread(j + 1)
            if j < KERNEL:
                turn_main(st_a, wa_main, i, j)
        return carry

    lax.fori_loop(0, KERNEL, rest_a, 0)

    def conv_a(row0):
        acc = None
        for di in range(KERNEL):
            rows = pl.ds(row0 + LANES * di, TILE)
            for src, ref in enumerate((x_u, x_s)):
                base = N3072 * src + PACK * di
                part = dot(ref[rows, 0:PACK], wa_main[base : base + PACK, :])
                acc = part if acc is None else acc + part
        return acc

    def put_a(acc, row0, first_row, slot):
        main = valid_rows(jnp.maximum(acc + bias_row(b_d1a, 0, TILE), 0.0), first_row, LANES)
        tail = valid_rows(jnp.maximum(rest_sum(y_rest, row0, TILE) + bias_rest(b_d1a), 0.0), first_row, LANES)
        put3_320(x_d, row0, main, low_lanes(tail), LANES, stage.at[slot])

    late[...] = jnp.zeros_like(late)

    def dec1a(i, carry):
        base = pl.multiple_of(i * PACK, PACK)
        put_a(late[...], pl.multiple_of(jnp.maximum(base - TILE, 0), TILE), STRIP_ROWS * strip - KERNEL + STRIPS * i, 1)
        for j in range(IN_CH):
            acc = conv_a(base + TILE * j)
            if j == KERNEL:
                late[...] = acc
            else:
                put_a(acc, base + TILE * j, STRIP_ROWS * strip - 1 + STRIPS * i + 2 * j, j % 2)
        return carry

    lax.fori_loop(0, IN_CH, dec1a, 0)
    put_a(late[...], N3840, STRIP_ROWS * strip + N29, 1)
    put_a(conv_a(N4096), N4096, STRIP_ROWS * strip + N31, 0)

    copy_b.wait()
    pack_weights(st_b, wb_main, wb_rest)
    head_bias = jnp.zeros((IN_CH, LANES), F32)
    for channel in range(IN_CH):
        head_bias = jnp.where(lax.broadcasted_iota(jnp.int32, (IN_CH, LANES), 0) == channel, b_head[channel], head_bias)

    pending[...] = jnp.zeros_like(pending)

    def head(hidden, row0):
        line = lax.dot_general(w_head[...], hidden, (((1,), (1,)), ((), ())), preferred_element_type=F32)
        for r in range(2):
            part = line[:, LANES * r : LANES * r + LANES] + head_bias
            result[0, row0 + r] = part[:, 0:REST]
            result[1, row0 + r] = part[:, REST:LANES]

    def dec1b(i, carry):
        base = pl.multiple_of(i * PACK, PACK)

        def rest(j):
            y_rest[TILE * j : TILE * j + TILE, :] = dot(x_d[pl.ds(base + TILE * j, TILE), 0:PACK], wb_rest[...])

        rest(0)
        waiting = pending[...]
        for j in range(IN_CH):
            rest(j + 1)
            acc = dot(x_d[pl.ds(base + TILE * j, TILE), 0:PACK], wb_main[0:PACK, :])
            acc = acc + dot(x_d[pl.ds(base + TILE * j + LANES, TILE), 0:PACK], wb_main[PACK:N2048, :])
            acc = acc + dot(x_d[pl.ds(base + TILE * j + TILE, TILE), 0:PACK], wb_main[N2048:N3072, :])
            head(waiting, jnp.maximum(STRIPS * i + 2 * j - 2, 0))
            main = jnp.maximum(acc + bias_row(b_d1b, 0, TILE), 0.0).astype(BF16)
            tail = jnp.maximum(rest_sum(y_rest, TILE * j, TILE) + bias_rest(b_d1b), 0.0).astype(BF16)
            waiting = jnp.concatenate([main, tail[:, 0:REST]], axis=1)
        pending[...] = waiting
        return carry

    pushes = []
    for part, first, rows in ((0, 0, N22), (1, N22, N10)):
        for side in range(2):
            pushes.append(
                Push(
                    result.at[side, pl.ds(first, rows)],
                    out.at[pl.ds(STRIP_ROWS * (strip % 2) + first, rows)],
                    send_sem.at[part, side],
                    recv_sem.at[part, strip % 2],
                    (lax.axis_index("data"), side, strip // 2),
                    (strip // 2 == row) & (col == side),
                )
            )

    lax.fori_loop(0, KERNEL, dec1b, 0)
    pl.semaphore_wait(barrier, STRIPS)
    for push in pushes[0:2]:
        push.start()
    lax.fori_loop(KERNEL, IN_CH, dec1b, 0)
    head(pending[...], N30)

    for push in pushes[2:IN_CH]:
        push.start()
    for push in pushes:
        push.wait_send()
    for part, first, rows in ((0, 0, N22), (1, N22, N10)):
        for half in range(2):
            Push(
                result.at[0, pl.ds(first, rows)], out.at[pl.ds(STRIP_ROWS * half + first, rows)],
                send_sem.at[part, 0], recv_sem.at[part, half], strip_device(strip), strip < 0,
            ).wait_recv()


def solution(mesh):
    tile_spec = P(("data", "row"), "col", None)

    def body(image_tile, *params):
        (w_enc1a, b_enc1a, w_enc1b, b_enc1b, w_enc2a, b_enc2a, w_enc2b, b_enc2b,
         w_mid_a, b_mid_a, w_mid_b, b_mid_b, w_up2, w_dec2a, b_dec2a, w_dec2b, b_dec2b,
         w_up1, w_dec1a, b_dec1a, w_dec1b, b_dec1b, w_head, b_head) = params
        def flat(weight):
            return weight.reshape(-1, weight.shape[-1])

        vmem = pl.BlockSpec(memory_space=pltpu.VMEM)
        hbm = pl.BlockSpec(memory_space=pl.ANY)
        dma = pltpu.SemaphoreType.DMA
        s1, p1 = pl.pallas_call(
            enc1_kernel,
            grid=(KERNEL,),
            out_shape=(jax.ShapeDtypeStruct((N4608, BASE_PAD), BF16), jax.ShapeDtypeStruct((N1152, N1152), BF16)),
            in_specs=[vmem, vmem, vmem, hbm, vmem],
            out_specs=(pl.BlockSpec((N1536, BASE_PAD), lambda i: (i, 0)), pl.BlockSpec((BASE_PAD, N1152), lambda i: (i, 0))),
            scratch_shapes=[
                pltpu.VMEM((2, N40, IN_CH, REST), BF16),
                pltpu.VMEM((N42, STRIP_ROWS, LANES), BF16),
                pltpu.VMEM((N96, BASE_PAD), BF16),
                pltpu.VMEM((N2880, BASE), BF16),
                pltpu.VMEM((N5120, N1152), BF16),
                pltpu.VMEM((N1792, TILE), F32),
                pltpu.VMEM((N3072, TILE), BF16),
                pltpu.VMEM((PACK, TILE), BF16),
                pltpu.VMEM((2, LANES, LANES), F32),
                pltpu.VMEM((2, KERNEL, N288, LANES), F32),
                pltpu.VMEM((2, KERNEL, N80, LANES), F32),
                dma, dma((IN_CH,)), dma((2, 2)),
            ],
            compiler_params=pltpu.CompilerParams(
                vmem_limit_bytes=VMEM_LIMIT, collective_id=1, has_side_effects=True, dimension_semantics=("arbitrary",)
            ),
            name="enc1",
        )(image_tile.transpose(0, 2, 1), w_enc1a, b_enc1a, flat(w_enc1b), b_enc1b)

        d2 = pl.pallas_call(
            mid_kernel,
            out_shape=jax.ShapeDtypeStruct((N1152, MIDDLE), BF16),
            in_specs=[hbm] * STRIPS + [vmem] * SIX,
            out_specs=hbm,
            scratch_shapes=[
                pltpu.VMEM((N1152, N1152), BF16),
                pltpu.VMEM((N3072, MIDDLE), BF16),
                pltpu.VMEM((RING_ROWS, DEEP), BF16),
                pltpu.VMEM((N1152, MIDDLE3), BF16),
                pltpu.VMEM((N1152, MIDDLE3), BF16),
                pltpu.VMEM((N1152, MIDDLE3), BF16),
                pltpu.VMEM((BASE, MIDDLE3), BF16),
                pltpu.VMEM((BASE, N3840), BF16),
                pltpu.VMEM((TILE, DEEP), BF16),
                pltpu.VMEM((N1152, MIDDLE), BF16),
                pltpu.VMEM((TILE, DEEP), F32),
                pltpu.VMEM((FIVE, N512, LANES), F32),
                pltpu.VMEM((LANES, LANES), F32),
                dma((N18,)), dma((TAPS,)), dma((KERNEL,)), dma((TAPS,)), dma((IN_CH,)), dma((TAPS,)), dma((TAPS,)), dma, dma,
                dma((LAST_STRIP, 2)), dma((LAST_STRIP, 2)),
            ],
            compiler_params=pltpu.CompilerParams(
                vmem_limit_bytes=VMEM_LIMIT, collective_id=0, has_side_effects=True
            ),
            name="mid",
        )(
            p1, flat(w_enc2a), flat(w_enc2b), flat(w_mid_a), flat(w_mid_b), flat(w_up2), flat(w_dec2a), flat(w_dec2b),
            b_enc2a, b_enc2b, b_mid_a, b_mid_b, b_dec2a, b_dec2b,
        )

        def turned(weight):
            return weight.transpose(0, 1, KERNEL, 2).reshape(-1, weight.shape[2])

        y = pl.pallas_call(
            dec1_kernel,
            out_shape=jax.ShapeDtypeStruct((REST, IN_CH, REST), F32),
            in_specs=[hbm] * FIVE + [vmem] * KERNEL + [pl.BlockSpec(memory_space=pltpu.SMEM)],
            out_specs=hbm,
            scratch_shapes=[
                pltpu.VMEM((N4608, N1152), BF16),
                pltpu.VMEM((N4608, N1152), BF16),
                pltpu.VMEM((N4352, N1152), BF16),
                pltpu.VMEM((N4608, TILE), F32),
                pltpu.VMEM((DEEP, MIDDLE), BF16),
                pltpu.VMEM((N2880, MIDDLE), BF16),
                pltpu.VMEM((N2880, BASE), BF16),
                pltpu.VMEM((N2560, TILE), BF16),
                pltpu.VMEM((MIDDLE, TILE), BF16),
                pltpu.VMEM((N6144, TILE), BF16),
                pltpu.VMEM((N2048, TILE), BF16),
                pltpu.VMEM((N3072, TILE), BF16),
                pltpu.VMEM((PACK, TILE), BF16),
                pltpu.VMEM((2, KERNEL, REST_AT, LANES), F32),
                pltpu.VMEM((2, STRIP_ROWS, IN_CH, REST), F32),
                pltpu.VMEM((TILE, BASE), BF16),
                pltpu.VMEM((2, KERNEL, N288, LANES), F32),
                pltpu.VMEM((N4608, BASE_PAD), BF16),
                pltpu.VMEM((N1152, MIDDLE), BF16),
                pltpu.VMEM((TILE, TILE), F32),
                dma((FIVE,)), dma((2, 2)), dma((2, 2)),
            ],
            compiler_params=pltpu.CompilerParams(vmem_limit_bytes=VMEM_LIMIT, collective_id=2, has_side_effects=True),
            name="dec1",
        )(d2, s1, turned(w_up1), turned(w_dec1a), flat(w_dec1b), b_dec1a, b_dec1b, w_head.T, b_head)
        return y.transpose(0, 2, 1)

    def program(image, *params):
        mapped = jax.shard_map(
            body, mesh=mesh, in_specs=(tile_spec,) + (P(),) * len(params), out_specs=tile_spec, check_vma=False
        )
        return mapped(image, *params)

    return program
```

```python
import functools

import jax
import jax.numpy as jnp
from jax import lax
from jax.experimental import pallas as pl
from jax.experimental.pallas import tpu as pltpu
from jax.sharding import PartitionSpec as P

KERNEL = 3
IN_CH = 4
FIVE = 5
SIX = 6
LAST_STRIP = 7
STRIPS = 8
TAPS = 9
N10 = 10
N12 = 12
N14 = 14
N16 = 16
N18 = 18
N22 = 22
N28 = 28
N29 = 29
N30 = 30
N31 = 31
STRIP_ROWS = 32
N36 = 36
N40 = 40
N42 = 42
N60 = 60
REST = 64
N80 = 80
N96 = 96
N127 = 127
LANES = 128
N192 = 192
N224 = 224
TILE = 256
N288 = 288
BASE = 320
BASE_PAD = 384
N512 = 512
MIDDLE = 640
REST_AT = 768
PACK_USED = 960
PACK = 1024
N1152 = 1152
N1168 = 1168
DEEP = 1280
N1536 = 1536
N1792 = 1792
MIDDLE3 = 1920
N2048 = 2048
N2560 = 2560
N2880 = 2880
N3072 = 3072
N3200 = 3200
N3840 = 3840
N4096 = 4096
N4352 = 4352
N4368 = 4368
N4608 = 4608
N4624 = 4624
N5136 = 5136
N6144 = 6144
N6400 = 6400
N8960 = 8960
N10240 = 10240
N11520 = 11520
BF16 = jnp.bfloat16
F32 = jnp.float32
MESH = pl.DeviceIdType.MESH
VMEM_LIMIT = 66_900_000
RING_ROWS = N11520


def strip_index():
    col = lax.axis_index("col")
    row = lax.axis_index("row")
    return row + col * (LAST_STRIP - 2 * row)


def strip_device(position):
    col = position // IN_CH
    rest = position % IN_CH
    return (lax.axis_index("data"), col, rest + col * (KERNEL - 2 * rest))


def dot(a, b):
    return jnp.dot(a, b, preferred_element_type=F32)


def shifted(value, width, step):
    if step == 1:
        return value
    rows = value.shape[0]
    column = lax.broadcasted_iota(jnp.int32, value.shape, 0) % width
    if step == 0:
        return jnp.where(column == 0, 0.0, pltpu.roll(value, 1, axis=0))
    return jnp.where(column == width - 1, 0.0, pltpu.roll(value, rows - 1, axis=0))


def put3(dst, row0, lane0, channels, value, width):
    rows, lanes = value.shape
    for step in range(KERNEL):
        dst[pl.ds(row0, rows), pl.ds(step * channels + lane0, lanes)] = shifted(value, width, step).astype(BF16)


def put3_320(dst, row0, main, rest, width, stage=None):
    rows = main.shape[0]
    pitch = width + N16
    planes = [main[:, 0:LANES], main[:, LANES:TILE], rest]
    for t, plane in enumerate(planes if stage is not None else []):
        for r in range(rows // width):
            stage[t, pitch * r + STRIPS : pitch * r + STRIPS + width, :] = plane[width * r : width * r + width]

    def moved(t, step):
        if stage is None:
            return shifted(planes[t], width, step)
        first = LAST_STRIP + step
        parts = [stage[t, pitch * r + first : pitch * r + first + width, :] for r in range(rows // width)]
        return jnp.concatenate(parts, axis=0) if len(parts) > 1 else parts[0]

    for step in range(KERNEL):
        for t in range(2):
            dst[2 * step + t, pl.ds(row0, rows), :] = moved(t, step).astype(BF16)
    first = moved(2, 0) + pltpu.roll(moved(2, 1), REST, axis=1)
    dst[SIX, pl.ds(row0, rows), :] = first.astype(BF16)
    dst[LAST_STRIP, pl.ds(row0, rows), :] = moved(2, 2).astype(BF16)


def packed_rows(ref, row0, rows):
    return jnp.concatenate([ref[t, pl.ds(row0, rows), :] for t in range(STRIPS)], axis=1)


def low_lanes(value):
    return jnp.where(lax.broadcasted_iota(jnp.int32, value.shape, 1) < REST, value, 0.0)


def pack_weights(staged, main_ref, rest_ref):
    for dj in range(KERNEL):
        for start, size, row in ((0, TILE, TILE * dj), (TILE, REST, REST_AT + REST * dj)):
            parts = []
            for di in range(KERNEL):
                base = (KERNEL * di + dj) * BASE + start
                main_ref[pl.ds(PACK * di + row, size), :] = staged[pl.ds(base, size), 0:TILE]
                parts.append(staged[pl.ds(base, size), TILE:BASE])
            parts.append(jnp.zeros((size, REST), BF16))
            rest_ref[pl.ds(row, size), :] = jnp.concatenate(parts, axis=1)
    clear_pad(main_ref, KERNEL)
    clear_pad(rest_ref, 1)


def clear_pad(ref, groups):
    for group in range(groups):
        ref[pl.ds(PACK * group + PACK_USED, REST), :] = jnp.zeros((REST, ref.shape[1]), BF16)


def turn_main(staged, main_ref, di, dj):
    turned = staged[pl.ds(pl.multiple_of(PACK_USED * di + BASE * dj, REST), TILE), :].T
    for src in range(2):
        base = N3072 * src + PACK * di
        main_ref[pl.ds(pl.multiple_of(base + TILE * dj, REST), TILE), :] = turned[BASE * src : BASE * src + TILE]
        main_ref[pl.ds(pl.multiple_of(base + REST_AT + REST * dj, REST), REST), :] = turned[BASE * src + TILE : BASE * src + BASE]


def turn_rest(staged, main_ref, rest_ref):
    for dj in range(KERNEL):
        parts = [staged[pl.ds(PACK_USED * di + BASE * dj + TILE, REST), :] for di in range(KERNEL)] + [jnp.zeros((REST, MIDDLE), BF16)]
        turned = jnp.concatenate(parts, axis=0).T
        for src in range(2):
            rest_ref[pl.ds(PACK * src + TILE * dj, TILE), :] = turned[BASE * src : BASE * src + TILE]
            rest_ref[pl.ds(PACK * src + REST_AT + REST * dj, REST), :] = turned[BASE * src + TILE : BASE * src + BASE]
    clear_pad(main_ref, SIX)
    clear_pad(rest_ref, 2)


def bias_row(ref, start, size):
    return ref[pl.ds(start, size)].reshape(1, size)


def bias_rest(ref):
    return jnp.concatenate([bias_row(ref, TILE, REST), jnp.zeros((1, REST), F32)], axis=1)


def enter_barrier():
    barrier = pltpu.get_barrier_semaphore()
    for position in range(STRIPS):
        pl.semaphore_signal(barrier, inc=1, device_id=strip_device(position), device_id_type=MESH)
    return barrier


def fetch(sources, targets, sems):
    copies = [pltpu.make_async_copy(src, dst, sems.at[i]) for i, (src, dst) in enumerate(zip(sources, targets))]
    for copy in copies:
        copy.start()
    return copies


class Push:
    def __init__(self, src, dst, send_sem, recv_sem, device, here):
        self.here = here
        self.local = pltpu.make_async_copy(src, dst, recv_sem)
        self.remote = pltpu.make_async_remote_copy(
            src_ref=src, dst_ref=dst, send_sem=send_sem, recv_sem=recv_sem, device_id=device, device_id_type=MESH
        )

    def start(self):
        @pl.when(self.here)
        def _():
            self.local.start()

        @pl.when(jnp.logical_not(self.here))
        def _():
            self.remote.start()

    def wait_send(self):
        @pl.when(jnp.logical_not(self.here))
        def _():
            self.remote.wait_send()

    def wait_recv(self):
        self.remote.wait_recv()


def rest_sum(y_ref, row0, rows):
    total = y_ref[pl.ds(row0, rows), 0:LANES] + y_ref[pl.ds(row0 + TILE, rows), LANES:TILE]
    return total + pltpu.roll(y_ref[pl.ds(row0 + LANES, rows), 0:LANES], REST, axis=1)


def valid_rows(value, first_row, width):
    row = first_row + lax.broadcasted_iota(jnp.int32, value.shape, 0) // width
    return jnp.where((row >= 0) & (row < TILE), value, 0.0)


def pooled(value, width, scratch):
    rows, lanes = value.shape
    tall = jnp.concatenate(
        [jnp.maximum(value[s : s + width], value[s + width : s + 2 * width]) for s in range(0, rows, 2 * width)], axis=0
    )
    halves = []
    for start in range(0, lanes, LANES):
        scratch[0 : rows // 2, :] = tall[:, start : start + LANES]
        halves.append(
            jnp.maximum(scratch[pl.ds(0, rows // IN_CH, stride=2), :], scratch[pl.ds(1, rows // IN_CH, stride=2), :])
        )
    return jnp.concatenate(halves, axis=1) if len(halves) > 1 else halves[0]


def enc1_kernel(
    image_hbm, w_a_hbm, b_a_hbm, w_b, b_b_hbm, s1_out, p1_out,
    image, w_a, b_a, b_b, halves, planes, w_stem, staged, x_a, y_rest, w_main, w_rest, pool_buf, stage, stage_p, w_sem, small_sem, send_sem, recv_sem,
):
    step = pl.program_id(0)
    strip = strip_index()

    @pl.when(step == 0)
    def _():
        row = lax.axis_index("row")
        col = lax.axis_index("col")
        barrier = enter_barrier()
        small = fetch((image_hbm, w_a_hbm, b_a_hbm, b_b_hbm), (image, w_a, b_a, b_b), small_sem)
        copy_w = pltpu.make_async_copy(w_b, staged, w_sem)
        copy_w.start()
        stage[...] = jnp.zeros_like(stage)
        stage_p[...] = jnp.zeros_like(stage_p)

        for copy in small:
            copy.wait()
        for di in range(KERNEL):
            taps = []
            for dj in range(KERNEL):
                tap = jnp.concatenate([w_a[di, dj].astype(F32), jnp.zeros((IN_CH, BASE), F32)], axis=0)
                taps.append(jnp.concatenate([tap, jnp.zeros((STRIPS, REST), F32)], axis=1))
            taps.append(jnp.zeros((STRIPS, BASE_PAD), F32))
            w_stem[STRIP_ROWS * di : STRIP_ROWS * di + STRIP_ROWS, :] = jnp.concatenate(taps, axis=0).astype(BF16)
        planes[N40:N42, :, :] = jnp.zeros((2, STRIP_ROWS, LANES), BF16)

        pl.semaphore_wait(barrier, STRIPS)
        pushes = []
        for index, (target, src_row, dst_row, rows) in enumerate(
            ((2 * row, 0, IN_CH, N36), (2 * row + 1, N28, 0, N36), ((2 * row + 2) % STRIPS, N60, 0, IN_CH), ((2 * row + LAST_STRIP) % STRIPS, 0, N36, IN_CH))
        ):
            pushes.append(
                Push(
                    image.at[pl.ds(src_row, rows)],
                    halves.at[col, pl.ds(dst_row, rows)],
                    send_sem.at[index],
                    recv_sem.at[index // 2, col],
                    strip_device(target),
                    target == strip,
                )
            )
        for push in pushes:
            push.start()
        copy_w.wait()
        pack_weights(staged, w_main, w_rest)
        for push in pushes:
            push.wait_send()
        for kind, rows in ((0, N36), (1, IN_CH)):
            for side in range(2):
                Push(
                    image.at[pl.ds(0, rows)], halves.at[side, pl.ds(0, rows)],
                    send_sem.at[0], recv_sem.at[kind, side], strip_device(strip), strip < 0,
                ).wait_recv()

        def expand(i, carry):
            for j in range(STRIPS):
                r = STRIPS * i + j
                both = jnp.concatenate([halves[0, r].astype(F32), halves[1, r].astype(F32)], axis=1)
                image_row = STRIP_ROWS * strip - IN_CH + r
                both = jnp.where((image_row >= 0) & (image_row < TILE), both, 0.0)
                both = jnp.concatenate([both, jnp.zeros((IN_CH, LANES), F32)], axis=0)
                column = lax.broadcasted_iota(jnp.int32, (STRIPS, LANES), 1)
                before = jnp.where(column == 0, 0.0, pltpu.roll(both, 1, axis=1))
                after = jnp.where(column == N127, 0.0, pltpu.roll(both, N127, axis=1))
                planes[r] = jnp.concatenate([before, both, after, jnp.zeros((STRIPS, LANES), F32)], axis=0).astype(BF16)
            return carry

        lax.fori_loop(0, FIVE, expand, 0)

        def stem(i, carry):
            for j in range(STRIPS):
                r = STRIPS * i + j
                patch = jnp.concatenate([planes[r + di] for di in range(KERNEL)], axis=0)
                acc = lax.dot_general(patch, w_stem[...], (((0,), (0,)), ((), ())), preferred_element_type=F32)
                image_row = STRIP_ROWS * strip - KERNEL + r
                inside = (image_row >= 0) & (image_row < TILE)
                main = jnp.where(inside, jnp.maximum(acc[:, 0:TILE] + bias_row(b_a, 0, TILE), 0.0), 0.0)
                tail = jnp.where(inside, jnp.maximum(acc[:, TILE:BASE_PAD] + bias_rest(b_a), 0.0), 0.0)
                put3_320(x_a, pl.multiple_of(r * LANES, LANES), main, tail, LANES, stage.at[j % 2])
            return carry

        lax.fori_loop(0, FIVE, stem, 0)

    base = pl.multiple_of(step * N1536, N512)

    def rest(j):
        y_rest[TILE * j : TILE * j + TILE, :] = dot(packed_rows(x_a, base + TILE * j, TILE), w_rest[...])

    rest(0)
    for j in range(SIX):
        rest(j + 1)
        acc = dot(packed_rows(x_a, base + TILE * j, TILE), w_main[0:PACK, :])
        acc = acc + dot(packed_rows(x_a, base + TILE * j + LANES, TILE), w_main[PACK:N2048, :])
        acc = acc + dot(packed_rows(x_a, base + TILE * j + TILE, TILE), w_main[N2048:N3072, :])
        first_row = STRIP_ROWS * strip - 2 + N12 * step + 2 * j
        main = valid_rows(jnp.maximum(acc + bias_row(b_b, 0, TILE), 0.0), first_row, LANES)
        tail = jnp.maximum(rest_sum(y_rest, TILE * j, TILE) + bias_rest(b_b), 0.0)
        tail = low_lanes(valid_rows(tail, first_row, LANES))
        s1_out[TILE * j : TILE * j + TILE, 0:TILE] = main.astype(BF16)
        s1_out[TILE * j : TILE * j + TILE, TILE:BASE_PAD] = tail.astype(BF16)
        put3_320(p1_out, REST * j, pooled(main, LANES, pool_buf.at[j % 2]), pooled(tail, LANES, pool_buf.at[j % 2]), REST, stage_p.at[j % 2])


def mid_kernel(
    p1_hbm, w_2a, w_2b, w_ma, w_mb, w_u2, w_d2a, w_d2b, b_2a_h, b_2b_h, b_ma_h, b_mb_h, b_d2a_h, b_d2b_h, out,
    b_2a, b_2b, b_ma, b_mb, b_d2a, b_d2b,
    p1, first_w, ring, x_a, x_s, x_u, m_1, m_2, m_o, d_2, acc_ref, wide, pool_buf,
    sem_2a, sem_2b, sem_ma, sem_mb, sem_u2, sem_d2a, sem_d2b, sem_p1, sem_out, small_sem, send_sem, recv_sem,
):
    strip = strip_index()
    prev_dev = strip_device((strip + LAST_STRIP) % STRIPS)
    next_dev = strip_device((strip + 1) % STRIPS)

    def exchange(buf, width, lane0, lanes, rows, index, target=None):
        target = buf if target is None else target
        lane = pl.ds(lane0, lanes)
        copies = []
        for side, src_row, dst_row, device in ((0, 1, rows + 1, prev_dev), (1, rows, 0, next_dev)):
            copies.append(
                pltpu.make_async_remote_copy(
                    src_ref=buf.at[pl.ds(src_row * width, width), lane],
                    dst_ref=target.at[pl.ds(dst_row * width, width), lane],
                    send_sem=send_sem.at[index, side],
                    recv_sem=recv_sem.at[index, side],
                    device_id=device,
                    device_id_type=MESH,
                )
            )
        return copies

    def start(copies):
        for copy in copies:
            copy.start()

    def finish(copies):
        for copy in copies:
            copy.wait()

    def halo(buf, width, channels, rows):
        for row, inside in ((0, strip > 0), (rows + 1, strip < LAST_STRIP)):
            value = buf[pl.ds(row * width, width), pl.ds(channels, channels)].astype(F32)
            put3(buf, row * width, 0, channels, jnp.where(inside, value, 0.0), width)

    copies_2a = []
    for tap in range(TAPS):
        di, dj = tap // KERNEL, tap % KERNEL
        for part, (start_row, size, row) in enumerate(((0, TILE, TILE * dj), (TILE, REST, REST_AT + REST * dj))):
            copies_2a.append(
                pltpu.make_async_copy(
                    w_2a.at[pl.ds(BASE * tap + start_row, size), :],
                    first_w.at[pl.ds(PACK * di + row, size), :],
                    sem_2a.at[2 * tap + part],
                )
            )

    def tap_copies(src, rows, base, sem):
        return [
            pltpu.make_async_copy(
                src.at[pl.ds(rows * tap, rows), :],
                ring.at[pl.ds(base + rows * (tap // 2), rows), pl.ds(MIDDLE * (tap % 2), MIDDLE)],
                sem.at[tap],
            )
            for tap in range(src.shape[0] // rows)
        ]

    copies_2b = tap_copies(w_2b, MIDDLE, 0, sem_2b)
    copies_ma = [
        pltpu.make_async_copy(w_ma.at[pl.ds(MIDDLE3 * di, MIDDLE3), :], ring.at[pl.ds(N3200 + MIDDLE3 * t, MIDDLE3), :], sem_ma.at[t])
        for t, di in enumerate((1, 0, 2))
    ]

    def mb_row(k):
        return (N8960 + DEEP * k) % RING_ROWS

    copies_mb = [
        pltpu.make_async_copy(
            w_mb.at[pl.ds(DEEP * (KERNEL * (1, 0, 2)[k // KERNEL] + k % KERNEL), DEEP), :], ring.at[pl.ds(mb_row(k), DEEP), :], sem_mb.at[k]
        )
        for k in range(TAPS)
    ]
    copies_u2 = [
        pltpu.make_async_copy(
            w_u2.at[pl.ds(DEEP * tap, DEEP), :],
            first_w.at[pl.ds(DEEP * tap, DEEP), :] if tap < 2 else ring.at[pl.ds(N8960, DEEP), pl.ds(MIDDLE * (tap - 2), MIDDLE)],
            sem_u2.at[tap],
        )
        for tap in range(IN_CH)
    ]
    copies_d2a = tap_copies(w_d2a, DEEP, 0, sem_d2a)
    copies_d2b = tap_copies(w_d2b, MIDDLE, N6400, sem_d2b)

    copy_p1 = pltpu.make_async_copy(p1_hbm, p1.at[:, pl.ds(0, N1152), :], sem_p1)
    barrier = pltpu.get_barrier_semaphore()
    for device in (prev_dev, next_dev):
        pl.semaphore_signal(barrier, inc=1, device_id=device, device_id_type=MESH)
    copy_p1.start()
    start(copies_2a)
    small = fetch(
        (b_2a_h, b_2b_h, b_ma_h, b_mb_h, b_d2a_h, b_d2b_h), (b_2a, b_2b, b_ma, b_mb, b_d2a, b_d2b), small_sem
    )
    pl.semaphore_wait(barrier, 2)

    for di in range(KERNEL):
        first_w[PACK * di + PACK_USED : PACK * di + PACK, :] = jnp.zeros((REST, MIDDLE), BF16)
    copy_p1.wait()
    finish(small)
    finish(copies_2a)
    start(copies_2b)
    start(copies_ma)

    ex_a = exchange(x_a, REST, MIDDLE, MIDDLE, N16, 0)
    ex_s = exchange(x_s, REST, MIDDLE, MIDDLE, N16, 1)
    ex_m1 = exchange(m_1, STRIP_ROWS, MIDDLE, MIDDLE, STRIPS, 2)
    ex_m2 = exchange(m_2, STRIP_ROWS, DEEP, DEEP, STRIPS, KERNEL)
    ex_u = exchange(x_u, REST, MIDDLE, MIDDLE, N16, IN_CH)
    ex_b = exchange(x_a, REST, MIDDLE, MIDDLE, N16, FIVE)
    ex_d = exchange(d_2, REST, 0, MIDDLE, N16, SIX, out)
    tiles = ((0, TILE), (TILE, TILE), (N512, LANES))

    def enc2a(i, carry):
        @pl.when(i == 1)
        def _():
            start(ex_a)

        for block in (i, KERNEL - i):
            row0 = pl.multiple_of(block * TILE, TILE)
            for lane0, lanes in tiles:
                acc = dot(packed_rows(p1, row0, TILE), first_w[0:PACK, pl.ds(lane0, lanes)])
                for di in (1, 2):
                    acc = acc + dot(
                        packed_rows(p1, row0 + REST * di, TILE),
                        first_w[PACK * di : PACK * di + PACK, pl.ds(lane0, lanes)],
                    )
                value = jnp.maximum(acc + bias_row(b_2a, lane0, lanes), 0.0)
                put3(x_a, row0 + REST, lane0, MIDDLE, value, REST)
        return carry

    lax.fori_loop(0, 2, enc2a, 0)
    finish(copies_2b)
    start(copies_mb[0:2])
    start(copies_u2[0:2])

    def conv640(src, row0, base, lane0, lanes):
        acc = None
        for di in range(KERNEL):
            weights = jnp.concatenate(
                [
                    ring[base + MIDDLE * (t // 2) : base + MIDDLE * (t // 2) + MIDDLE, pl.ds(MIDDLE * (t % 2) + lane0, lanes)]
                    for t in range(KERNEL * di, KERNEL * di + KERNEL)
                ],
                axis=0,
            )
            part = dot(src[pl.ds(row0 + REST * di, TILE), :], weights)
            acc = part if acc is None else acc + part
        return acc

    def enc2b(i, carry):
        block = i + 1 - 2 * (i % 2)
        row0 = pl.multiple_of(block * TILE, TILE)

        @pl.when(i == 1)
        def _():
            finish(ex_a)
            halo(x_a, REST, MIDDLE, N16)

        @pl.when(i == KERNEL)
        def _():
            start(ex_m1)
            start(ex_s)

        for lane0, lanes in tiles:
            value = jnp.maximum(conv640(x_a, row0, 0, lane0, lanes) + bias_row(b_2b, lane0, lanes), 0.0)
            put3(x_s, row0 + REST, lane0, MIDDLE, value, REST)
            put3(m_1, pl.multiple_of(block * REST + STRIP_ROWS, STRIP_ROWS), lane0, MIDDLE, pooled(value, REST, pool_buf), STRIP_ROWS)
        return carry

    lax.fori_loop(0, IN_CH, enc2b, 0)
    start(copies_mb[2:IN_CH])

    acc_ref[...] = jnp.zeros_like(acc_ref)
    finish(copies_ma)

    def mid_a(t, carry):
        di = (t + 1) % 2 + 2 * (t // 2) - t // 2

        @pl.when(t == 1)
        def _():
            start(copies_mb[IN_CH:SIX])
            finish(ex_m1)
            halo(m_1, STRIP_ROWS, MIDDLE, STRIPS)

        @pl.when(t == 2)
        def _():
            start(copies_mb[SIX:LAST_STRIP])

        base = pl.multiple_of(N3200 + MIDDLE3 * t, LANES)
        lhs_row = pl.multiple_of(STRIP_ROWS * di, STRIP_ROWS)
        for lane0 in range(0, DEEP, TILE):
            acc_ref[:, pl.ds(lane0, TILE)] += dot(
                m_1[pl.ds(lhs_row, TILE), :], ring[pl.ds(base, MIDDLE3), pl.ds(lane0, TILE)]
            )
        return carry

    lax.fori_loop(0, KERNEL, mid_a, 0)
    start(copies_mb[LAST_STRIP:TAPS])

    def mid_a_rows(first, rows):
        for lane0 in range(0, DEEP, TILE):
            value = jnp.maximum(acc_ref[pl.ds(first, rows), pl.ds(lane0, TILE)] + bias_row(b_ma, lane0, TILE), 0.0)
            put3(m_2, STRIP_ROWS + first, lane0, DEEP, value, STRIP_ROWS)

    mid_a_rows(0, STRIP_ROWS)
    mid_a_rows(N224, STRIP_ROWS)
    start(ex_m2)
    mid_a_rows(STRIP_ROWS, N192)
    acc_ref[...] = jnp.zeros_like(acc_ref)

    def mid_b(t, carry):
        di = (t + 1) % 2 + 2 * (t // 2) - t // 2

        for j in range(KERNEL):
            @pl.when(t == j)
            def _(j=j):
                finish(copies_mb[KERNEL * j : KERNEL * j + KERNEL])

        @pl.when(t == 1)
        def _():
            start(copies_u2[2:IN_CH])
            start(copies_d2a[0:2])
            finish(ex_m2)
            halo(m_2, STRIP_ROWS, DEEP, STRIPS)

        @pl.when(t == 2)
        def _():
            start(copies_d2a[2:STRIPS])

        lhs_row = pl.multiple_of(STRIP_ROWS * di, STRIP_ROWS)
        for lane0 in range(0, DEEP, TILE):
            acc = None
            for dj in range(KERNEL):
                base = pl.multiple_of(mb_row(KERNEL * t + dj), LANES)
                part = dot(
                    m_2[pl.ds(lhs_row, TILE), DEEP * dj : DEEP * dj + DEEP], ring[pl.ds(base, DEEP), pl.ds(lane0, TILE)]
                )
                acc = part if acc is None else acc + part
            acc_ref[:, pl.ds(lane0, TILE)] += acc
        return carry

    lax.fori_loop(0, KERNEL, mid_b, 0)
    start(copies_d2a[STRIPS:TAPS])
    for lane0 in range(0, DEEP, TILE):
        value = jnp.maximum(acc_ref[:, pl.ds(lane0, TILE)] + bias_row(b_mb, lane0, TILE), 0.0)
        m_o[:, pl.ds(lane0, TILE)] = value.astype(BF16)

    finish(copies_u2)
    for p in range(2):
        for q in range(2):
            for lane0, lanes in tiles:
                if p == 0:
                    weights = first_w[DEEP * q : DEEP * q + DEEP, pl.ds(lane0, lanes)]
                else:
                    weights = ring[N8960:N10240, pl.ds(MIDDLE * q + lane0, lanes)]
                part = dot(m_o[...], weights)
                for lane in range(0, lanes, LANES):
                    wide[(lane0 + lane) // LANES, pl.ds(q, TILE, stride=2), :] = part[:, lane : lane + LANES]

        def place(i, carry):
            src = pl.multiple_of(REST * i, REST)
            dst = pl.multiple_of(REST * (1 + 2 * i + p), REST)
            for lane0 in range(0, MIDDLE, LANES):
                put3(x_u, dst, lane0, MIDDLE, wide[lane0 // LANES, pl.ds(src, REST), :], REST)
            return carry

        lax.fori_loop(0, STRIPS, place, 0)
    start(ex_u)
    start(copies_d2b)
    finish(ex_s)
    halo(x_s, REST, MIDDLE, N16)
    finish(copies_d2a)

    def dec2a(i, carry):
        block = i + 1 - 2 * (i % 2)
        row0 = pl.multiple_of(block * TILE, TILE)

        @pl.when(i == 1)
        def _():
            finish(ex_u)
            halo(x_u, REST, MIDDLE, N16)

        @pl.when(i == KERNEL)
        def _():
            start(ex_b)

        for lane0, lanes in tiles:
            acc = None
            for tap in range(TAPS):
                rows = pl.ds(row0 + REST * (tap // KERNEL), TILE)
                cols = pl.ds(MIDDLE * (tap % KERNEL), MIDDLE)
                lhs = jnp.concatenate([x_u[rows, cols], x_s[rows, cols]], axis=1)
                base = DEEP * (tap // 2)
                part = dot(lhs, ring[base : base + DEEP, pl.ds(MIDDLE * (tap % 2) + lane0, lanes)])
                acc = part if acc is None else acc + part
            value = jnp.maximum(acc + bias_row(b_d2a, lane0, lanes), 0.0)
            put3(x_a, row0 + REST, lane0, MIDDLE, value, REST)
        return carry

    lax.fori_loop(0, IN_CH, dec2a, 0)
    finish(copies_d2b)

    def dec2b(i, carry):
        block = i + 1 - 2 * (i % 2)
        row0 = pl.multiple_of(block * TILE, TILE)

        @pl.when(i == 1)
        def _():
            finish(ex_b)
            halo(x_a, REST, MIDDLE, N16)

        @pl.when(i == KERNEL)
        def _():
            start(ex_d)

        for lane0, lanes in tiles:
            value = jnp.maximum(conv640(x_a, row0, N6400, lane0, lanes) + bias_row(b_d2b, lane0, lanes), 0.0)
            d_2[pl.ds(row0 + REST, TILE), pl.ds(lane0, lanes)] = value.astype(BF16)
        return carry

    lax.fori_loop(0, IN_CH, dec2b, 0)
    result = pltpu.make_async_copy(d_2.at[pl.ds(REST, PACK), :], out.at[pl.ds(REST, PACK), :], sem_out)
    result.start()
    finish(ex_d)
    result.wait()


def dec1_kernel(
    d_2, s1, w_u1, w_d1a, w_d1b, b_d1a_h, b_d1b_h, w_head_h, b_head_h, out,
    b_d1a, b_d1b, w_head, b_head, x_u, x_s, x_d, y_rest, st_u, st_a, st_b, wu_main, wu_rest, wa_main, wa_rest, wb_main, wb_rest, wide, result, pending, stage, skip, low, late,
    sem, small_sem, send_sem, recv_sem,
):
    strip = strip_index()
    row = lax.axis_index("row")
    col = lax.axis_index("col")
    copy_u = pltpu.make_async_copy(w_u1, st_u, sem.at[0])
    copy_a = pltpu.make_async_copy(w_d1a, st_a, sem.at[1])
    copy_s = pltpu.make_async_copy(s1, skip, sem.at[2])
    copy_b = pltpu.make_async_copy(w_d1b, st_b, sem.at[KERNEL])
    copy_d = pltpu.make_async_copy(d_2, low, sem.at[IN_CH])
    barrier = enter_barrier()
    copy_u.start()
    copy_d.start()
    small = fetch((b_d1a_h, b_d1b_h, w_head_h, b_head_h), (b_d1a, b_d1b, w_head, b_head), small_sem)

    stage[...] = jnp.zeros_like(stage)
    copy_u.wait()
    copy_a.start()
    copy_s.start()
    copy_b.start()
    for tap in range(IN_CH):
        wu_main[MIDDLE * tap : MIDDLE * tap + MIDDLE, :] = st_u[BASE * tap : BASE * tap + TILE, :].T
    wu_rest[...] = jnp.concatenate([st_u[BASE * tap + TILE : BASE * tap + BASE, :] for tap in range(IN_CH)], axis=0).T
    copy_d.wait()
    for copy in small:
        copy.wait()

    def up1(i, carry):
        row0 = pl.multiple_of(i * BASE_PAD, LANES)
        lhs = low[pl.ds(row0, BASE_PAD), :]
        rest = dot(lhs, wu_rest[...])
        for p in range(2):
            part = rest[:, LANES * p : LANES * p + LANES]
            buf = wide.at[p]
            buf[2, pl.ds(0, BASE_PAD, stride=2), :] = low_lanes(part)
            buf[2, pl.ds(1, BASE_PAD, stride=2), :] = low_lanes(pltpu.roll(part, REST, axis=1))
            for q in range(2):
                tap = 2 * p + q
                main = dot(lhs, wu_main[MIDDLE * tap : MIDDLE * tap + MIDDLE, :])
                buf[0, pl.ds(q, BASE_PAD, stride=2), :] = main[:, 0:LANES]
                buf[1, pl.ds(q, BASE_PAD, stride=2), :] = main[:, LANES:TILE]
            for r in range(SIX):
                main = jnp.concatenate([buf[0, LANES * r : LANES * r + LANES, :], buf[1, LANES * r : LANES * r + LANES, :]], axis=1)
                put3_320(
                    x_u, pl.multiple_of((N12 * i + 2 * r + p) * LANES, LANES), main, buf[2, LANES * r : LANES * r + LANES, :], LANES
                )
        return carry

    lax.fori_loop(0, KERNEL, up1, 0)

    @pl.when(strip == 0)
    def _():
        x_u[:, 0:TILE, :] = jnp.zeros((STRIPS, TILE, LANES), BF16)

    @pl.when(strip == LAST_STRIP)
    def _():
        x_u[:, N4352:N4608, :] = jnp.zeros((STRIPS, TILE, LANES), BF16)

    copy_a.wait()
    turn_rest(st_a, wa_main, wa_rest)
    copy_s.wait()

    def rest_a(i, carry):
        base = pl.multiple_of(i * N1536, N512)

        def spread(j):
            rows = pl.ds(base + TILE * j, TILE)
            put3_320(
                x_s, base + TILE * j, skip[rows, 0:TILE].astype(F32), skip[rows, TILE:BASE_PAD].astype(F32), LANES, stage.at[j % 2]
            )

        spread(0)
        for j in range(SIX):
            rows = pl.ds(base + TILE * j, TILE)
            y_rest[rows, :] = dot(packed_rows(x_u, base + TILE * j, TILE), wa_rest[0:PACK, :]) + dot(
                packed_rows(x_s, base + TILE * j, TILE), wa_rest[PACK:N2048, :]
            )
            if j < FIVE:
                spread(j + 1)
            if j < KERNEL:
                turn_main(st_a, wa_main, i, j)
        return carry

    lax.fori_loop(0, KERNEL, rest_a, 0)

    def conv_a(row0):
        acc = None
        for di in range(KERNEL):
            for src, ref in enumerate((x_u, x_s)):
                base = N3072 * src + PACK * di
                part = dot(packed_rows(ref, row0 + LANES * di, TILE), wa_main[base : base + PACK, :])
                acc = part if acc is None else acc + part
        return acc

    def put_a(acc, row0, first_row, slot):
        main = valid_rows(jnp.maximum(acc + bias_row(b_d1a, 0, TILE), 0.0), first_row, LANES)
        tail = valid_rows(jnp.maximum(rest_sum(y_rest, row0, TILE) + bias_rest(b_d1a), 0.0), first_row, LANES)
        put3_320(x_d, row0, main, low_lanes(tail), LANES, stage.at[slot])

    late[...] = jnp.zeros_like(late)

    def dec1a(i, carry):
        base = pl.multiple_of(i * PACK, PACK)
        put_a(late[...], pl.multiple_of(jnp.maximum(base - TILE, 0), TILE), STRIP_ROWS * strip - KERNEL + STRIPS * i, 1)
        for j in range(IN_CH):
            acc = conv_a(base + TILE * j)
            if j == KERNEL:
                late[...] = acc
            else:
                put_a(acc, base + TILE * j, STRIP_ROWS * strip - 1 + STRIPS * i + 2 * j, j % 2)
        return carry

    lax.fori_loop(0, IN_CH, dec1a, 0)
    put_a(late[...], N3840, STRIP_ROWS * strip + N29, 1)
    put_a(conv_a(N4096), N4096, STRIP_ROWS * strip + N31, 0)

    copy_b.wait()
    pack_weights(st_b, wb_main, wb_rest)
    head_bias = jnp.zeros((IN_CH, LANES), F32)
    for channel in range(IN_CH):
        head_bias = jnp.where(lax.broadcasted_iota(jnp.int32, (IN_CH, LANES), 0) == channel, b_head[channel], head_bias)

    pending[...] = jnp.zeros_like(pending)

    def head(hidden, row0):
        line = lax.dot_general(w_head[...], hidden, (((1,), (1,)), ((), ())), preferred_element_type=F32)
        for r in range(2):
            part = line[:, LANES * r : LANES * r + LANES] + head_bias
            result[0, row0 + r] = part[:, 0:REST]
            result[1, row0 + r] = part[:, REST:LANES]

    def dec1b(i, carry):
        base = pl.multiple_of(i * PACK, PACK)

        def rest(j):
            y_rest[TILE * j : TILE * j + TILE, :] = dot(packed_rows(x_d, base + TILE * j, TILE), wb_rest[...])

        rest(0)
        waiting = pending[...]
        for j in range(IN_CH):
            rest(j + 1)
            acc = dot(packed_rows(x_d, base + TILE * j, TILE), wb_main[0:PACK, :])
            acc = acc + dot(packed_rows(x_d, base + TILE * j + LANES, TILE), wb_main[PACK:N2048, :])
            acc = acc + dot(packed_rows(x_d, base + TILE * j + TILE, TILE), wb_main[N2048:N3072, :])
            head(waiting, jnp.maximum(STRIPS * i + 2 * j - 2, 0))
            main = jnp.maximum(acc + bias_row(b_d1b, 0, TILE), 0.0).astype(BF16)
            tail = jnp.maximum(rest_sum(y_rest, TILE * j, TILE) + bias_rest(b_d1b), 0.0).astype(BF16)
            waiting = jnp.concatenate([main, tail[:, 0:REST]], axis=1)
        pending[...] = waiting
        return carry

    pushes = []
    for part, first, rows in ((0, 0, N22), (1, N22, N10)):
        for side in range(2):
            pushes.append(
                Push(
                    result.at[side, pl.ds(first, rows)],
                    out.at[pl.ds(STRIP_ROWS * (strip % 2) + first, rows)],
                    send_sem.at[part, side],
                    recv_sem.at[part, strip % 2],
                    (lax.axis_index("data"), side, strip // 2),
                    (strip // 2 == row) & (col == side),
                )
            )

    lax.fori_loop(0, KERNEL, dec1b, 0)
    pl.semaphore_wait(barrier, STRIPS)
    for push in pushes[0:2]:
        push.start()
    lax.fori_loop(KERNEL, IN_CH, dec1b, 0)
    head(pending[...], N30)

    for push in pushes[2:IN_CH]:
        push.start()
    for push in pushes:
        push.wait_send()
    for part, first, rows in ((0, 0, N22), (1, N22, N10)):
        for half in range(2):
            Push(
                result.at[0, pl.ds(first, rows)], out.at[pl.ds(STRIP_ROWS * half + first, rows)],
                send_sem.at[part, 0], recv_sem.at[part, half], strip_device(strip), strip < 0,
            ).wait_recv()


def solution(mesh):
    tile_spec = P(("data", "row"), "col", None)

    def body(image_tile, *params):
        (w_enc1a, b_enc1a, w_enc1b, b_enc1b, w_enc2a, b_enc2a, w_enc2b, b_enc2b,
         w_mid_a, b_mid_a, w_mid_b, b_mid_b, w_up2, w_dec2a, b_dec2a, w_dec2b, b_dec2b,
         w_up1, w_dec1a, b_dec1a, w_dec1b, b_dec1b, w_head, b_head) = params
        def flat(weight):
            return weight.reshape(-1, weight.shape[-1])

        hbm = pl.BlockSpec(memory_space=pl.ANY)
        dma = pltpu.SemaphoreType.DMA
        s1, p1 = pl.pallas_call(
            enc1_kernel,
            grid=(KERNEL,),
            out_shape=(jax.ShapeDtypeStruct((N4608, BASE_PAD), BF16), jax.ShapeDtypeStruct((STRIPS, N1152, LANES), BF16)),
            in_specs=[hbm] * FIVE,
            out_specs=(pl.BlockSpec((N1536, BASE_PAD), lambda i: (i, 0)), pl.BlockSpec((STRIPS, BASE_PAD, LANES), lambda i: (0, i, 0))),
            scratch_shapes=[
                pltpu.VMEM((REST, IN_CH, REST), BF16),
                pltpu.VMEM((KERNEL, KERNEL, IN_CH, BASE), BF16),
                pltpu.VMEM((BASE,), F32),
                pltpu.VMEM((BASE,), F32),
                pltpu.VMEM((2, N40, IN_CH, REST), BF16),
                pltpu.VMEM((N42, STRIP_ROWS, LANES), BF16),
                pltpu.VMEM((N96, BASE_PAD), BF16),
                pltpu.VMEM((N2880, BASE), BF16),
                pltpu.VMEM((STRIPS, N5136, LANES), BF16),
                pltpu.VMEM((N1792, TILE), F32),
                pltpu.VMEM((N3072, TILE), BF16),
                pltpu.VMEM((PACK, TILE), BF16),
                pltpu.VMEM((2, LANES, LANES), F32),
                pltpu.VMEM((2, KERNEL, N288, LANES), F32),
                pltpu.VMEM((2, KERNEL, N80, LANES), F32),
                dma, dma((IN_CH,)), dma((IN_CH,)), dma((2, 2)),
            ],
            compiler_params=pltpu.CompilerParams(
                vmem_limit_bytes=VMEM_LIMIT, collective_id=1, has_side_effects=True, dimension_semantics=("arbitrary",)
            ),
            name="enc1",
        )(image_tile.transpose(0, 2, 1), w_enc1a, b_enc1a, flat(w_enc1b), b_enc1b)

        d2 = pl.pallas_call(
            mid_kernel,
            out_shape=jax.ShapeDtypeStruct((N1152, MIDDLE), BF16),
            in_specs=[hbm] * N14,
            out_specs=hbm,
            scratch_shapes=[
                *[pltpu.VMEM((size,), F32) for size in (MIDDLE, MIDDLE, DEEP, DEEP, MIDDLE, MIDDLE)],
                pltpu.VMEM((STRIPS, N1168, LANES), BF16),
                pltpu.VMEM((N3072, MIDDLE), BF16),
                pltpu.VMEM((RING_ROWS, DEEP), BF16),
                pltpu.VMEM((N1152, MIDDLE3), BF16),
                pltpu.VMEM((N1152, MIDDLE3), BF16),
                pltpu.VMEM((N1152, MIDDLE3), BF16),
                pltpu.VMEM((BASE, MIDDLE3), BF16),
                pltpu.VMEM((BASE, N3840), BF16),
                pltpu.VMEM((TILE, DEEP), BF16),
                pltpu.VMEM((N1152, MIDDLE), BF16),
                pltpu.VMEM((TILE, DEEP), F32),
                pltpu.VMEM((FIVE, N512, LANES), F32),
                pltpu.VMEM((LANES, LANES), F32),
                dma((N18,)), dma((TAPS,)), dma((KERNEL,)), dma((TAPS,)), dma((IN_CH,)), dma((TAPS,)), dma((TAPS,)), dma, dma, dma((SIX,)),
                dma((LAST_STRIP, 2)), dma((LAST_STRIP, 2)),
            ],
            compiler_params=pltpu.CompilerParams(
                vmem_limit_bytes=VMEM_LIMIT, collective_id=0, has_side_effects=True
            ),
            name="mid",
        )(
            p1, flat(w_enc2a), flat(w_enc2b), flat(w_mid_a), flat(w_mid_b), flat(w_up2), flat(w_dec2a), flat(w_dec2b),
            b_enc2a, b_enc2b, b_mid_a, b_mid_b, b_dec2a, b_dec2b,
        )

        def turned(weight):
            return weight.transpose(0, 1, KERNEL, 2).reshape(-1, weight.shape[2])

        y = pl.pallas_call(
            dec1_kernel,
            out_shape=jax.ShapeDtypeStruct((REST, IN_CH, REST), F32),
            in_specs=[hbm] * TAPS,
            out_specs=hbm,
            scratch_shapes=[
                pltpu.VMEM((BASE,), F32),
                pltpu.VMEM((BASE,), F32),
                pltpu.VMEM((IN_CH, BASE), BF16),
                pltpu.SMEM((IN_CH,), F32),
                pltpu.VMEM((STRIPS, N4624, LANES), BF16),
                pltpu.VMEM((STRIPS, N4624, LANES), BF16),
                pltpu.VMEM((STRIPS, N4368, LANES), BF16),
                pltpu.VMEM((N4608, TILE), F32),
                pltpu.VMEM((DEEP, MIDDLE), BF16),
                pltpu.VMEM((N2880, MIDDLE), BF16),
                pltpu.VMEM((N2880, BASE), BF16),
                pltpu.VMEM((N2560, TILE), BF16),
                pltpu.VMEM((MIDDLE, TILE), BF16),
                pltpu.VMEM((N6144, TILE), BF16),
                pltpu.VMEM((N2048, TILE), BF16),
                pltpu.VMEM((N3072, TILE), BF16),
                pltpu.VMEM((PACK, TILE), BF16),
                pltpu.VMEM((2, KERNEL, REST_AT, LANES), F32),
                pltpu.VMEM((2, STRIP_ROWS, IN_CH, REST), F32),
                pltpu.VMEM((TILE, BASE), BF16),
                pltpu.VMEM((2, KERNEL, N288, LANES), F32),
                pltpu.VMEM((N4608, BASE_PAD), BF16),
                pltpu.VMEM((N1152, MIDDLE), BF16),
                pltpu.VMEM((TILE, TILE), F32),
                dma((FIVE,)), dma((IN_CH,)), dma((2, 2)), dma((2, 2)),
            ],
            compiler_params=pltpu.CompilerParams(vmem_limit_bytes=VMEM_LIMIT, collective_id=2, has_side_effects=True),
            name="dec1",
        )(d2, s1, turned(w_up1), turned(w_dec1a), flat(w_dec1b), b_dec1a, b_dec1b, w_head.T, b_head)
        return y.transpose(0, 2, 1)

    def program(image, *params):
        mapped = jax.shard_map(
            body, mesh=mesh, in_specs=(tile_spec,) + (P(),) * len(params), out_specs=tile_spec, check_vma=False
        )
        return mapped(image, *params)

    return program
```

```python
import functools

import jax
import jax.numpy as jnp
from jax import lax
from jax.experimental import pallas as pl
from jax.experimental.pallas import tpu as pltpu
from jax.sharding import PartitionSpec as P

KERNEL = 3
IN_CH = 4
FIVE = 5
SIX = 6
LAST_STRIP = 7
STRIPS = 8
TAPS = 9
N10 = 10
N11 = 11
N12 = 12
N16 = 16
N18 = 18
N22 = 22
N28 = 28
N29 = 29
N30 = 30
N31 = 31
STRIP_ROWS = 32
N36 = 36
N40 = 40
N42 = 42
N60 = 60
REST = 64
N80 = 80
N96 = 96
N127 = 127
LANES = 128
N192 = 192
N224 = 224
TILE = 256
N288 = 288
BASE = 320
BASE_PAD = 384
N512 = 512
MIDDLE = 640
REST_AT = 768
PACK_USED = 960
PACK = 1024
N1152 = 1152
N1168 = 1168
DEEP = 1280
N1536 = 1536
N1792 = 1792
MIDDLE3 = 1920
N2048 = 2048
N2560 = 2560
N2880 = 2880
N3072 = 3072
N3200 = 3200
N3840 = 3840
N4096 = 4096
N4352 = 4352
N4368 = 4368
N4608 = 4608
N4624 = 4624
N5136 = 5136
N6144 = 6144
N6400 = 6400
N8960 = 8960
N10240 = 10240
N11520 = 11520
BF16 = jnp.bfloat16
F32 = jnp.float32
MESH = pl.DeviceIdType.MESH
VMEM_LIMIT = 66_900_000
RING_ROWS = N11520


def strip_index():
    col = lax.axis_index("col")
    row = lax.axis_index("row")
    return row + col * (LAST_STRIP - 2 * row)


def strip_device(position):
    col = position // IN_CH
    rest = position % IN_CH
    return (lax.axis_index("data"), col, rest + col * (KERNEL - 2 * rest))


def dot(a, b):
    return jnp.dot(a, b, preferred_element_type=F32)


def shifted(value, width, step):
    if step == 1:
        return value
    rows = value.shape[0]
    column = lax.broadcasted_iota(jnp.int32, value.shape, 0) % width
    if step == 0:
        return jnp.where(column == 0, 0.0, pltpu.roll(value, 1, axis=0))
    return jnp.where(column == width - 1, 0.0, pltpu.roll(value, rows - 1, axis=0))


def put3(dst, row0, lane0, channels, value, width):
    rows, lanes = value.shape
    for step in range(KERNEL):
        dst[pl.ds(row0, rows), pl.ds(step * channels + lane0, lanes)] = shifted(value, width, step).astype(BF16)


def put3_320(dst, row0, main, rest, width, stage=None):
    rows = main.shape[0]
    pitch = width + N16
    planes = [main[:, 0:LANES], main[:, LANES:TILE], rest]
    for t, plane in enumerate(planes if stage is not None else []):
        for r in range(rows // width):
            stage[t, pitch * r + STRIPS : pitch * r + STRIPS + width, :] = plane[width * r : width * r + width]

    def moved(t, step):
        if stage is None:
            return shifted(planes[t], width, step)
        first = LAST_STRIP + step
        parts = [stage[t, pitch * r + first : pitch * r + first + width, :] for r in range(rows // width)]
        return jnp.concatenate(parts, axis=0) if len(parts) > 1 else parts[0]

    for step in range(KERNEL):
        for t in range(2):
            dst[2 * step + t, pl.ds(row0, rows), :] = moved(t, step).astype(BF16)
    first = moved(2, 0) + pltpu.roll(moved(2, 1), REST, axis=1)
    dst[SIX, pl.ds(row0, rows), :] = first.astype(BF16)
    dst[LAST_STRIP, pl.ds(row0, rows), :] = moved(2, 2).astype(BF16)


def packed_rows(ref, row0, rows):
    return jnp.concatenate([ref[t, pl.ds(row0, rows), :] for t in range(STRIPS)], axis=1)


def low_lanes(value):
    return jnp.where(lax.broadcasted_iota(jnp.int32, value.shape, 1) < REST, value, 0.0)


def pack_weights(staged, main_ref, rest_ref):
    for dj in range(KERNEL):
        for start, size, row in ((0, TILE, TILE * dj), (TILE, REST, REST_AT + REST * dj)):
            parts = []
            for di in range(KERNEL):
                base = (KERNEL * di + dj) * BASE + start
                main_ref[pl.ds(PACK * di + row, size), :] = staged[pl.ds(base, size), 0:TILE]
                parts.append(staged[pl.ds(base, size), TILE:BASE])
            parts.append(jnp.zeros((size, REST), BF16))
            rest_ref[pl.ds(row, size), :] = jnp.concatenate(parts, axis=1)
    clear_pad(main_ref, KERNEL)
    clear_pad(rest_ref, 1)


def clear_pad(ref, groups):
    for group in range(groups):
        ref[pl.ds(PACK * group + PACK_USED, REST), :] = jnp.zeros((REST, ref.shape[1]), BF16)


def turn_main(staged, main_ref, di, dj):
    turned = staged[pl.ds(pl.multiple_of(PACK_USED * di + BASE * dj, REST), TILE), :].T
    for src in range(2):
        base = N3072 * src + PACK * di
        main_ref[pl.ds(pl.multiple_of(base + TILE * dj, REST), TILE), :] = turned[BASE * src : BASE * src + TILE]
        main_ref[pl.ds(pl.multiple_of(base + REST_AT + REST * dj, REST), REST), :] = turned[BASE * src + TILE : BASE * src + BASE]


def turn_rest(staged, rest_ref, dj):
    parts = [staged[pl.ds(pl.multiple_of(PACK_USED * di + BASE * dj + TILE, REST), REST), :] for di in range(KERNEL)]
    turned = jnp.concatenate(parts + [jnp.zeros((REST, MIDDLE), BF16)], axis=0).T
    for src in range(2):
        rest_ref[pl.ds(pl.multiple_of(PACK * src + TILE * dj, REST), TILE), :] = turned[BASE * src : BASE * src + TILE]
        rest_ref[pl.ds(pl.multiple_of(PACK * src + REST_AT + REST * dj, REST), REST), :] = turned[BASE * src + TILE : BASE * src + BASE]


def bias_row(ref, start, size):
    return ref[pl.ds(start, size)].reshape(1, size)


def bias_rest(ref):
    return jnp.concatenate([bias_row(ref, TILE, REST), jnp.zeros((1, REST), F32)], axis=1)


def enter_barrier():
    barrier = pltpu.get_barrier_semaphore()
    for position in range(STRIPS):
        pl.semaphore_signal(barrier, inc=1, device_id=strip_device(position), device_id_type=MESH)
    return barrier


def fetch(sources, targets, sems):
    copies = [pltpu.make_async_copy(src, dst, sems.at[i]) for i, (src, dst) in enumerate(zip(sources, targets))]
    for copy in copies:
        copy.start()
    return copies


class Push:
    def __init__(self, src, dst, send_sem, recv_sem, device, here):
        self.here = here
        self.local = pltpu.make_async_copy(src, dst, recv_sem)
        self.remote = pltpu.make_async_remote_copy(
            src_ref=src, dst_ref=dst, send_sem=send_sem, recv_sem=recv_sem, device_id=device, device_id_type=MESH
        )

    def start(self):
        @pl.when(self.here)
        def _():
            self.local.start()

        @pl.when(jnp.logical_not(self.here))
        def _():
            self.remote.start()

    def wait_send(self):
        @pl.when(jnp.logical_not(self.here))
        def _():
            self.remote.wait_send()

    def wait_recv(self):
        self.remote.wait_recv()


def rest_sum(y_ref, row0, rows):
    total = y_ref[pl.ds(row0, rows), 0:LANES] + y_ref[pl.ds(row0 + TILE, rows), LANES:TILE]
    return total + pltpu.roll(y_ref[pl.ds(row0 + LANES, rows), 0:LANES], REST, axis=1)


def valid_rows(value, first_row, width):
    row = first_row + lax.broadcasted_iota(jnp.int32, value.shape, 0) // width
    return jnp.where((row >= 0) & (row < TILE), value, 0.0)


def pooled(value, width, scratch):
    rows, lanes = value.shape
    tall = jnp.concatenate(
        [jnp.maximum(value[s : s + width], value[s + width : s + 2 * width]) for s in range(0, rows, 2 * width)], axis=0
    )
    halves = []
    for start in range(0, lanes, LANES):
        scratch[0 : rows // 2, :] = tall[:, start : start + LANES]
        halves.append(
            jnp.maximum(scratch[pl.ds(0, rows // IN_CH, stride=2), :], scratch[pl.ds(1, rows // IN_CH, stride=2), :])
        )
    return jnp.concatenate(halves, axis=1) if len(halves) > 1 else halves[0]


def enc1_kernel(
    image_hbm, w_a_hbm, b_a_hbm, w_b, b_b_hbm, s1_out, p1_out,
    image, w_a, b_a, b_b, halves, planes, w_stem, staged, x_a, y_rest, w_main, w_rest, pool_buf, stage, stage_p, w_sem, small_sem, send_sem, recv_sem,
):
    step = pl.program_id(0)
    strip = strip_index()

    @pl.when(step == 0)
    def _():
        row = lax.axis_index("row")
        col = lax.axis_index("col")
        barrier = enter_barrier()
        small = fetch((image_hbm, w_a_hbm, b_a_hbm, b_b_hbm), (image, w_a, b_a, b_b), small_sem)
        copy_w = pltpu.make_async_copy(w_b, staged, w_sem)
        copy_w.start()
        stage[...] = jnp.zeros_like(stage)
        stage_p[...] = jnp.zeros_like(stage_p)

        for copy in small:
            copy.wait()
        for di in range(KERNEL):
            taps = []
            for dj in range(KERNEL):
                tap = jnp.concatenate([w_a[di, dj].astype(F32), jnp.zeros((IN_CH, BASE), F32)], axis=0)
                taps.append(jnp.concatenate([tap, jnp.zeros((STRIPS, REST), F32)], axis=1))
            taps.append(jnp.zeros((STRIPS, BASE_PAD), F32))
            w_stem[STRIP_ROWS * di : STRIP_ROWS * di + STRIP_ROWS, :] = jnp.concatenate(taps, axis=0).astype(BF16)
        planes[N40:N42, :, :] = jnp.zeros((2, STRIP_ROWS, LANES), BF16)

        pl.semaphore_wait(barrier, STRIPS)
        pushes = []
        for index, (target, src_row, dst_row, rows) in enumerate(
            ((2 * row, 0, IN_CH, N36), (2 * row + 1, N28, 0, N36), ((2 * row + 2) % STRIPS, N60, 0, IN_CH), ((2 * row + LAST_STRIP) % STRIPS, 0, N36, IN_CH))
        ):
            pushes.append(
                Push(
                    image.at[pl.ds(src_row, rows)],
                    halves.at[col, pl.ds(dst_row, rows)],
                    send_sem.at[index],
                    recv_sem.at[index // 2, col],
                    strip_device(target),
                    target == strip,
                )
            )
        for push in pushes:
            push.start()
        copy_w.wait()
        pack_weights(staged, w_main, w_rest)
        for push in pushes:
            push.wait_send()
        for kind, rows in ((0, N36), (1, IN_CH)):
            for side in range(2):
                Push(
                    image.at[pl.ds(0, rows)], halves.at[side, pl.ds(0, rows)],
                    send_sem.at[0], recv_sem.at[kind, side], strip_device(strip), strip < 0,
                ).wait_recv()

        def expand(i, carry):
            for j in range(STRIPS):
                r = STRIPS * i + j
                both = jnp.concatenate([halves[0, r].astype(F32), halves[1, r].astype(F32)], axis=1)
                image_row = STRIP_ROWS * strip - IN_CH + r
                both = jnp.where((image_row >= 0) & (image_row < TILE), both, 0.0)
                both = jnp.concatenate([both, jnp.zeros((IN_CH, LANES), F32)], axis=0)
                column = lax.broadcasted_iota(jnp.int32, (STRIPS, LANES), 1)
                before = jnp.where(column == 0, 0.0, pltpu.roll(both, 1, axis=1))
                after = jnp.where(column == N127, 0.0, pltpu.roll(both, N127, axis=1))
                planes[r] = jnp.concatenate([before, both, after, jnp.zeros((STRIPS, LANES), F32)], axis=0).astype(BF16)
            return carry

        lax.fori_loop(0, FIVE, expand, 0)

        def stem(i, carry):
            for j in range(STRIPS):
                r = STRIPS * i + j
                patch = jnp.concatenate([planes[r + di] for di in range(KERNEL)], axis=0)
                acc = lax.dot_general(patch, w_stem[...], (((0,), (0,)), ((), ())), preferred_element_type=F32)
                image_row = STRIP_ROWS * strip - KERNEL + r
                inside = (image_row >= 0) & (image_row < TILE)
                main = jnp.where(inside, jnp.maximum(acc[:, 0:TILE] + bias_row(b_a, 0, TILE), 0.0), 0.0)
                tail = jnp.where(inside, jnp.maximum(acc[:, TILE:BASE_PAD] + bias_rest(b_a), 0.0), 0.0)
                put3_320(x_a, pl.multiple_of(r * LANES, LANES), main, tail, LANES, stage.at[j % 2])
            return carry

        lax.fori_loop(0, FIVE, stem, 0)

    base = pl.multiple_of(step * N1536, N512)

    def rest(j):
        y_rest[TILE * j : TILE * j + TILE, :] = dot(packed_rows(x_a, base + TILE * j, TILE), w_rest[...])

    rest(0)
    for j in range(SIX):
        rest(j + 1)
        acc = dot(packed_rows(x_a, base + TILE * j, TILE), w_main[0:PACK, :])
        acc = acc + dot(packed_rows(x_a, base + TILE * j + LANES, TILE), w_main[PACK:N2048, :])
        acc = acc + dot(packed_rows(x_a, base + TILE * j + TILE, TILE), w_main[N2048:N3072, :])
        first_row = STRIP_ROWS * strip - 2 + N12 * step + 2 * j
        main = valid_rows(jnp.maximum(acc + bias_row(b_b, 0, TILE), 0.0), first_row, LANES)
        tail = jnp.maximum(rest_sum(y_rest, TILE * j, TILE) + bias_rest(b_b), 0.0)
        tail = low_lanes(valid_rows(tail, first_row, LANES))
        s1_out[TILE * j : TILE * j + TILE, 0:TILE] = main.astype(BF16)
        s1_out[TILE * j : TILE * j + TILE, TILE:BASE_PAD] = tail.astype(BF16)
        put3_320(p1_out, REST * j, pooled(main, LANES, pool_buf.at[j % 2]), pooled(tail, LANES, pool_buf.at[j % 2]), REST, stage_p.at[j % 2])


def mid_kernel(
    p1_hbm, w_2a, w_2b, w_ma, w_mb, w_u2, w_d2a, w_d2b, w_u1, w_d1a, b_2a_h, b_2b_h, b_ma_h, b_mb_h, b_d2a_h, b_d2b_h,
    out, um_out, ur_out, am_out, ar_out,
    b_2a, b_2b, b_ma, b_mb, b_d2a, b_d2b, wu_main, wu_rest, wa_main, wa_rest,
    p1, first_w, ring, x_a, x_s, x_u, m_1, m_2, m_o, d_2, acc_ref, wide, pool_buf,
    sem_2a, sem_2b, sem_ma, sem_mb, sem_u2, sem_d2a, sem_d2b, sem_p1, sem_out, turn_sem, small_sem, send_sem, recv_sem,
):
    strip = strip_index()
    prev_dev = strip_device((strip + LAST_STRIP) % STRIPS)
    next_dev = strip_device((strip + 1) % STRIPS)

    def exchange(buf, width, lane0, lanes, rows, index, target=None):
        target = buf if target is None else target
        lane = pl.ds(lane0, lanes)
        copies = []
        for side, src_row, dst_row, device in ((0, 1, rows + 1, prev_dev), (1, rows, 0, next_dev)):
            copies.append(
                pltpu.make_async_remote_copy(
                    src_ref=buf.at[pl.ds(src_row * width, width), lane],
                    dst_ref=target.at[pl.ds(dst_row * width, width), lane],
                    send_sem=send_sem.at[index, side],
                    recv_sem=recv_sem.at[index, side],
                    device_id=device,
                    device_id_type=MESH,
                )
            )
        return copies

    def start(copies):
        for copy in copies:
            copy.start()

    def finish(copies):
        for copy in copies:
            copy.wait()

    def halo(buf, width, channels, rows):
        for row, inside in ((0, strip > 0), (rows + 1, strip < LAST_STRIP)):
            value = buf[pl.ds(row * width, width), pl.ds(channels, channels)].astype(F32)
            put3(buf, row * width, 0, channels, jnp.where(inside, value, 0.0), width)

    copies_2a = []
    for tap in range(TAPS):
        di, dj = tap // KERNEL, tap % KERNEL
        for part, (start_row, size, row) in enumerate(((0, TILE, TILE * dj), (TILE, REST, REST_AT + REST * dj))):
            copies_2a.append(
                pltpu.make_async_copy(
                    w_2a.at[pl.ds(BASE * tap + start_row, size), :],
                    first_w.at[pl.ds(PACK * di + row, size), :],
                    sem_2a.at[2 * tap + part],
                )
            )

    def tap_copies(src, rows, base, sem):
        return [
            pltpu.make_async_copy(
                src.at[pl.ds(rows * tap, rows), :],
                ring.at[pl.ds(base + rows * (tap // 2), rows), pl.ds(MIDDLE * (tap % 2), MIDDLE)],
                sem.at[tap],
            )
            for tap in range(src.shape[0] // rows)
        ]

    copies_2b = tap_copies(w_2b, MIDDLE, 0, sem_2b)
    copies_ma = [
        pltpu.make_async_copy(w_ma.at[pl.ds(MIDDLE3 * di, MIDDLE3), :], ring.at[pl.ds(N3200 + MIDDLE3 * t, MIDDLE3), :], sem_ma.at[t])
        for t, di in enumerate((1, 0, 2))
    ]

    def mb_row(k):
        return (N8960 + DEEP * k) % RING_ROWS

    copies_mb = [
        pltpu.make_async_copy(
            w_mb.at[pl.ds(DEEP * (KERNEL * (1, 0, 2)[k // KERNEL] + k % KERNEL), DEEP), :], ring.at[pl.ds(mb_row(k), DEEP), :], sem_mb.at[k]
        )
        for k in range(TAPS)
    ]
    copies_u2 = [
        pltpu.make_async_copy(
            w_u2.at[pl.ds(DEEP * tap, DEEP), :],
            first_w.at[pl.ds(DEEP * tap, DEEP), :] if tap < 2 else ring.at[pl.ds(N8960, DEEP), pl.ds(MIDDLE * (tap - 2), MIDDLE)],
            sem_u2.at[tap],
        )
        for tap in range(IN_CH)
    ]
    st_u = ring.at[pl.ds(N10240, DEEP), pl.ds(0, MIDDLE)]
    copies_turn = [
        pltpu.make_async_copy(w_u1, st_u, turn_sem.at[0]),
        pltpu.make_async_copy(w_d1a, first_w.at[pl.ds(0, N2880), :], turn_sem.at[1]),
    ]
    copies_d2a = tap_copies(w_d2a, DEEP, 0, sem_d2a)
    copies_d2b = tap_copies(w_d2b, MIDDLE, N6400, sem_d2b)

    copy_p1 = pltpu.make_async_copy(p1_hbm, p1.at[:, pl.ds(0, N1152), :], sem_p1)
    barrier = pltpu.get_barrier_semaphore()
    for device in (prev_dev, next_dev):
        pl.semaphore_signal(barrier, inc=1, device_id=device, device_id_type=MESH)
    copy_p1.start()
    start(copies_2a)
    small = fetch(
        (b_2a_h, b_2b_h, b_ma_h, b_mb_h, b_d2a_h, b_d2b_h), (b_2a, b_2b, b_ma, b_mb, b_d2a, b_d2b), small_sem
    )
    pl.semaphore_wait(barrier, 2)

    for di in range(KERNEL):
        first_w[PACK * di + PACK_USED : PACK * di + PACK, :] = jnp.zeros((REST, MIDDLE), BF16)
    copy_p1.wait()
    finish(small)
    finish(copies_2a)
    start(copies_2b)
    start(copies_ma)

    ex_a = exchange(x_a, REST, MIDDLE, MIDDLE, N16, 0)
    ex_s = exchange(x_s, REST, MIDDLE, MIDDLE, N16, 1)
    ex_m1 = exchange(m_1, STRIP_ROWS, MIDDLE, MIDDLE, STRIPS, 2)
    ex_m2 = exchange(m_2, STRIP_ROWS, DEEP, DEEP, STRIPS, KERNEL)
    ex_u = exchange(x_u, REST, MIDDLE, MIDDLE, N16, IN_CH)
    ex_b = exchange(x_a, REST, MIDDLE, MIDDLE, N16, FIVE)
    ex_d = exchange(d_2, REST, 0, MIDDLE, N16, SIX, out)
    tiles = ((0, TILE), (TILE, TILE), (N512, LANES))

    def enc2a(i, carry):
        @pl.when(i == 1)
        def _():
            start(ex_a)

        for block in (i, KERNEL - i):
            row0 = pl.multiple_of(block * TILE, TILE)
            for lane0, lanes in tiles:
                acc = dot(packed_rows(p1, row0, TILE), first_w[0:PACK, pl.ds(lane0, lanes)])
                for di in (1, 2):
                    acc = acc + dot(
                        packed_rows(p1, row0 + REST * di, TILE),
                        first_w[PACK * di : PACK * di + PACK, pl.ds(lane0, lanes)],
                    )
                value = jnp.maximum(acc + bias_row(b_2a, lane0, lanes), 0.0)
                put3(x_a, row0 + REST, lane0, MIDDLE, value, REST)
        return carry

    lax.fori_loop(0, 2, enc2a, 0)
    finish(copies_2b)
    start(copies_mb[0:2])
    start(copies_u2[0:2])

    def conv640(src, row0, base, lane0, lanes):
        weights = jnp.concatenate(
            [
                ring[base + MIDDLE * (t // 2) : base + MIDDLE * (t // 2) + MIDDLE, pl.ds(MIDDLE * (t % 2) + lane0, lanes)]
                for t in range(TAPS)
            ],
            axis=0,
        )
        rows = jnp.concatenate([src[pl.ds(row0 + REST * di, TILE), :] for di in range(KERNEL)], axis=1)
        return dot(rows, weights)

    def enc2b(i, carry):
        block = i + 1 - 2 * (i % 2)
        row0 = pl.multiple_of(block * TILE, TILE)

        @pl.when(i == 1)
        def _():
            finish(ex_a)
            halo(x_a, REST, MIDDLE, N16)

        @pl.when(i == KERNEL)
        def _():
            start(ex_m1)
            start(ex_s)

        for lane0, lanes in tiles:
            value = jnp.maximum(conv640(x_a, row0, 0, lane0, lanes) + bias_row(b_2b, lane0, lanes), 0.0)
            put3(x_s, row0 + REST, lane0, MIDDLE, value, REST)
            put3(m_1, pl.multiple_of(block * REST + STRIP_ROWS, STRIP_ROWS), lane0, MIDDLE, pooled(value, REST, pool_buf), STRIP_ROWS)
        return carry

    lax.fori_loop(0, IN_CH, enc2b, 0)
    start(copies_mb[2:IN_CH])

    acc_ref[...] = jnp.zeros_like(acc_ref)
    finish(copies_ma)

    def mid_a(t, carry):
        di = (t + 1) % 2 + 2 * (t // 2) - t // 2

        @pl.when(t == 1)
        def _():
            start(copies_mb[IN_CH:SIX])
            finish(ex_m1)
            halo(m_1, STRIP_ROWS, MIDDLE, STRIPS)

        @pl.when(t == 2)
        def _():
            start(copies_mb[SIX:LAST_STRIP])

        base = pl.multiple_of(N3200 + MIDDLE3 * t, LANES)
        lhs_row = pl.multiple_of(STRIP_ROWS * di, STRIP_ROWS)
        for lane0 in range(0, DEEP, TILE):
            acc_ref[:, pl.ds(lane0, TILE)] += dot(
                m_1[pl.ds(lhs_row, TILE), :], ring[pl.ds(base, MIDDLE3), pl.ds(lane0, TILE)]
            )
        return carry

    lax.fori_loop(0, KERNEL, mid_a, 0)
    start(copies_mb[LAST_STRIP:TAPS])

    def mid_a_rows(first, rows):
        for lane0 in range(0, DEEP, TILE):
            value = jnp.maximum(acc_ref[pl.ds(first, rows), pl.ds(lane0, TILE)] + bias_row(b_ma, lane0, TILE), 0.0)
            put3(m_2, STRIP_ROWS + first, lane0, DEEP, value, STRIP_ROWS)

    mid_a_rows(0, STRIP_ROWS)
    mid_a_rows(N224, STRIP_ROWS)
    start(ex_m2)
    mid_a_rows(STRIP_ROWS, N192)
    acc_ref[...] = jnp.zeros_like(acc_ref)

    def mid_b(t, carry):
        di = (t + 1) % 2 + 2 * (t // 2) - t // 2

        for j in range(KERNEL):
            @pl.when(t == j)
            def _(j=j):
                finish(copies_mb[KERNEL * j : KERNEL * j + KERNEL])

        @pl.when(t == 1)
        def _():
            start(copies_u2[2:IN_CH])
            start(copies_d2a[0:2])
            finish(ex_m2)
            halo(m_2, STRIP_ROWS, DEEP, STRIPS)

        @pl.when(t == 2)
        def _():
            start(copies_d2a[2:STRIPS])

        lhs_row = pl.multiple_of(STRIP_ROWS * di, STRIP_ROWS)
        for lane0 in range(0, DEEP, TILE):
            acc = None
            for dj in range(KERNEL):
                base = pl.multiple_of(mb_row(KERNEL * t + dj), LANES)
                part = dot(
                    m_2[pl.ds(lhs_row, TILE), DEEP * dj : DEEP * dj + DEEP], ring[pl.ds(base, DEEP), pl.ds(lane0, TILE)]
                )
                acc = part if acc is None else acc + part
            acc_ref[:, pl.ds(lane0, TILE)] += acc
        return carry

    lax.fori_loop(0, KERNEL, mid_b, 0)
    start(copies_d2a[STRIPS:TAPS])
    for lane0 in range(0, DEEP, TILE):
        value = jnp.maximum(acc_ref[:, pl.ds(lane0, TILE)] + bias_row(b_mb, lane0, TILE), 0.0)
        m_o[:, pl.ds(lane0, TILE)] = value.astype(BF16)

    finish(copies_u2)
    for p in range(2):
        for q in range(2):
            for lane0, lanes in tiles:
                if p == 0:
                    weights = first_w[DEEP * q : DEEP * q + DEEP, pl.ds(lane0, lanes)]
                else:
                    weights = ring[N8960:N10240, pl.ds(MIDDLE * q + lane0, lanes)]
                part = dot(m_o[...], weights)
                for lane in range(0, lanes, LANES):
                    wide[(lane0 + lane) // LANES, pl.ds(q, TILE, stride=2), :] = part[:, lane : lane + LANES]

        if p == 0:
            start(copies_turn)

        def place(i, carry):
            src = pl.multiple_of(REST * i, REST)
            dst = pl.multiple_of(REST * (1 + 2 * i + p), REST)
            for lane0 in range(0, MIDDLE, LANES):
                put3(x_u, dst, lane0, MIDDLE, wide[lane0 // LANES, pl.ds(src, REST), :], REST)
            return carry

        lax.fori_loop(0, STRIPS, place, 0)
    start(ex_u)
    start(copies_d2b)
    finish(ex_s)
    halo(x_s, REST, MIDDLE, N16)
    finish(copies_d2a)
    finish(copies_turn)
    clear_pad(wa_main, SIX)
    clear_pad(wa_rest, 2)

    def dec2a(i, carry):
        block = i + 1 - 2 * (i % 2)
        row0 = pl.multiple_of(block * TILE, TILE)

        @pl.when(i == 1)
        def _():
            finish(ex_u)
            halo(x_u, REST, MIDDLE, N16)

        @pl.when(i == KERNEL)
        def _():
            start(ex_b)

        for lane0, lanes in tiles:
            acc = None
            for tap in range(TAPS):
                rows = pl.ds(row0 + REST * (tap // KERNEL), TILE)
                cols = pl.ds(MIDDLE * (tap % KERNEL), MIDDLE)
                lhs = jnp.concatenate([x_u[rows, cols], x_s[rows, cols]], axis=1)
                base = DEEP * (tap // 2)
                part = dot(lhs, ring[base : base + DEEP, pl.ds(MIDDLE * (tap % 2) + lane0, lanes)])
                acc = part if acc is None else acc + part
            value = jnp.maximum(acc + bias_row(b_d2a, lane0, lanes), 0.0)
            put3(x_a, row0 + REST, lane0, MIDDLE, value, REST)

        part = jnp.minimum(i, 2)
        for dj in range(KERNEL):
            turn_main(first_w, wa_main, part, dj)
        turn_rest(first_w, wa_rest, part)
        wu_main[pl.ds(pl.multiple_of(MIDDLE * i, REST), MIDDLE), :] = st_u[pl.ds(pl.multiple_of(BASE * i, REST), TILE), :].T
        wu_rest[...] = jnp.concatenate([st_u[BASE * tap + TILE : BASE * tap + BASE, :] for tap in range(IN_CH)], axis=0).T
        return carry

    lax.fori_loop(0, IN_CH, dec2a, 0)
    turned = [
        pltpu.make_async_copy(src, dst, turn_sem.at[2 + index])
        for index, (src, dst) in enumerate(((wu_main, um_out), (wu_rest, ur_out), (wa_main, am_out), (wa_rest, ar_out)))
    ]
    start(turned)
    finish(copies_d2b)

    def dec2b(i, carry):
        block = i + 1 - 2 * (i % 2)
        row0 = pl.multiple_of(block * TILE, TILE)

        @pl.when(i == 1)
        def _():
            finish(ex_b)
            halo(x_a, REST, MIDDLE, N16)

        @pl.when(i == KERNEL)
        def _():
            start(ex_d)

        for lane0, lanes in tiles:
            value = jnp.maximum(conv640(x_a, row0, N6400, lane0, lanes) + bias_row(b_d2b, lane0, lanes), 0.0)
            d_2[pl.ds(row0 + REST, TILE), pl.ds(lane0, lanes)] = value.astype(BF16)
        return carry

    lax.fori_loop(0, IN_CH, dec2b, 0)
    result = pltpu.make_async_copy(d_2.at[pl.ds(REST, PACK), :], out.at[pl.ds(REST, PACK), :], sem_out)
    result.start()
    finish(turned)
    finish(ex_d)
    result.wait()


def dec1_kernel(
    d_2, s1, um_h, ur_h, am_h, ar_h, w_d1b, b_d1a_h, b_d1b_h, w_head_h, b_head_h, out,
    b_d1a, b_d1b, w_head, b_head, x_u, x_s, x_d, y_rest, st_b, wu_main, wu_rest, wa_main, wa_rest, wb_main, wb_rest, wide, result, pending, stage, skip, low, late,
    sem, small_sem, send_sem, recv_sem,
):
    strip = strip_index()
    row = lax.axis_index("row")
    col = lax.axis_index("col")
    copy_um = pltpu.make_async_copy(um_h, wu_main, sem.at[0])
    copy_ur = pltpu.make_async_copy(ur_h, wu_rest, sem.at[1])
    copy_am = pltpu.make_async_copy(am_h, wa_main, sem.at[FIVE])
    copy_ar = pltpu.make_async_copy(ar_h, wa_rest, sem.at[SIX])
    copy_s = pltpu.make_async_copy(s1, skip, sem.at[2])
    copy_b = pltpu.make_async_copy(w_d1b, st_b, sem.at[KERNEL])
    copy_d = pltpu.make_async_copy(d_2, low, sem.at[IN_CH])
    barrier = enter_barrier()
    copy_um.start()
    copy_ur.start()
    copy_d.start()
    small = fetch((b_d1a_h, b_d1b_h, w_head_h, b_head_h), (b_d1a, b_d1b, w_head, b_head), small_sem)

    stage[...] = jnp.zeros_like(stage)
    copy_um.wait()
    copy_ur.wait()
    copy_s.start()
    copy_ar.start()
    copy_am.start()
    copy_b.start()
    copy_d.wait()
    for copy in small:
        copy.wait()

    def up1(i, carry):
        row0 = pl.multiple_of(i * BASE_PAD, LANES)
        lhs = low[pl.ds(row0, BASE_PAD), :]
        rest = dot(lhs, wu_rest[...])
        for p in range(2):
            part = rest[:, LANES * p : LANES * p + LANES]
            buf = wide.at[p]
            buf[2, pl.ds(0, BASE_PAD, stride=2), :] = low_lanes(part)
            buf[2, pl.ds(1, BASE_PAD, stride=2), :] = low_lanes(pltpu.roll(part, REST, axis=1))
            for q in range(2):
                tap = 2 * p + q
                main = dot(lhs, wu_main[MIDDLE * tap : MIDDLE * tap + MIDDLE, :])
                buf[0, pl.ds(q, BASE_PAD, stride=2), :] = main[:, 0:LANES]
                buf[1, pl.ds(q, BASE_PAD, stride=2), :] = main[:, LANES:TILE]
            for r in range(SIX):
                main = jnp.concatenate([buf[0, LANES * r : LANES * r + LANES, :], buf[1, LANES * r : LANES * r + LANES, :]], axis=1)
                put3_320(
                    x_u, pl.multiple_of((N12 * i + 2 * r + p) * LANES, LANES), main, buf[2, LANES * r : LANES * r + LANES, :], LANES
                )
        return carry

    lax.fori_loop(0, KERNEL, up1, 0)

    @pl.when(strip == 0)
    def _():
        x_u[:, 0:TILE, :] = jnp.zeros((STRIPS, TILE, LANES), BF16)

    @pl.when(strip == LAST_STRIP)
    def _():
        x_u[:, N4352:N4608, :] = jnp.zeros((STRIPS, TILE, LANES), BF16)

    copy_s.wait()
    copy_ar.wait()

    def rest_a(i, carry):
        base = pl.multiple_of(i * N1536, N512)

        def spread(j):
            rows = pl.ds(base + TILE * j, TILE)
            put3_320(
                x_s, base + TILE * j, skip[rows, 0:TILE].astype(F32), skip[rows, TILE:BASE_PAD].astype(F32), LANES, stage.at[j % 2]
            )

        spread(0)
        for j in range(SIX):
            rows = pl.ds(base + TILE * j, TILE)
            y_rest[rows, :] = dot(packed_rows(x_u, base + TILE * j, TILE), wa_rest[0:PACK, :]) + dot(
                packed_rows(x_s, base + TILE * j, TILE), wa_rest[PACK:N2048, :]
            )
            if j < FIVE:
                spread(j + 1)
        return carry

    lax.fori_loop(0, KERNEL, rest_a, 0)
    copy_am.wait()

    def conv_a(row0):
        acc = None
        for di in range(KERNEL):
            for src, ref in enumerate((x_u, x_s)):
                base = N3072 * src + PACK * di
                part = dot(packed_rows(ref, row0 + LANES * di, TILE), wa_main[base : base + PACK, :])
                acc = part if acc is None else acc + part
        return acc

    def put_a(acc, row0, first_row, slot):
        main = valid_rows(jnp.maximum(acc + bias_row(b_d1a, 0, TILE), 0.0), first_row, LANES)
        tail = valid_rows(jnp.maximum(rest_sum(y_rest, row0, TILE) + bias_rest(b_d1a), 0.0), first_row, LANES)
        put3_320(x_d, row0, main, low_lanes(tail), LANES, stage.at[slot])

    late[...] = jnp.zeros_like(late)

    def dec1a(i, carry):
        base = pl.multiple_of(i * PACK, PACK)
        put_a(late[...], pl.multiple_of(jnp.maximum(base - TILE, 0), TILE), STRIP_ROWS * strip - KERNEL + STRIPS * i, 1)
        for j in range(IN_CH):
            acc = conv_a(base + TILE * j)
            if j == KERNEL:
                late[...] = acc
            else:
                put_a(acc, base + TILE * j, STRIP_ROWS * strip - 1 + STRIPS * i + 2 * j, j % 2)
        return carry

    lax.fori_loop(0, IN_CH, dec1a, 0)
    put_a(late[...], N3840, STRIP_ROWS * strip + N29, 1)
    put_a(conv_a(N4096), N4096, STRIP_ROWS * strip + N31, 0)

    copy_b.wait()
    pack_weights(st_b, wb_main, wb_rest)
    head_bias = jnp.zeros((IN_CH, LANES), F32)
    for channel in range(IN_CH):
        head_bias = jnp.where(lax.broadcasted_iota(jnp.int32, (IN_CH, LANES), 0) == channel, b_head[channel], head_bias)

    pending[...] = jnp.zeros_like(pending)

    def head(hidden, row0):
        line = lax.dot_general(w_head[...], hidden, (((1,), (1,)), ((), ())), preferred_element_type=F32)
        for r in range(2):
            part = line[:, LANES * r : LANES * r + LANES] + head_bias
            result[0, row0 + r] = part[:, 0:REST]
            result[1, row0 + r] = part[:, REST:LANES]

    def dec1b(i, carry):
        base = pl.multiple_of(i * PACK, PACK)

        def rest(j):
            y_rest[TILE * j : TILE * j + TILE, :] = dot(packed_rows(x_d, base + TILE * j, TILE), wb_rest[...])

        rest(0)
        waiting = pending[...]
        for j in range(IN_CH):
            rest(j + 1)
            acc = dot(packed_rows(x_d, base + TILE * j, TILE), wb_main[0:PACK, :])
            acc = acc + dot(packed_rows(x_d, base + TILE * j + LANES, TILE), wb_main[PACK:N2048, :])
            acc = acc + dot(packed_rows(x_d, base + TILE * j + TILE, TILE), wb_main[N2048:N3072, :])
            head(waiting, jnp.maximum(STRIPS * i + 2 * j - 2, 0))
            main = jnp.maximum(acc + bias_row(b_d1b, 0, TILE), 0.0).astype(BF16)
            tail = jnp.maximum(rest_sum(y_rest, TILE * j, TILE) + bias_rest(b_d1b), 0.0).astype(BF16)
            waiting = jnp.concatenate([main, tail[:, 0:REST]], axis=1)
        pending[...] = waiting
        return carry

    pushes = []
    for part, first, rows in ((0, 0, N22), (1, N22, N10)):
        for side in range(2):
            pushes.append(
                Push(
                    result.at[side, pl.ds(first, rows)],
                    out.at[pl.ds(STRIP_ROWS * (strip % 2) + first, rows)],
                    send_sem.at[part, side],
                    recv_sem.at[part, strip % 2],
                    (lax.axis_index("data"), side, strip // 2),
                    (strip // 2 == row) & (col == side),
                )
            )

    lax.fori_loop(0, KERNEL, dec1b, 0)
    pl.semaphore_wait(barrier, STRIPS)
    for push in pushes[0:2]:
        push.start()
    lax.fori_loop(KERNEL, IN_CH, dec1b, 0)
    head(pending[...], N30)

    for push in pushes[2:IN_CH]:
        push.start()
    for push in pushes:
        push.wait_send()
    for part, first, rows in ((0, 0, N22), (1, N22, N10)):
        for half in range(2):
            Push(
                result.at[0, pl.ds(first, rows)], out.at[pl.ds(STRIP_ROWS * half + first, rows)],
                send_sem.at[part, 0], recv_sem.at[part, half], strip_device(strip), strip < 0,
            ).wait_recv()


def solution(mesh):
    tile_spec = P(("data", "row"), "col", None)

    def body(image_tile, *params):
        (w_enc1a, b_enc1a, w_enc1b, b_enc1b, w_enc2a, b_enc2a, w_enc2b, b_enc2b,
         w_mid_a, b_mid_a, w_mid_b, b_mid_b, w_up2, w_dec2a, b_dec2a, w_dec2b, b_dec2b,
         w_up1, w_dec1a, b_dec1a, w_dec1b, b_dec1b, w_head, b_head) = params
        def flat(weight):
            return weight.reshape(-1, weight.shape[-1])

        hbm = pl.BlockSpec(memory_space=pl.ANY)
        dma = pltpu.SemaphoreType.DMA
        s1, p1 = pl.pallas_call(
            enc1_kernel,
            grid=(KERNEL,),
            out_shape=(jax.ShapeDtypeStruct((N4608, BASE_PAD), BF16), jax.ShapeDtypeStruct((STRIPS, N1152, LANES), BF16)),
            in_specs=[hbm] * FIVE,
            out_specs=(pl.BlockSpec((N1536, BASE_PAD), lambda i: (i, 0)), pl.BlockSpec((STRIPS, BASE_PAD, LANES), lambda i: (0, i, 0))),
            scratch_shapes=[
                pltpu.VMEM((REST, IN_CH, REST), BF16),
                pltpu.VMEM((KERNEL, KERNEL, IN_CH, BASE), BF16),
                pltpu.VMEM((BASE,), F32),
                pltpu.VMEM((BASE,), F32),
                pltpu.VMEM((2, N40, IN_CH, REST), BF16),
                pltpu.VMEM((N42, STRIP_ROWS, LANES), BF16),
                pltpu.VMEM((N96, BASE_PAD), BF16),
                pltpu.VMEM((N2880, BASE), BF16),
                pltpu.VMEM((STRIPS, N5136, LANES), BF16),
                pltpu.VMEM((N1792, TILE), F32),
                pltpu.VMEM((N3072, TILE), BF16),
                pltpu.VMEM((PACK, TILE), BF16),
                pltpu.VMEM((2, LANES, LANES), F32),
                pltpu.VMEM((2, KERNEL, N288, LANES), F32),
                pltpu.VMEM((2, KERNEL, N80, LANES), F32),
                dma, dma((IN_CH,)), dma((IN_CH,)), dma((2, 2)),
            ],
            compiler_params=pltpu.CompilerParams(
                vmem_limit_bytes=VMEM_LIMIT, collective_id=1, has_side_effects=True, dimension_semantics=("arbitrary",)
            ),
            name="enc1",
        )(image_tile.transpose(0, 2, 1), w_enc1a, b_enc1a, flat(w_enc1b), b_enc1b)

        turned_shapes = ((N2560, TILE), (MIDDLE, TILE), (N6144, TILE), (N2048, TILE))

        def turned(weight):
            return weight.transpose(0, 1, KERNEL, 2).reshape(-1, weight.shape[2])

        d2, *level_one = pl.pallas_call(
            mid_kernel,
            out_shape=[jax.ShapeDtypeStruct(shape, BF16) for shape in ((N1152, MIDDLE),) + turned_shapes],
            in_specs=[hbm] * N16,
            out_specs=[hbm] * FIVE,
            scratch_shapes=[
                *[pltpu.VMEM((size,), F32) for size in (MIDDLE, MIDDLE, DEEP, DEEP, MIDDLE, MIDDLE)],
                *[pltpu.VMEM(shape, BF16) for shape in turned_shapes],
                pltpu.VMEM((STRIPS, N1168, LANES), BF16),
                pltpu.VMEM((N3072, MIDDLE), BF16),
                pltpu.VMEM((RING_ROWS, DEEP), BF16),
                pltpu.VMEM((N1152, MIDDLE3), BF16),
                pltpu.VMEM((N1152, MIDDLE3), BF16),
                pltpu.VMEM((N1152, MIDDLE3), BF16),
                pltpu.VMEM((BASE, MIDDLE3), BF16),
                pltpu.VMEM((BASE, N3840), BF16),
                pltpu.VMEM((TILE, DEEP), BF16),
                pltpu.VMEM((N1152, MIDDLE), BF16),
                pltpu.VMEM((TILE, DEEP), F32),
                pltpu.VMEM((FIVE, N512, LANES), F32),
                pltpu.VMEM((LANES, LANES), F32),
                dma((N18,)), dma((TAPS,)), dma((KERNEL,)), dma((TAPS,)), dma((IN_CH,)), dma((TAPS,)), dma((TAPS,)), dma, dma, dma((SIX,)), dma((SIX,)),
                dma((LAST_STRIP, 2)), dma((LAST_STRIP, 2)),
            ],
            compiler_params=pltpu.CompilerParams(
                vmem_limit_bytes=VMEM_LIMIT, collective_id=0, has_side_effects=True
            ),
            name="mid",
        )(
            p1, flat(w_enc2a), flat(w_enc2b), flat(w_mid_a), flat(w_mid_b), flat(w_up2), flat(w_dec2a), flat(w_dec2b),
            turned(w_up1), turned(w_dec1a),
            b_enc2a, b_enc2b, b_mid_a, b_mid_b, b_dec2a, b_dec2b,
        )

        y = pl.pallas_call(
            dec1_kernel,
            out_shape=jax.ShapeDtypeStruct((REST, IN_CH, REST), F32),
            in_specs=[hbm] * N11,
            out_specs=hbm,
            scratch_shapes=[
                pltpu.VMEM((BASE,), F32),
                pltpu.VMEM((BASE,), F32),
                pltpu.VMEM((IN_CH, BASE), BF16),
                pltpu.SMEM((IN_CH,), F32),
                pltpu.VMEM((STRIPS, N4624, LANES), BF16),
                pltpu.VMEM((STRIPS, N4624, LANES), BF16),
                pltpu.VMEM((STRIPS, N4368, LANES), BF16),
                pltpu.VMEM((N4608, TILE), F32),
                pltpu.VMEM((N2880, BASE), BF16),
                pltpu.VMEM((N2560, TILE), BF16),
                pltpu.VMEM((MIDDLE, TILE), BF16),
                pltpu.VMEM((N6144, TILE), BF16),
                pltpu.VMEM((N2048, TILE), BF16),
                pltpu.VMEM((N3072, TILE), BF16),
                pltpu.VMEM((PACK, TILE), BF16),
                pltpu.VMEM((2, KERNEL, REST_AT, LANES), F32),
                pltpu.VMEM((2, STRIP_ROWS, IN_CH, REST), F32),
                pltpu.VMEM((TILE, BASE), BF16),
                pltpu.VMEM((2, KERNEL, N288, LANES), F32),
                pltpu.VMEM((N4608, BASE_PAD), BF16),
                pltpu.VMEM((N1152, MIDDLE), BF16),
                pltpu.VMEM((TILE, TILE), F32),
                dma((LAST_STRIP,)), dma((IN_CH,)), dma((2, 2)), dma((2, 2)),
            ],
            compiler_params=pltpu.CompilerParams(vmem_limit_bytes=VMEM_LIMIT, collective_id=2, has_side_effects=True),
            name="dec1",
        )(d2, s1, *level_one, flat(w_dec1b), b_dec1a, b_dec1b, w_head.T, b_head)
        return y.transpose(0, 2, 1)

    def program(image, *params):
        mapped = jax.shard_map(
            body, mesh=mesh, in_specs=(tile_spec,) + (P(),) * len(params), out_specs=tile_spec, check_vma=False
        )
        return mapped(image, *params)

    return program
```

```python
import functools

import jax
import jax.numpy as jnp
from jax import lax
from jax.experimental import pallas as pl
from jax.experimental.pallas import tpu as pltpu
from jax.sharding import PartitionSpec as P

KERNEL = 3
IN_CH = 4
FIVE = 5
SIX = 6
LAST_STRIP = 7
STRIPS = 8
TAPS = 9
N10 = 10
N11 = 11
N12 = 12
N16 = 16
N17 = 17
N18 = 18
N22 = 22
N28 = 28
N29 = 29
N30 = 30
N31 = 31
STRIP_ROWS = 32
N36 = 36
N40 = 40
N42 = 42
N50 = 50
N60 = 60
REST = 64
N80 = 80
N96 = 96
N127 = 127
LANES = 128
N192 = 192
N224 = 224
TILE = 256
N288 = 288
BASE = 320
BASE_PAD = 384
N512 = 512
MIDDLE = 640
REST_AT = 768
PACK_USED = 960
PACK = 1024
N1152 = 1152
N1168 = 1168
DEEP = 1280
N1536 = 1536
N1792 = 1792
MIDDLE3 = 1920
N2048 = 2048
N2560 = 2560
N2880 = 2880
N3072 = 3072
N3200 = 3200
N3840 = 3840
N4096 = 4096
N4368 = 4368
N4608 = 4608
N4624 = 4624
N5136 = 5136
N6144 = 6144
N6400 = 6400
N8960 = 8960
N10240 = 10240
N11520 = 11520
BF16 = jnp.bfloat16
F32 = jnp.float32
MESH = pl.DeviceIdType.MESH
VMEM_LIMIT = 66_900_000
RING_ROWS = N11520


def strip_index():
    col = lax.axis_index("col")
    row = lax.axis_index("row")
    return row + col * (LAST_STRIP - 2 * row)


def strip_device(position):
    col = position // IN_CH
    rest = position % IN_CH
    return (lax.axis_index("data"), col, rest + col * (KERNEL - 2 * rest))


def dot(a, b):
    return jnp.dot(a, b, preferred_element_type=F32)


def shifted(value, width, step):
    if step == 1:
        return value
    rows = value.shape[0]
    column = lax.broadcasted_iota(jnp.int32, value.shape, 0) % width
    if step == 0:
        return jnp.where(column == 0, 0.0, pltpu.roll(value, 1, axis=0))
    return jnp.where(column == width - 1, 0.0, pltpu.roll(value, rows - 1, axis=0))


def put3(dst, row0, lane0, channels, value, width):
    rows, lanes = value.shape
    for step in range(KERNEL):
        dst[pl.ds(row0, rows), pl.ds(step * channels + lane0, lanes)] = shifted(value, width, step).astype(BF16)


def put3_320(dst, row0, main, rest, width, stage=None):
    rows = main.shape[0]
    pitch = width + N16
    planes = [main[:, 0:LANES], main[:, LANES:TILE], rest]
    for t, plane in enumerate(planes if stage is not None else []):
        for r in range(rows // width):
            stage[t, pitch * r + STRIPS : pitch * r + STRIPS + width, :] = plane[width * r : width * r + width]

    def moved(t, step):
        if stage is None:
            return shifted(planes[t], width, step)
        first = LAST_STRIP + step
        parts = [stage[t, pitch * r + first : pitch * r + first + width, :] for r in range(rows // width)]
        return jnp.concatenate(parts, axis=0) if len(parts) > 1 else parts[0]

    for step in range(KERNEL):
        for t in range(2):
            dst[2 * step + t, pl.ds(row0, rows), :] = moved(t, step).astype(BF16)
    first = moved(2, 0) + pltpu.roll(moved(2, 1), REST, axis=1)
    dst[SIX, pl.ds(row0, rows), :] = first.astype(BF16)
    dst[LAST_STRIP, pl.ds(row0, rows), :] = moved(2, 2).astype(BF16)


def packed_rows(ref, row0, rows):
    return jnp.concatenate([ref[t, pl.ds(row0, rows), :] for t in range(STRIPS)], axis=1)


def low_lanes(value):
    return jnp.where(lax.broadcasted_iota(jnp.int32, value.shape, 1) < REST, value, 0.0)


def pack_weights(staged, main_ref, rest_ref):
    for dj in range(KERNEL):
        for start, size, row in ((0, TILE, TILE * dj), (TILE, REST, REST_AT + REST * dj)):
            parts = []
            for di in range(KERNEL):
                base = (KERNEL * di + dj) * BASE + start
                main_ref[pl.ds(PACK * di + row, size), :] = staged[pl.ds(base, size), 0:TILE]
                parts.append(staged[pl.ds(base, size), TILE:BASE])
            parts.append(jnp.zeros((size, REST), BF16))
            rest_ref[pl.ds(row, size), :] = jnp.concatenate(parts, axis=1)
    clear_pad(main_ref, KERNEL)
    clear_pad(rest_ref, 1)


def clear_pad(ref, groups):
    for group in range(groups):
        ref[pl.ds(PACK * group + PACK_USED, REST), :] = jnp.zeros((REST, ref.shape[1]), BF16)


def turn_main(staged, main_ref, di, dj):
    turned = staged[pl.ds(pl.multiple_of(PACK_USED * di + BASE * dj, REST), TILE), :].T
    for src in range(2):
        base = N3072 * src + PACK * di
        main_ref[pl.ds(pl.multiple_of(base + TILE * dj, REST), TILE), :] = turned[BASE * src : BASE * src + TILE]
        main_ref[pl.ds(pl.multiple_of(base + REST_AT + REST * dj, REST), REST), :] = turned[BASE * src + TILE : BASE * src + BASE]


def turn_rest(staged, rest_ref, dj):
    parts = [staged[pl.ds(pl.multiple_of(PACK_USED * di + BASE * dj + TILE, REST), REST), :] for di in range(KERNEL)]
    turned = jnp.concatenate(parts + [jnp.zeros((REST, MIDDLE), BF16)], axis=0).T
    for src in range(2):
        rest_ref[pl.ds(pl.multiple_of(PACK * src + TILE * dj, REST), TILE), :] = turned[BASE * src : BASE * src + TILE]
        rest_ref[pl.ds(pl.multiple_of(PACK * src + REST_AT + REST * dj, REST), REST), :] = turned[BASE * src + TILE : BASE * src + BASE]


def bias_row(ref, start, size):
    return ref[pl.ds(start, size)].reshape(1, size)


def bias_rest(ref):
    return jnp.concatenate([bias_row(ref, TILE, REST), jnp.zeros((1, REST), F32)], axis=1)


def enter_barrier():
    barrier = pltpu.get_barrier_semaphore()
    for position in range(STRIPS):
        pl.semaphore_signal(barrier, inc=1, device_id=strip_device(position), device_id_type=MESH)
    return barrier


def fetch(sources, targets, sems):
    copies = [pltpu.make_async_copy(src, dst, sems.at[i]) for i, (src, dst) in enumerate(zip(sources, targets))]
    for copy in copies:
        copy.start()
    return copies


class Push:
    def __init__(self, src, dst, send_sem, recv_sem, device, here):
        self.here = here
        self.local = pltpu.make_async_copy(src, dst, recv_sem)
        self.remote = pltpu.make_async_remote_copy(
            src_ref=src, dst_ref=dst, send_sem=send_sem, recv_sem=recv_sem, device_id=device, device_id_type=MESH
        )

    def start(self):
        @pl.when(self.here)
        def _():
            self.local.start()

        @pl.when(jnp.logical_not(self.here))
        def _():
            self.remote.start()

    def wait_send(self):
        @pl.when(jnp.logical_not(self.here))
        def _():
            self.remote.wait_send()

    def wait_recv(self):
        self.remote.wait_recv()


def rest_sum(y_ref, row0, rows):
    total = y_ref[pl.ds(row0, rows), 0:LANES] + y_ref[pl.ds(row0 + TILE, rows), LANES:TILE]
    return total + pltpu.roll(y_ref[pl.ds(row0 + LANES, rows), 0:LANES], REST, axis=1)


def valid_rows(value, first_row, width):
    row = first_row + lax.broadcasted_iota(jnp.int32, value.shape, 0) // width
    return jnp.where((row >= 0) & (row < TILE), value, 0.0)


def pooled(value, width, scratch):
    rows, lanes = value.shape
    tall = jnp.concatenate(
        [jnp.maximum(value[s : s + width], value[s + width : s + 2 * width]) for s in range(0, rows, 2 * width)], axis=0
    )
    halves = []
    for start in range(0, lanes, LANES):
        scratch[0 : rows // 2, :] = tall[:, start : start + LANES]
        halves.append(
            jnp.maximum(scratch[pl.ds(0, rows // IN_CH, stride=2), :], scratch[pl.ds(1, rows // IN_CH, stride=2), :])
        )
    return jnp.concatenate(halves, axis=1) if len(halves) > 1 else halves[0]


def enc1_kernel(
    image_hbm, w_a_hbm, b_a_hbm, w_b, b_b_hbm, s1_out, p1_out,
    image, w_a, b_a, b_b, halves, planes, w_stem, staged, x_a, y_rest, w_main, w_rest, pool_buf, stage, stage_p, w_sem, small_sem, send_sem, recv_sem,
):
    step = pl.program_id(0)
    strip = strip_index()

    @pl.when(step == 0)
    def _():
        row = lax.axis_index("row")
        col = lax.axis_index("col")
        barrier = enter_barrier()
        small = fetch((image_hbm, w_a_hbm, b_a_hbm, b_b_hbm), (image, w_a, b_a, b_b), small_sem)
        copy_w = pltpu.make_async_copy(w_b, staged, w_sem)
        copy_w.start()
        stage[...] = jnp.zeros_like(stage)
        stage_p[...] = jnp.zeros_like(stage_p)

        for copy in small:
            copy.wait()
        for di in range(KERNEL):
            taps = []
            for dj in range(KERNEL):
                tap = jnp.concatenate([w_a[di, dj].astype(F32), jnp.zeros((IN_CH, BASE), F32)], axis=0)
                taps.append(jnp.concatenate([tap, jnp.zeros((STRIPS, REST), F32)], axis=1))
            taps.append(jnp.zeros((STRIPS, BASE_PAD), F32))
            w_stem[STRIP_ROWS * di : STRIP_ROWS * di + STRIP_ROWS, :] = jnp.concatenate(taps, axis=0).astype(BF16)

        planes[N40:N42, :, :] = jnp.zeros((2, STRIP_ROWS, LANES), BF16)

        pl.semaphore_wait(barrier, STRIPS)
        pushes = []
        for index, (target, src_row, dst_row, rows) in enumerate(
            ((2 * row, 0, IN_CH, N36), (2 * row + 1, N28, 0, N36), ((2 * row + 2) % STRIPS, N60, 0, IN_CH), ((2 * row + LAST_STRIP) % STRIPS, 0, N36, IN_CH))
        ):
            pushes.append(
                Push(
                    image.at[pl.ds(src_row, rows)],
                    halves.at[col, pl.ds(dst_row, rows)],
                    send_sem.at[index],
                    recv_sem.at[index // 2, col],
                    strip_device(target),
                    target == strip,
                )
            )
        for push in pushes:
            push.start()
        copy_w.wait()
        pack_weights(staged, w_main, w_rest)
        for push in pushes:
            push.wait_send()
        for kind, rows in ((0, N36), (1, IN_CH)):
            for side in range(2):
                Push(
                    image.at[pl.ds(0, rows)], halves.at[side, pl.ds(0, rows)],
                    send_sem.at[0], recv_sem.at[kind, side], strip_device(strip), strip < 0,
                ).wait_recv()

        def expand(i, carry):
            for j in range(STRIPS):
                r = STRIPS * i + j
                both = jnp.concatenate([halves[0, r].astype(F32), halves[1, r].astype(F32)], axis=1)
                image_row = STRIP_ROWS * strip - IN_CH + r
                both = jnp.where((image_row >= 0) & (image_row < TILE), both, 0.0)
                both = jnp.concatenate([both, jnp.zeros((IN_CH, LANES), F32)], axis=0)
                column = lax.broadcasted_iota(jnp.int32, (STRIPS, LANES), 1)
                before = jnp.where(column == 0, 0.0, pltpu.roll(both, 1, axis=1))
                after = jnp.where(column == N127, 0.0, pltpu.roll(both, N127, axis=1))
                planes[r] = jnp.concatenate([before, both, after, jnp.zeros((STRIPS, LANES), F32)], axis=0).astype(BF16)
            return carry

        lax.fori_loop(0, FIVE, expand, 0)

        def stem(i, carry):
            for j in range(STRIPS):
                r = STRIPS * i + j
                patch = jnp.concatenate([planes[r + di] for di in range(KERNEL)], axis=0)
                acc = lax.dot_general(patch, w_stem[...], (((0,), (0,)), ((), ())), preferred_element_type=F32)
                image_row = STRIP_ROWS * strip - KERNEL + r
                inside = (image_row >= 0) & (image_row < TILE)
                main = jnp.where(inside, jnp.maximum(acc[:, 0:TILE] + bias_row(b_a, 0, TILE), 0.0), 0.0)
                tail = jnp.where(inside, jnp.maximum(acc[:, TILE:BASE_PAD] + bias_rest(b_a), 0.0), 0.0)
                put3_320(x_a, pl.multiple_of(r * LANES, LANES), main, tail, LANES, stage.at[j % 2])
            return carry

        lax.fori_loop(0, FIVE, stem, 0)

    base = pl.multiple_of(step * N1536, N512)

    def rest(j):
        y_rest[TILE * j : TILE * j + TILE, :] = dot(packed_rows(x_a, base + TILE * j, TILE), w_rest[...])

    rest(0)
    for j in range(SIX):
        rest(j + 1)
        acc = dot(packed_rows(x_a, base + TILE * j, TILE), w_main[0:PACK, :])
        acc = acc + dot(packed_rows(x_a, base + TILE * j + LANES, TILE), w_main[PACK:N2048, :])
        acc = acc + dot(packed_rows(x_a, base + TILE * j + TILE, TILE), w_main[N2048:N3072, :])
        first_row = STRIP_ROWS * strip - 2 + N12 * step + 2 * j
        main = valid_rows(jnp.maximum(acc + bias_row(b_b, 0, TILE), 0.0), first_row, LANES)
        tail = jnp.maximum(rest_sum(y_rest, TILE * j, TILE) + bias_rest(b_b), 0.0)
        tail = low_lanes(valid_rows(tail, first_row, LANES))
        s1_out[TILE * j : TILE * j + TILE, 0:TILE] = main.astype(BF16)
        s1_out[TILE * j : TILE * j + TILE, TILE:BASE_PAD] = tail.astype(BF16)
        put3_320(p1_out, REST * j, pooled(main, LANES, pool_buf.at[j % 2]), pooled(tail, LANES, pool_buf.at[j % 2]), REST, stage_p.at[j % 2])


def mid_kernel(
    p1_hbm, w_2a, w_2b, w_ma, w_mb, w_u2, w_d2a, w_d2b, w_u1, w_d1a, b_2a_h, b_2b_h, b_ma_h, b_mb_h, b_d2a_h, b_d2b_h,
    out, um_out, ur_out, am_out, ar_out,
    b_2a, b_2b, b_ma, b_mb, b_d2a, b_d2b, wu_main, wu_rest, wa_main, wa_rest,
    p1, first_w, ring, x_a, x_s, x_u, m_1, m_2, m_o, d_2, acc_ref, wide, pool_buf,
    sem_2a, sem_2b, sem_ma, sem_mb, sem_u2, sem_d2a, sem_d2b, sem_p1, sem_out, turn_sem, small_sem, send_sem, recv_sem,
):
    strip = strip_index()
    prev_dev = strip_device((strip + LAST_STRIP) % STRIPS)
    next_dev = strip_device((strip + 1) % STRIPS)

    def exchange(buf, width, lane0, lanes, rows, index, target=None):
        target = buf if target is None else target
        lane = pl.ds(lane0, lanes)
        copies = []
        for side, src_row, dst_row, device in ((0, 1, rows + 1, prev_dev), (1, rows, 0, next_dev)):
            copies.append(
                pltpu.make_async_remote_copy(
                    src_ref=buf.at[pl.ds(src_row * width, width), lane],
                    dst_ref=target.at[pl.ds(dst_row * width, width), lane],
                    send_sem=send_sem.at[index, side],
                    recv_sem=recv_sem.at[index, side],
                    device_id=device,
                    device_id_type=MESH,
                )
            )
        return copies

    def start(copies):
        for copy in copies:
            copy.start()

    def finish(copies):
        for copy in copies:
            copy.wait()

    def halo(buf, width, channels, rows):
        for row, inside in ((0, strip > 0), (rows + 1, strip < LAST_STRIP)):
            value = buf[pl.ds(row * width, width), pl.ds(channels, channels)].astype(F32)
            put3(buf, row * width, 0, channels, jnp.where(inside, value, 0.0), width)

    copies_2a = []
    for tap in range(TAPS):
        di, dj = tap // KERNEL, tap % KERNEL
        for part, (start_row, size, row) in enumerate(((0, TILE, TILE * dj), (TILE, REST, REST_AT + REST * dj))):
            copies_2a.append(
                pltpu.make_async_copy(
                    w_2a.at[pl.ds(BASE * tap + start_row, size), :],
                    first_w.at[pl.ds(PACK * di + row, size), :],
                    sem_2a.at[2 * tap + part],
                )
            )

    def tap_copies(src, rows, base, sem):
        return [
            pltpu.make_async_copy(
                src.at[pl.ds(rows * tap, rows), :],
                ring.at[pl.ds(base + rows * (tap // 2), rows), pl.ds(MIDDLE * (tap % 2), MIDDLE)],
                sem.at[tap],
            )
            for tap in range(src.shape[0] // rows)
        ]

    copies_2b = tap_copies(w_2b, MIDDLE, 0, sem_2b)
    copies_ma = [
        pltpu.make_async_copy(w_ma.at[pl.ds(MIDDLE3 * di, MIDDLE3), :], ring.at[pl.ds(N3200 + MIDDLE3 * t, MIDDLE3), :], sem_ma.at[t])
        for t, di in enumerate((1, 0, 2))
    ]

    def mb_row(k):
        return (N8960 + DEEP * k) % RING_ROWS

    copies_mb = [
        pltpu.make_async_copy(
            w_mb.at[pl.ds(DEEP * (KERNEL * (1, 0, 2)[k // KERNEL] + k % KERNEL), DEEP), :], ring.at[pl.ds(mb_row(k), DEEP), :], sem_mb.at[k]
        )
        for k in range(TAPS)
    ]
    copies_u2 = [
        pltpu.make_async_copy(
            w_u2.at[pl.ds(DEEP * tap, DEEP), :],
            first_w.at[pl.ds(DEEP * tap, DEEP), :] if tap < 2 else ring.at[pl.ds(N8960, DEEP), pl.ds(MIDDLE * (tap - 2), MIDDLE)],
            sem_u2.at[tap],
        )
        for tap in range(IN_CH)
    ]
    st_u = ring.at[pl.ds(N10240, DEEP), pl.ds(0, MIDDLE)]
    copies_turn = [
        pltpu.make_async_copy(w_u1, st_u, turn_sem.at[0]),
        pltpu.make_async_copy(w_d1a, first_w.at[pl.ds(0, N2880), :], turn_sem.at[1]),
    ]
    copies_d2a = tap_copies(w_d2a, DEEP, 0, sem_d2a)
    copies_d2b = tap_copies(w_d2b, MIDDLE, N6400, sem_d2b)

    copy_p1 = pltpu.make_async_copy(p1_hbm, p1.at[:, pl.ds(0, N1152), :], sem_p1)
    barrier = pltpu.get_barrier_semaphore()
    for device in (prev_dev, next_dev):
        pl.semaphore_signal(barrier, inc=1, device_id=device, device_id_type=MESH)
    copy_p1.start()
    start(copies_2a)
    small = fetch(
        (b_2a_h, b_2b_h, b_ma_h, b_mb_h, b_d2a_h, b_d2b_h), (b_2a, b_2b, b_ma, b_mb, b_d2a, b_d2b), small_sem
    )
    pl.semaphore_wait(barrier, 2)

    for di in range(KERNEL):
        first_w[PACK * di + PACK_USED : PACK * di + PACK, :] = jnp.zeros((REST, MIDDLE), BF16)
    copy_p1.wait()
    finish(small)
    finish(copies_2a)
    start(copies_2b)
    start(copies_ma)

    ex_a = exchange(x_a, REST, MIDDLE, MIDDLE, N16, 0)
    ex_s = exchange(x_s, REST, MIDDLE, MIDDLE, N16, 1)
    ex_m1 = exchange(m_1, STRIP_ROWS, MIDDLE, MIDDLE, STRIPS, 2)
    ex_m2 = exchange(m_2, STRIP_ROWS, DEEP, DEEP, STRIPS, KERNEL)
    ex_u = exchange(x_u, REST, MIDDLE, MIDDLE, N16, IN_CH)
    ex_b = exchange(x_a, REST, MIDDLE, MIDDLE, N16, FIVE)
    ex_d = exchange(d_2, REST, 0, MIDDLE, N16, SIX, out)
    tiles = ((0, TILE), (TILE, TILE), (N512, LANES))

    def enc2a(i, carry):
        @pl.when(i == 1)
        def _():
            start(ex_a)

        for block in (i, KERNEL - i):
            row0 = pl.multiple_of(block * TILE, TILE)
            for lane0, lanes in tiles:
                acc = dot(packed_rows(p1, row0, TILE), first_w[0:PACK, pl.ds(lane0, lanes)])
                for di in (1, 2):
                    acc = acc + dot(
                        packed_rows(p1, row0 + REST * di, TILE),
                        first_w[PACK * di : PACK * di + PACK, pl.ds(lane0, lanes)],
                    )
                value = jnp.maximum(acc + bias_row(b_2a, lane0, lanes), 0.0)
                put3(x_a, row0 + REST, lane0, MIDDLE, value, REST)
        return carry

    lax.fori_loop(0, 2, enc2a, 0)
    finish(copies_2b)
    start(copies_mb[0:2])
    start(copies_u2[0:2])

    def conv640(src, row0, base, lane0, lanes):
        weights = jnp.concatenate(
            [
                ring[base + MIDDLE * (t // 2) : base + MIDDLE * (t // 2) + MIDDLE, pl.ds(MIDDLE * (t % 2) + lane0, lanes)]
                for t in range(TAPS)
            ],
            axis=0,
        )
        rows = jnp.concatenate([src[pl.ds(row0 + REST * di, TILE), :] for di in range(KERNEL)], axis=1)
        return dot(rows, weights)

    def enc2b(i, carry):
        block = i + 1 - 2 * (i % 2)
        row0 = pl.multiple_of(block * TILE, TILE)

        @pl.when(i == 1)
        def _():
            finish(ex_a)
            halo(x_a, REST, MIDDLE, N16)

        @pl.when(i == KERNEL)
        def _():
            start(ex_m1)
            start(ex_s)

        for lane0, lanes in tiles:
            value = jnp.maximum(conv640(x_a, row0, 0, lane0, lanes) + bias_row(b_2b, lane0, lanes), 0.0)
            put3(x_s, row0 + REST, lane0, MIDDLE, value, REST)
            put3(m_1, pl.multiple_of(block * REST + STRIP_ROWS, STRIP_ROWS), lane0, MIDDLE, pooled(value, REST, pool_buf), STRIP_ROWS)
        return carry

    lax.fori_loop(0, IN_CH, enc2b, 0)
    start(copies_mb[2:IN_CH])

    acc_ref[...] = jnp.zeros_like(acc_ref)
    finish(copies_ma)

    def mid_a(t, carry):
        di = (t + 1) % 2 + 2 * (t // 2) - t // 2

        @pl.when(t == 1)
        def _():
            start(copies_mb[IN_CH:SIX])
            finish(ex_m1)
            halo(m_1, STRIP_ROWS, MIDDLE, STRIPS)

        @pl.when(t == 2)
        def _():
            start(copies_mb[SIX:LAST_STRIP])

        base = pl.multiple_of(N3200 + MIDDLE3 * t, LANES)
        lhs_row = pl.multiple_of(STRIP_ROWS * di, STRIP_ROWS)
        for lane0 in range(0, DEEP, TILE):
            acc_ref[:, pl.ds(lane0, TILE)] += dot(
                m_1[pl.ds(lhs_row, TILE), :], ring[pl.ds(base, MIDDLE3), pl.ds(lane0, TILE)]
            )
        return carry

    lax.fori_loop(0, KERNEL, mid_a, 0)
    start(copies_mb[LAST_STRIP:TAPS])

    def mid_a_rows(first, rows):
        for lane0 in range(0, DEEP, TILE):
            value = jnp.maximum(acc_ref[pl.ds(first, rows), pl.ds(lane0, TILE)] + bias_row(b_ma, lane0, TILE), 0.0)
            put3(m_2, STRIP_ROWS + first, lane0, DEEP, value, STRIP_ROWS)

    mid_a_rows(0, STRIP_ROWS)
    mid_a_rows(N224, STRIP_ROWS)
    start(ex_m2)
    mid_a_rows(STRIP_ROWS, N192)
    acc_ref[...] = jnp.zeros_like(acc_ref)

    def mid_b(t, carry):
        di = (t + 1) % 2 + 2 * (t // 2) - t // 2

        for j in range(KERNEL):
            @pl.when(t == j)
            def _(j=j):
                finish(copies_mb[KERNEL * j : KERNEL * j + KERNEL])

        @pl.when(t == 1)
        def _():
            start(copies_u2[2:IN_CH])
            start(copies_d2a[0:2])
            finish(ex_m2)
            halo(m_2, STRIP_ROWS, DEEP, STRIPS)

        @pl.when(t == 2)
        def _():
            start(copies_d2a[2:STRIPS])

        lhs_row = pl.multiple_of(STRIP_ROWS * di, STRIP_ROWS)
        for lane0 in range(0, DEEP, TILE):
            acc = None
            for dj in range(KERNEL):
                base = pl.multiple_of(mb_row(KERNEL * t + dj), LANES)
                part = dot(
                    m_2[pl.ds(lhs_row, TILE), DEEP * dj : DEEP * dj + DEEP], ring[pl.ds(base, DEEP), pl.ds(lane0, TILE)]
                )
                acc = part if acc is None else acc + part
            acc_ref[:, pl.ds(lane0, TILE)] += acc
        return carry

    lax.fori_loop(0, KERNEL, mid_b, 0)
    start(copies_d2a[STRIPS:TAPS])
    for lane0 in range(0, DEEP, TILE):
        value = jnp.maximum(acc_ref[:, pl.ds(lane0, TILE)] + bias_row(b_mb, lane0, TILE), 0.0)
        m_o[:, pl.ds(lane0, TILE)] = value.astype(BF16)

    finish(copies_u2)
    for p in range(2):
        for q in range(2):
            for lane0, lanes in tiles:
                if p == 0:
                    weights = first_w[DEEP * q : DEEP * q + DEEP, pl.ds(lane0, lanes)]
                else:
                    weights = ring[N8960:N10240, pl.ds(MIDDLE * q + lane0, lanes)]
                part = dot(m_o[...], weights)
                for lane in range(0, lanes, LANES):
                    wide[(lane0 + lane) // LANES, pl.ds(q, TILE, stride=2), :] = part[:, lane : lane + LANES]

        if p == 0:
            start(copies_turn)

        def place(i, carry):
            src = pl.multiple_of(REST * i, REST)
            dst = pl.multiple_of(REST * (1 + 2 * i + p), REST)
            for lane0 in range(0, MIDDLE, LANES):
                put3(x_u, dst, lane0, MIDDLE, wide[lane0 // LANES, pl.ds(src, REST), :], REST)
            return carry

        lax.fori_loop(0, STRIPS, place, 0)
    start(ex_u)
    start(copies_d2b)
    finish(ex_s)
    halo(x_s, REST, MIDDLE, N16)
    finish(copies_d2a)
    finish(copies_turn)
    clear_pad(wa_main, SIX)
    clear_pad(wa_rest, 2)

    def dec2a(i, carry):
        block = i + 1 - 2 * (i % 2)
        row0 = pl.multiple_of(block * TILE, TILE)

        @pl.when(i == 1)
        def _():
            finish(ex_u)
            halo(x_u, REST, MIDDLE, N16)

        @pl.when(i == KERNEL)
        def _():
            start(ex_b)

        for lane0, lanes in tiles:
            acc = None
            for tap in range(TAPS):
                rows = pl.ds(row0 + REST * (tap // KERNEL), TILE)
                cols = pl.ds(MIDDLE * (tap % KERNEL), MIDDLE)
                lhs = jnp.concatenate([x_u[rows, cols], x_s[rows, cols]], axis=1)
                base = DEEP * (tap // 2)
                part = dot(lhs, ring[base : base + DEEP, pl.ds(MIDDLE * (tap % 2) + lane0, lanes)])
                acc = part if acc is None else acc + part
            value = jnp.maximum(acc + bias_row(b_d2a, lane0, lanes), 0.0)
            put3(x_a, row0 + REST, lane0, MIDDLE, value, REST)

        part = jnp.minimum(i, 2)
        for dj in range(KERNEL):
            turn_main(first_w, wa_main, part, dj)
        turn_rest(first_w, wa_rest, part)
        wu_main[pl.ds(pl.multiple_of(MIDDLE * i, REST), MIDDLE), :] = st_u[pl.ds(pl.multiple_of(BASE * i, REST), TILE), :].T
        wu_rest[...] = jnp.concatenate([st_u[BASE * tap + TILE : BASE * tap + BASE, :] for tap in range(IN_CH)], axis=0).T
        return carry

    lax.fori_loop(0, IN_CH, dec2a, 0)
    turned = [
        pltpu.make_async_copy(src, dst, turn_sem.at[2 + index])
        for index, (src, dst) in enumerate(((wu_main, um_out), (wu_rest, ur_out), (wa_main, am_out), (wa_rest, ar_out)))
    ]
    start(turned)
    finish(copies_d2b)

    def dec2b(i, carry):
        block = i + 1 - 2 * (i % 2)
        row0 = pl.multiple_of(block * TILE, TILE)

        @pl.when(i == 1)
        def _():
            finish(ex_b)
            halo(x_a, REST, MIDDLE, N16)

        @pl.when(i == KERNEL)
        def _():
            start(ex_d)

        for lane0, lanes in tiles:
            value = jnp.maximum(conv640(x_a, row0, N6400, lane0, lanes) + bias_row(b_d2b, lane0, lanes), 0.0)
            d_2[pl.ds(row0 + REST, TILE), pl.ds(lane0, lanes)] = value.astype(BF16)
        return carry

    lax.fori_loop(0, IN_CH, dec2b, 0)
    result = pltpu.make_async_copy(d_2.at[pl.ds(REST, PACK), :], out.at[pl.ds(REST, PACK), :], sem_out)
    result.start()
    finish(turned)
    finish(ex_d)
    result.wait()


def dec1_kernel(
    d_2, s1, um_h, ur_h, am_h, ar_h, w_d1b, b_d1a_h, b_d1b_h, w_head_h, b_head_h, out,
    b_d1a, b_d1b, w_head, b_head, x_u, x_s, x_d, y_rest, st_b, wu_main, wu_rest, wa_main, wa_rest, wb_main, wb_rest, wide, result, pending, stage, skip, low, late,
    sem, small_sem, send_sem, recv_sem,
):
    strip = strip_index()
    row = lax.axis_index("row")
    col = lax.axis_index("col")
    copy_um = pltpu.make_async_copy(um_h, wu_main, sem.at[0])
    copy_ur = pltpu.make_async_copy(ur_h, wu_rest, sem.at[1])
    copy_am = pltpu.make_async_copy(am_h, wa_main, sem.at[FIVE])
    copy_ar = pltpu.make_async_copy(ar_h, wa_rest, sem.at[SIX])
    copy_s = pltpu.make_async_copy(s1, skip, sem.at[2])
    copy_b = pltpu.make_async_copy(w_d1b, st_b, sem.at[KERNEL])
    copy_d = pltpu.make_async_copy(d_2, low, sem.at[IN_CH])
    barrier = enter_barrier()
    copy_um.start()
    copy_ur.start()
    copy_d.start()
    small = fetch((b_d1a_h, b_d1b_h, w_head_h, b_head_h), (b_d1a, b_d1b, w_head, b_head), small_sem)

    stage[...] = jnp.zeros_like(stage)
    copy_um.wait()
    copy_ur.wait()
    copy_s.start()
    copy_ar.start()
    copy_am.start()
    copy_b.start()
    copy_d.wait()
    for copy in small:
        copy.wait()

    def up1(i):
        lhs = low[BASE_PAD * i : BASE_PAD * i + BASE_PAD, :]
        rest = dot(lhs, wu_rest[...])
        for p in range(2):
            part = rest[:, LANES * p : LANES * p + LANES]
            buf = wide.at[2 * i + p]
            buf[2, pl.ds(0, BASE_PAD, stride=2), :] = low_lanes(part)
            buf[2, pl.ds(1, BASE_PAD, stride=2), :] = low_lanes(pltpu.roll(part, REST, axis=1))
            for q in range(2):
                tap = 2 * p + q
                main = dot(lhs, wu_main[MIDDLE * tap : MIDDLE * tap + MIDDLE, :])
                buf[0, pl.ds(q, BASE_PAD, stride=2), :] = main[:, 0:LANES]
                buf[1, pl.ds(q, BASE_PAD, stride=2), :] = main[:, LANES:TILE]
            for r in range(SIX):
                main = jnp.concatenate([buf[0, LANES * r : LANES * r + LANES, :], buf[1, LANES * r : LANES * r + LANES, :]], axis=1)
                tail = buf[2, LANES * r : LANES * r + LANES, :]
                if (i, r) == (0, 0):
                    main, tail = jnp.where(strip > 0, main, 0.0), jnp.where(strip > 0, tail, 0.0)
                if (i, r) == (2, FIVE):
                    main, tail = jnp.where(strip < LAST_STRIP, main, 0.0), jnp.where(strip < LAST_STRIP, tail, 0.0)
                put3_320(x_u, (N12 * i + 2 * r + p) * LANES, main, tail, LANES)

    def spread(j):
        rows = pl.ds(TILE * j, TILE)
        put3_320(x_s, TILE * j, skip[rows, 0:TILE].astype(F32), skip[rows, TILE:BASE_PAD].astype(F32), LANES, stage.at[j % 2])

    def rest_a(i):
        for j in range(SIX * i, SIX * i + SIX):
            y_rest[TILE * j : TILE * j + TILE, :] = dot(packed_rows(x_u, TILE * j, TILE), wa_rest[0:PACK, :]) + dot(
                packed_rows(x_s, TILE * j, TILE), wa_rest[PACK:N2048, :]
            )
            if j < N17:
                spread(j + 1)

    up1(0)
    up1(1)
    copy_s.wait()
    copy_ar.wait()
    spread(0)
    up1(2)
    for i in range(KERNEL):
        rest_a(i)
    copy_am.wait()

    def conv_a(row0):
        acc = None
        for di in range(KERNEL):
            for src, ref in enumerate((x_u, x_s)):
                base = N3072 * src + PACK * di
                part = dot(packed_rows(ref, row0 + LANES * di, TILE), wa_main[base : base + PACK, :])
                acc = part if acc is None else acc + part
        return acc

    def put_a(acc, row0, first_row, slot):
        main = valid_rows(jnp.maximum(acc + bias_row(b_d1a, 0, TILE), 0.0), first_row, LANES)
        tail = valid_rows(jnp.maximum(rest_sum(y_rest, row0, TILE) + bias_rest(b_d1a), 0.0), first_row, LANES)
        put3_320(x_d, row0, main, low_lanes(tail), LANES, stage.at[slot])

    late[...] = jnp.zeros_like(late)

    def dec1a(i, carry):
        base = pl.multiple_of(i * PACK, PACK)
        put_a(late[...], pl.multiple_of(jnp.maximum(base - TILE, 0), TILE), STRIP_ROWS * strip - KERNEL + STRIPS * i, 1)
        for j in range(IN_CH):
            acc = conv_a(base + TILE * j)
            if j == KERNEL:
                late[...] = acc
            else:
                put_a(acc, base + TILE * j, STRIP_ROWS * strip - 1 + STRIPS * i + 2 * j, j % 2)
        return carry

    copy_b.wait()
    lax.fori_loop(0, IN_CH, dec1a, 0)
    pack_weights(st_b, wb_main, wb_rest)
    put_a(late[...], N3840, STRIP_ROWS * strip + N29, 1)
    put_a(conv_a(N4096), N4096, STRIP_ROWS * strip + N31, 0)

    head_bias = jnp.zeros((IN_CH, LANES), F32)
    for channel in range(IN_CH):
        head_bias = jnp.where(lax.broadcasted_iota(jnp.int32, (IN_CH, LANES), 0) == channel, b_head[channel], head_bias)

    pending[...] = jnp.zeros_like(pending)

    def head(hidden, row0):
        line = lax.dot_general(w_head[...], hidden, (((1,), (1,)), ((), ())), preferred_element_type=F32)
        for r in range(2):
            part = line[:, LANES * r : LANES * r + LANES] + head_bias
            result[0, row0 + r] = part[:, 0:REST]
            result[1, row0 + r] = part[:, REST:LANES]

    pushes = []
    for part, first, rows in ((0, 0, N22), (1, N22, N10)):
        for side in range(2):
            pushes.append(
                Push(
                    result.at[side, pl.ds(first, rows)],
                    out.at[pl.ds(STRIP_ROWS * (strip % 2) + first, rows)],
                    send_sem.at[part, side],
                    recv_sem.at[part, strip % 2],
                    (lax.axis_index("data"), side, strip // 2),
                    (strip // 2 == row) & (col == side),
                )
            )

    def dec1b(i, carry):
        base = pl.multiple_of(i * PACK, PACK)

        @pl.when(i == KERNEL)
        def _():
            pl.semaphore_wait(barrier, STRIPS)
            for push in pushes[0:2]:
                push.start()

        def rest(j):
            y_rest[TILE * j : TILE * j + TILE, :] = dot(packed_rows(x_d, base + TILE * j, TILE), wb_rest[...])

        rest(0)
        waiting = pending[...]
        for j in range(IN_CH):
            rest(j + 1)
            acc = dot(packed_rows(x_d, base + TILE * j, TILE), wb_main[0:PACK, :])
            acc = acc + dot(packed_rows(x_d, base + TILE * j + LANES, TILE), wb_main[PACK:N2048, :])
            acc = acc + dot(packed_rows(x_d, base + TILE * j + TILE, TILE), wb_main[N2048:N3072, :])
            head(waiting, jnp.maximum(STRIPS * i + 2 * j - 2, 0))
            main = jnp.maximum(acc + bias_row(b_d1b, 0, TILE), 0.0).astype(BF16)
            tail = jnp.maximum(rest_sum(y_rest, TILE * j, TILE) + bias_rest(b_d1b), 0.0).astype(BF16)
            waiting = jnp.concatenate([main, tail[:, 0:REST]], axis=1)
        pending[...] = waiting
        return carry

    lax.fori_loop(0, IN_CH, dec1b, 0)
    head(pending[...], N30)

    for push in pushes[2:IN_CH]:
        push.start()
    for push in pushes:
        push.wait_send()
    for part, first, rows in ((0, 0, N22), (1, N22, N10)):
        for half in range(2):
            Push(
                result.at[0, pl.ds(first, rows)], out.at[pl.ds(STRIP_ROWS * half + first, rows)],
                send_sem.at[part, 0], recv_sem.at[part, half], strip_device(strip), strip < 0,
            ).wait_recv()


def solution(mesh):
    tile_spec = P(("data", "row"), "col", None)

    def body(image_tile, *params):
        (w_enc1a, b_enc1a, w_enc1b, b_enc1b, w_enc2a, b_enc2a, w_enc2b, b_enc2b,
         w_mid_a, b_mid_a, w_mid_b, b_mid_b, w_up2, w_dec2a, b_dec2a, w_dec2b, b_dec2b,
         w_up1, w_dec1a, b_dec1a, w_dec1b, b_dec1b, w_head, b_head) = params
        def flat(weight):
            return weight.reshape(-1, weight.shape[-1])

        hbm = pl.BlockSpec(memory_space=pl.ANY)
        dma = pltpu.SemaphoreType.DMA
        s1, p1 = pl.pallas_call(
            enc1_kernel,
            grid=(KERNEL,),
            out_shape=(jax.ShapeDtypeStruct((N4608, BASE_PAD), BF16), jax.ShapeDtypeStruct((STRIPS, N1152, LANES), BF16)),
            in_specs=[hbm] * FIVE,
            out_specs=(pl.BlockSpec((N1536, BASE_PAD), lambda i: (i, 0)), pl.BlockSpec((STRIPS, BASE_PAD, LANES), lambda i: (0, i, 0))),
            scratch_shapes=[
                pltpu.VMEM((REST, IN_CH, REST), BF16),
                pltpu.VMEM((KERNEL, KERNEL, IN_CH, BASE), BF16),
                pltpu.VMEM((BASE,), F32),
                pltpu.VMEM((BASE,), F32),
                pltpu.VMEM((2, N40, IN_CH, REST), BF16),
                pltpu.VMEM((N50, STRIP_ROWS, LANES), BF16),
                pltpu.VMEM((N96, BASE_PAD), BF16),
                pltpu.VMEM((N2880, BASE), BF16),
                pltpu.VMEM((STRIPS, N5136, LANES), BF16),
                pltpu.VMEM((N1792, TILE), F32),
                pltpu.VMEM((N3072, TILE), BF16),
                pltpu.VMEM((PACK, TILE), BF16),
                pltpu.VMEM((2, LANES, LANES), F32),
                pltpu.VMEM((2, KERNEL, N288, LANES), F32),
                pltpu.VMEM((2, KERNEL, N80, LANES), F32),
                dma, dma((IN_CH,)), dma((IN_CH,)), dma((2, 2)),
            ],
            compiler_params=pltpu.CompilerParams(
                vmem_limit_bytes=VMEM_LIMIT, collective_id=1, has_side_effects=True, dimension_semantics=("arbitrary",)
            ),
            name="enc1",
        )(image_tile.transpose(0, 2, 1), w_enc1a, b_enc1a, flat(w_enc1b), b_enc1b)

        turned_shapes = ((N2560, TILE), (MIDDLE, TILE), (N6144, TILE), (N2048, TILE))

        def turned(weight):
            return weight.transpose(0, 1, KERNEL, 2).reshape(-1, weight.shape[2])

        d2, *level_one = pl.pallas_call(
            mid_kernel,
            out_shape=[jax.ShapeDtypeStruct(shape, BF16) for shape in ((N1152, MIDDLE),) + turned_shapes],
            in_specs=[hbm] * N16,
            out_specs=[hbm] * FIVE,
            scratch_shapes=[
                *[pltpu.VMEM((size,), F32) for size in (MIDDLE, MIDDLE, DEEP, DEEP, MIDDLE, MIDDLE)],
                *[pltpu.VMEM(shape, BF16) for shape in turned_shapes],
                pltpu.VMEM((STRIPS, N1168, LANES), BF16),
                pltpu.VMEM((N3072, MIDDLE), BF16),
                pltpu.VMEM((RING_ROWS, DEEP), BF16),
                pltpu.VMEM((N1152, MIDDLE3), BF16),
                pltpu.VMEM((N1152, MIDDLE3), BF16),
                pltpu.VMEM((N1152, MIDDLE3), BF16),
                pltpu.VMEM((BASE, MIDDLE3), BF16),
                pltpu.VMEM((BASE, N3840), BF16),
                pltpu.VMEM((TILE, DEEP), BF16),
                pltpu.VMEM((N1152, MIDDLE), BF16),
                pltpu.VMEM((TILE, DEEP), F32),
                pltpu.VMEM((FIVE, N512, LANES), F32),
                pltpu.VMEM((LANES, LANES), F32),
                dma((N18,)), dma((TAPS,)), dma((KERNEL,)), dma((TAPS,)), dma((IN_CH,)), dma((TAPS,)), dma((TAPS,)), dma, dma, dma((SIX,)), dma((SIX,)),
                dma((LAST_STRIP, 2)), dma((LAST_STRIP, 2)),
            ],
            compiler_params=pltpu.CompilerParams(
                vmem_limit_bytes=VMEM_LIMIT, collective_id=0, has_side_effects=True
            ),
            name="mid",
        )(
            p1, flat(w_enc2a), flat(w_enc2b), flat(w_mid_a), flat(w_mid_b), flat(w_up2), flat(w_dec2a), flat(w_dec2b),
            turned(w_up1), turned(w_dec1a),
            b_enc2a, b_enc2b, b_mid_a, b_mid_b, b_dec2a, b_dec2b,
        )

        y = pl.pallas_call(
            dec1_kernel,
            out_shape=jax.ShapeDtypeStruct((REST, IN_CH, REST), F32),
            in_specs=[hbm] * N11,
            out_specs=hbm,
            scratch_shapes=[
                pltpu.VMEM((BASE,), F32),
                pltpu.VMEM((BASE,), F32),
                pltpu.VMEM((IN_CH, BASE), BF16),
                pltpu.SMEM((IN_CH,), F32),
                pltpu.VMEM((STRIPS, N4624, LANES), BF16),
                pltpu.VMEM((STRIPS, N4624, LANES), BF16),
                pltpu.VMEM((STRIPS, N4368, LANES), BF16),
                pltpu.VMEM((N4608, TILE), F32),
                pltpu.VMEM((N2880, BASE), BF16),
                pltpu.VMEM((N2560, TILE), BF16),
                pltpu.VMEM((MIDDLE, TILE), BF16),
                pltpu.VMEM((N6144, TILE), BF16),
                pltpu.VMEM((N2048, TILE), BF16),
                pltpu.VMEM((N3072, TILE), BF16),
                pltpu.VMEM((PACK, TILE), BF16),
                pltpu.VMEM((SIX, KERNEL, REST_AT, LANES), F32),
                pltpu.VMEM((2, STRIP_ROWS, IN_CH, REST), F32),
                pltpu.VMEM((TILE, BASE), BF16),
                pltpu.VMEM((2, KERNEL, N288, LANES), F32),
                pltpu.VMEM((N4608, BASE_PAD), BF16),
                pltpu.VMEM((N1152, MIDDLE), BF16),
                pltpu.VMEM((TILE, TILE), F32),
                dma((LAST_STRIP,)), dma((IN_CH,)), dma((2, 2)), dma((2, 2)),
            ],
            compiler_params=pltpu.CompilerParams(vmem_limit_bytes=VMEM_LIMIT, collective_id=2, has_side_effects=True),
            name="dec1",
        )(d2, s1, *level_one, flat(w_dec1b), b_dec1a, b_dec1b, w_head.T, b_head)
        return y.transpose(0, 2, 1)

    def program(image, *params):
        mapped = jax.shard_map(
            body, mesh=mesh, in_specs=(tile_spec,) + (P(),) * len(params), out_specs=tile_spec, check_vma=False
        )
        return mapped(image, *params)

    return program
```

```python
import functools

import jax
import jax.numpy as jnp
from jax import lax
from jax.experimental import pallas as pl
from jax.experimental.pallas import tpu as pltpu
from jax.sharding import PartitionSpec as P

KERNEL = 3
IN_CH = 4
FIVE = 5
SIX = 6
LAST_STRIP = 7
STRIPS = 8
TAPS = 9
N10 = 10
N11 = 11
N12 = 12
N16 = 16
N17 = 17
N18 = 18
N20 = 20
N22 = 22
N28 = 28
N29 = 29
N30 = 30
N31 = 31
STRIP_ROWS = 32
N36 = 36
N40 = 40
N42 = 42
N50 = 50
N60 = 60
REST = 64
N80 = 80
N96 = 96
N127 = 127
LANES = 128
N192 = 192
N224 = 224
TILE = 256
N288 = 288
BASE = 320
BASE_PAD = 384
N512 = 512
MIDDLE = 640
REST_AT = 768
PACK_USED = 960
PACK = 1024
N1152 = 1152
N1168 = 1168
DEEP = 1280
N1536 = 1536
N1792 = 1792
MIDDLE3 = 1920
N2048 = 2048
N2560 = 2560
N2880 = 2880
N3072 = 3072
N3200 = 3200
N3840 = 3840
N4096 = 4096
N4368 = 4368
N4608 = 4608
N4624 = 4624
N5136 = 5136
N6144 = 6144
N6400 = 6400
N8960 = 8960
N10240 = 10240
N11520 = 11520
BF16 = jnp.bfloat16
F32 = jnp.float32
MESH = pl.DeviceIdType.MESH
VMEM_LIMIT = 66_900_000
RING_ROWS = N11520


def strip_index():
    col = lax.axis_index("col")
    row = lax.axis_index("row")
    return row + col * (LAST_STRIP - 2 * row)


def strip_device(position):
    col = position // IN_CH
    rest = position % IN_CH
    return (lax.axis_index("data"), col, rest + col * (KERNEL - 2 * rest))


def dot(a, b):
    return jnp.dot(a, b, preferred_element_type=F32)


def shifted(value, width, step):
    if step == 1:
        return value
    rows = value.shape[0]
    column = lax.broadcasted_iota(jnp.int32, value.shape, 0) % width
    if step == 0:
        return jnp.where(column == 0, 0.0, pltpu.roll(value, 1, axis=0))
    return jnp.where(column == width - 1, 0.0, pltpu.roll(value, rows - 1, axis=0))


def put3(dst, row0, lane0, channels, value, width):
    rows, lanes = value.shape
    for step in range(KERNEL):
        dst[pl.ds(row0, rows), pl.ds(step * channels + lane0, lanes)] = shifted(value, width, step).astype(BF16)


def put3_320(dst, row0, main, rest, width, stage=None):
    rows = main.shape[0]
    pitch = width + N16
    planes = [main[:, 0:LANES], main[:, LANES:TILE], rest]
    for t, plane in enumerate(planes if stage is not None else []):
        for r in range(rows // width):
            stage[t, pitch * r + STRIPS : pitch * r + STRIPS + width, :] = plane[width * r : width * r + width]

    def moved(t, step):
        if stage is None:
            return shifted(planes[t], width, step)
        first = LAST_STRIP + step
        parts = [stage[t, pitch * r + first : pitch * r + first + width, :] for r in range(rows // width)]
        return jnp.concatenate(parts, axis=0) if len(parts) > 1 else parts[0]

    for step in range(KERNEL):
        for t in range(2):
            dst[2 * step + t, pl.ds(row0, rows), :] = moved(t, step).astype(BF16)
    first = moved(2, 0) + pltpu.roll(moved(2, 1), REST, axis=1)
    dst[SIX, pl.ds(row0, rows), :] = first.astype(BF16)
    dst[LAST_STRIP, pl.ds(row0, rows), :] = moved(2, 2).astype(BF16)


def packed_rows(ref, row0, rows):
    return jnp.concatenate([ref[t, pl.ds(row0, rows), :] for t in range(STRIPS)], axis=1)


def low_lanes(value):
    return jnp.where(lax.broadcasted_iota(jnp.int32, value.shape, 1) < REST, value, 0.0)


def pack_weights(staged, main_ref, rest_ref):
    for dj in range(KERNEL):
        for start, size, row in ((0, TILE, TILE * dj), (TILE, REST, REST_AT + REST * dj)):
            parts = []
            for di in range(KERNEL):
                base = (KERNEL * di + dj) * BASE + start
                main_ref[pl.ds(PACK * di + row, size), :] = staged[pl.ds(base, size), 0:TILE]
                parts.append(staged[pl.ds(base, size), TILE:BASE])
            parts.append(jnp.zeros((size, REST), BF16))
            rest_ref[pl.ds(row, size), :] = jnp.concatenate(parts, axis=1)
    clear_pad(main_ref, KERNEL)
    clear_pad(rest_ref, 1)


def clear_pad(ref, groups):
    for group in range(groups):
        ref[pl.ds(PACK * group + PACK_USED, REST), :] = jnp.zeros((REST, ref.shape[1]), BF16)


def turn_main(staged, main_ref, di, dj):
    turned = staged[pl.ds(pl.multiple_of(PACK_USED * di + BASE * dj, REST), TILE), :].T
    for src in range(2):
        base = N3072 * src + PACK * di
        main_ref[pl.ds(pl.multiple_of(base + TILE * dj, REST), TILE), :] = turned[BASE * src : BASE * src + TILE]
        main_ref[pl.ds(pl.multiple_of(base + REST_AT + REST * dj, REST), REST), :] = turned[BASE * src + TILE : BASE * src + BASE]


def turn_rest(staged, rest_ref, dj):
    parts = [staged[pl.ds(pl.multiple_of(PACK_USED * di + BASE * dj + TILE, REST), REST), :] for di in range(KERNEL)]
    turned = jnp.concatenate(parts + [jnp.zeros((REST, MIDDLE), BF16)], axis=0).T
    for src in range(2):
        rest_ref[pl.ds(pl.multiple_of(PACK * src + TILE * dj, REST), TILE), :] = turned[BASE * src : BASE * src + TILE]
        rest_ref[pl.ds(pl.multiple_of(PACK * src + REST_AT + REST * dj, REST), REST), :] = turned[BASE * src + TILE : BASE * src + BASE]


def bias_row(ref, start, size):
    return ref[pl.ds(start, size)].reshape(1, size)


def bias_rest(ref):
    return jnp.concatenate([bias_row(ref, TILE, REST), jnp.zeros((1, REST), F32)], axis=1)


def enter_barrier():
    barrier = pltpu.get_barrier_semaphore()
    for position in range(STRIPS):
        pl.semaphore_signal(barrier, inc=1, device_id=strip_device(position), device_id_type=MESH)
    return barrier


def fetch(sources, targets, sems):
    copies = [pltpu.make_async_copy(src, dst, sems.at[i]) for i, (src, dst) in enumerate(zip(sources, targets))]
    for copy in copies:
        copy.start()
    return copies


class Push:
    def __init__(self, src, dst, send_sem, recv_sem, device, here):
        self.here = here
        self.local = pltpu.make_async_copy(src, dst, recv_sem)
        self.remote = pltpu.make_async_remote_copy(
            src_ref=src, dst_ref=dst, send_sem=send_sem, recv_sem=recv_sem, device_id=device, device_id_type=MESH
        )

    def start(self):
        @pl.when(self.here)
        def _():
            self.local.start()

        @pl.when(jnp.logical_not(self.here))
        def _():
            self.remote.start()

    def wait_send(self):
        @pl.when(jnp.logical_not(self.here))
        def _():
            self.remote.wait_send()

    def wait_recv(self):
        self.remote.wait_recv()


def rest_sum(y_ref, row0, rows):
    total = y_ref[pl.ds(row0, rows), 0:LANES] + y_ref[pl.ds(row0 + TILE, rows), LANES:TILE]
    return total + pltpu.roll(y_ref[pl.ds(row0 + LANES, rows), 0:LANES], REST, axis=1)


def valid_rows(value, first_row, width):
    row = first_row + lax.broadcasted_iota(jnp.int32, value.shape, 0) // width
    return jnp.where((row >= 0) & (row < TILE), value, 0.0)


def pooled(value, width, scratch):
    rows, lanes = value.shape
    tall = jnp.concatenate(
        [jnp.maximum(value[s : s + width], value[s + width : s + 2 * width]) for s in range(0, rows, 2 * width)], axis=0
    )
    halves = []
    for start in range(0, lanes, LANES):
        scratch[0 : rows // 2, :] = tall[:, start : start + LANES]
        halves.append(
            jnp.maximum(scratch[pl.ds(0, rows // IN_CH, stride=2), :], scratch[pl.ds(1, rows // IN_CH, stride=2), :])
        )
    return jnp.concatenate(halves, axis=1) if len(halves) > 1 else halves[0]


def enc1_kernel(
    image_hbm, w_a_hbm, b_a_hbm, w_b, b_b_hbm, s1_out, p1_out,
    image, w_a, b_a, b_b, halves, planes, w_stem, staged, x_a, y_rest, w_main, w_rest, pool_buf, stage, stage_p, w_sem, small_sem, send_sem, recv_sem,
):
    step = pl.program_id(0)
    strip = strip_index()

    @pl.when(step == 0)
    def _():
        row = lax.axis_index("row")
        col = lax.axis_index("col")
        barrier = enter_barrier()
        small = fetch((image_hbm, w_a_hbm, b_a_hbm, b_b_hbm), (image, w_a, b_a, b_b), small_sem)
        copy_w = pltpu.make_async_copy(w_b, staged, w_sem)
        copy_w.start()
        stage[...] = jnp.zeros_like(stage)
        stage_p[...] = jnp.zeros_like(stage_p)

        for copy in small:
            copy.wait()
        for di in range(KERNEL):
            taps = []
            for dj in range(KERNEL):
                tap = jnp.concatenate([w_a[di, dj].astype(F32), jnp.zeros((IN_CH, BASE), F32)], axis=0)
                taps.append(jnp.concatenate([tap, jnp.zeros((STRIPS, REST), F32)], axis=1))
            taps.append(jnp.zeros((STRIPS, BASE_PAD), F32))
            w_stem[STRIP_ROWS * di : STRIP_ROWS * di + STRIP_ROWS, :] = jnp.concatenate(taps, axis=0).astype(BF16)

        planes[N40:N42, :, :] = jnp.zeros((2, STRIP_ROWS, LANES), BF16)

        pl.semaphore_wait(barrier, STRIPS)
        pushes = []
        for index, (target, src_row, dst_row, rows) in enumerate(
            ((2 * row, 0, IN_CH, N36), (2 * row + 1, N28, 0, N36), ((2 * row + 2) % STRIPS, N60, 0, IN_CH), ((2 * row + LAST_STRIP) % STRIPS, 0, N36, IN_CH))
        ):
            pushes.append(
                Push(
                    image.at[pl.ds(src_row, rows)],
                    halves.at[col, pl.ds(dst_row, rows)],
                    send_sem.at[index],
                    recv_sem.at[index // 2, col],
                    strip_device(target),
                    target == strip,
                )
            )
        for push in pushes:
            push.start()
        copy_w.wait()
        pack_weights(staged, w_main, w_rest)
        for push in pushes:
            push.wait_send()
        for kind, rows in ((0, N36), (1, IN_CH)):
            for side in range(2):
                Push(
                    image.at[pl.ds(0, rows)], halves.at[side, pl.ds(0, rows)],
                    send_sem.at[0], recv_sem.at[kind, side], strip_device(strip), strip < 0,
                ).wait_recv()

        def expand(i, carry):
            for j in range(N20):
                r = N20 * i + j
                both = jnp.concatenate([halves[0, r].astype(F32), halves[1, r].astype(F32)], axis=1)
                image_row = STRIP_ROWS * strip - IN_CH + r
                both = jnp.where((image_row >= 0) & (image_row < TILE), both, 0.0)
                both = jnp.concatenate([both, jnp.zeros((IN_CH, LANES), F32)], axis=0)
                column = lax.broadcasted_iota(jnp.int32, (STRIPS, LANES), 1)
                before = jnp.where(column == 0, 0.0, pltpu.roll(both, 1, axis=1))
                after = jnp.where(column == N127, 0.0, pltpu.roll(both, N127, axis=1))
                planes[r] = jnp.concatenate([before, both, after, jnp.zeros((STRIPS, LANES), F32)], axis=0).astype(BF16)
            return carry

        lax.fori_loop(0, 2, expand, 0)

        def stem(i, carry):
            for j in range(STRIPS):
                r = STRIPS * i + j
                patch = jnp.concatenate([planes[r + di] for di in range(KERNEL)], axis=0)
                acc = lax.dot_general(patch, w_stem[...], (((0,), (0,)), ((), ())), preferred_element_type=F32)
                image_row = STRIP_ROWS * strip - KERNEL + r
                inside = (image_row >= 0) & (image_row < TILE)
                main = jnp.where(inside, jnp.maximum(acc[:, 0:TILE] + bias_row(b_a, 0, TILE), 0.0), 0.0)
                tail = jnp.where(inside, jnp.maximum(acc[:, TILE:BASE_PAD] + bias_rest(b_a), 0.0), 0.0)
                put3_320(x_a, pl.multiple_of(r * LANES, LANES), main, tail, LANES, stage.at[j % 2])
            return carry

        lax.fori_loop(0, FIVE, stem, 0)

    base = pl.multiple_of(step * N1536, N512)

    def rest(j):
        y_rest[TILE * j : TILE * j + TILE, :] = dot(packed_rows(x_a, base + TILE * j, TILE), w_rest[...])

    rest(0)
    for j in range(SIX):
        rest(j + 1)
        acc = dot(packed_rows(x_a, base + TILE * j, TILE), w_main[0:PACK, :])
        acc = acc + dot(packed_rows(x_a, base + TILE * j + LANES, TILE), w_main[PACK:N2048, :])
        acc = acc + dot(packed_rows(x_a, base + TILE * j + TILE, TILE), w_main[N2048:N3072, :])
        first_row = STRIP_ROWS * strip - 2 + N12 * step + 2 * j
        main = valid_rows(jnp.maximum(acc + bias_row(b_b, 0, TILE), 0.0), first_row, LANES)
        tail = jnp.maximum(rest_sum(y_rest, TILE * j, TILE) + bias_rest(b_b), 0.0)
        tail = low_lanes(valid_rows(tail, first_row, LANES))
        s1_out[TILE * j : TILE * j + TILE, 0:TILE] = main.astype(BF16)
        s1_out[TILE * j : TILE * j + TILE, TILE:BASE_PAD] = tail.astype(BF16)
        put3_320(p1_out, REST * j, pooled(main, LANES, pool_buf.at[j % 2]), pooled(tail, LANES, pool_buf.at[j % 2]), REST, stage_p.at[j % 2])


def mid_kernel(
    p1_hbm, w_2a, w_2b, w_ma, w_mb, w_u2, w_d2a, w_d2b, w_u1, w_d1a, b_2a_h, b_2b_h, b_ma_h, b_mb_h, b_d2a_h, b_d2b_h,
    out, um_out, ur_out, am_out, ar_out,
    b_2a, b_2b, b_ma, b_mb, b_d2a, b_d2b, wu_main, wu_rest, wa_main, wa_rest,
    p1, first_w, ring, x_a, x_s, x_u, m_1, m_2, m_o, d_2, acc_ref, wide, pool_buf,
    sem_2a, sem_2b, sem_ma, sem_mb, sem_u2, sem_d2a, sem_d2b, sem_p1, sem_out, turn_sem, small_sem, send_sem, recv_sem,
):
    strip = strip_index()
    prev_dev = strip_device((strip + LAST_STRIP) % STRIPS)
    next_dev = strip_device((strip + 1) % STRIPS)

    def exchange(buf, width, lane0, lanes, rows, index, target=None):
        target = buf if target is None else target
        lane = pl.ds(lane0, lanes)
        copies = []
        for side, src_row, dst_row, device in ((0, 1, rows + 1, prev_dev), (1, rows, 0, next_dev)):
            copies.append(
                pltpu.make_async_remote_copy(
                    src_ref=buf.at[pl.ds(src_row * width, width), lane],
                    dst_ref=target.at[pl.ds(dst_row * width, width), lane],
                    send_sem=send_sem.at[index, side],
                    recv_sem=recv_sem.at[index, side],
                    device_id=device,
                    device_id_type=MESH,
                )
            )
        return copies

    def start(copies):
        for copy in copies:
            copy.start()

    def finish(copies):
        for copy in copies:
            copy.wait()

    def halo(buf, width, channels, rows):
        for row, inside in ((0, strip > 0), (rows + 1, strip < LAST_STRIP)):
            value = buf[pl.ds(row * width, width), pl.ds(channels, channels)].astype(F32)
            put3(buf, row * width, 0, channels, jnp.where(inside, value, 0.0), width)

    copies_2a = []
    for tap in range(TAPS):
        di, dj = tap // KERNEL, tap % KERNEL
        for part, (start_row, size, row) in enumerate(((0, TILE, TILE * dj), (TILE, REST, REST_AT + REST * dj))):
            copies_2a.append(
                pltpu.make_async_copy(
                    w_2a.at[pl.ds(BASE * tap + start_row, size), :],
                    first_w.at[pl.ds(PACK * di + row, size), :],
                    sem_2a.at[2 * tap + part],
                )
            )

    def tap_copies(src, rows, base, sem):
        return [
            pltpu.make_async_copy(
                src.at[pl.ds(rows * tap, rows), :],
                ring.at[pl.ds(base + rows * (tap // 2), rows), pl.ds(MIDDLE * (tap % 2), MIDDLE)],
                sem.at[tap],
            )
            for tap in range(src.shape[0] // rows)
        ]

    copies_2b = tap_copies(w_2b, MIDDLE, 0, sem_2b)
    copies_ma = [
        pltpu.make_async_copy(w_ma.at[pl.ds(MIDDLE3 * di, MIDDLE3), :], ring.at[pl.ds(N3200 + MIDDLE3 * t, MIDDLE3), :], sem_ma.at[t])
        for t, di in enumerate((1, 0, 2))
    ]

    def mb_row(k):
        return (N8960 + DEEP * k) % RING_ROWS

    copies_mb = [
        pltpu.make_async_copy(
            w_mb.at[pl.ds(DEEP * (KERNEL * (1, 0, 2)[k // KERNEL] + k % KERNEL), DEEP), :], ring.at[pl.ds(mb_row(k), DEEP), :], sem_mb.at[k]
        )
        for k in range(TAPS)
    ]
    copies_u2 = [
        pltpu.make_async_copy(
            w_u2.at[pl.ds(DEEP * tap, DEEP), :],
            first_w.at[pl.ds(DEEP * tap, DEEP), :] if tap < 2 else ring.at[pl.ds(N8960, DEEP), pl.ds(MIDDLE * (tap - 2), MIDDLE)],
            sem_u2.at[tap],
        )
        for tap in range(IN_CH)
    ]
    st_u = ring.at[pl.ds(N10240, DEEP), pl.ds(0, MIDDLE)]
    copies_turn = [
        pltpu.make_async_copy(w_u1, st_u, turn_sem.at[0]),
        pltpu.make_async_copy(w_d1a, first_w.at[pl.ds(0, N2880), :], turn_sem.at[1]),
    ]
    copies_d2a = tap_copies(w_d2a, DEEP, 0, sem_d2a)
    copies_d2b = tap_copies(w_d2b, MIDDLE, N6400, sem_d2b)

    copy_p1 = pltpu.make_async_copy(p1_hbm, p1.at[:, pl.ds(0, N1152), :], sem_p1)
    barrier = pltpu.get_barrier_semaphore()
    for device in (prev_dev, next_dev):
        pl.semaphore_signal(barrier, inc=1, device_id=device, device_id_type=MESH)
    copy_p1.start()
    start(copies_2a)
    small = fetch(
        (b_2a_h, b_2b_h, b_ma_h, b_mb_h, b_d2a_h, b_d2b_h), (b_2a, b_2b, b_ma, b_mb, b_d2a, b_d2b), small_sem
    )
    pl.semaphore_wait(barrier, 2)

    for di in range(KERNEL):
        first_w[PACK * di + PACK_USED : PACK * di + PACK, :] = jnp.zeros((REST, MIDDLE), BF16)
    copy_p1.wait()
    finish(small)
    finish(copies_2a)
    start(copies_2b)
    start(copies_ma)

    ex_a = exchange(x_a, REST, MIDDLE, MIDDLE, N16, 0)
    ex_s = exchange(x_s, REST, MIDDLE, MIDDLE, N16, 1)
    ex_m1 = exchange(m_1, STRIP_ROWS, MIDDLE, MIDDLE, STRIPS, 2)
    ex_m2 = exchange(m_2, STRIP_ROWS, DEEP, DEEP, STRIPS, KERNEL)
    ex_u = exchange(x_u, REST, MIDDLE, MIDDLE, N16, IN_CH)
    ex_b = exchange(x_a, REST, MIDDLE, MIDDLE, N16, FIVE)
    ex_d = exchange(d_2, REST, 0, MIDDLE, N16, SIX, out)
    tiles = ((0, TILE), (TILE, TILE), (N512, LANES))

    def enc2a(i, carry):
        @pl.when(i == 1)
        def _():
            start(ex_a)

        for block in (i, KERNEL - i):
            row0 = pl.multiple_of(block * TILE, TILE)
            for lane0, lanes in tiles:
                acc = dot(packed_rows(p1, row0, TILE), first_w[0:PACK, pl.ds(lane0, lanes)])
                for di in (1, 2):
                    acc = acc + dot(
                        packed_rows(p1, row0 + REST * di, TILE),
                        first_w[PACK * di : PACK * di + PACK, pl.ds(lane0, lanes)],
                    )
                value = jnp.maximum(acc + bias_row(b_2a, lane0, lanes), 0.0)
                put3(x_a, row0 + REST, lane0, MIDDLE, value, REST)
        return carry

    lax.fori_loop(0, 2, enc2a, 0)
    finish(copies_2b)
    start(copies_mb[0:2])
    start(copies_u2[0:2])

    def conv640(src, row0, base, lane0, lanes):
        weights = jnp.concatenate(
            [
                ring[base + MIDDLE * (t // 2) : base + MIDDLE * (t // 2) + MIDDLE, pl.ds(MIDDLE * (t % 2) + lane0, lanes)]
                for t in range(TAPS)
            ],
            axis=0,
        )
        rows = jnp.concatenate([src[pl.ds(row0 + REST * di, TILE), :] for di in range(KERNEL)], axis=1)
        return dot(rows, weights)

    def enc2b(i, carry):
        block = i + 1 - 2 * (i % 2)
        row0 = pl.multiple_of(block * TILE, TILE)

        @pl.when(i == 1)
        def _():
            finish(ex_a)
            halo(x_a, REST, MIDDLE, N16)

        @pl.when(i == KERNEL)
        def _():
            start(ex_m1)
            start(ex_s)

        for lane0, lanes in tiles:
            value = jnp.maximum(conv640(x_a, row0, 0, lane0, lanes) + bias_row(b_2b, lane0, lanes), 0.0)
            put3(x_s, row0 + REST, lane0, MIDDLE, value, REST)
            put3(m_1, pl.multiple_of(block * REST + STRIP_ROWS, STRIP_ROWS), lane0, MIDDLE, pooled(value, REST, pool_buf), STRIP_ROWS)
        return carry

    lax.fori_loop(0, IN_CH, enc2b, 0)
    start(copies_mb[2:IN_CH])

    acc_ref[...] = jnp.zeros_like(acc_ref)
    finish(copies_ma)

    def mid_a(t, carry):
        di = (t + 1) % 2 + 2 * (t // 2) - t // 2

        @pl.when(t == 1)
        def _():
            start(copies_mb[IN_CH:SIX])
            finish(ex_m1)
            halo(m_1, STRIP_ROWS, MIDDLE, STRIPS)

        @pl.when(t == 2)
        def _():
            start(copies_mb[SIX:LAST_STRIP])

        base = pl.multiple_of(N3200 + MIDDLE3 * t, LANES)
        lhs_row = pl.multiple_of(STRIP_ROWS * di, STRIP_ROWS)
        for lane0 in range(0, DEEP, TILE):
            acc_ref[:, pl.ds(lane0, TILE)] += dot(
                m_1[pl.ds(lhs_row, TILE), :], ring[pl.ds(base, MIDDLE3), pl.ds(lane0, TILE)]
            )
        return carry

    lax.fori_loop(0, KERNEL, mid_a, 0)
    start(copies_mb[LAST_STRIP:TAPS])

    def mid_a_rows(first, rows):
        for lane0 in range(0, DEEP, TILE):
            value = jnp.maximum(acc_ref[pl.ds(first, rows), pl.ds(lane0, TILE)] + bias_row(b_ma, lane0, TILE), 0.0)
            put3(m_2, STRIP_ROWS + first, lane0, DEEP, value, STRIP_ROWS)

    mid_a_rows(0, STRIP_ROWS)
    mid_a_rows(N224, STRIP_ROWS)
    start(ex_m2)
    mid_a_rows(STRIP_ROWS, N192)
    acc_ref[...] = jnp.zeros_like(acc_ref)

    def mid_b(t, carry):
        di = (t + 1) % 2 + 2 * (t // 2) - t // 2

        for j in range(KERNEL):
            @pl.when(t == j)
            def _(j=j):
                finish(copies_mb[KERNEL * j : KERNEL * j + KERNEL])

        @pl.when(t == 1)
        def _():
            start(copies_u2[2:IN_CH])
            start(copies_d2a[0:2])
            finish(ex_m2)
            halo(m_2, STRIP_ROWS, DEEP, STRIPS)

        @pl.when(t == 2)
        def _():
            start(copies_d2a[2:STRIPS])

        lhs_row = pl.multiple_of(STRIP_ROWS * di, STRIP_ROWS)
        for lane0 in range(0, DEEP, TILE):
            acc = None
            for dj in range(KERNEL):
                base = pl.multiple_of(mb_row(KERNEL * t + dj), LANES)
                part = dot(
                    m_2[pl.ds(lhs_row, TILE), DEEP * dj : DEEP * dj + DEEP], ring[pl.ds(base, DEEP), pl.ds(lane0, TILE)]
                )
                acc = part if acc is None else acc + part
            acc_ref[:, pl.ds(lane0, TILE)] += acc
        return carry

    lax.fori_loop(0, KERNEL, mid_b, 0)
    start(copies_d2a[STRIPS:TAPS])
    for lane0 in range(0, DEEP, TILE):
        value = jnp.maximum(acc_ref[:, pl.ds(lane0, TILE)] + bias_row(b_mb, lane0, TILE), 0.0)
        m_o[:, pl.ds(lane0, TILE)] = value.astype(BF16)

    finish(copies_u2)
    for p in range(2):
        for q in range(2):
            for lane0, lanes in tiles:
                if p == 0:
                    weights = first_w[DEEP * q : DEEP * q + DEEP, pl.ds(lane0, lanes)]
                else:
                    weights = ring[N8960:N10240, pl.ds(MIDDLE * q + lane0, lanes)]
                part = dot(m_o[...], weights)
                for lane in range(0, lanes, LANES):
                    wide[(lane0 + lane) // LANES, pl.ds(q, TILE, stride=2), :] = part[:, lane : lane + LANES]

        if p == 0:
            start(copies_turn)

        def place(i, carry):
            src = pl.multiple_of(REST * i, REST)
            dst = pl.multiple_of(REST * (1 + 2 * i + p), REST)
            for lane0 in range(0, MIDDLE, LANES):
                put3(x_u, dst, lane0, MIDDLE, wide[lane0 // LANES, pl.ds(src, REST), :], REST)
            return carry

        lax.fori_loop(0, STRIPS, place, 0)
    start(ex_u)
    start(copies_d2b)
    finish(ex_s)
    halo(x_s, REST, MIDDLE, N16)
    finish(copies_d2a)
    finish(copies_turn)
    clear_pad(wa_main, SIX)
    clear_pad(wa_rest, 2)

    def dec2a(i, carry):
        block = i + 1 - 2 * (i % 2)
        row0 = pl.multiple_of(block * TILE, TILE)

        @pl.when(i == 1)
        def _():
            finish(ex_u)
            halo(x_u, REST, MIDDLE, N16)

        @pl.when(i == KERNEL)
        def _():
            start(ex_b)

        for lane0, lanes in tiles:
            acc = None
            for tap in range(TAPS):
                rows = pl.ds(row0 + REST * (tap // KERNEL), TILE)
                cols = pl.ds(MIDDLE * (tap % KERNEL), MIDDLE)
                lhs = jnp.concatenate([x_u[rows, cols], x_s[rows, cols]], axis=1)
                base = DEEP * (tap // 2)
                part = dot(lhs, ring[base : base + DEEP, pl.ds(MIDDLE * (tap % 2) + lane0, lanes)])
                acc = part if acc is None else acc + part
            value = jnp.maximum(acc + bias_row(b_d2a, lane0, lanes), 0.0)
            put3(x_a, row0 + REST, lane0, MIDDLE, value, REST)

        part = jnp.minimum(i, 2)
        for dj in range(KERNEL):
            turn_main(first_w, wa_main, part, dj)
        turn_rest(first_w, wa_rest, part)
        wu_main[pl.ds(pl.multiple_of(MIDDLE * i, REST), MIDDLE), :] = st_u[pl.ds(pl.multiple_of(BASE * i, REST), TILE), :].T
        wu_rest[...] = jnp.concatenate([st_u[BASE * tap + TILE : BASE * tap + BASE, :] for tap in range(IN_CH)], axis=0).T
        return carry

    lax.fori_loop(0, IN_CH, dec2a, 0)
    turned = [
        pltpu.make_async_copy(src, dst, turn_sem.at[2 + index])
        for index, (src, dst) in enumerate(((wu_main, um_out), (wu_rest, ur_out), (wa_main, am_out), (wa_rest, ar_out)))
    ]
    start(turned)
    finish(copies_d2b)

    def dec2b(i, carry):
        block = i + 1 - 2 * (i % 2)
        row0 = pl.multiple_of(block * TILE, TILE)

        @pl.when(i == 1)
        def _():
            finish(ex_b)
            halo(x_a, REST, MIDDLE, N16)

        @pl.when(i == KERNEL)
        def _():
            start(ex_d)

        for lane0, lanes in tiles:
            value = jnp.maximum(conv640(x_a, row0, N6400, lane0, lanes) + bias_row(b_d2b, lane0, lanes), 0.0)
            d_2[pl.ds(row0 + REST, TILE), pl.ds(lane0, lanes)] = value.astype(BF16)
        return carry

    lax.fori_loop(0, IN_CH, dec2b, 0)
    result = pltpu.make_async_copy(d_2.at[pl.ds(REST, PACK), :], out.at[pl.ds(REST, PACK), :], sem_out)
    result.start()
    finish(turned)
    finish(ex_d)
    result.wait()


def dec1_kernel(
    d_2, s1, um_h, ur_h, am_h, ar_h, w_d1b, b_d1a_h, b_d1b_h, w_head_h, b_head_h, out,
    b_d1a, b_d1b, w_head, b_head, x_u, x_s, x_d, y_rest, st_b, wu_main, wu_rest, wa_main, wa_rest, wb_main, wb_rest, wide, result, pending, stage, skip, low, late,
    sem, small_sem, send_sem, recv_sem,
):
    strip = strip_index()
    row = lax.axis_index("row")
    col = lax.axis_index("col")
    copy_um = pltpu.make_async_copy(um_h, wu_main, sem.at[0])
    copy_ur = pltpu.make_async_copy(ur_h, wu_rest, sem.at[1])
    copy_am = pltpu.make_async_copy(am_h, wa_main, sem.at[FIVE])
    copy_ar = pltpu.make_async_copy(ar_h, wa_rest, sem.at[SIX])
    copy_s = pltpu.make_async_copy(s1, skip, sem.at[2])
    copy_b = pltpu.make_async_copy(w_d1b, st_b, sem.at[KERNEL])
    copy_d = pltpu.make_async_copy(d_2, low, sem.at[IN_CH])
    barrier = enter_barrier()
    copy_um.start()
    copy_ur.start()
    copy_d.start()
    small = fetch((b_d1a_h, b_d1b_h, w_head_h, b_head_h), (b_d1a, b_d1b, w_head, b_head), small_sem)

    stage[...] = jnp.zeros_like(stage)
    copy_um.wait()
    copy_ur.wait()
    copy_s.start()
    copy_ar.start()
    copy_am.start()
    copy_b.start()
    copy_d.wait()
    for copy in small:
        copy.wait()

    def up1(i):
        lhs = low[BASE_PAD * i : BASE_PAD * i + BASE_PAD, :]
        rest = dot(lhs, wu_rest[...])
        for p in range(2):
            part = rest[:, LANES * p : LANES * p + LANES]
            buf = wide.at[2 * i + p]
            buf[2, pl.ds(0, BASE_PAD, stride=2), :] = low_lanes(part)
            buf[2, pl.ds(1, BASE_PAD, stride=2), :] = low_lanes(pltpu.roll(part, REST, axis=1))
            for q in range(2):
                tap = 2 * p + q
                main = dot(lhs, wu_main[MIDDLE * tap : MIDDLE * tap + MIDDLE, :])
                buf[0, pl.ds(q, BASE_PAD, stride=2), :] = main[:, 0:LANES]
                buf[1, pl.ds(q, BASE_PAD, stride=2), :] = main[:, LANES:TILE]
            for r in range(SIX):
                main = jnp.concatenate([buf[0, LANES * r : LANES * r + LANES, :], buf[1, LANES * r : LANES * r + LANES, :]], axis=1)
                tail = buf[2, LANES * r : LANES * r + LANES, :]
                if (i, r) == (0, 0):
                    main, tail = jnp.where(strip > 0, main, 0.0), jnp.where(strip > 0, tail, 0.0)
                if (i, r) == (2, FIVE):
                    main, tail = jnp.where(strip < LAST_STRIP, main, 0.0), jnp.where(strip < LAST_STRIP, tail, 0.0)
                put3_320(x_u, (N12 * i + 2 * r + p) * LANES, main, tail, LANES)

    def spread(j):
        rows = pl.ds(TILE * j, TILE)
        put3_320(x_s, TILE * j, skip[rows, 0:TILE].astype(F32), skip[rows, TILE:BASE_PAD].astype(F32), LANES, stage.at[j % 2])

    def rest_a(i):
        for j in range(SIX * i, SIX * i + SIX):
            y_rest[TILE * j : TILE * j + TILE, :] = dot(packed_rows(x_u, TILE * j, TILE), wa_rest[0:PACK, :]) + dot(
                packed_rows(x_s, TILE * j, TILE), wa_rest[PACK:N2048, :]
            )
            if j < N17:
                spread(j + 1)

    up1(0)
    up1(1)
    copy_s.wait()
    copy_ar.wait()
    spread(0)
    up1(2)
    for i in range(KERNEL):
        rest_a(i)
    copy_am.wait()

    def conv_a(row0):
        acc = None
        for di in range(KERNEL):
            for src, ref in enumerate((x_u, x_s)):
                base = N3072 * src + PACK * di
                part = dot(packed_rows(ref, row0 + LANES * di, TILE), wa_main[base : base + PACK, :])
                acc = part if acc is None else acc + part
        return acc

    def put_a(acc, row0, first_row, slot):
        main = valid_rows(jnp.maximum(acc + bias_row(b_d1a, 0, TILE), 0.0), first_row, LANES)
        tail = valid_rows(jnp.maximum(rest_sum(y_rest, row0, TILE) + bias_rest(b_d1a), 0.0), first_row, LANES)
        put3_320(x_d, row0, main, low_lanes(tail), LANES, stage.at[slot])

    late[...] = jnp.zeros_like(late)

    def dec1a(i, carry):
        base = pl.multiple_of(i * PACK, PACK)
        put_a(late[...], pl.multiple_of(jnp.maximum(base - TILE, 0), TILE), STRIP_ROWS * strip - KERNEL + STRIPS * i, 1)
        for j in range(IN_CH):
            acc = conv_a(base + TILE * j)
            if j == KERNEL:
                late[...] = acc
            else:
                put_a(acc, base + TILE * j, STRIP_ROWS * strip - 1 + STRIPS * i + 2 * j, j % 2)
        return carry

    copy_b.wait()
    lax.fori_loop(0, IN_CH, dec1a, 0)
    pack_weights(st_b, wb_main, wb_rest)
    put_a(late[...], N3840, STRIP_ROWS * strip + N29, 1)
    put_a(conv_a(N4096), N4096, STRIP_ROWS * strip + N31, 0)

    head_bias = jnp.zeros((IN_CH, LANES), F32)
    for channel in range(IN_CH):
        head_bias = jnp.where(lax.broadcasted_iota(jnp.int32, (IN_CH, LANES), 0) == channel, b_head[channel], head_bias)

    pending[...] = jnp.zeros_like(pending)

    def head(hidden, row0):
        line = lax.dot_general(w_head[...], hidden, (((1,), (1,)), ((), ())), preferred_element_type=F32)
        for r in range(2):
            part = line[:, LANES * r : LANES * r + LANES] + head_bias
            result[0, row0 + r] = part[:, 0:REST]
            result[1, row0 + r] = part[:, REST:LANES]

    pushes = []
    for part, first, rows in ((0, 0, N22), (1, N22, N10)):
        for side in range(2):
            pushes.append(
                Push(
                    result.at[side, pl.ds(first, rows)],
                    out.at[pl.ds(STRIP_ROWS * (strip % 2) + first, rows)],
                    send_sem.at[part, side],
                    recv_sem.at[part, strip % 2],
                    (lax.axis_index("data"), side, strip // 2),
                    (strip // 2 == row) & (col == side),
                )
            )

    def dec1b(i, carry):
        base = pl.multiple_of(i * PACK, PACK)

        @pl.when(i == KERNEL)
        def _():
            pl.semaphore_wait(barrier, STRIPS)
            for push in pushes[0:2]:
                push.start()

        def rest(j):
            y_rest[TILE * j : TILE * j + TILE, :] = dot(packed_rows(x_d, base + TILE * j, TILE), wb_rest[...])

        rest(0)
        waiting = pending[...]
        for j in range(IN_CH):
            rest(j + 1)
            acc = dot(packed_rows(x_d, base + TILE * j, TILE), wb_main[0:PACK, :])
            acc = acc + dot(packed_rows(x_d, base + TILE * j + LANES, TILE), wb_main[PACK:N2048, :])
            acc = acc + dot(packed_rows(x_d, base + TILE * j + TILE, TILE), wb_main[N2048:N3072, :])
            head(waiting, jnp.maximum(STRIPS * i + 2 * j - 2, 0))
            main = jnp.maximum(acc + bias_row(b_d1b, 0, TILE), 0.0).astype(BF16)
            tail = jnp.maximum(rest_sum(y_rest, TILE * j, TILE) + bias_rest(b_d1b), 0.0).astype(BF16)
            waiting = jnp.concatenate([main, tail[:, 0:REST]], axis=1)
        pending[...] = waiting
        return carry

    lax.fori_loop(0, IN_CH, dec1b, 0)
    head(pending[...], N30)

    for push in pushes[2:IN_CH]:
        push.start()
    for push in pushes:
        push.wait_send()
    for part, first, rows in ((0, 0, N22), (1, N22, N10)):
        for half in range(2):
            Push(
                result.at[0, pl.ds(first, rows)], out.at[pl.ds(STRIP_ROWS * half + first, rows)],
                send_sem.at[part, 0], recv_sem.at[part, half], strip_device(strip), strip < 0,
            ).wait_recv()


def solution(mesh):
    tile_spec = P(("data", "row"), "col", None)

    def body(image_tile, *params):
        (w_enc1a, b_enc1a, w_enc1b, b_enc1b, w_enc2a, b_enc2a, w_enc2b, b_enc2b,
         w_mid_a, b_mid_a, w_mid_b, b_mid_b, w_up2, w_dec2a, b_dec2a, w_dec2b, b_dec2b,
         w_up1, w_dec1a, b_dec1a, w_dec1b, b_dec1b, w_head, b_head) = params
        def flat(weight):
            return weight.reshape(-1, weight.shape[-1])

        hbm = pl.BlockSpec(memory_space=pl.ANY)
        dma = pltpu.SemaphoreType.DMA
        s1, p1 = pl.pallas_call(
            enc1_kernel,
            grid=(KERNEL,),
            out_shape=(jax.ShapeDtypeStruct((N4608, BASE_PAD), BF16), jax.ShapeDtypeStruct((STRIPS, N1152, LANES), BF16)),
            in_specs=[hbm] * FIVE,
            out_specs=(pl.BlockSpec((N1536, BASE_PAD), lambda i: (i, 0)), pl.BlockSpec((STRIPS, BASE_PAD, LANES), lambda i: (0, i, 0))),
            scratch_shapes=[
                pltpu.VMEM((REST, IN_CH, REST), BF16),
                pltpu.VMEM((KERNEL, KERNEL, IN_CH, BASE), BF16),
                pltpu.VMEM((BASE,), F32),
                pltpu.VMEM((BASE,), F32),
                pltpu.VMEM((2, N40, IN_CH, REST), BF16),
                pltpu.VMEM((N50, STRIP_ROWS, LANES), BF16),
                pltpu.VMEM((N96, BASE_PAD), BF16),
                pltpu.VMEM((N2880, BASE), BF16),
                pltpu.VMEM((STRIPS, N5136, LANES), BF16),
                pltpu.VMEM((N1792, TILE), F32),
                pltpu.VMEM((N3072, TILE), BF16),
                pltpu.VMEM((PACK, TILE), BF16),
                pltpu.VMEM((2, LANES, LANES), F32),
                pltpu.VMEM((2, KERNEL, N288, LANES), F32),
                pltpu.VMEM((2, KERNEL, N80, LANES), F32),
                dma, dma((IN_CH,)), dma((IN_CH,)), dma((2, 2)),
            ],
            compiler_params=pltpu.CompilerParams(
                vmem_limit_bytes=VMEM_LIMIT, collective_id=1, has_side_effects=True, dimension_semantics=("arbitrary",)
            ),
            name="enc1",
        )(image_tile.transpose(0, 2, 1), w_enc1a, b_enc1a, flat(w_enc1b), b_enc1b)

        turned_shapes = ((N2560, TILE), (MIDDLE, TILE), (N6144, TILE), (N2048, TILE))

        def turned(weight):
            return weight.transpose(0, 1, KERNEL, 2).reshape(-1, weight.shape[2])

        d2, *level_one = pl.pallas_call(
            mid_kernel,
            out_shape=[jax.ShapeDtypeStruct(shape, BF16) for shape in ((N1152, MIDDLE),) + turned_shapes],
            in_specs=[hbm] * N16,
            out_specs=[hbm] * FIVE,
            scratch_shapes=[
                *[pltpu.VMEM((size,), F32) for size in (MIDDLE, MIDDLE, DEEP, DEEP, MIDDLE, MIDDLE)],
                *[pltpu.VMEM(shape, BF16) for shape in turned_shapes],
                pltpu.VMEM((STRIPS, N1168, LANES), BF16),
                pltpu.VMEM((N3072, MIDDLE), BF16),
                pltpu.VMEM((RING_ROWS, DEEP), BF16),
                pltpu.VMEM((N1152, MIDDLE3), BF16),
                pltpu.VMEM((N1152, MIDDLE3), BF16),
                pltpu.VMEM((N1152, MIDDLE3), BF16),
                pltpu.VMEM((BASE, MIDDLE3), BF16),
                pltpu.VMEM((BASE, N3840), BF16),
                pltpu.VMEM((TILE, DEEP), BF16),
                pltpu.VMEM((N1152, MIDDLE), BF16),
                pltpu.VMEM((TILE, DEEP), F32),
                pltpu.VMEM((FIVE, N512, LANES), F32),
                pltpu.VMEM((LANES, LANES), F32),
                dma((N18,)), dma((TAPS,)), dma((KERNEL,)), dma((TAPS,)), dma((IN_CH,)), dma((TAPS,)), dma((TAPS,)), dma, dma, dma((SIX,)), dma((SIX,)),
                dma((LAST_STRIP, 2)), dma((LAST_STRIP, 2)),
            ],
            compiler_params=pltpu.CompilerParams(
                vmem_limit_bytes=VMEM_LIMIT, collective_id=0, has_side_effects=True
            ),
            name="mid",
        )(
            p1, flat(w_enc2a), flat(w_enc2b), flat(w_mid_a), flat(w_mid_b), flat(w_up2), flat(w_dec2a), flat(w_dec2b),
            turned(w_up1), turned(w_dec1a),
            b_enc2a, b_enc2b, b_mid_a, b_mid_b, b_dec2a, b_dec2b,
        )

        y = pl.pallas_call(
            dec1_kernel,
            out_shape=jax.ShapeDtypeStruct((REST, IN_CH, REST), F32),
            in_specs=[hbm] * N11,
            out_specs=hbm,
            scratch_shapes=[
                pltpu.VMEM((BASE,), F32),
                pltpu.VMEM((BASE,), F32),
                pltpu.VMEM((IN_CH, BASE), BF16),
                pltpu.SMEM((IN_CH,), F32),
                pltpu.VMEM((STRIPS, N4624, LANES), BF16),
                pltpu.VMEM((STRIPS, N4624, LANES), BF16),
                pltpu.VMEM((STRIPS, N4368, LANES), BF16),
                pltpu.VMEM((N4608, TILE), F32),
                pltpu.VMEM((N2880, BASE), BF16),
                pltpu.VMEM((N2560, TILE), BF16),
                pltpu.VMEM((MIDDLE, TILE), BF16),
                pltpu.VMEM((N6144, TILE), BF16),
                pltpu.VMEM((N2048, TILE), BF16),
                pltpu.VMEM((N3072, TILE), BF16),
                pltpu.VMEM((PACK, TILE), BF16),
                pltpu.VMEM((SIX, KERNEL, REST_AT, LANES), F32),
                pltpu.VMEM((2, STRIP_ROWS, IN_CH, REST), F32),
                pltpu.VMEM((TILE, BASE), BF16),
                pltpu.VMEM((2, KERNEL, N288, LANES), F32),
                pltpu.VMEM((N4608, BASE_PAD), BF16),
                pltpu.VMEM((N1152, MIDDLE), BF16),
                pltpu.VMEM((TILE, TILE), F32),
                dma((LAST_STRIP,)), dma((IN_CH,)), dma((2, 2)), dma((2, 2)),
            ],
            compiler_params=pltpu.CompilerParams(vmem_limit_bytes=VMEM_LIMIT, collective_id=2, has_side_effects=True),
            name="dec1",
        )(d2, s1, *level_one, flat(w_dec1b), b_dec1a, b_dec1b, w_head.T, b_head)
        return y.transpose(0, 2, 1)

    def program(image, *params):
        mapped = jax.shard_map(
            body, mesh=mesh, in_specs=(tile_spec,) + (P(),) * len(params), out_specs=tile_spec, check_vma=False
        )
        return mapped(image, *params)

    return program
```

```python
import functools

import jax
import jax.numpy as jnp
from jax import lax
from jax.experimental import pallas as pl
from jax.experimental.pallas import tpu as pltpu
from jax.sharding import PartitionSpec as P

KERNEL = 3
IN_CH = 4
FIVE = 5
SIX = 6
LAST_STRIP = 7
STRIPS = 8
TAPS = 9
N10 = 10
N11 = 11
N12 = 12
N16 = 16
N17 = 17
N18 = 18
N20 = 20
N22 = 22
N28 = 28
N29 = 29
N30 = 30
N31 = 31
STRIP_ROWS = 32
N36 = 36
N40 = 40
N42 = 42
N50 = 50
N60 = 60
REST = 64
N80 = 80
N96 = 96
N127 = 127
LANES = 128
N192 = 192
N224 = 224
TILE = 256
N288 = 288
BASE = 320
BASE_PAD = 384
N512 = 512
MIDDLE = 640
REST_AT = 768
PACK_USED = 960
PACK = 1024
N1152 = 1152
N1168 = 1168
DEEP = 1280
N1536 = 1536
N1792 = 1792
MIDDLE3 = 1920
N2048 = 2048
N2560 = 2560
N2880 = 2880
N3072 = 3072
N3200 = 3200
N3840 = 3840
N4096 = 4096
N4368 = 4368
N4608 = 4608
N4624 = 4624
N5136 = 5136
N6144 = 6144
N6400 = 6400
N8960 = 8960
N10240 = 10240
N11520 = 11520
BF16 = jnp.bfloat16
F32 = jnp.float32
MESH = pl.DeviceIdType.MESH
VMEM_LIMIT = 66_900_000
RING_ROWS = N11520


def strip_index():
    col = lax.axis_index("col")
    row = lax.axis_index("row")
    return row + col * (LAST_STRIP - 2 * row)


def strip_device(position):
    col = position // IN_CH
    rest = position % IN_CH
    return (lax.axis_index("data"), col, rest + col * (KERNEL - 2 * rest))


def dot(a, b):
    return jnp.dot(a, b, preferred_element_type=F32)


def shifted(value, width, step):
    if step == 1:
        return value
    rows = value.shape[0]
    column = lax.broadcasted_iota(jnp.int32, value.shape, 0) % width
    if step == 0:
        return jnp.where(column == 0, 0.0, pltpu.roll(value, 1, axis=0))
    return jnp.where(column == width - 1, 0.0, pltpu.roll(value, rows - 1, axis=0))


def put3(dst, row0, lane0, channels, value, width):
    rows, lanes = value.shape
    for step in range(KERNEL):
        dst[pl.ds(row0, rows), pl.ds(step * channels + lane0, lanes)] = shifted(value, width, step).astype(BF16)


def put3_320(dst, row0, main, rest, width, stage=None):
    rows = main.shape[0]
    pitch = width + N16
    planes = [main[:, 0:LANES], main[:, LANES:TILE], rest]
    for t, plane in enumerate(planes if stage is not None else []):
        for r in range(rows // width):
            stage[t, pitch * r + STRIPS : pitch * r + STRIPS + width, :] = plane[width * r : width * r + width]

    def moved(t, step):
        if stage is None:
            return shifted(planes[t], width, step)
        first = LAST_STRIP + step
        parts = [stage[t, pitch * r + first : pitch * r + first + width, :] for r in range(rows // width)]
        return jnp.concatenate(parts, axis=0) if len(parts) > 1 else parts[0]

    for step in range(KERNEL):
        for t in range(2):
            dst[2 * step + t, pl.ds(row0, rows), :] = moved(t, step).astype(BF16)
    first = moved(2, 0) + pltpu.roll(moved(2, 1), REST, axis=1)
    dst[SIX, pl.ds(row0, rows), :] = first.astype(BF16)
    dst[LAST_STRIP, pl.ds(row0, rows), :] = moved(2, 2).astype(BF16)


def packed_rows(ref, row0, rows):
    return jnp.concatenate([ref[t, pl.ds(row0, rows), :] for t in range(STRIPS)], axis=1)


def low_lanes(value):
    return jnp.where(lax.broadcasted_iota(jnp.int32, value.shape, 1) < REST, value, 0.0)


def pack_weights(staged, main_ref, rest_ref):
    for dj in range(KERNEL):
        for start, size, row in ((0, TILE, TILE * dj), (TILE, REST, REST_AT + REST * dj)):
            parts = []
            for di in range(KERNEL):
                base = (KERNEL * di + dj) * BASE + start
                main_ref[pl.ds(PACK * di + row, size), :] = staged[pl.ds(base, size), 0:TILE]
                parts.append(staged[pl.ds(base, size), TILE:BASE])
            parts.append(jnp.zeros((size, REST), BF16))
            rest_ref[pl.ds(row, size), :] = jnp.concatenate(parts, axis=1)
    clear_pad(main_ref, KERNEL)
    clear_pad(rest_ref, 1)


def clear_pad(ref, groups):
    for group in range(groups):
        ref[pl.ds(PACK * group + PACK_USED, REST), :] = jnp.zeros((REST, ref.shape[1]), BF16)


def turn_main(staged, main_ref, di, dj):
    turned = staged[pl.ds(pl.multiple_of(PACK_USED * di + BASE * dj, REST), TILE), :].T
    for src in range(2):
        base = N3072 * src + PACK * di
        main_ref[pl.ds(pl.multiple_of(base + TILE * dj, REST), TILE), :] = turned[BASE * src : BASE * src + TILE]
        main_ref[pl.ds(pl.multiple_of(base + REST_AT + REST * dj, REST), REST), :] = turned[BASE * src + TILE : BASE * src + BASE]


def turn_rest(staged, rest_ref, dj):
    parts = [staged[pl.ds(pl.multiple_of(PACK_USED * di + BASE * dj + TILE, REST), REST), :] for di in range(KERNEL)]
    turned = jnp.concatenate(parts + [jnp.zeros((REST, MIDDLE), BF16)], axis=0).T
    for src in range(2):
        rest_ref[pl.ds(pl.multiple_of(PACK * src + TILE * dj, REST), TILE), :] = turned[BASE * src : BASE * src + TILE]
        rest_ref[pl.ds(pl.multiple_of(PACK * src + REST_AT + REST * dj, REST), REST), :] = turned[BASE * src + TILE : BASE * src + BASE]


def bias_row(ref, start, size):
    return ref[pl.ds(start, size)].reshape(1, size)


def bias_rest(ref):
    return jnp.concatenate([bias_row(ref, TILE, REST), jnp.zeros((1, REST), F32)], axis=1)


def enter_barrier():
    barrier = pltpu.get_barrier_semaphore()
    for position in range(STRIPS):
        pl.semaphore_signal(barrier, inc=1, device_id=strip_device(position), device_id_type=MESH)
    return barrier


def fetch(sources, targets, sems):
    copies = [pltpu.make_async_copy(src, dst, sems.at[i]) for i, (src, dst) in enumerate(zip(sources, targets))]
    for copy in copies:
        copy.start()
    return copies


class Push:
    def __init__(self, src, dst, send_sem, recv_sem, device, here):
        self.here = here
        self.local = pltpu.make_async_copy(src, dst, recv_sem)
        self.remote = pltpu.make_async_remote_copy(
            src_ref=src, dst_ref=dst, send_sem=send_sem, recv_sem=recv_sem, device_id=device, device_id_type=MESH
        )

    def start(self):
        @pl.when(self.here)
        def _():
            self.local.start()

        @pl.when(jnp.logical_not(self.here))
        def _():
            self.remote.start()

    def wait_send(self):
        @pl.when(jnp.logical_not(self.here))
        def _():
            self.remote.wait_send()

    def wait_recv(self):
        self.remote.wait_recv()


def rest_sum(y_ref, row0, rows):
    total = y_ref[pl.ds(row0, rows), 0:LANES] + y_ref[pl.ds(row0 + TILE, rows), LANES:TILE]
    return total + pltpu.roll(y_ref[pl.ds(row0 + LANES, rows), 0:LANES], REST, axis=1)


def valid_rows(value, first_row, width):
    row = first_row + lax.broadcasted_iota(jnp.int32, value.shape, 0) // width
    return jnp.where((row >= 0) & (row < TILE), value, 0.0)


def pooled(value, width, scratch):
    rows, lanes = value.shape
    tall = jnp.concatenate(
        [jnp.maximum(value[s : s + width], value[s + width : s + 2 * width]) for s in range(0, rows, 2 * width)], axis=0
    )
    halves = []
    for start in range(0, lanes, LANES):
        scratch[0 : rows // 2, :] = tall[:, start : start + LANES]
        halves.append(
            jnp.maximum(scratch[pl.ds(0, rows // IN_CH, stride=2), :], scratch[pl.ds(1, rows // IN_CH, stride=2), :])
        )
    return jnp.concatenate(halves, axis=1) if len(halves) > 1 else halves[0]


def enc1_kernel(
    image_hbm, w_a_hbm, b_a_hbm, w_b, b_b_hbm, s1_out, p1_out,
    image, w_a, b_a, b_b, halves, planes, w_stem, staged, x_a, y_rest, w_main, w_rest, pool_buf, stage, stage_p, w_sem, small_sem, send_sem, recv_sem,
):
    step = pl.program_id(0)
    strip = strip_index()

    @pl.when(step == 0)
    def _():
        row = lax.axis_index("row")
        col = lax.axis_index("col")
        barrier = enter_barrier()
        small = fetch((image_hbm, w_a_hbm, b_a_hbm, b_b_hbm), (image, w_a, b_a, b_b), small_sem)
        copy_w = pltpu.make_async_copy(w_b, staged, w_sem)
        copy_w.start()
        stage[...] = jnp.zeros_like(stage)
        stage_p[...] = jnp.zeros_like(stage_p)

        for copy in small:
            copy.wait()
        for di in range(KERNEL):
            taps = []
            for dj in range(KERNEL):
                tap = jnp.concatenate([w_a[di, dj].astype(F32), jnp.zeros((IN_CH, BASE), F32)], axis=0)
                taps.append(jnp.concatenate([tap, jnp.zeros((STRIPS, REST), F32)], axis=1))
            taps.append(jnp.zeros((STRIPS, BASE_PAD), F32))
            w_stem[STRIP_ROWS * di : STRIP_ROWS * di + STRIP_ROWS, :] = jnp.concatenate(taps, axis=0).astype(BF16)

        planes[N40:N42, :, :] = jnp.zeros((2, STRIP_ROWS, LANES), BF16)

        pl.semaphore_wait(barrier, STRIPS)
        pushes = []
        for index, (target, src_row, dst_row, rows) in enumerate(
            ((2 * row, 0, IN_CH, N36), (2 * row + 1, N28, 0, N36), ((2 * row + 2) % STRIPS, N60, 0, IN_CH), ((2 * row + LAST_STRIP) % STRIPS, 0, N36, IN_CH))
        ):
            pushes.append(
                Push(
                    image.at[pl.ds(src_row, rows)],
                    halves.at[col, pl.ds(dst_row, rows)],
                    send_sem.at[index],
                    recv_sem.at[index // 2, col],
                    strip_device(target),
                    target == strip,
                )
            )
        for push in pushes:
            push.start()
        copy_w.wait()
        pack_weights(staged, w_main, w_rest)
        for push in pushes:
            push.wait_send()
        for kind, rows in ((0, N36), (1, IN_CH)):
            for side in range(2):
                Push(
                    image.at[pl.ds(0, rows)], halves.at[side, pl.ds(0, rows)],
                    send_sem.at[0], recv_sem.at[kind, side], strip_device(strip), strip < 0,
                ).wait_recv()

        def expand(i, carry):
            for j in range(N20):
                r = N20 * i + j
                both = jnp.concatenate([halves[0, r].astype(F32), halves[1, r].astype(F32)], axis=1)
                image_row = STRIP_ROWS * strip - IN_CH + r
                both = jnp.where((image_row >= 0) & (image_row < TILE), both, 0.0)
                both = jnp.concatenate([both, jnp.zeros((IN_CH, LANES), F32)], axis=0)
                column = lax.broadcasted_iota(jnp.int32, (STRIPS, LANES), 1)
                before = jnp.where(column == 0, 0.0, pltpu.roll(both, 1, axis=1))
                after = jnp.where(column == N127, 0.0, pltpu.roll(both, N127, axis=1))
                planes[r] = jnp.concatenate([before, both, after, jnp.zeros((STRIPS, LANES), F32)], axis=0).astype(BF16)
            return carry

        lax.fori_loop(0, 2, expand, 0)

        def stem(i, carry):
            for j in range(STRIPS):
                r = STRIPS * i + j
                patch = jnp.concatenate([planes[r + di] for di in range(KERNEL)], axis=0)
                acc = lax.dot_general(patch, w_stem[...], (((0,), (0,)), ((), ())), preferred_element_type=F32)
                image_row = STRIP_ROWS * strip - KERNEL + r
                inside = (image_row >= 0) & (image_row < TILE)
                main = jnp.where(inside, jnp.maximum(acc[:, 0:TILE] + bias_row(b_a, 0, TILE), 0.0), 0.0)
                tail = jnp.where(inside, jnp.maximum(acc[:, TILE:BASE_PAD] + bias_rest(b_a), 0.0), 0.0)
                put3_320(x_a, pl.multiple_of(r * LANES, LANES), main, tail, LANES, stage.at[j % 2])
            return carry

        lax.fori_loop(0, FIVE, stem, 0)

    base = pl.multiple_of(step * N1536, N512)

    def rest(j):
        y_rest[TILE * j : TILE * j + TILE, :] = dot(packed_rows(x_a, base + TILE * j, TILE), w_rest[...])

    rest(0)
    for j in range(SIX):
        rest(j + 1)
        acc = dot(packed_rows(x_a, base + TILE * j, TILE), w_main[0:PACK, :])
        acc = acc + dot(packed_rows(x_a, base + TILE * j + LANES, TILE), w_main[PACK:N2048, :])
        acc = acc + dot(packed_rows(x_a, base + TILE * j + TILE, TILE), w_main[N2048:N3072, :])
        first_row = STRIP_ROWS * strip - 2 + N12 * step + 2 * j
        main = valid_rows(jnp.maximum(acc + bias_row(b_b, 0, TILE), 0.0), first_row, LANES)
        tail = jnp.maximum(rest_sum(y_rest, TILE * j, TILE) + bias_rest(b_b), 0.0)
        tail = low_lanes(valid_rows(tail, first_row, LANES))
        s1_out[TILE * j : TILE * j + TILE, 0:TILE] = main.astype(BF16)
        s1_out[TILE * j : TILE * j + TILE, TILE:BASE_PAD] = tail.astype(BF16)
        put3_320(p1_out, REST * j, pooled(main, LANES, pool_buf.at[j % 2]), pooled(tail, LANES, pool_buf.at[j % 2]), REST, stage_p.at[j % 2])


def mid_kernel(
    p1_hbm, w_2a, w_2b, w_ma, w_mb, w_u2, w_d2a, w_d2b, w_u1, w_d1a, b_2a_h, b_2b_h, b_ma_h, b_mb_h, b_d2a_h, b_d2b_h,
    out, um_out, ur_out, am_out, ar_out,
    b_2a, b_2b, b_ma, b_mb, b_d2a, b_d2b, wu_main, wu_rest, wa_main, wa_rest,
    p1, first_w, ring, x_a, x_s, x_u, m_1, m_2, m_o, d_2, acc_ref, wide, pool_buf,
    sem_2a, sem_2b, sem_ma, sem_mb, sem_u2, sem_d2a, sem_d2b, sem_p1, sem_out, turn_sem, small_sem, send_sem, recv_sem,
):
    strip = strip_index()
    prev_dev = strip_device((strip + LAST_STRIP) % STRIPS)
    next_dev = strip_device((strip + 1) % STRIPS)

    def exchange(buf, width, lane0, lanes, rows, index, target=None):
        target = buf if target is None else target
        lane = pl.ds(lane0, lanes)
        copies = []
        for side, src_row, dst_row, device in ((0, 1, rows + 1, prev_dev), (1, rows, 0, next_dev)):
            copies.append(
                pltpu.make_async_remote_copy(
                    src_ref=buf.at[pl.ds(src_row * width, width), lane],
                    dst_ref=target.at[pl.ds(dst_row * width, width), lane],
                    send_sem=send_sem.at[index, side],
                    recv_sem=recv_sem.at[index, side],
                    device_id=device,
                    device_id_type=MESH,
                )
            )
        return copies

    def start(copies):
        for copy in copies:
            copy.start()

    def finish(copies):
        for copy in copies:
            copy.wait()

    def halo(buf, width, channels, rows):
        for row, inside in ((0, strip > 0), (rows + 1, strip < LAST_STRIP)):
            value = buf[pl.ds(row * width, width), pl.ds(channels, channels)].astype(F32)
            put3(buf, row * width, 0, channels, jnp.where(inside, value, 0.0), width)

    copies_2a = []
    for tap in range(TAPS):
        di, dj = tap // KERNEL, tap % KERNEL
        for part, (start_row, size, row) in enumerate(((0, TILE, TILE * dj), (TILE, REST, REST_AT + REST * dj))):
            copies_2a.append(
                pltpu.make_async_copy(
                    w_2a.at[pl.ds(BASE * tap + start_row, size), :],
                    first_w.at[pl.ds(PACK * di + row, size), :],
                    sem_2a.at[2 * tap + part],
                )
            )

    def tap_copies(src, rows, base, sem):
        return [
            pltpu.make_async_copy(
                src.at[pl.ds(rows * tap, rows), :],
                ring.at[pl.ds(base + rows * (tap // 2), rows), pl.ds(MIDDLE * (tap % 2), MIDDLE)],
                sem.at[tap],
            )
            for tap in range(src.shape[0] // rows)
        ]

    copies_2b = tap_copies(w_2b, MIDDLE, 0, sem_2b)
    copies_ma = [
        pltpu.make_async_copy(w_ma.at[pl.ds(MIDDLE3 * di, MIDDLE3), :], ring.at[pl.ds(N3200 + MIDDLE3 * t, MIDDLE3), :], sem_ma.at[t])
        for t, di in enumerate((1, 0, 2))
    ]

    def mb_row(k):
        return (N8960 + DEEP * k) % RING_ROWS

    copies_mb = [
        pltpu.make_async_copy(
            w_mb.at[pl.ds(DEEP * (KERNEL * (1, 0, 2)[k // KERNEL] + k % KERNEL), DEEP), :], ring.at[pl.ds(mb_row(k), DEEP), :], sem_mb.at[k]
        )
        for k in range(TAPS)
    ]
    copies_u2 = [
        pltpu.make_async_copy(
            w_u2.at[pl.ds(DEEP * tap, DEEP), :],
            first_w.at[pl.ds(DEEP * tap, DEEP), :] if tap < 2 else ring.at[pl.ds(N8960, DEEP), pl.ds(MIDDLE * (tap - 2), MIDDLE)],
            sem_u2.at[tap],
        )
        for tap in range(IN_CH)
    ]
    st_u = ring.at[pl.ds(N10240, DEEP), pl.ds(0, MIDDLE)]
    copies_turn = [
        pltpu.make_async_copy(w_u1, st_u, turn_sem.at[0]),
        pltpu.make_async_copy(w_d1a, first_w.at[pl.ds(0, N2880), :], turn_sem.at[1]),
    ]
    copies_d2a = tap_copies(w_d2a, DEEP, 0, sem_d2a)
    copies_d2b = tap_copies(w_d2b, MIDDLE, N6400, sem_d2b)

    copy_p1 = pltpu.make_async_copy(p1_hbm, p1.at[:, pl.ds(0, N1152), :], sem_p1)
    barrier = pltpu.get_barrier_semaphore()
    for device in (prev_dev, next_dev):
        pl.semaphore_signal(barrier, inc=1, device_id=device, device_id_type=MESH)
    copy_p1.start()
    start(copies_2a)
    small = fetch(
        (b_2a_h, b_2b_h, b_ma_h, b_mb_h, b_d2a_h, b_d2b_h), (b_2a, b_2b, b_ma, b_mb, b_d2a, b_d2b), small_sem
    )
    pl.semaphore_wait(barrier, 2)

    for di in range(KERNEL):
        first_w[PACK * di + PACK_USED : PACK * di + PACK, :] = jnp.zeros((REST, MIDDLE), BF16)
    copy_p1.wait()
    finish(small)
    finish(copies_2a)
    start(copies_2b)
    start(copies_ma)

    ex_a = exchange(x_a, REST, MIDDLE, MIDDLE, N16, 0)
    ex_s = exchange(x_s, REST, MIDDLE, MIDDLE, N16, 1)
    ex_m1 = exchange(m_1, STRIP_ROWS, MIDDLE, MIDDLE, STRIPS, 2)
    ex_m2 = exchange(m_2, STRIP_ROWS, DEEP, DEEP, STRIPS, KERNEL)
    ex_u = exchange(x_u, REST, MIDDLE, MIDDLE, N16, IN_CH)
    ex_b = exchange(x_a, REST, MIDDLE, MIDDLE, N16, FIVE)
    ex_d = exchange(d_2, REST, 0, MIDDLE, N16, SIX, out)
    tiles = ((0, TILE), (TILE, TILE), (N512, LANES))

    def enc2a(i, carry):
        @pl.when(i == 1)
        def _():
            start(ex_a)

        for block in (i, KERNEL - i):
            row0 = pl.multiple_of(block * TILE, TILE)
            for lane0, lanes in tiles:
                acc = dot(packed_rows(p1, row0, TILE), first_w[0:PACK, pl.ds(lane0, lanes)])
                for di in (1, 2):
                    acc = acc + dot(
                        packed_rows(p1, row0 + REST * di, TILE),
                        first_w[PACK * di : PACK * di + PACK, pl.ds(lane0, lanes)],
                    )
                value = jnp.maximum(acc + bias_row(b_2a, lane0, lanes), 0.0)
                put3(x_a, row0 + REST, lane0, MIDDLE, value, REST)
        return carry

    lax.fori_loop(0, 2, enc2a, 0)
    finish(copies_2b)
    start(copies_mb[0:2])
    start(copies_u2[0:2])

    def conv640(src, row0, base, lane0, lanes):
        weights = jnp.concatenate(
            [
                ring[base + MIDDLE * (t // 2) : base + MIDDLE * (t // 2) + MIDDLE, pl.ds(MIDDLE * (t % 2) + lane0, lanes)]
                for t in range(TAPS)
            ],
            axis=0,
        )
        rows = jnp.concatenate([src[pl.ds(row0 + REST * di, TILE), :] for di in range(KERNEL)], axis=1)
        return dot(rows, weights)

    def enc2b(i, carry):
        block = i + 1 - 2 * (i % 2)
        row0 = pl.multiple_of(block * TILE, TILE)

        @pl.when(i == 1)
        def _():
            finish(ex_a)
            halo(x_a, REST, MIDDLE, N16)

        @pl.when(i == KERNEL)
        def _():
            start(ex_m1)
            start(ex_s)

        for lane0, lanes in tiles:
            value = jnp.maximum(conv640(x_a, row0, 0, lane0, lanes) + bias_row(b_2b, lane0, lanes), 0.0)
            put3(x_s, row0 + REST, lane0, MIDDLE, value, REST)
            put3(m_1, pl.multiple_of(block * REST + STRIP_ROWS, STRIP_ROWS), lane0, MIDDLE, pooled(value, REST, pool_buf), STRIP_ROWS)
        return carry

    lax.fori_loop(0, IN_CH, enc2b, 0)
    start(copies_mb[2:IN_CH])

    acc_ref[...] = jnp.zeros_like(acc_ref)
    finish(copies_ma)

    def mid_a(t, carry):
        di = (t + 1) % 2 + 2 * (t // 2) - t // 2

        @pl.when(t == 1)
        def _():
            start(copies_mb[IN_CH:SIX])
            finish(ex_m1)
            halo(m_1, STRIP_ROWS, MIDDLE, STRIPS)

        @pl.when(t == 2)
        def _():
            start(copies_mb[SIX:LAST_STRIP])

        base = pl.multiple_of(N3200 + MIDDLE3 * t, LANES)
        lhs_row = pl.multiple_of(STRIP_ROWS * di, STRIP_ROWS)
        for lane0 in range(0, DEEP, TILE):
            acc_ref[:, pl.ds(lane0, TILE)] += dot(
                m_1[pl.ds(lhs_row, TILE), :], ring[pl.ds(base, MIDDLE3), pl.ds(lane0, TILE)]
            )
        return carry

    lax.fori_loop(0, KERNEL, mid_a, 0)
    start(copies_mb[LAST_STRIP:TAPS])

    def mid_a_rows(first, rows):
        for lane0 in range(0, DEEP, TILE):
            value = jnp.maximum(acc_ref[pl.ds(first, rows), pl.ds(lane0, TILE)] + bias_row(b_ma, lane0, TILE), 0.0)
            put3(m_2, STRIP_ROWS + first, lane0, DEEP, value, STRIP_ROWS)

    mid_a_rows(0, STRIP_ROWS)
    mid_a_rows(N224, STRIP_ROWS)
    start(ex_m2)
    mid_a_rows(STRIP_ROWS, N192)
    acc_ref[...] = jnp.zeros_like(acc_ref)

    def mid_b(t, carry):
        di = (t + 1) % 2 + 2 * (t // 2) - t // 2

        for j in range(KERNEL):
            @pl.when(t == j)
            def _(j=j):
                finish(copies_mb[KERNEL * j : KERNEL * j + KERNEL])

        @pl.when(t == 1)
        def _():
            start(copies_u2[2:IN_CH])
            start(copies_d2a[0:2])
            finish(ex_m2)
            halo(m_2, STRIP_ROWS, DEEP, STRIPS)

        @pl.when(t == 2)
        def _():
            start(copies_d2a[2:STRIPS])

        lhs_row = pl.multiple_of(STRIP_ROWS * di, STRIP_ROWS)
        for lane0 in range(0, DEEP, TILE):
            acc = None
            for dj in range(KERNEL):
                base = pl.multiple_of(mb_row(KERNEL * t + dj), LANES)
                part = dot(
                    m_2[pl.ds(lhs_row, TILE), DEEP * dj : DEEP * dj + DEEP], ring[pl.ds(base, DEEP), pl.ds(lane0, TILE)]
                )
                acc = part if acc is None else acc + part
            acc_ref[:, pl.ds(lane0, TILE)] += acc
        return carry

    lax.fori_loop(0, KERNEL, mid_b, 0)
    start(copies_d2a[STRIPS:TAPS])
    for lane0 in range(0, DEEP, TILE):
        value = jnp.maximum(acc_ref[:, pl.ds(lane0, TILE)] + bias_row(b_mb, lane0, TILE), 0.0)
        m_o[:, pl.ds(lane0, TILE)] = value.astype(BF16)

    finish(copies_u2)
    for p in range(2):
        for q in range(2):
            for lane0, lanes in tiles:
                if p == 0:
                    weights = first_w[DEEP * q : DEEP * q + DEEP, pl.ds(lane0, lanes)]
                else:
                    weights = ring[N8960:N10240, pl.ds(MIDDLE * q + lane0, lanes)]
                part = dot(m_o[...], weights)
                for lane in range(0, lanes, LANES):
                    wide[(lane0 + lane) // LANES, pl.ds(q, TILE, stride=2), :] = part[:, lane : lane + LANES]

        if p == 0:
            start(copies_turn)

        def place(i, carry):
            src = pl.multiple_of(REST * i, REST)
            dst = pl.multiple_of(REST * (1 + 2 * i + p), REST)
            for lane0 in range(0, MIDDLE, LANES):
                put3(x_u, dst, lane0, MIDDLE, wide[lane0 // LANES, pl.ds(src, REST), :], REST)
            return carry

        lax.fori_loop(0, STRIPS, place, 0)
    start(ex_u)
    start(copies_d2b)
    finish(ex_s)
    halo(x_s, REST, MIDDLE, N16)
    finish(copies_d2a)
    finish(copies_turn)
    clear_pad(wa_main, SIX)
    clear_pad(wa_rest, 2)

    def dec2a(i, carry):
        block = i + 1 - 2 * (i % 2)
        row0 = pl.multiple_of(block * TILE, TILE)

        @pl.when(i == 1)
        def _():
            finish(ex_u)
            halo(x_u, REST, MIDDLE, N16)

        @pl.when(i == KERNEL)
        def _():
            start(ex_b)

        for lane0, lanes in tiles:
            acc = None
            for tap in range(TAPS):
                rows = pl.ds(row0 + REST * (tap // KERNEL), TILE)
                cols = pl.ds(MIDDLE * (tap % KERNEL), MIDDLE)
                lhs = jnp.concatenate([x_u[rows, cols], x_s[rows, cols]], axis=1)
                base = DEEP * (tap // 2)
                part = dot(lhs, ring[base : base + DEEP, pl.ds(MIDDLE * (tap % 2) + lane0, lanes)])
                acc = part if acc is None else acc + part
            value = jnp.maximum(acc + bias_row(b_d2a, lane0, lanes), 0.0)
            put3(x_a, row0 + REST, lane0, MIDDLE, value, REST)

        part = jnp.minimum(i, 2)
        for dj in range(KERNEL):
            turn_main(first_w, wa_main, part, dj)
        turn_rest(first_w, wa_rest, part)
        wu_main[pl.ds(pl.multiple_of(MIDDLE * i, REST), MIDDLE), :] = st_u[pl.ds(pl.multiple_of(BASE * i, REST), TILE), :].T
        wu_rest[...] = jnp.concatenate([st_u[BASE * tap + TILE : BASE * tap + BASE, :] for tap in range(IN_CH)], axis=0).T
        return carry

    lax.fori_loop(0, IN_CH, dec2a, 0)
    turned = [
        pltpu.make_async_copy(src, dst, turn_sem.at[2 + index])
        for index, (src, dst) in enumerate(((wu_main, um_out), (wu_rest, ur_out), (wa_main, am_out), (wa_rest, ar_out)))
    ]
    start(turned)
    finish(copies_d2b)

    def dec2b(i, carry):
        block = i + 1 - 2 * (i % 2)
        row0 = pl.multiple_of(block * TILE, TILE)

        @pl.when(i == 1)
        def _():
            finish(ex_b)
            halo(x_a, REST, MIDDLE, N16)

        @pl.when(i == KERNEL)
        def _():
            start(ex_d)

        for lane0, lanes in tiles:
            value = jnp.maximum(conv640(x_a, row0, N6400, lane0, lanes) + bias_row(b_d2b, lane0, lanes), 0.0)
            d_2[pl.ds(row0 + REST, TILE), pl.ds(lane0, lanes)] = value.astype(BF16)
        return carry

    lax.fori_loop(0, IN_CH, dec2b, 0)
    result = pltpu.make_async_copy(d_2.at[pl.ds(REST, PACK), :], out.at[pl.ds(REST, PACK), :], sem_out)
    result.start()
    finish(turned)
    finish(ex_d)
    result.wait()


def dec1_kernel(
    d_2, s1, um_h, ur_h, am_h, ar_h, w_d1b, b_d1a_h, b_d1b_h, w_head_h, b_head_h, out,
    b_d1a, b_d1b, w_head, b_head, x_u, x_s, x_d, y_rest, st_b, wu_main, wu_rest, wa_main, wa_rest, wb_main, wb_rest, wide, result, pending, stage, skip, low, late,
    sem, small_sem, send_sem, recv_sem,
):
    strip = strip_index()
    row = lax.axis_index("row")
    col = lax.axis_index("col")
    copy_um = pltpu.make_async_copy(um_h, wu_main, sem.at[0])
    copy_ur = pltpu.make_async_copy(ur_h, wu_rest, sem.at[1])
    copy_am = pltpu.make_async_copy(am_h, wa_main, sem.at[FIVE])
    copy_ar = pltpu.make_async_copy(ar_h, wa_rest, sem.at[SIX])
    copy_s = pltpu.make_async_copy(s1, skip, sem.at[2])
    copy_b = pltpu.make_async_copy(w_d1b, st_b, sem.at[KERNEL])
    copy_d = pltpu.make_async_copy(d_2, low, sem.at[IN_CH])
    barrier = enter_barrier()
    copy_um.start()
    copy_ur.start()
    copy_d.start()
    small = fetch((b_d1a_h, b_d1b_h, w_head_h, b_head_h), (b_d1a, b_d1b, w_head, b_head), small_sem)

    stage[...] = jnp.zeros_like(stage)
    copy_um.wait()
    copy_ur.wait()
    copy_s.start()
    copy_ar.start()
    copy_d.wait()
    for copy in small:
        copy.wait()

    def up1(i):
        lhs = low[BASE_PAD * i : BASE_PAD * i + BASE_PAD, :]
        rest = dot(lhs, wu_rest[...])
        for p in range(2):
            part = rest[:, LANES * p : LANES * p + LANES]
            buf = wide.at[2 * i + p]
            buf[2, pl.ds(0, BASE_PAD, stride=2), :] = low_lanes(part)
            buf[2, pl.ds(1, BASE_PAD, stride=2), :] = low_lanes(pltpu.roll(part, REST, axis=1))
            for q in range(2):
                tap = 2 * p + q
                main = dot(lhs, wu_main[MIDDLE * tap : MIDDLE * tap + MIDDLE, :])
                buf[0, pl.ds(q, BASE_PAD, stride=2), :] = main[:, 0:LANES]
                buf[1, pl.ds(q, BASE_PAD, stride=2), :] = main[:, LANES:TILE]
            for r in range(SIX):
                main = jnp.concatenate([buf[0, LANES * r : LANES * r + LANES, :], buf[1, LANES * r : LANES * r + LANES, :]], axis=1)
                tail = buf[2, LANES * r : LANES * r + LANES, :]
                if (i, r) == (0, 0):
                    main, tail = jnp.where(strip > 0, main, 0.0), jnp.where(strip > 0, tail, 0.0)
                if (i, r) == (2, FIVE):
                    main, tail = jnp.where(strip < LAST_STRIP, main, 0.0), jnp.where(strip < LAST_STRIP, tail, 0.0)
                put3_320(x_u, (N12 * i + 2 * r + p) * LANES, main, tail, LANES)

    def spread(j):
        rows = pl.ds(TILE * j, TILE)
        put3_320(x_s, TILE * j, skip[rows, 0:TILE].astype(F32), skip[rows, TILE:BASE_PAD].astype(F32), LANES, stage.at[j % 2])

    def rest_a(i):
        for j in range(SIX * i, SIX * i + SIX):
            y_rest[TILE * j : TILE * j + TILE, :] = dot(packed_rows(x_u, TILE * j, TILE), wa_rest[0:PACK, :]) + dot(
                packed_rows(x_s, TILE * j, TILE), wa_rest[PACK:N2048, :]
            )
            if j < N17:
                spread(j + 1)

    up1(0)
    up1(1)
    copy_s.wait()
    copy_ar.wait()
    copy_am.start()
    copy_b.start()
    spread(0)
    up1(2)
    for i in range(KERNEL):
        rest_a(i)
    copy_am.wait()

    def conv_a(row0):
        acc = None
        for di in range(KERNEL):
            for src, ref in enumerate((x_u, x_s)):
                base = N3072 * src + PACK * di
                part = dot(packed_rows(ref, row0 + LANES * di, TILE), wa_main[base : base + PACK, :])
                acc = part if acc is None else acc + part
        return acc

    def put_a(acc, row0, first_row, slot):
        main = valid_rows(jnp.maximum(acc + bias_row(b_d1a, 0, TILE), 0.0), first_row, LANES)
        tail = valid_rows(jnp.maximum(rest_sum(y_rest, row0, TILE) + bias_rest(b_d1a), 0.0), first_row, LANES)
        put3_320(x_d, row0, main, low_lanes(tail), LANES, stage.at[slot])

    late[...] = jnp.zeros_like(late)

    def dec1a(i, carry):
        base = pl.multiple_of(i * PACK, PACK)
        put_a(late[...], pl.multiple_of(jnp.maximum(base - TILE, 0), TILE), STRIP_ROWS * strip - KERNEL + STRIPS * i, 1)
        for j in range(IN_CH):
            acc = conv_a(base + TILE * j)
            if j == KERNEL:
                late[...] = acc
            else:
                put_a(acc, base + TILE * j, STRIP_ROWS * strip - 1 + STRIPS * i + 2 * j, j % 2)
        return carry

    copy_b.wait()
    lax.fori_loop(0, IN_CH, dec1a, 0)
    pack_weights(st_b, wb_main, wb_rest)
    put_a(late[...], N3840, STRIP_ROWS * strip + N29, 1)
    put_a(conv_a(N4096), N4096, STRIP_ROWS * strip + N31, 0)

    head_bias = jnp.zeros((IN_CH, LANES), F32)
    for channel in range(IN_CH):
        head_bias = jnp.where(lax.broadcasted_iota(jnp.int32, (IN_CH, LANES), 0) == channel, b_head[channel], head_bias)

    pending[...] = jnp.zeros_like(pending)

    def head(hidden, row0):
        line = lax.dot_general(w_head[...], hidden, (((1,), (1,)), ((), ())), preferred_element_type=F32)
        for r in range(2):
            part = line[:, LANES * r : LANES * r + LANES] + head_bias
            result[0, row0 + r] = part[:, 0:REST]
            result[1, row0 + r] = part[:, REST:LANES]

    pushes = []
    for part, first, rows in ((0, 0, N22), (1, N22, N10)):
        for side in range(2):
            pushes.append(
                Push(
                    result.at[side, pl.ds(first, rows)],
                    out.at[pl.ds(STRIP_ROWS * (strip % 2) + first, rows)],
                    send_sem.at[part, side],
                    recv_sem.at[part, strip % 2],
                    (lax.axis_index("data"), side, strip // 2),
                    (strip // 2 == row) & (col == side),
                )
            )

    def dec1b(i, carry):
        base = pl.multiple_of(i * PACK, PACK)

        @pl.when(i == KERNEL)
        def _():
            pl.semaphore_wait(barrier, STRIPS)
            for push in pushes[0:2]:
                push.start()

        def rest(j):
            y_rest[TILE * j : TILE * j + TILE, :] = dot(packed_rows(x_d, base + TILE * j, TILE), wb_rest[...])

        rest(0)
        waiting = pending[...]
        for j in range(IN_CH):
            rest(j + 1)
            acc = dot(packed_rows(x_d, base + TILE * j, TILE), wb_main[0:PACK, :])
            acc = acc + dot(packed_rows(x_d, base + TILE * j + LANES, TILE), wb_main[PACK:N2048, :])
            acc = acc + dot(packed_rows(x_d, base + TILE * j + TILE, TILE), wb_main[N2048:N3072, :])
            head(waiting, jnp.maximum(STRIPS * i + 2 * j - 2, 0))
            main = jnp.maximum(acc + bias_row(b_d1b, 0, TILE), 0.0).astype(BF16)
            tail = jnp.maximum(rest_sum(y_rest, TILE * j, TILE) + bias_rest(b_d1b), 0.0).astype(BF16)
            waiting = jnp.concatenate([main, tail[:, 0:REST]], axis=1)
        pending[...] = waiting
        return carry

    lax.fori_loop(0, IN_CH, dec1b, 0)
    head(pending[...], N30)

    for push in pushes[2:IN_CH]:
        push.start()
    for push in pushes:
        push.wait_send()
    for part, first, rows in ((0, 0, N22), (1, N22, N10)):
        for half in range(2):
            Push(
                result.at[0, pl.ds(first, rows)], out.at[pl.ds(STRIP_ROWS * half + first, rows)],
                send_sem.at[part, 0], recv_sem.at[part, half], strip_device(strip), strip < 0,
            ).wait_recv()


def solution(mesh):
    tile_spec = P(("data", "row"), "col", None)

    def body(image_tile, *params):
        (w_enc1a, b_enc1a, w_enc1b, b_enc1b, w_enc2a, b_enc2a, w_enc2b, b_enc2b,
         w_mid_a, b_mid_a, w_mid_b, b_mid_b, w_up2, w_dec2a, b_dec2a, w_dec2b, b_dec2b,
         w_up1, w_dec1a, b_dec1a, w_dec1b, b_dec1b, w_head, b_head) = params
        def flat(weight):
            return weight.reshape(-1, weight.shape[-1])

        hbm = pl.BlockSpec(memory_space=pl.ANY)
        dma = pltpu.SemaphoreType.DMA
        s1, p1 = pl.pallas_call(
            enc1_kernel,
            grid=(KERNEL,),
            out_shape=(jax.ShapeDtypeStruct((N4608, BASE_PAD), BF16), jax.ShapeDtypeStruct((STRIPS, N1152, LANES), BF16)),
            in_specs=[hbm] * FIVE,
            out_specs=(pl.BlockSpec((N1536, BASE_PAD), lambda i: (i, 0)), pl.BlockSpec((STRIPS, BASE_PAD, LANES), lambda i: (0, i, 0))),
            scratch_shapes=[
                pltpu.VMEM((REST, IN_CH, REST), BF16),
                pltpu.VMEM((KERNEL, KERNEL, IN_CH, BASE), BF16),
                pltpu.VMEM((BASE,), F32),
                pltpu.VMEM((BASE,), F32),
                pltpu.VMEM((2, N40, IN_CH, REST), BF16),
                pltpu.VMEM((N50, STRIP_ROWS, LANES), BF16),
                pltpu.VMEM((N96, BASE_PAD), BF16),
                pltpu.VMEM((N2880, BASE), BF16),
                pltpu.VMEM((STRIPS, N5136, LANES), BF16),
                pltpu.VMEM((N1792, TILE), F32),
                pltpu.VMEM((N3072, TILE), BF16),
                pltpu.VMEM((PACK, TILE), BF16),
                pltpu.VMEM((2, LANES, LANES), F32),
                pltpu.VMEM((2, KERNEL, N288, LANES), F32),
                pltpu.VMEM((2, KERNEL, N80, LANES), F32),
                dma, dma((IN_CH,)), dma((IN_CH,)), dma((2, 2)),
            ],
            compiler_params=pltpu.CompilerParams(
                vmem_limit_bytes=VMEM_LIMIT, collective_id=1, has_side_effects=True, dimension_semantics=("arbitrary",)
            ),
            name="enc1",
        )(image_tile.transpose(0, 2, 1), w_enc1a, b_enc1a, flat(w_enc1b), b_enc1b)

        turned_shapes = ((N2560, TILE), (MIDDLE, TILE), (N6144, TILE), (N2048, TILE))

        def turned(weight):
            return weight.transpose(0, 1, KERNEL, 2).reshape(-1, weight.shape[2])

        d2, *level_one = pl.pallas_call(
            mid_kernel,
            out_shape=[jax.ShapeDtypeStruct(shape, BF16) for shape in ((N1152, MIDDLE),) + turned_shapes],
            in_specs=[hbm] * N16,
            out_specs=[hbm] * FIVE,
            scratch_shapes=[
                *[pltpu.VMEM((size,), F32) for size in (MIDDLE, MIDDLE, DEEP, DEEP, MIDDLE, MIDDLE)],
                *[pltpu.VMEM(shape, BF16) for shape in turned_shapes],
                pltpu.VMEM((STRIPS, N1168, LANES), BF16),
                pltpu.VMEM((N3072, MIDDLE), BF16),
                pltpu.VMEM((RING_ROWS, DEEP), BF16),
                pltpu.VMEM((N1152, MIDDLE3), BF16),
                pltpu.VMEM((N1152, MIDDLE3), BF16),
                pltpu.VMEM((N1152, MIDDLE3), BF16),
                pltpu.VMEM((BASE, MIDDLE3), BF16),
                pltpu.VMEM((BASE, N3840), BF16),
                pltpu.VMEM((TILE, DEEP), BF16),
                pltpu.VMEM((N1152, MIDDLE), BF16),
                pltpu.VMEM((TILE, DEEP), F32),
                pltpu.VMEM((FIVE, N512, LANES), F32),
                pltpu.VMEM((LANES, LANES), F32),
                dma((N18,)), dma((TAPS,)), dma((KERNEL,)), dma((TAPS,)), dma((IN_CH,)), dma((TAPS,)), dma((TAPS,)), dma, dma, dma((SIX,)), dma((SIX,)),
                dma((LAST_STRIP, 2)), dma((LAST_STRIP, 2)),
            ],
            compiler_params=pltpu.CompilerParams(
                vmem_limit_bytes=VMEM_LIMIT, collective_id=0, has_side_effects=True
            ),
            name="mid",
        )(
            p1, flat(w_enc2a), flat(w_enc2b), flat(w_mid_a), flat(w_mid_b), flat(w_up2), flat(w_dec2a), flat(w_dec2b),
            turned(w_up1), turned(w_dec1a),
            b_enc2a, b_enc2b, b_mid_a, b_mid_b, b_dec2a, b_dec2b,
        )

        y = pl.pallas_call(
            dec1_kernel,
            out_shape=jax.ShapeDtypeStruct((REST, IN_CH, REST), F32),
            in_specs=[hbm] * N11,
            out_specs=hbm,
            scratch_shapes=[
                pltpu.VMEM((BASE,), F32),
                pltpu.VMEM((BASE,), F32),
                pltpu.VMEM((IN_CH, BASE), BF16),
                pltpu.SMEM((IN_CH,), F32),
                pltpu.VMEM((STRIPS, N4624, LANES), BF16),
                pltpu.VMEM((STRIPS, N4624, LANES), BF16),
                pltpu.VMEM((STRIPS, N4368, LANES), BF16),
                pltpu.VMEM((N4608, TILE), F32),
                pltpu.VMEM((N2880, BASE), BF16),
                pltpu.VMEM((N2560, TILE), BF16),
                pltpu.VMEM((MIDDLE, TILE), BF16),
                pltpu.VMEM((N6144, TILE), BF16),
                pltpu.VMEM((N2048, TILE), BF16),
                pltpu.VMEM((N3072, TILE), BF16),
                pltpu.VMEM((PACK, TILE), BF16),
                pltpu.VMEM((SIX, KERNEL, REST_AT, LANES), F32),
                pltpu.VMEM((2, STRIP_ROWS, IN_CH, REST), F32),
                pltpu.VMEM((TILE, BASE), BF16),
                pltpu.VMEM((2, KERNEL, N288, LANES), F32),
                pltpu.VMEM((N4608, BASE_PAD), BF16),
                pltpu.VMEM((N1152, MIDDLE), BF16),
                pltpu.VMEM((TILE, TILE), F32),
                dma((LAST_STRIP,)), dma((IN_CH,)), dma((2, 2)), dma((2, 2)),
            ],
            compiler_params=pltpu.CompilerParams(vmem_limit_bytes=VMEM_LIMIT, collective_id=2, has_side_effects=True),
            name="dec1",
        )(d2, s1, *level_one, flat(w_dec1b), b_dec1a, b_dec1b, w_head.T, b_head)
        return y.transpose(0, 2, 1)

    def program(image, *params):
        mapped = jax.shard_map(
            body, mesh=mesh, in_specs=(tile_spec,) + (P(),) * len(params), out_specs=tile_spec, check_vma=False
        )
        return mapped(image, *params)

    return program
```
